512 devices in a mesh: seqa: 16 (over z_lo, core), seqb: 8 (over x, z_hi), dp: 4 (over y).
Axes of the slice: x: 4, y: 4, z: 16 (z_hi: 2, z_lo: 8; z = z_hi * 8 + z_lo), core: 2. Of those that a mesh axis runs over, the one named last changes fastest.
Arguments:
- queries: bfloat16 [16384, 128, 64], P(('dp', 'seqa', 'seqb')), parts along dimension 0, may hold values from -6 to 6
- keys: bfloat16 [16384, 128, 64], P(('dp', 'seqa', 'seqb')), parts along dimension 0, may hold values from -6 to 6
- values: bfloat16 [16384, 128, 64], P(('dp', 'seqa', 'seqb')), parts along dimension 0, may hold values from -6 to 6
- doc_bounds: int32 [36], P('dp'), parts along dimension 0, may hold values from 0 to 4096, as said below
- q_gain: float32 [64], replicated, may hold values from 0.25 to 1.75
- k_gain: float32 [64], replicated, may hold values from 0.25 to 1.75
Outputs:
- attended: bfloat16 [16384, 128, 64], P(('dp', 'seqa', 'seqb')), parts along dimension 0
The draws below stay inside these ranges and needn't reach their ends.
There are 4 independent parts, one for each index of `dp`. The reference program is written for one: setup_inputs(seed, part) draws one part's arguments, and reference() takes and returns one part's arrays. A program takes and returns all parts, laid end to end along the dimension named above; an argument that names none is the same for every part. Nothing has to cross between parts.
Inputs may be any that keep to these rules, and one draw needn't show every extreme that they name: doc_bounds[0] is 0, doc_bounds[8] is 4096, and the entries rise strictly.
All inputs are finite; a program needn't handle non-finite values.
Results may differ from the reference program's by a relative error of at most 0.0015.
Values may be sent and summed in bfloat16 or wider, within the bound.
No kernel may reach another device: no remote copies, remote signals or barrier semaphores. Data moves between devices by JAX's collectives and lax.ppermute only.
A program may use at most 64 MiB of HBM per device.

```python
import jax
import jax.numpy as jnp
from jax import lax

HD = 64
DOCS = 8
SEQ = 4096
HEADS = 128


def draw_doc_bounds(key, part):
    shuffled = jax.random.permutation(key, SEQ - 1).astype(jnp.int32) + 1
    cuts = jnp.sort(shuffled[:DOCS - 1])
    return jnp.concatenate([jnp.zeros((1,), jnp.int32), cuts, jnp.full((1,), SEQ, jnp.int32)]).astype(jnp.int32)


def level_of(stream_key, shape, cuts, least, top_value):
    def one(dim, parts):
        heights = jax.random.uniform(jax.random.fold_in(jax.random.fold_in(stream_key, 6), dim), (parts,), jnp.float32, least / len(cuts), top_value / len(cuts))
        return jnp.repeat(jnp.exp(heights), shape[dim] // parts).reshape((-1,) + (1,) * (len(shape) - dim - 1))

    level = one(*cuts[0])
    for cut in cuts[1:]:
        level = level * one(*cut)
    return level


def normal_values(stream_key, dims, scale, bound, shards=(), kind=jnp.bfloat16):
    values = scale * jax.random.normal(stream_key, dims, jnp.float32)
    if shards:
        values = values * level_of(stream_key, dims, shards, -0.22, 0.18)
    return jnp.clip(values, -bound, bound).astype(kind)


def setup_inputs(seed: int = 0, part: int = 0) -> dict:
    streams_of = jax.random.split(jax.random.key(seed), 7)
    part_keys = jax.random.split(jax.random.fold_in(streams_of[6], part), 7)
    queries = normal_values(part_keys[0], (SEQ, HEADS, HD), 1.0, 6.0, ((0, 128),))
    keys = normal_values(part_keys[1], (SEQ, HEADS, HD), 1.0, 6.0, ((0, 128),))
    values = normal_values(part_keys[2], (SEQ, HEADS, HD), 1.0, 6.0, ((0, 128),))
    doc_bounds = draw_doc_bounds(jax.random.fold_in(jax.random.fold_in(streams_of[6], part), 71), part)
    q_gain = jnp.clip(1.0 + 0.15 * jax.random.normal(streams_of[4], (HD,), jnp.float32), 0.25, 1.75)
    k_gain = jnp.clip(1.0 + 0.15 * jax.random.normal(streams_of[5], (HD,), jnp.float32), 0.25, 1.75)
    return {"queries": queries, "keys": keys, "values": values, "doc_bounds": doc_bounds, "q_gain": q_gain, "k_gain": k_gain}


def prepare(block, gain, positions):
    values32 = block.astype(jnp.float32)
    scale = lax.rsqrt(lax.optimization_barrier(jnp.mean(values32 * values32, axis=-1, keepdims=True)) + 1e-06)
    normed = values32 * scale * gain
    half = normed.shape[-1] // 2
    freq = jnp.exp(-jnp.log(10000.0) * jnp.arange(half, dtype=jnp.float32) * 2.0 / normed.shape[-1])
    angle = positions.astype(jnp.float32)[:, None] * freq[None, :]
    first = normed[:, :half]
    second = normed[:, half:]
    cosine = jnp.cos(angle)
    sine = jnp.sin(angle)
    rotated = jnp.concatenate([first * cosine - second * sine, first * sine + second * cosine], axis=-1)
    return rotated.astype(jnp.bfloat16)

def reference(queries, keys, values, doc_bounds, q_gain, k_gain):
    length = queries.shape[0]
    width = queries.shape[2]
    places = jnp.arange(length, dtype=jnp.int32)
    doc = lax.optimization_barrier(jnp.sum((places[:, None] >= doc_bounds[None, 1:DOCS]).astype(jnp.int32), axis=1)).astype(jnp.int32)
    positions = places - doc_bounds[doc]
    allowed = (doc[:, None] == doc[None, :]) & (places[None, :] <= places[:, None])

    def one_head(items):
        query_head, key_head, value_head = items
        qr = prepare(query_head, q_gain, positions)
        kr = prepare(key_head, k_gain, positions)
        scores = jnp.dot(qr, kr.T, preferred_element_type=jnp.float32) / jnp.sqrt(jnp.float32(width))
        scores = jnp.where(allowed, scores, jnp.float32(-1e+30))
        top = lax.optimization_barrier(jnp.max(scores, axis=1, keepdims=True))
        expo = jnp.where(allowed, jnp.exp(scores - top), jnp.float32(0.0))
        weights = (expo / lax.optimization_barrier(jnp.sum(expo, axis=1, keepdims=True))).astype(jnp.bfloat16)
        return jnp.dot(weights, value_head, preferred_element_type=jnp.float32).astype(jnp.bfloat16)
    outputs = lax.map(one_head, (jnp.transpose(queries, (1, 0, 2)), jnp.transpose(keys, (1, 0, 2)), jnp.transpose(values, (1, 0, 2))))
    return jnp.transpose(outputs, (1, 0, 2))
```

```python
import functools

import jax
import jax.numpy as jnp
from jax import lax
from jax.experimental import pallas as pl
from jax.experimental.pallas import tpu as pltpu
from jax.sharding import PartitionSpec as P

AXES = ("seqa", "seqb")
TOK = 32
HALF_TOK = 16
HD = 64
HEADS = 128
DOCS = 8
SEQ = 4096
BLK = 256
PAIRS = BLK // 2
NBLK = SEQ // BLK
SRC = BLK // TOK
NT = (((1,), (1,)), ((), ()))
NN = (((1,), (0,)), ((), ()))
SCALE = 1.4426950408889634 / 8.0
FIRST = -9.210340371976184


def dot(a, b, dims):
    return lax.dot_general(a, b, dims, preferred_element_type=jnp.float32)


def starts_of(token, bounds_ref):
    start = jnp.zeros_like(token)
    for d in range(1, DOCS):
        start = jnp.where(token >= bounds_ref[d], bounds_ref[d], start)
    return start


def identity(n):
    return (
        lax.broadcasted_iota(jnp.int32, (n, n), 0) == lax.broadcasted_iota(jnp.int32, (n, n), 1)
    ).astype(jnp.float32).astype(jnp.bfloat16)


def interleave():
    row = lax.broadcasted_iota(jnp.int32, (256, 256), 0)
    col = lax.broadcasted_iota(jnp.int32, (256, 256), 1)
    return (col == (row % 16) * 16 + row // 16).astype(jnp.float32).astype(jnp.bfloat16)


def send_kernel(base_ref, bounds_ref, q_ref, k_ref, v_ref, qg_ref, kg_ref, o_ref, rot, turned):
    lane = lax.broadcasted_iota(jnp.int32, (HD // 2, 128), 1)
    token = base_ref[0] + lane
    place = (token - starts_of(token, bounds_ref)).astype(jnp.float32)
    index = lax.broadcasted_iota(jnp.int32, (HD // 2, 128), 0).astype(jnp.float32)
    angle = place * jnp.exp(jnp.float32(FIRST) * index * 2.0 / HD)
    cosine = jnp.cos(angle)
    sine = jnp.sin(angle)
    gains = [jnp.transpose(jnp.broadcast_to(g[...], (HEADS, HD))) for g in (qg_ref, kg_ref)]
    for t in range(TOK):
        c = jnp.broadcast_to(cosine[:, t : t + 1], (HD // 2, HEADS))
        s = jnp.broadcast_to(sine[:, t : t + 1], (HD // 2, HEADS))
        for n, (x_ref, gain) in enumerate(zip((q_ref, k_ref), gains)):
            x = x_ref[t].astype(jnp.float32)
            scale = lax.rsqrt(jnp.mean(x * x, axis=0, keepdims=True) + 1e-06)
            x = x * scale * gain
            a, b = x[: HD // 2], x[HD // 2 :]
            row = pl.ds((t // HALF_TOK) * HD, HD)
            rot[n, t % HALF_TOK, row, :] = jnp.concatenate([a * c - b * s, a * s + b * c], axis=0).astype(
                jnp.bfloat16
            )
    for t in range(TOK):
        rot[2, t % HALF_TOK, pl.ds((t // HALF_TOK) * HD, HD), :] = v_ref[t]
    eye = identity(HEADS)
    for n in range(3):
        for r in range(0, HALF_TOK, 2):
            both = dot(eye, rot[n, r : r + 2].reshape(256, HEADS), NT).astype(jnp.bfloat16)
            turned[n, r] = both[:, :128]
            turned[n, r + 1] = both[:, 128:]
    mix = interleave()
    for n in range(3):
        for h in range(0, HEADS, 16):
            part = turned[n, :, h : h + 16, :].reshape(256, 128)
            o_ref[h : h + 16, 16 * n : 16 * n + 16, :] = (
                dot(mix, part, NN).astype(jnp.bfloat16).reshape(16, 16, 128)
            )


def attend_kernel(bounds_ref, x_ref, o_ref, vt, expo):
    eye = identity(128)
    for j in range(NBLK):
        v2 = x_ref[SRC * j : SRC * j + SRC, 32:48, :].reshape(PAIRS, 128)
        vt[j] = dot(eye, v2, NT).astype(jnp.bfloat16)
    low = lax.broadcasted_iota(jnp.int32, (PAIRS, 128), 1) < HD
    lane = lax.broadcasted_iota(jnp.int32, (1, BLK), 1)
    pair = lane % PAIRS
    q_off = (pair // 16) * 32 + pair % 16 + (lane // PAIRS) * 16
    row = lax.broadcasted_iota(jnp.int32, (PAIRS, BLK), 0)
    k_off = (row // 16) * 32 + row % 16

    def query_block(i, _):
        q2 = x_ref[pl.ds(SRC * i, SRC), 0:16, :].reshape(PAIRS, 128).astype(jnp.float32)
        swap = pltpu.roll(q2, HD, 1)
        zero = jnp.zeros_like(q2)
        rhs_lo = jnp.concatenate([jnp.where(low, q2, zero), jnp.where(low, swap, zero)], axis=0).astype(jnp.bfloat16)
        rhs_hi = jnp.concatenate([jnp.where(low, zero, swap), jnp.where(low, zero, q2)], axis=0).astype(jnp.bfloat16)
        q_tok = BLK * i + q_off
        q_start = starts_of(q_tok, bounds_ref)
        first = BLK * i
        start = jnp.int32(0)
        for d in range(1, DOCS):
            start = jnp.where(first >= bounds_ref[d], bounds_ref[d], start)
        j0 = start // BLK

        def scores(j, total):
            k2 = x_ref[pl.ds(SRC * j, SRC), 16:32, :].reshape(PAIRS, 128)
            for n, rhs in enumerate((rhs_lo, rhs_hi)):
                s = dot(k2, rhs, NT)
                k_tok = BLK * j + 16 * n + k_off
                allowed = (k_tok <= q_tok) & (k_tok >= q_start)
                e = jnp.where(allowed, jnp.exp2(s * jnp.float32(SCALE)), jnp.float32(0.0))
                expo[j - j0, n] = e
                total = total + jnp.sum(e, axis=0, keepdims=True)
            return total

        total = lax.fori_loop(j0, i + 1, scores, jnp.zeros((1, BLK), jnp.float32))
        inverse = 1.0 / total

        def weigh(j, out):
            for n in range(2):
                w = (expo[j - j0, n] * inverse).astype(jnp.bfloat16)
                out = out + dot(vt[j, HD * n : HD * n + HD, :], w, NN)
            return out

        out = lax.fori_loop(j0, i + 1, weigh, jnp.zeros((HD, BLK), jnp.float32))
        both = jnp.concatenate([out[:, :PAIRS], out[:, PAIRS:]], axis=0)
        o_ref[pl.ds(SRC * i, SRC)] = jnp.transpose(both).astype(jnp.bfloat16).reshape(SRC, 16, 128)
        return 0

    lax.fori_loop(0, NBLK, query_block, 0)


def take_kernel(x_ref, o_ref, turned):
    mix = interleave()
    for h in range(0, HEADS, 16):
        part = x_ref[h : h + 16].reshape(256, 128)
        turned[:, h : h + 16, :] = dot(mix, part, NN).astype(jnp.bfloat16).reshape(16, 16, 128)
    eye = identity(128)
    for r in range(HALF_TOK):
        both = dot(eye, turned[r], NT).astype(jnp.bfloat16)
        o_ref[r] = both[:HD]
        o_ref[r + HALF_TOK] = both[HD:]


SMEM = pl.BlockSpec(memory_space=pltpu.SMEM)
VMEM = pl.BlockSpec(memory_space=pltpu.VMEM)


def body(queries, keys, values, doc_bounds, q_gain, k_gain):
    group = lax.axis_size("seqa") * lax.axis_size("seqb")
    index = lax.axis_index("seqa") * lax.axis_size("seqb") + lax.axis_index("seqb")
    base = (index * TOK).astype(jnp.int32).reshape(1)
    turn = lambda x: jnp.transpose(x, (0, 2, 1))
    packed = pl.pallas_call(
        send_kernel,
        out_shape=jax.ShapeDtypeStruct((HEADS, 48, 128), jnp.bfloat16),
        in_specs=[SMEM, SMEM, VMEM, VMEM, VMEM, VMEM, VMEM],
        out_specs=VMEM,
        scratch_shapes=[
            pltpu.VMEM((3, HALF_TOK, 128, HEADS), jnp.bfloat16),
            pltpu.VMEM((3, HALF_TOK, HEADS, 128), jnp.bfloat16),
        ],
        compiler_params=pltpu.CompilerParams(vmem_limit_bytes=32 << 20),
        name="send_side",
    )(base, doc_bounds, turn(queries), turn(keys), turn(values), q_gain.reshape(1, HD), k_gain.reshape(1, HD))
    mine = lax.all_to_all(packed, AXES, split_axis=0, concat_axis=0, tiled=True)
    result = pl.pallas_call(
        attend_kernel,
        out_shape=jax.ShapeDtypeStruct((group, HALF_TOK, 128), jnp.bfloat16),
        in_specs=[SMEM, VMEM],
        out_specs=VMEM,
        scratch_shapes=[
            pltpu.VMEM((NBLK, 128, PAIRS), jnp.bfloat16),
            pltpu.VMEM((NBLK, 2, PAIRS, BLK), jnp.float32),
        ],
        compiler_params=pltpu.CompilerParams(vmem_limit_bytes=32 << 20),
        name="attend",
    )(doc_bounds, mine)
    back = lax.all_to_all(result, AXES, split_axis=0, concat_axis=0, tiled=True)
    out = pl.pallas_call(
        take_kernel,
        out_shape=jax.ShapeDtypeStruct((TOK, HD, HEADS), jnp.bfloat16),
        in_specs=[VMEM],
        out_specs=VMEM,
        scratch_shapes=[pltpu.VMEM((HALF_TOK, HEADS, 128), jnp.bfloat16)],
        compiler_params=pltpu.CompilerParams(vmem_limit_bytes=32 << 20),
        name="take_side",
    )(back)
    return turn(out)


def solution(mesh):
    tokens = P(("dp", "seqa", "seqb"), None, None)
    return jax.shard_map(
        body,
        mesh=mesh,
        in_specs=(tokens, tokens, tokens, P("dp"), P(), P()),
        out_specs=tokens,
        check_vma=False,
    )
```

```python
import jax
import jax.numpy as jnp
from jax import lax
from jax.experimental import pallas as pl
from jax.experimental.pallas import tpu as pltpu
from jax.sharding import PartitionSpec as P

AXES = ("seqa", "seqb")
TOK = 32
ROWS = 16
HD = 64
HEADS = 128
DOCS = 8
SEQ = 4096
BLK = 256
PAIRS = BLK // 2
NBLK = SEQ // BLK
SRC = BLK // TOK
UNROLL = 4
GROUP = 8
FAR = (NBLK - 2) * (NBLK - 1) // 2 + UNROLL
NT = (((1,), (1,)), ((), ()))
NN = (((1,), (0,)), ((), ()))
SCALE = 1.4426950408889634 / 8.0
FIRST = -9.210340371976184


def dot(a, b, dims=NN):
    return lax.dot_general(a, b, dims, preferred_element_type=jnp.float32)


def starts_of(token, bounds_ref):
    start = jnp.zeros_like(token)
    for d in range(1, DOCS):
        start = jnp.where(token >= bounds_ref[d], bounds_ref[d], start)
    return start


def identity(n):
    row = lax.broadcasted_iota(jnp.int32, (n, n), 0)
    col = lax.broadcasted_iota(jnp.int32, (n, n), 1)
    return (row == col).astype(jnp.float32).astype(jnp.bfloat16)


def interleave():
    row = lax.broadcasted_iota(jnp.int32, (256, 256), 0)
    col = lax.broadcasted_iota(jnp.int32, (256, 256), 1)
    return (col == (row % 16) * 16 + row // 16).astype(jnp.float32).astype(jnp.bfloat16)


def send_kernel(
    base_ref, bounds_hbm, q_hbm, k_hbm, v_hbm, qg_hbm, kg_hbm, o_hbm, bounds_ref, x_ref, g_ref, rot, turned, packed, sems, out_sems
):
    arriving = [
        pltpu.make_async_copy(source, target, sems.at[n])
        for n, (source, target) in enumerate(
            (
                (bounds_hbm, bounds_ref),
                (qg_hbm, g_ref.at[0]),
                (kg_hbm, g_ref.at[1]),
                (q_hbm, x_ref.at[0]),
                (k_hbm, x_ref.at[1]),
                (v_hbm, x_ref.at[2]),
            )
        )
    ]
    for c in arriving:
        c.start()
    for c in arriving[:3]:
        c.wait()
    lane = lax.broadcasted_iota(jnp.int32, (HD // 2, 128), 1)
    token = base_ref[0] + lane
    place = (token - starts_of(token, bounds_ref)).astype(jnp.float32)
    index = lax.broadcasted_iota(jnp.int32, (HD // 2, 128), 0).astype(jnp.float32)
    angle = place * jnp.exp(jnp.float32(FIRST) * index * 2.0 / HD)
    cosine = jnp.cos(angle)
    sine = jnp.sin(angle)
    gains = [jnp.transpose(jnp.broadcast_to(g_ref[n], (HEADS, HD))) for n in range(2)]
    eye = identity(HEADS)
    mix = interleave()
    for c in arriving[3:]:
        c.wait()

    def turn(n, r, rows):
        both = dot(eye, rows, NT).astype(jnp.bfloat16)
        turned[n, r] = both[:, :128]
        turned[n, r + 1] = both[:, 128:]

    leaving = []

    def leave(heads, rows):
        copy = pltpu.make_async_copy(packed.at[heads, rows], o_hbm.at[heads, rows], out_sems.at[len(leaving)])
        copy.start()
        leaving.append(copy)

    for r in range(0, ROWS, 2):
        turn(2, r, jnp.concatenate([x_ref[2, t] for t in (r, r + ROWS, r + 1, r + 1 + ROWS)], axis=0))
    for h in range(0, HEADS, 32):
        part = jnp.concatenate([turned[2, :, h + m : h + m + 16, :].reshape(256, 128) for m in (0, 16)], axis=1)
        both = dot(mix, part).astype(jnp.bfloat16)
        for m in range(2):
            packed[h + 16 * m : h + 16 * m + 16, 32:48, :] = both[:, 128 * m : 128 * m + 128].reshape(16, 16, 128)
    leave(pl.ds(0, HEADS), pl.ds(32, 16))
    for r in range(0, ROWS, 2):
        for t in (r, r + ROWS, r + 1, r + 1 + ROWS):
            c = jnp.broadcast_to(cosine[:, t : t + 1], (HD // 2, HEADS))
            s = jnp.broadcast_to(sine[:, t : t + 1], (HD // 2, HEADS))
            for n in range(2):
                x = x_ref[n, t].astype(jnp.float32)
                scale = lax.rsqrt(jnp.mean(x * x, axis=0, keepdims=True) + 1e-06)
                x = x * scale * gains[n]
                a, b = x[: HD // 2], x[HD // 2 :]
                y = jnp.concatenate([a * c - b * s, a * s + b * c], axis=0)
                rot[n, t % ROWS, pl.ds((t // ROWS) * HD, HD), :] = y.astype(jnp.bfloat16)
        for n in range(2):
            turn(n, r, rot[n, r : r + 2].reshape(256, HEADS))
    for h in range(0, HEADS, 16):
        part = jnp.concatenate([turned[n, :, h : h + 16, :].reshape(256, 128) for n in range(2)], axis=1)
        both = dot(mix, part).astype(jnp.bfloat16)
        for n in range(2):
            packed[h : h + 16, 16 * n : 16 * n + 16, :] = both[:, 128 * n : 128 * n + 128].reshape(16, 16, 128)
        if h % 32 == 16:
            leave(pl.ds(h - 16, 32), pl.ds(0, 32))
    for c in leaving:
        c.wait()


def attend_kernel(bounds_ref, x_ref, o_ref, qt, vt, starts, near, far, total, summed, item_i, item_j):
    lane = lax.broadcasted_iota(jnp.int32, (1, BLK), 1)
    pair = lane % PAIRS
    q_off = (pair // 16) * 32 + pair % 16 + (lane // PAIRS) * 16
    row = lax.broadcasted_iota(jnp.int32, (2 * PAIRS, BLK), 0)
    k_off = ((row % PAIRS) // 16) * 32 + row % 16 + (row // PAIRS) * 16
    below = k_off <= q_off

    def list_block(i, n):
        def add(j, n):
            item_i[n] = i
            item_j[n] = j
            return n + 1

        return lax.fori_loop(starts_of(BLK * i, bounds_ref) // BLK, i - 1, add, n)

    n_far = lax.fori_loop(2, NBLK, list_block, jnp.int32(0))
    for u in range(UNROLL - 1):
        item_i[n_far + u] = NBLK
        item_j[n_far + u] = 0
    trips = (n_far + UNROLL - 1) // UNROLL
    zero = jnp.zeros((HD, BLK), jnp.bfloat16)

    def wide(x):
        t = jnp.transpose(x.astype(jnp.float32)).astype(jnp.bfloat16)
        return jnp.concatenate([t[:HD], t[HD:]], axis=1)

    def scores(j, q, allowed):
        k2 = x_ref[pl.ds(SRC * j, SRC), 16:32, :].reshape(PAIRS, 128)
        low = dot(k2, jnp.concatenate([q, zero], axis=0))
        high = dot(k2, jnp.concatenate([zero, q], axis=0))
        s = jnp.concatenate([low, high], axis=0)
        return jnp.where(allowed, jnp.exp2(s * jnp.float32(SCALE)), jnp.float32(0.0))

    def partial_sum(e):
        return jnp.sum(e.reshape(BLK // 8, 8, BLK), axis=0)

    def near_scores(g, _):
        for u in range(GROUP):
            i = GROUP * g + u
            q = wide(x_ref[pl.ds(SRC * i, SRC), 0:16, :].reshape(PAIRS, 128))
            qt[i] = q
            vt[i] = wide(x_ref[pl.ds(SRC * i, SRC), 32:48, :].reshape(PAIRS, 128))
            start = starts_of(BLK * i + q_off, bounds_ref)
            starts[i] = start
            e1 = scores(i, q, below & (k_off >= start - BLK * i))
            e0 = scores(jnp.maximum(i - 1, 0), q, k_off >= start - BLK * (i - 1))
            near[i, 0] = e0
            near[i, 1] = e1
            total[i] = partial_sum(e0) + partial_sum(e1)
        return 0

    lax.fori_loop(0, NBLK // GROUP, near_scores, 0)

    def far_scores(w, _):
        for u in range(UNROLL):
            n = UNROLL * w + u
            i, j = item_i[n], item_j[n]
            e = scores(j, qt[i], k_off >= starts[i] - BLK * j)
            far[n] = e
            total[i] += partial_sum(e)
        return 0

    lax.fori_loop(0, trips, far_scores, 0)

    def near_values(g, _):
        for u in range(GROUP):
            i = GROUP * g + u
            inverse = 1.0 / jnp.sum(total[i], axis=0, keepdims=True)
            total[i] = jnp.broadcast_to(inverse, (8, BLK))
            w = jnp.concatenate([(near[i, n] * inverse).astype(jnp.bfloat16) for n in range(2)], axis=0)
            summed[i] = dot(jnp.concatenate([vt[jnp.maximum(i - 1, 0)], vt[i]], axis=1), w)
        return 0

    lax.fori_loop(0, NBLK // GROUP, near_values, 0)

    def far_values(w, _):
        for u in range(UNROLL):
            n = UNROLL * w + u
            i, j = item_i[n], item_j[n]
            summed[i] += dot(vt[j], (far[n] * total[i][0:1]).astype(jnp.bfloat16))
        return 0

    lax.fori_loop(0, trips, far_values, 0)

    def finish(g, _):
        for u in range(GROUP):
            i = GROUP * g + u
            out = summed[i]
            both = jnp.transpose(jnp.concatenate([out[:, :PAIRS], out[:, PAIRS:]], axis=0))
            o_ref[pl.ds(SRC * i, SRC)] = both.astype(jnp.bfloat16).reshape(SRC, 16, 128)
        return 0

    lax.fori_loop(0, NBLK // GROUP, finish, 0)


def take_kernel(x_ref, o_hbm, turned, out, sems):
    mix = interleave()
    eye = identity(128)
    for h in range(0, HEADS, 32):
        part = jnp.concatenate([x_ref[h + m : h + m + 16].reshape(256, 128) for m in (0, 16)], axis=1)
        both = dot(mix, part).astype(jnp.bfloat16)
        for m in range(2):
            turned[:, h + 16 * m : h + 16 * m + 16, :] = both[:, 128 * m : 128 * m + 128].reshape(16, 16, 128)
    copies = []
    for r in range(0, ROWS, 2):
        both = dot(eye, turned[r : r + 2].reshape(256, 128), NT).astype(jnp.bfloat16)
        for m in range(2):
            out[r + m] = both[:HD, 128 * m : 128 * m + 128]
            out[r + m + ROWS] = both[HD:, 128 * m : 128 * m + 128]
        if r % 8 == 6:
            for first in (r - 6, r - 6 + ROWS):
                copy = pltpu.make_async_copy(
                    out.at[pl.ds(first, 8)], o_hbm.at[pl.ds(first, 8)], sems.at[len(copies)]
                )
                copy.start()
                copies.append(copy)
    for copy in copies:
        copy.wait()


SMEM = pl.BlockSpec(memory_space=pltpu.SMEM)
VMEM = pl.BlockSpec(memory_space=pltpu.VMEM)
HBM = pl.BlockSpec(memory_space=pltpu.HBM)


def send_call(base, doc_bounds, q, k, v, q_gain, k_gain):
    return pl.pallas_call(
        send_kernel,
        out_shape=jax.ShapeDtypeStruct((HEADS, 48, 128), jnp.bfloat16),
        in_specs=[SMEM] + [HBM] * 6,
        out_specs=HBM,
        scratch_shapes=[
            pltpu.SMEM((DOCS + 1,), jnp.int32),
            pltpu.VMEM((3, TOK, HD, HEADS), jnp.bfloat16),
            pltpu.VMEM((2, 1, HD), jnp.float32),
            pltpu.VMEM((2, ROWS, 128, HEADS), jnp.bfloat16),
            pltpu.VMEM((3, ROWS, HEADS, 128), jnp.bfloat16),
            pltpu.VMEM((HEADS, 48, 128), jnp.bfloat16),
            pltpu.SemaphoreType.DMA((6,)),
            pltpu.SemaphoreType.DMA((5,)),
        ],
        compiler_params=pltpu.CompilerParams(vmem_limit_bytes=60 << 20),
        name="send_side",
    )(base, doc_bounds, q, k, v, q_gain.reshape(1, HD), k_gain.reshape(1, HD))


def attend_call(doc_bounds, mine):
    return pl.pallas_call(
        attend_kernel,
        out_shape=jax.ShapeDtypeStruct((SEQ // TOK, ROWS, 128), jnp.bfloat16),
        in_specs=[SMEM, VMEM],
        out_specs=VMEM,
        scratch_shapes=[
            pltpu.VMEM((NBLK + 1, HD, BLK), jnp.bfloat16),
            pltpu.VMEM((NBLK, HD, BLK), jnp.bfloat16),
            pltpu.VMEM((NBLK + 1, 1, BLK), jnp.int32),
            pltpu.VMEM((NBLK, 2, BLK, BLK), jnp.float32),
            pltpu.VMEM((FAR, BLK, BLK), jnp.float32),
            pltpu.VMEM((NBLK + 1, 8, BLK), jnp.float32),
            pltpu.VMEM((NBLK + 1, HD, BLK), jnp.float32),
            pltpu.SMEM((FAR,), jnp.int32),
            pltpu.SMEM((FAR,), jnp.int32),
        ],
        compiler_params=pltpu.CompilerParams(vmem_limit_bytes=40 << 20),
        name="attend",
    )(doc_bounds, mine)


def take_call(back):
    return pl.pallas_call(
        take_kernel,
        out_shape=jax.ShapeDtypeStruct((TOK, HD, HEADS), jnp.bfloat16),
        in_specs=[VMEM],
        out_specs=HBM,
        scratch_shapes=[
            pltpu.VMEM((ROWS, HEADS, 128), jnp.bfloat16),
            pltpu.VMEM((TOK, HD, HEADS), jnp.bfloat16),
            pltpu.SemaphoreType.DMA((4,)),
        ],
        compiler_params=pltpu.CompilerParams(vmem_limit_bytes=32 << 20),
        name="take_side",
    )(back)


def body(queries, keys, values, doc_bounds, q_gain, k_gain):
    index = lax.axis_index("seqa") * lax.axis_size("seqb") + lax.axis_index("seqb")
    base = (index * TOK).astype(jnp.int32).reshape(1)
    inputs = [jnp.transpose(x, (0, 2, 1)) for x in (queries, keys, values)]
    packed = send_call(base, doc_bounds, *inputs, q_gain, k_gain)
    mine = lax.all_to_all(packed, AXES, split_axis=0, concat_axis=0, tiled=True)
    result = attend_call(doc_bounds, mine)
    back = lax.all_to_all(result, AXES, split_axis=0, concat_axis=0, tiled=True)
    return jnp.transpose(take_call(back), (0, 2, 1))


def solution(mesh):
    tokens = P(("dp", "seqa", "seqb"), None, None)
    return jax.shard_map(
        body,
        mesh=mesh,
        in_specs=(tokens, tokens, tokens, P("dp"), P(), P()),
        out_specs=tokens,
        check_vma=False,
    )
```

```python
import jax
import jax.numpy as jnp
from jax import lax
from jax.experimental import pallas as pl
from jax.experimental.pallas import tpu as pltpu
from jax.sharding import PartitionSpec as P

AXES = ("seqa", "seqb")
TOK = 32
ROWS = 16
HD = 64
HEADS = 128
DOCS = 8
SEQ = 4096
BLK = 256
PAIRS = BLK // 2
NBLK = SEQ // BLK
SRC = BLK // TOK
UNROLL = 8
GROUP = 16
FAR = (NBLK - 2) * (NBLK - 1) // 2 + UNROLL
NT = (((1,), (1,)), ((), ()))
NN = (((1,), (0,)), ((), ()))
BIG = 32768.0
SCALE = 1.4426950408889634 / 8.0
FIRST = -9.210340371976184


def dot(a, b, dims=NN):
    return lax.dot_general(a, b, dims, preferred_element_type=jnp.float32)


def starts_of(token, bounds_ref):
    start = jnp.zeros_like(token)
    for d in range(1, DOCS):
        start = jnp.where(token >= bounds_ref[d], bounds_ref[d], start)
    return start


def identity(n):
    row = lax.broadcasted_iota(jnp.int32, (n, n), 0)
    col = lax.broadcasted_iota(jnp.int32, (n, n), 1)
    return (row == col).astype(jnp.float32).astype(jnp.bfloat16)


def interleave():
    row = lax.broadcasted_iota(jnp.int32, (256, 256), 0)
    col = lax.broadcasted_iota(jnp.int32, (256, 256), 1)
    return (col == (row % 16) * 16 + row // 16).astype(jnp.float32).astype(jnp.bfloat16)


def send_kernel(
    base_ref, bounds_hbm, q_hbm, k_hbm, v_hbm, qg_hbm, kg_hbm, o_ref, bounds_ref, x_ref, g_ref, rot, turned, sems
):
    arriving = [
        pltpu.make_async_copy(source, target, sems.at[n])
        for n, (source, target) in enumerate(
            (
                (bounds_hbm, bounds_ref),
                (qg_hbm, g_ref.at[0]),
                (kg_hbm, g_ref.at[1]),
                (q_hbm, x_ref.at[0]),
                (v_hbm, x_ref.at[2]),
                (k_hbm, x_ref.at[1]),
            )
        )
    ]
    for c in arriving:
        c.start()
    for c in arriving[:3]:
        c.wait()
    lane = lax.broadcasted_iota(jnp.int32, (HD // 2, 128), 1)
    token = base_ref[0] + lane
    place = (token - starts_of(token, bounds_ref)).astype(jnp.float32)
    index = lax.broadcasted_iota(jnp.int32, (HD // 2, 128), 0).astype(jnp.float32)
    angle = place * jnp.exp(jnp.float32(FIRST) * index * 2.0 / HD)
    cosine = jnp.cos(angle)
    sine = jnp.sin(angle)
    eye = identity(HEADS)
    mix = interleave()

    def turn(n, r, rows):
        both = dot(eye, rows, NT).astype(jnp.bfloat16)
        turned[n, r] = both[:, :128]
        turned[n, r + 1] = both[:, 128:]

    def rotate(n):
        gain = jnp.transpose(jnp.broadcast_to(g_ref[n], (HEADS, HD)))
        for r in range(0, ROWS, 2):
            for t in (r, r + ROWS, r + 1, r + 1 + ROWS):
                c = jnp.broadcast_to(cosine[:, t : t + 1], (HD // 2, HEADS))
                s = jnp.broadcast_to(sine[:, t : t + 1], (HD // 2, HEADS))
                x = x_ref[n, t].astype(jnp.float32)
                scale = lax.rsqrt(jnp.mean(x * x, axis=0, keepdims=True) + 1e-06)
                x = x * scale * gain
                a, b = x[: HD // 2], x[HD // 2 :]
                y = jnp.concatenate([a * c - b * s, a * s + b * c], axis=0)
                rot[n, t % ROWS, pl.ds((t // ROWS) * HD, HD), :] = y.astype(jnp.bfloat16)
            turn(n, r, rot[n, r : r + 2].reshape(256, HEADS))

    def spread(n):
        for h in range(0, HEADS, 32):
            part = jnp.concatenate([turned[n, :, h + m : h + m + 16, :].reshape(256, 128) for m in (0, 16)], axis=1)
            both = dot(mix, part).astype(jnp.bfloat16)
            for m in range(2):
                heads = slice(h + 16 * m, h + 16 * m + 16)
                o_ref[heads, 16 * n : 16 * n + 16, :] = both[:, 128 * m : 128 * m + 128].reshape(16, 16, 128)

    arriving[3].wait()
    arriving[4].wait()
    for r in range(0, ROWS, 2):
        turn(2, r, jnp.concatenate([x_ref[2, t] for t in (r, r + ROWS, r + 1, r + 1 + ROWS)], axis=0))
    spread(2)
    rotate(0)
    arriving[5].wait()
    spread(0)
    rotate(1)
    spread(1)


def attend_kernel(bounds_ref, x_ref, o_ref, qt, kf, vt, near, far, total, summed, item_i, item_j):
    def offsets(shape, axis):
        n = lax.broadcasted_iota(jnp.int32, shape, axis)
        return ((n % PAIRS) // 16) * 32 + n % 16 + (n // PAIRS) * 16

    below = offsets((BLK, BLK), 0) <= offsets((BLK, BLK), 1)
    q_off = offsets((16, BLK), 1)
    k_off = offsets((BLK, 128), 0)

    def bounds_along(shape, axis):
        n = lax.broadcasted_iota(jnp.int32, shape, axis)
        out = jnp.full(shape, SEQ, jnp.int32)
        for d in range(1, DOCS):
            out = jnp.where(n == d, bounds_ref[d], out)
        return out

    q_bounds = bounds_along((16, BLK), 0)
    k_bounds = bounds_along((1, 128), 1)

    def list_block(i, n):
        def add(j, n):
            item_i[n] = i
            item_j[n] = j
            return n + 1

        return lax.fori_loop(starts_of(BLK * i, bounds_ref) // BLK, i - 1, add, n)

    n_far = lax.fori_loop(2, NBLK, list_block, jnp.int32(0))
    for u in range(UNROLL - 1):
        item_i[n_far + u] = NBLK
        item_j[n_far + u] = 0
    trips = (n_far + UNROLL - 1) // UNROLL
    zero = jnp.zeros((HD, BLK), jnp.bfloat16)
    rest = jnp.zeros((128 - 16, BLK), jnp.bfloat16)

    def wide(x):
        t = jnp.transpose(x.astype(jnp.float32)).astype(jnp.bfloat16)
        return jnp.concatenate([t[:HD], t[HD:]], axis=1)

    def scores(j, q, flags):
        k2 = x_ref[pl.ds(SRC * j, SRC), 16:32, :].reshape(PAIRS, 128)
        low = dot(jnp.concatenate([k2, kf[j, :PAIRS]], axis=1), jnp.concatenate([q, zero, flags, rest], axis=0))
        high = dot(jnp.concatenate([k2, kf[j, PAIRS:]], axis=1), jnp.concatenate([zero, q, flags, rest], axis=0))
        return jnp.exp2(jnp.concatenate([low, high], axis=0) * jnp.float32(SCALE))

    def flags_of(i):
        return jnp.where(BLK * i + q_off >= q_bounds, jnp.float32(-BIG), jnp.float32(0.0)).astype(jnp.bfloat16)

    def partial_sum(e):
        return jnp.sum(e.reshape(BLK // 8, 8, BLK), axis=0)

    def near_scores():
        for i in range(NBLK):
            q = wide(x_ref[pl.ds(SRC * i, SRC), 0:16, :].reshape(PAIRS, 128))
            qt[i] = q
            vt[i] = wide(x_ref[pl.ds(SRC * i, SRC), 32:48, :].reshape(PAIRS, 128))
            flags = flags_of(i)
            kf[i] = jnp.where(BLK * i + k_off < k_bounds, jnp.float32(1.0), jnp.float32(0.0)).astype(jnp.bfloat16)
            e1 = jnp.where(below, scores(i, q, flags), jnp.float32(0.0))
            e0 = scores(max(i - 1, 0), q, flags)
            if i == 0:
                e0 = jnp.zeros_like(e0)
            near[i, 0] = e0
            near[i, 1] = e1
            total[i] = partial_sum(e0) + partial_sum(e1)

    near_scores()

    def far_scores(w, _):
        for u in range(UNROLL):
            n = UNROLL * w + u
            i, j = item_i[n], item_j[n]
            e = scores(j, qt[i], flags_of(i))
            far[n] = e
            total[i] += partial_sum(e)
        return 0

    lax.fori_loop(0, trips, far_scores, 0)

    def near_values(g, _):
        for u in range(GROUP):
            i = GROUP * g + u
            inverse = 1.0 / jnp.sum(total[i], axis=0, keepdims=True)
            total[i] = jnp.broadcast_to(inverse, (8, BLK))
            w = jnp.concatenate([(near[i, n] * inverse).astype(jnp.bfloat16) for n in range(2)], axis=0)
            summed[i] = dot(jnp.concatenate([vt[jnp.maximum(i - 1, 0)], vt[i]], axis=1), w)
        return 0

    lax.fori_loop(0, NBLK // GROUP, near_values, 0)

    def far_values(w, _):
        for u in range(UNROLL):
            n = UNROLL * w + u
            i, j = item_i[n], item_j[n]
            summed[i] += dot(vt[j], (far[n] * total[i][0:1]).astype(jnp.bfloat16))
        return 0

    lax.fori_loop(0, trips, far_values, 0)

    def finish(g, _):
        for u in range(GROUP):
            i = GROUP * g + u
            out = summed[i]
            both = jnp.transpose(jnp.concatenate([out[:, :PAIRS], out[:, PAIRS:]], axis=0))
            o_ref[pl.ds(SRC * i, SRC)] = both.astype(jnp.bfloat16).reshape(SRC, 16, 128)
        return 0

    lax.fori_loop(0, NBLK // GROUP, finish, 0)


def take_kernel(x_ref, o_hbm, turned, out, sems):
    mix = interleave()
    eye = identity(128)
    for h in range(0, HEADS, 32):
        part = jnp.concatenate([x_ref[h + m : h + m + 16].reshape(256, 128) for m in (0, 16)], axis=1)
        both = dot(mix, part).astype(jnp.bfloat16)
        for m in range(2):
            turned[:, h + 16 * m : h + 16 * m + 16, :] = both[:, 128 * m : 128 * m + 128].reshape(16, 16, 128)
    copies = []
    for r in range(0, ROWS, 2):
        both = dot(eye, turned[r : r + 2].reshape(256, 128), NT).astype(jnp.bfloat16)
        for m in range(2):
            out[r + m] = both[:HD, 128 * m : 128 * m + 128]
            out[r + m + ROWS] = both[HD:, 128 * m : 128 * m + 128]
        if r % 8 == 6:
            for first in (r - 6, r - 6 + ROWS):
                copy = pltpu.make_async_copy(
                    out.at[pl.ds(first, 8)], o_hbm.at[pl.ds(first, 8)], sems.at[len(copies)]
                )
                copy.start()
                copies.append(copy)
    for copy in copies:
        copy.wait()


SMEM = pl.BlockSpec(memory_space=pltpu.SMEM)
VMEM = pl.BlockSpec(memory_space=pltpu.VMEM)
HBM = pl.BlockSpec(memory_space=pltpu.HBM)


def in_hbm(x):
    return pltpu.with_memory_space_constraint(x, pltpu.HBM)


def send_call(base, doc_bounds, q, k, v, q_gain, k_gain):
    return pl.pallas_call(
        send_kernel,
        out_shape=jax.ShapeDtypeStruct((HEADS, 48, 128), jnp.bfloat16),
        in_specs=[SMEM] + [HBM] * 6,
        out_specs=VMEM,
        scratch_shapes=[
            pltpu.SMEM((DOCS + 1,), jnp.int32),
            pltpu.VMEM((3, TOK, HD, HEADS), jnp.bfloat16),
            pltpu.VMEM((2, 1, HD), jnp.float32),
            pltpu.VMEM((2, ROWS, 128, HEADS), jnp.bfloat16),
            pltpu.VMEM((3, ROWS, HEADS, 128), jnp.bfloat16),
            pltpu.SemaphoreType.DMA((6,)),
        ],
        compiler_params=pltpu.CompilerParams(vmem_limit_bytes=32 << 20),
        name="send_side",
    )(base, *(in_hbm(x) for x in (doc_bounds, q, k, v, q_gain.reshape(1, HD), k_gain.reshape(1, HD))))


def attend_call(doc_bounds, mine):
    return pl.pallas_call(
        attend_kernel,
        out_shape=jax.ShapeDtypeStruct((SEQ // TOK, ROWS, 128), jnp.bfloat16),
        in_specs=[SMEM, VMEM],
        out_specs=VMEM,
        scratch_shapes=[
            pltpu.VMEM((NBLK + 1, HD, BLK), jnp.bfloat16),
            pltpu.VMEM((NBLK, BLK, 128), jnp.bfloat16),
            pltpu.VMEM((NBLK, HD, BLK), jnp.bfloat16),
            pltpu.VMEM((NBLK, 2, BLK, BLK), jnp.float32),
            pltpu.VMEM((FAR, BLK, BLK), jnp.float32),
            pltpu.VMEM((NBLK + 1, 8, BLK), jnp.float32),
            pltpu.VMEM((NBLK + 1, HD, BLK), jnp.float32),
            pltpu.SMEM((FAR,), jnp.int32),
            pltpu.SMEM((FAR,), jnp.int32),
        ],
        compiler_params=pltpu.CompilerParams(vmem_limit_bytes=44 << 20),
        name="attend",
    )(doc_bounds, mine)


def take_call(back):
    return pl.pallas_call(
        take_kernel,
        out_shape=jax.ShapeDtypeStruct((TOK, HD, HEADS), jnp.bfloat16),
        in_specs=[VMEM],
        out_specs=HBM,
        scratch_shapes=[
            pltpu.VMEM((ROWS, HEADS, 128), jnp.bfloat16),
            pltpu.VMEM((TOK, HD, HEADS), jnp.bfloat16),
            pltpu.SemaphoreType.DMA((4,)),
        ],
        compiler_params=pltpu.CompilerParams(vmem_limit_bytes=32 << 20),
        name="take_side",
    )(back)


def body(queries, keys, values, doc_bounds, q_gain, k_gain):
    index = lax.axis_index("seqa") * lax.axis_size("seqb") + lax.axis_index("seqb")
    base = (index * TOK).astype(jnp.int32).reshape(1)
    inputs = [jnp.transpose(x, (0, 2, 1)) for x in (queries, keys, values)]
    packed = send_call(base, doc_bounds, *inputs, q_gain, k_gain)
    mine = lax.all_to_all(packed, AXES, split_axis=0, concat_axis=0, tiled=True)
    result = attend_call(doc_bounds, mine)
    back = lax.all_to_all(result, AXES, split_axis=0, concat_axis=0, tiled=True)
    return jnp.transpose(take_call(back), (0, 2, 1))


def solution(mesh):
    tokens = P(("dp", "seqa", "seqb"), None, None)
    return jax.shard_map(
        body,
        mesh=mesh,
        in_specs=(tokens, tokens, tokens, P("dp"), P(), P()),
        out_specs=tokens,
        check_vma=False,
    )
```

```python
import jax
import jax.numpy as jnp
from jax import lax
from jax.experimental import pallas as pl
from jax.experimental.pallas import tpu as pltpu
from jax.sharding import PartitionSpec as P

AXES = ("seqa", "seqb")
TOK = 32
ROWS = 16
HD = 64
HEADS = 128
DOCS = 8
SEQ = 4096
BLK = 256
PAIRS = BLK // 2
NBLK = SEQ // BLK
SRC = BLK // TOK
UNROLL = 8
GROUP = 16
FAR = (NBLK - 2) * (NBLK - 1) // 2 + UNROLL
NT = (((1,), (1,)), ((), ()))
NN = (((1,), (0,)), ((), ()))
BIG = 32768.0
SCALE = 1.4426950408889634 / 8.0
FIRST = -9.210340371976184


def dot(a, b, dims=NN):
    return lax.dot_general(a, b, dims, preferred_element_type=jnp.float32)


def starts_of(token, bound):
    start = jnp.zeros_like(token)
    for d in range(1, DOCS):
        start = jnp.where(token >= bound(d), bound(d), start)
    return start


def identity(n):
    row = lax.broadcasted_iota(jnp.int32, (n, n), 0)
    col = lax.broadcasted_iota(jnp.int32, (n, n), 1)
    return (row == col).astype(jnp.float32).astype(jnp.bfloat16)


def interleave():
    row = lax.broadcasted_iota(jnp.int32, (256, 256), 0)
    col = lax.broadcasted_iota(jnp.int32, (256, 256), 1)
    return (col == (row % 16) * 16 + row // 16).astype(jnp.float32).astype(jnp.bfloat16)


def send_kernel(
    bounds_hbm, q_hbm, k_hbm, v_hbm, qg_hbm, kg_hbm, o_ref, bounds_ref, x_ref, g_ref, rot, turned, sems
):
    arriving = [
        pltpu.make_async_copy(source, target, sems.at[n])
        for n, (source, target) in enumerate(
            (
                (bounds_hbm, bounds_ref),
                (qg_hbm, g_ref.at[0]),
                (kg_hbm, g_ref.at[1]),
                (q_hbm, x_ref.at[0]),
                (v_hbm, x_ref.at[2]),
                (k_hbm, x_ref.at[1]),
            )
        )
    ]
    for c in arriving:
        c.start()
    for c in arriving[:3]:
        c.wait()
    lane = lax.broadcasted_iota(jnp.int32, (HD // 2, 128), 1)
    index = lax.axis_index("seqa") * lax.axis_size("seqb") + lax.axis_index("seqb")
    token = index * TOK + lane
    start = starts_of(token, lambda d: bounds_ref[:, d : d + 1])
    place = (token - start).astype(jnp.float32)
    index = lax.broadcasted_iota(jnp.int32, (HD // 2, 128), 0).astype(jnp.float32)
    angle = place * jnp.exp(jnp.float32(FIRST) * index * 2.0 / HD)
    cosine = jnp.cos(angle)
    sine = jnp.sin(angle)
    eye = identity(HEADS)
    mix = interleave()

    def turn(n, r, rows):
        both = dot(eye, rows, NT).astype(jnp.bfloat16)
        turned[n, r] = both[:, :128]
        turned[n, r + 1] = both[:, 128:]

    def rotate(n):
        gain = jnp.transpose(jnp.broadcast_to(g_ref[n], (HEADS, HD)))
        for r in range(0, ROWS, 2):
            for t in (r, r + ROWS, r + 1, r + 1 + ROWS):
                c = jnp.broadcast_to(cosine[:, t : t + 1], (HD // 2, HEADS))
                s = jnp.broadcast_to(sine[:, t : t + 1], (HD // 2, HEADS))
                x = x_ref[n, t].astype(jnp.float32)
                scale = lax.rsqrt(jnp.mean(x * x, axis=0, keepdims=True) + 1e-06)
                x = x * scale * gain
                a, b = x[: HD // 2], x[HD // 2 :]
                y = jnp.concatenate([a * c - b * s, a * s + b * c], axis=0)
                rot[n, t % ROWS, pl.ds((t // ROWS) * HD, HD), :] = y.astype(jnp.bfloat16)
            turn(n, r, rot[n, r : r + 2].reshape(256, HEADS))

    def spread(n):
        for h in range(0, HEADS, 32):
            part = jnp.concatenate([turned[n, :, h + m : h + m + 16, :].reshape(256, 128) for m in (0, 16)], axis=1)
            both = dot(mix, part).astype(jnp.bfloat16)
            for m in range(2):
                heads = slice(h + 16 * m, h + 16 * m + 16)
                o_ref[heads, 16 * n : 16 * n + 16, :] = both[:, 128 * m : 128 * m + 128].reshape(16, 16, 128)

    arriving[3].wait()
    arriving[4].wait()
    for r in range(0, ROWS, 2):
        turn(2, r, jnp.concatenate([x_ref[2, t] for t in (r, r + ROWS, r + 1, r + 1 + ROWS)], axis=0))
    spread(2)
    rotate(0)
    arriving[5].wait()
    spread(0)
    rotate(1)
    spread(1)


def attend_kernel(bounds_ref, x_ref, o_ref, qt, kf, vt, near, far, total, summed, items, scalars, sem):
    copy = pltpu.make_async_copy(bounds_ref, scalars, sem)
    copy.start()

    def offsets(shape, axis):
        n = lax.broadcasted_iota(jnp.int32, shape, axis)
        return ((n % PAIRS) // 16) * 32 + n % 16 + (n // PAIRS) * 16

    below = offsets((BLK, BLK), 0) <= offsets((BLK, BLK), 1)
    q_off = offsets((16, BLK), 1)
    k_off = offsets((BLK, 128), 0)

    def bounds_along(shape, axis):
        n = lax.broadcasted_iota(jnp.int32, shape, axis)
        out = jnp.full(shape, SEQ, jnp.int32)
        for d in range(1, DOCS):
            out = jnp.where(n == d, bounds_ref[:, d : d + 1], out)
        return out

    q_bounds = bounds_along((16, BLK), 0)
    k_bounds = bounds_along((1, 128), 1)

    zero = jnp.zeros((HD, BLK), jnp.bfloat16)
    rest = jnp.zeros((128 - 16, BLK), jnp.bfloat16)

    def wide(x):
        t = jnp.transpose(x.astype(jnp.float32)).astype(jnp.bfloat16)
        return jnp.concatenate([t[:HD], t[HD:]], axis=1)

    def scores(j, q, flags):
        k2 = x_ref[pl.ds(SRC * j, SRC), 16:32, :].reshape(PAIRS, 128)
        low = dot(jnp.concatenate([k2, kf[j, :PAIRS]], axis=1), jnp.concatenate([q, zero, flags, rest], axis=0))
        high = dot(jnp.concatenate([k2, kf[j, PAIRS:]], axis=1), jnp.concatenate([zero, q, flags, rest], axis=0))
        return jnp.exp2(jnp.concatenate([low, high], axis=0) * jnp.float32(SCALE))

    def flags_of(i):
        return jnp.where(BLK * i + q_off >= q_bounds, jnp.float32(-BIG), jnp.float32(0.0)).astype(jnp.bfloat16)

    def partial_sum(e):
        return jnp.sum(e.reshape(BLK // 8, 8, BLK), axis=0)

    def near_scores(blocks):
        for i in blocks:
            q = wide(x_ref[pl.ds(SRC * i, SRC), 0:16, :].reshape(PAIRS, 128))
            qt[i] = q
            vt[i] = wide(x_ref[pl.ds(SRC * i, SRC), 32:48, :].reshape(PAIRS, 128))
            flags = flags_of(i)
            kf[i] = jnp.where(BLK * i + k_off < k_bounds, jnp.float32(1.0), jnp.float32(0.0)).astype(jnp.bfloat16)
            e1 = jnp.where(below, scores(i, q, flags), jnp.float32(0.0))
            e0 = scores(max(i - 1, 0), q, flags)
            if i == 0:
                e0 = jnp.zeros_like(e0)
            near[i, 0] = e0
            near[i, 1] = e1
            total[i] = partial_sum(e0) + partial_sum(e1)

    near_scores(range(3))
    copy.wait()
    n_far = jnp.int32(0)
    for i in range(2, NBLK):
        start = starts_of(jnp.int32(BLK * i), lambda d: scalars[0, d])
        for j in range(i - 2, -1, -1):
            items[n_far] = NBLK * i + j
            n_far += (start < BLK * (j + 1)).astype(jnp.int32)
    near_scores(range(3, NBLK))
    for u in range(UNROLL - 1):
        items[n_far + u] = NBLK * NBLK
    trips = (n_far + UNROLL - 1) // UNROLL

    def far_scores(w, _):
        for u in range(UNROLL):
            n = UNROLL * w + u
            i, j = items[n] >> 4, items[n] & 15
            e = scores(j, qt[i], flags_of(i))
            far[n] = e
            total[i] += partial_sum(e)
        return 0

    lax.fori_loop(0, trips, far_scores, 0)

    for i in range(NBLK):
        inverse = 1.0 / jnp.sum(total[i], axis=0, keepdims=True)
        total[i] = jnp.broadcast_to(inverse, (8, BLK))
        summed[i] = jnp.zeros((HD, BLK), jnp.float32)

    def far_values(w, _):
        for u in range(UNROLL):
            n = UNROLL * w + u
            i, j = items[n] >> 4, items[n] & 15
            summed[i] += dot(vt[j], (far[n] * total[i][0:1]).astype(jnp.bfloat16))
        return 0

    lax.fori_loop(0, trips, far_values, 0)

    for i in range(NBLK):
        w = jnp.concatenate([(near[i, n] * total[i][0:1]).astype(jnp.bfloat16) for n in range(2)], axis=0)
        out = dot(jnp.concatenate([vt[max(i - 1, 0)], vt[i]], axis=1), w) + summed[i]
        both = jnp.transpose(jnp.concatenate([out[:, :PAIRS], out[:, PAIRS:]], axis=0))
        o_ref[SRC * i : SRC * i + SRC] = both.astype(jnp.bfloat16).reshape(SRC, 16, 128)


def take_kernel(x_ref, o_hbm, turned, out, sems):
    mix = interleave()
    eye = identity(128)
    for h in range(0, HEADS, 32):
        part = jnp.concatenate([x_ref[h + m : h + m + 16].reshape(256, 128) for m in (0, 16)], axis=1)
        both = dot(mix, part).astype(jnp.bfloat16)
        for m in range(2):
            turned[:, h + 16 * m : h + 16 * m + 16, :] = both[:, 128 * m : 128 * m + 128].reshape(16, 16, 128)
    copies = []
    for r in range(0, ROWS, 2):
        both = dot(eye, turned[r : r + 2].reshape(256, 128), NT).astype(jnp.bfloat16)
        for m in range(2):
            out[r + m] = both[:HD, 128 * m : 128 * m + 128]
            out[r + m + ROWS] = both[HD:, 128 * m : 128 * m + 128]
        if r % 8 == 6:
            for first in (r - 6, r - 6 + ROWS):
                copy = pltpu.make_async_copy(
                    out.at[pl.ds(first, 8)], o_hbm.at[pl.ds(first, 8)], sems.at[len(copies)]
                )
                copy.start()
                copies.append(copy)
    for copy in copies:
        copy.wait()


VMEM = pl.BlockSpec(memory_space=pltpu.VMEM)
HBM = pl.BlockSpec(memory_space=pltpu.HBM)


def in_hbm(x):
    return pltpu.with_memory_space_constraint(x, pltpu.HBM)


def send_call(doc_bounds, q, k, v, q_gain, k_gain):
    return pl.pallas_call(
        send_kernel,
        out_shape=jax.ShapeDtypeStruct((HEADS, 48, 128), jnp.bfloat16),
        in_specs=[HBM] * 6,
        out_specs=VMEM,
        scratch_shapes=[
            pltpu.VMEM((1, DOCS + 1), jnp.int32),
            pltpu.VMEM((3, TOK, HD, HEADS), jnp.bfloat16),
            pltpu.VMEM((2, 1, HD), jnp.float32),
            pltpu.VMEM((2, ROWS, 128, HEADS), jnp.bfloat16),
            pltpu.VMEM((3, ROWS, HEADS, 128), jnp.bfloat16),
            pltpu.SemaphoreType.DMA((6,)),
        ],
        compiler_params=pltpu.CompilerParams(vmem_limit_bytes=32 << 20),
        name="send_side",
    )(*(in_hbm(x) for x in (doc_bounds, q, k, v, q_gain.reshape(1, HD), k_gain.reshape(1, HD))))


def attend_call(doc_bounds, mine):
    return pl.pallas_call(
        attend_kernel,
        out_shape=jax.ShapeDtypeStruct((SEQ // TOK, ROWS, 128), jnp.bfloat16),
        in_specs=[VMEM, VMEM],
        out_specs=VMEM,
        scratch_shapes=[
            pltpu.VMEM((NBLK + 1, HD, BLK), jnp.bfloat16),
            pltpu.VMEM((NBLK, BLK, 128), jnp.bfloat16),
            pltpu.VMEM((NBLK, HD, BLK), jnp.bfloat16),
            pltpu.VMEM((NBLK, 2, BLK, BLK), jnp.float32),
            pltpu.VMEM((FAR, BLK, BLK), jnp.float32),
            pltpu.VMEM((NBLK + 1, 8, BLK), jnp.float32),
            pltpu.VMEM((NBLK + 1, HD, BLK), jnp.float32),
            pltpu.SMEM((FAR,), jnp.int32),
            pltpu.SMEM((1, DOCS + 1), jnp.int32),
            pltpu.SemaphoreType.DMA(()),
        ],
        compiler_params=pltpu.CompilerParams(vmem_limit_bytes=44 << 20),
        name="attend",
    )(doc_bounds, mine)


def take_call(back):
    return pl.pallas_call(
        take_kernel,
        out_shape=jax.ShapeDtypeStruct((TOK, HD, HEADS), jnp.bfloat16),
        in_specs=[VMEM],
        out_specs=HBM,
        scratch_shapes=[
            pltpu.VMEM((ROWS, HEADS, 128), jnp.bfloat16),
            pltpu.VMEM((TOK, HD, HEADS), jnp.bfloat16),
            pltpu.SemaphoreType.DMA((4,)),
        ],
        compiler_params=pltpu.CompilerParams(vmem_limit_bytes=32 << 20),
        name="take_side",
    )(back)


def body(queries, keys, values, doc_bounds, q_gain, k_gain):
    doc_bounds = doc_bounds.reshape(1, DOCS + 1)
    inputs = [jnp.transpose(x, (0, 2, 1)) for x in (queries, keys, values)]
    packed = send_call(doc_bounds, *inputs, q_gain, k_gain)
    mine = lax.all_to_all(packed, AXES, split_axis=0, concat_axis=0, tiled=True)
    result = attend_call(doc_bounds, mine)
    back = lax.all_to_all(result, AXES, split_axis=0, concat_axis=0, tiled=True)
    return jnp.transpose(take_call(back), (0, 2, 1))


def solution(mesh):
    tokens = P(("dp", "seqa", "seqb"), None, None)
    return jax.shard_map(
        body,
        mesh=mesh,
        in_specs=(tokens, tokens, tokens, P("dp"), P(), P()),
        out_specs=tokens,
        check_vma=False,
    )
```

```python
import jax
import jax.numpy as jnp
from jax import lax
from jax.experimental import pallas as pl
from jax.experimental.pallas import tpu as pltpu
from jax.sharding import PartitionSpec as P

AXES = ("seqa", "seqb")
TOK = 32
ROWS = 16
HD = 64
HEADS = 128
DOCS = 8
SEQ = 4096
BLK = 256
PAIRS = BLK // 2
NBLK = SEQ // BLK
SRC = BLK // TOK
LONG, MIDDLE, SHORT = 16, 8, 4
FAR = (NBLK - 2) * (NBLK - 1) // 2 + LONG
NT = (((1,), (1,)), ((), ()))
NN = (((1,), (0,)), ((), ()))
BIG = 32768.0
SCALE = 1.4426950408889634 / 8.0
FIRST = -9.210340371976184


def dot(a, b, dims=NN):
    return lax.dot_general(a, b, dims, preferred_element_type=jnp.float32)


def starts_of(token, bound):
    start = jnp.zeros_like(token)
    for d in range(1, DOCS):
        start = jnp.where(token >= bound(d), bound(d), start)
    return start


def identity(n):
    row = lax.broadcasted_iota(jnp.int32, (n, n), 0)
    col = lax.broadcasted_iota(jnp.int32, (n, n), 1)
    return (row == col).astype(jnp.float32).astype(jnp.bfloat16)


def interleave():
    row = lax.broadcasted_iota(jnp.int32, (256, 256), 0)
    col = lax.broadcasted_iota(jnp.int32, (256, 256), 1)
    return (col == (row % 16) * 16 + row // 16).astype(jnp.float32).astype(jnp.bfloat16)


def send_kernel(
    bounds_hbm, q_hbm, k_hbm, v_hbm, qg_hbm, kg_hbm, o_ref, bounds_ref, x_ref, g_ref, rot, turned, sems
):
    arriving = [
        pltpu.make_async_copy(source, target, sems.at[n])
        for n, (source, target) in enumerate(
            (
                (bounds_hbm, bounds_ref),
                (qg_hbm, g_ref.at[0]),
                (kg_hbm, g_ref.at[1]),
                (q_hbm, x_ref.at[0]),
                (v_hbm, x_ref.at[2]),
                (k_hbm, x_ref.at[1]),
            )
        )
    ]
    for c in arriving:
        c.start()
    for c in arriving[:3]:
        c.wait()
    lane = lax.broadcasted_iota(jnp.int32, (HD // 2, 128), 1)
    index = lax.axis_index("seqa") * lax.axis_size("seqb") + lax.axis_index("seqb")
    token = index * TOK + lane
    start = starts_of(token, lambda d: bounds_ref[:, d : d + 1])
    place = (token - start).astype(jnp.float32)
    index = lax.broadcasted_iota(jnp.int32, (HD // 2, 128), 0).astype(jnp.float32)
    angle = place * jnp.exp(jnp.float32(FIRST) * index * 2.0 / HD)
    cosine = jnp.cos(angle)
    sine = jnp.sin(angle)
    eye = identity(HEADS)
    mix = interleave()

    def turn(n, r, rows):
        both = dot(eye, rows, NT).astype(jnp.bfloat16)
        turned[n, r] = both[:, :128]
        turned[n, r + 1] = both[:, 128:]

    def rotate(n):
        gain = jnp.transpose(jnp.broadcast_to(g_ref[n], (HEADS, HD)))
        for r in range(0, ROWS, 2):
            for t in (r, r + ROWS, r + 1, r + 1 + ROWS):
                c = jnp.broadcast_to(cosine[:, t : t + 1], (HD // 2, HEADS))
                s = jnp.broadcast_to(sine[:, t : t + 1], (HD // 2, HEADS))
                x = x_ref[n, t].astype(jnp.float32)
                scale = lax.rsqrt(jnp.mean(x * x, axis=0, keepdims=True) + 1e-06)
                x = x * scale * gain
                a, b = x[: HD // 2], x[HD // 2 :]
                y = jnp.concatenate([a * c - b * s, a * s + b * c], axis=0)
                rot[n, t % ROWS, pl.ds((t // ROWS) * HD, HD), :] = y.astype(jnp.bfloat16)
            turn(n, r, rot[n, r : r + 2].reshape(256, HEADS))

    def spread(n):
        for h in range(0, HEADS, 32):
            part = jnp.concatenate([turned[n, :, h + m : h + m + 16, :].reshape(256, 128) for m in (0, 16)], axis=1)
            both = dot(mix, part).astype(jnp.bfloat16)
            for m in range(2):
                heads = slice(h + 16 * m, h + 16 * m + 16)
                o_ref[heads, 16 * n : 16 * n + 16, :] = both[:, 128 * m : 128 * m + 128].reshape(16, 16, 128)

    for c in arriving[3:]:
        c.wait()

    def turn_values():
        for r in range(0, ROWS, 2):
            turn(2, r, jnp.concatenate([x_ref[2, t] for t in (r, r + ROWS, r + 1, r + 1 + ROWS)], axis=0))

    turn_values()
    rotate(0)
    spread(2)
    rotate(1)
    spread(0)
    spread(1)


def attend_kernel(bounds_ref, x_ref, o_ref, qt, kf, vt, near, far, total, summed, items):

    def offsets(shape, axis):
        n = lax.broadcasted_iota(jnp.int32, shape, axis)
        return ((n % PAIRS) // 16) * 32 + n % 16 + (n // PAIRS) * 16

    below = offsets((BLK, BLK), 0) <= offsets((BLK, BLK), 1)
    q_off = offsets((16, BLK), 1)
    k_off = offsets((BLK, 128), 0)

    def bounds_along(shape, axis):
        n = lax.broadcasted_iota(jnp.int32, shape, axis)
        out = jnp.full(shape, SEQ, jnp.int32)
        for d in range(1, DOCS):
            out = jnp.where(n == d, bounds_ref[:, d : d + 1], out)
        return out

    q_bounds = bounds_along((16, BLK), 0)
    k_bounds = bounds_along((1, 128), 1)

    zero = jnp.zeros((HD, BLK), jnp.bfloat16)
    rest = jnp.zeros((128 - 16, BLK), jnp.bfloat16)

    def wide(x):
        t = jnp.transpose(x.astype(jnp.float32)).astype(jnp.bfloat16)
        return jnp.concatenate([t[:HD], t[HD:]], axis=1)

    def scores(j, q, flags):
        k2 = x_ref[pl.ds(SRC * j, SRC), 16:32, :].reshape(PAIRS, 128)
        low = dot(jnp.concatenate([k2, kf[j, :PAIRS]], axis=1), jnp.concatenate([q, zero, flags, rest], axis=0))
        high = dot(jnp.concatenate([k2, kf[j, PAIRS:]], axis=1), jnp.concatenate([zero, q, flags, rest], axis=0))
        return jnp.exp2(jnp.concatenate([low, high], axis=0) * jnp.float32(SCALE))

    def flags_of(i):
        return jnp.where(BLK * i + q_off >= q_bounds, jnp.float32(-BIG), jnp.float32(0.0)).astype(jnp.bfloat16)

    def partial_sum(e):
        return jnp.sum(e.reshape(BLK // 8, 8, BLK), axis=0)

    def near_scores(blocks):
        for i in blocks:
            q = wide(x_ref[pl.ds(SRC * i, SRC), 0:16, :].reshape(PAIRS, 128))
            qt[i] = q
            vt[i] = wide(x_ref[pl.ds(SRC * i, SRC), 32:48, :].reshape(PAIRS, 128))
            flags = flags_of(i)
            kf[i] = jnp.where(BLK * i + k_off < k_bounds, jnp.float32(1.0), jnp.float32(0.0)).astype(jnp.bfloat16)
            e1 = jnp.where(below, scores(i, q, flags), jnp.float32(0.0))
            e0 = scores(max(i - 1, 0), q, flags)
            if i == 0:
                e0 = jnp.zeros_like(e0)
            near[i, 0] = e0
            near[i, 1] = e1
            total[i] = partial_sum(e0) + partial_sum(e1)

    scalars = [jnp.max(bounds_ref[:, d : d + 1]) for d in range(DOCS)]
    n_far = jnp.int32(0)
    for i in range(2, NBLK):
        start = starts_of(jnp.int32(BLK * i), lambda d: scalars[d])
        for j in range(i - 2, -1, -1):
            items[n_far] = NBLK * i + j
            n_far += (start < BLK * (j + 1)).astype(jnp.int32)
    near_scores(range(NBLK))
    for u in range(LONG - 1):
        items[n_far + u] = NBLK * NBLK
    trips = (n_far + LONG - MIDDLE - 1) // LONG
    left = n_far - LONG * trips
    passes = (
        (0, trips, LONG),
        (LONG * trips, (left > SHORT).astype(jnp.int32), MIDDLE),
        (LONG * trips, ((left > 0) & (left <= SHORT)).astype(jnp.int32), SHORT),
    )

    def far_blocks(work):
        for begin, trips, length in passes:

            def trip(w, _, begin=begin, length=length):
                for u in range(length):
                    n = begin + length * w + u
                    work(n, items[n] >> 4, items[n] & 15)
                return 0

            lax.fori_loop(0, trips, trip, 0)

    def far_scores(n, i, j):
        e = scores(j, qt[i], flags_of(i))
        far[n] = e
        total[i] += partial_sum(e)

    far_blocks(far_scores)
    for i in range(NBLK):
        inverse = 1.0 / jnp.sum(total[i], axis=0, keepdims=True)
        total[i] = jnp.broadcast_to(inverse, (8, BLK))
        summed[i] = jnp.zeros((HD, BLK), jnp.float32)

    def far_values(n, i, j):
        summed[i] += dot(vt[j], (far[n] * total[i][0:1]).astype(jnp.bfloat16))

    far_blocks(far_values)

    for i in range(NBLK):
        w = jnp.concatenate([(near[i, n] * total[i][0:1]).astype(jnp.bfloat16) for n in range(2)], axis=0)
        out = dot(jnp.concatenate([vt[max(i - 1, 0)], vt[i]], axis=1), w) + summed[i]
        both = jnp.transpose(jnp.concatenate([out[:, :PAIRS], out[:, PAIRS:]], axis=0))
        o_ref[SRC * i : SRC * i + SRC] = both.astype(jnp.bfloat16).reshape(SRC, 16, 128)


def take_kernel(x_ref, o_hbm, turned, out, sems):
    mix = interleave()
    eye = identity(128)
    for h in range(0, HEADS, 32):
        part = jnp.concatenate([x_ref[h + m : h + m + 16].reshape(256, 128) for m in (0, 16)], axis=1)
        both = dot(mix, part).astype(jnp.bfloat16)
        for m in range(2):
            turned[:, h + 16 * m : h + 16 * m + 16, :] = both[:, 128 * m : 128 * m + 128].reshape(16, 16, 128)
    copies = []
    for r in range(0, ROWS, 2):
        both = dot(eye, turned[r : r + 2].reshape(256, 128), NT).astype(jnp.bfloat16)
        for m in range(2):
            out[r + m] = both[:HD, 128 * m : 128 * m + 128]
            out[r + m + ROWS] = both[HD:, 128 * m : 128 * m + 128]
        if r % 8 == 6:
            for first in (r - 6, r - 6 + ROWS):
                copy = pltpu.make_async_copy(
                    out.at[pl.ds(first, 8)], o_hbm.at[pl.ds(first, 8)], sems.at[len(copies)]
                )
                copy.start()
                copies.append(copy)
    for copy in copies:
        copy.wait()


VMEM = pl.BlockSpec(memory_space=pltpu.VMEM)
HBM = pl.BlockSpec(memory_space=pltpu.HBM)


def in_hbm(x):
    return pltpu.with_memory_space_constraint(x, pltpu.HBM)


def send_call(doc_bounds, q, k, v, q_gain, k_gain):
    return pl.pallas_call(
        send_kernel,
        out_shape=jax.ShapeDtypeStruct((HEADS, 48, 128), jnp.bfloat16),
        in_specs=[HBM] * 6,
        out_specs=VMEM,
        scratch_shapes=[
            pltpu.VMEM((1, DOCS + 1), jnp.int32),
            pltpu.VMEM((3, TOK, HD, HEADS), jnp.bfloat16),
            pltpu.VMEM((2, 1, HD), jnp.float32),
            pltpu.VMEM((2, ROWS, 128, HEADS), jnp.bfloat16),
            pltpu.VMEM((3, ROWS, HEADS, 128), jnp.bfloat16),
            pltpu.SemaphoreType.DMA((6,)),
        ],
        compiler_params=pltpu.CompilerParams(vmem_limit_bytes=32 << 20),
        name="send_side",
    )(*(in_hbm(x) for x in (doc_bounds, q, k, v, q_gain.reshape(1, HD), k_gain.reshape(1, HD))))


def attend_call(doc_bounds, mine):
    return pl.pallas_call(
        attend_kernel,
        out_shape=jax.ShapeDtypeStruct((SEQ // TOK, ROWS, 128), jnp.bfloat16),
        in_specs=[VMEM, VMEM],
        out_specs=VMEM,
        scratch_shapes=[
            pltpu.VMEM((NBLK + 1, HD, BLK), jnp.bfloat16),
            pltpu.VMEM((NBLK, BLK, 128), jnp.bfloat16),
            pltpu.VMEM((NBLK, HD, BLK), jnp.bfloat16),
            pltpu.VMEM((NBLK, 2, BLK, BLK), jnp.float32),
            pltpu.VMEM((FAR, BLK, BLK), jnp.float32),
            pltpu.VMEM((NBLK + 1, 8, BLK), jnp.float32),
            pltpu.VMEM((NBLK + 1, HD, BLK), jnp.float32),
            pltpu.SMEM((FAR,), jnp.int32),
        ],
        compiler_params=pltpu.CompilerParams(vmem_limit_bytes=44 << 20),
        name="attend",
    )(doc_bounds, mine)


def take_call(back):
    return pl.pallas_call(
        take_kernel,
        out_shape=jax.ShapeDtypeStruct((TOK, HD, HEADS), jnp.bfloat16),
        in_specs=[VMEM],
        out_specs=HBM,
        scratch_shapes=[
            pltpu.VMEM((ROWS, HEADS, 128), jnp.bfloat16),
            pltpu.VMEM((TOK, HD, HEADS), jnp.bfloat16),
            pltpu.SemaphoreType.DMA((4,)),
        ],
        compiler_params=pltpu.CompilerParams(vmem_limit_bytes=32 << 20),
        name="take_side",
    )(back)


def body(queries, keys, values, doc_bounds, q_gain, k_gain):
    doc_bounds = doc_bounds.reshape(1, DOCS + 1)
    inputs = [jnp.transpose(x, (0, 2, 1)) for x in (queries, keys, values)]
    packed = send_call(doc_bounds, *inputs, q_gain, k_gain)
    mine = lax.all_to_all(packed, AXES, split_axis=0, concat_axis=0, tiled=True)
    result = attend_call(doc_bounds, mine)
    back = lax.all_to_all(result, AXES, split_axis=0, concat_axis=0, tiled=True)
    return jnp.transpose(take_call(back), (0, 2, 1))


def solution(mesh):
    tokens = P(("dp", "seqa", "seqb"), None, None)
    return jax.shard_map(
        body,
        mesh=mesh,
        in_specs=(tokens, tokens, tokens, P("dp"), P(), P()),
        out_specs=tokens,
        check_vma=False,
    )
```

```python
import jax
import jax.numpy as jnp
from jax import lax
from jax.experimental import pallas as pl
from jax.experimental.pallas import tpu as pltpu
from jax.sharding import PartitionSpec as P

ORDER = ("zh", "zl", "x", "c")
TOK = 32
ROWS = 16
HD = 64
HEADS = 128
DOCS = 8
SEQ = 4096
BLK = 256
PAIRS = BLK // 2
NBLK = SEQ // BLK
SRC = BLK // TOK
LONG, MIDDLE, SHORT = 16, 8, 4
FAR = (NBLK - 2) * (NBLK - 1) // 2 + LONG
NT = (((1,), (1,)), ((), ()))
NN = (((1,), (0,)), ((), ()))
BIG = 32768.0
SCALE = 1.4426950408889634 / 8.0
FIRST = -9.210340371976184


def dot(a, b, dims=NN):
    return lax.dot_general(a, b, dims, preferred_element_type=jnp.float32)


def starts_of(token, bound):
    start = jnp.zeros_like(token)
    for d in range(1, DOCS):
        start = jnp.where(token >= bound(d), bound(d), start)
    return start


def identity(n):
    row = lax.broadcasted_iota(jnp.int32, (n, n), 0)
    col = lax.broadcasted_iota(jnp.int32, (n, n), 1)
    return (row == col).astype(jnp.float32).astype(jnp.bfloat16)


def interleave():
    row = lax.broadcasted_iota(jnp.int32, (256, 256), 0)
    col = lax.broadcasted_iota(jnp.int32, (256, 256), 1)
    return (col == (row % 16) * 16 + row // 16).astype(jnp.float32).astype(jnp.bfloat16)


def send_kernel(
    bounds_hbm, q_hbm, k_hbm, v_hbm, qg_hbm, kg_hbm, o_ref, bounds_ref, x_ref, g_ref, rot, turned, sems
):
    arriving = [
        pltpu.make_async_copy(source, target, sems.at[n])
        for n, (source, target) in enumerate(
            (
                (bounds_hbm, bounds_ref),
                (qg_hbm, g_ref.at[0]),
                (kg_hbm, g_ref.at[1]),
                (q_hbm, x_ref.at[0]),
                (v_hbm, x_ref.at[2]),
                (k_hbm, x_ref.at[1]),
            )
        )
    ]
    for c in arriving:
        c.start()
    for c in arriving[:3]:
        c.wait()
    lane = lax.broadcasted_iota(jnp.int32, (HD // 2, 128), 1)
    seqa = lax.axis_index("zl") * 2 + lax.axis_index("c")
    seqb = lax.axis_index("x") * 2 + lax.axis_index("zh")
    index = seqa * SRC + seqb
    token = index * TOK + lane
    start = starts_of(token, lambda d: bounds_ref[:, d : d + 1])
    place = (token - start).astype(jnp.float32)
    index = lax.broadcasted_iota(jnp.int32, (HD // 2, 128), 0).astype(jnp.float32)
    angle = place * jnp.exp(jnp.float32(FIRST) * index * 2.0 / HD)
    cosine = jnp.cos(angle)
    sine = jnp.sin(angle)
    eye = identity(HEADS)
    mix = interleave()

    def turn(n, r, rows):
        both = dot(eye, rows, NT).astype(jnp.bfloat16)
        turned[n, r] = both[:, :128]
        turned[n, r + 1] = both[:, 128:]

    def rotate(n):
        gain = jnp.transpose(jnp.broadcast_to(g_ref[n], (HEADS, HD)))
        for r in range(0, ROWS, 2):
            for t in (r, r + ROWS, r + 1, r + 1 + ROWS):
                c = jnp.broadcast_to(cosine[:, t : t + 1], (HD // 2, HEADS))
                s = jnp.broadcast_to(sine[:, t : t + 1], (HD // 2, HEADS))
                x = x_ref[n, t].astype(jnp.float32)
                scale = lax.rsqrt(jnp.mean(x * x, axis=0, keepdims=True) + 1e-06)
                x = x * scale * gain
                a, b = x[: HD // 2], x[HD // 2 :]
                y = jnp.concatenate([a * c - b * s, a * s + b * c], axis=0)
                rot[n, t % ROWS, pl.ds((t // ROWS) * HD, HD), :] = y.astype(jnp.bfloat16)
            turn(n, r, rot[n, r : r + 2].reshape(256, HEADS))

    def spread(n):
        for h in range(0, HEADS, 32):
            part = jnp.concatenate([turned[n, :, h + m : h + m + 16, :].reshape(256, 128) for m in (0, 16)], axis=1)
            both = dot(mix, part).astype(jnp.bfloat16)
            for m in range(2):
                heads = slice(h + 16 * m, h + 16 * m + 16)
                o_ref[heads, 16 * n : 16 * n + 16, :] = both[:, 128 * m : 128 * m + 128].reshape(16, 16, 128)

    for c in arriving[3:]:
        c.wait()

    def turn_values():
        for r in range(0, ROWS, 2):
            turn(2, r, jnp.concatenate([x_ref[2, t] for t in (r, r + ROWS, r + 1, r + 1 + ROWS)], axis=0))

    turn_values()
    rotate(0)
    spread(2)
    rotate(1)
    spread(0)
    spread(1)


def attend_kernel(bounds_ref, x_ref, o_ref, qt, kf, vt, near, far, total, summed, items):

    def offsets(shape, axis):
        n = lax.broadcasted_iota(jnp.int32, shape, axis)
        run = (n % PAIRS) // 16
        return (run % 4 * 2 + run // 4) * 32 + n % 16 + (n // PAIRS) * 16

    below = offsets((BLK, BLK), 0) <= offsets((BLK, BLK), 1)
    q_off = offsets((16, BLK), 1)
    k_off = offsets((BLK, 128), 0)

    def bounds_along(shape, axis):
        n = lax.broadcasted_iota(jnp.int32, shape, axis)
        out = jnp.full(shape, SEQ, jnp.int32)
        for d in range(1, DOCS):
            out = jnp.where(n == d, bounds_ref[:, d : d + 1], out)
        return out

    q_bounds = bounds_along((16, BLK), 0)
    k_bounds = bounds_along((1, 128), 1)

    zero = jnp.zeros((HD, BLK), jnp.bfloat16)
    rest = jnp.zeros((128 - 16, BLK), jnp.bfloat16)

    def wide(x):
        t = jnp.transpose(x.astype(jnp.float32)).astype(jnp.bfloat16)
        return jnp.concatenate([t[:HD], t[HD:]], axis=1)

    def scores(j, q, flags):
        k2 = x_ref[:, j >> 1, :, j & 1, 16:32, :].reshape(PAIRS, 128)
        low = dot(jnp.concatenate([k2, kf[j, :PAIRS]], axis=1), jnp.concatenate([q, zero, flags, rest], axis=0))
        high = dot(jnp.concatenate([k2, kf[j, PAIRS:]], axis=1), jnp.concatenate([zero, q, flags, rest], axis=0))
        return jnp.exp2(jnp.concatenate([low, high], axis=0) * jnp.float32(SCALE))

    def flags_of(i):
        return jnp.where(BLK * i + q_off >= q_bounds, jnp.float32(-BIG), jnp.float32(0.0)).astype(jnp.bfloat16)

    def partial_sum(e):
        return jnp.sum(e.reshape(BLK // 8, 8, BLK), axis=0)

    def near_scores(blocks):
        for i in blocks:
            q = wide(x_ref[:, i >> 1, :, i & 1, 0:16, :].reshape(PAIRS, 128))
            qt[i] = q
            vt[i] = wide(x_ref[:, i >> 1, :, i & 1, 32:48, :].reshape(PAIRS, 128))
            flags = flags_of(i)
            kf[i] = jnp.where(BLK * i + k_off < k_bounds, jnp.float32(1.0), jnp.float32(0.0)).astype(jnp.bfloat16)
            e1 = jnp.where(below, scores(i, q, flags), jnp.float32(0.0))
            e0 = scores(max(i - 1, 0), q, flags)
            if i == 0:
                e0 = jnp.zeros_like(e0)
            near[i, 0] = e0
            near[i, 1] = e1
            total[i] = partial_sum(e0) + partial_sum(e1)

    scalars = [jnp.max(bounds_ref[:, d : d + 1]) for d in range(DOCS)]
    n_far = jnp.int32(0)
    for i in range(2, NBLK):
        start = starts_of(jnp.int32(BLK * i), lambda d: scalars[d])
        for j in range(i - 2, -1, -1):
            items[n_far] = NBLK * i + j
            n_far += (start < BLK * (j + 1)).astype(jnp.int32)
    near_scores(range(NBLK))
    for u in range(LONG - 1):
        items[n_far + u] = NBLK * NBLK
    trips = (n_far + LONG - MIDDLE - 1) // LONG
    left = n_far - LONG * trips
    passes = (
        (0, trips, LONG),
        (LONG * trips, (left > SHORT).astype(jnp.int32), MIDDLE),
        (LONG * trips, ((left > 0) & (left <= SHORT)).astype(jnp.int32), SHORT),
    )

    def far_blocks(work):
        for begin, trips, length in passes:

            def trip(w, _, begin=begin, length=length):
                for u in range(length):
                    n = begin + length * w + u
                    work(n, items[n] >> 4, items[n] & 15)
                return 0

            lax.fori_loop(0, trips, trip, 0)

    def far_scores(n, i, j):
        e = scores(j, qt[i], flags_of(i))
        far[n] = e
        total[i] += partial_sum(e)

    far_blocks(far_scores)
    for i in range(NBLK):
        inverse = 1.0 / jnp.sum(total[i], axis=0, keepdims=True)
        total[i] = jnp.broadcast_to(inverse, (8, BLK))
        summed[i] = jnp.zeros((HD, BLK), jnp.float32)

    def far_values(n, i, j):
        summed[i] += dot(vt[j], (far[n] * total[i][0:1]).astype(jnp.bfloat16))

    far_blocks(far_values)

    for i in range(NBLK):
        w = jnp.concatenate([(near[i, n] * total[i][0:1]).astype(jnp.bfloat16) for n in range(2)], axis=0)
        out = dot(jnp.concatenate([vt[max(i - 1, 0)], vt[i]], axis=1), w) + summed[i]
        both = jnp.transpose(jnp.concatenate([out[:, :PAIRS], out[:, PAIRS:]], axis=0))
        o_ref[:, i >> 1, :, i & 1] = both.astype(jnp.bfloat16).reshape(2, 4, 16, 128)


def take_kernel(x_ref, o_hbm, turned, out, sems):
    mix = interleave()
    eye = identity(128)
    for h in range(0, HEADS, 32):
        part = jnp.concatenate([x_ref[h + m : h + m + 16].reshape(256, 128) for m in (0, 16)], axis=1)
        both = dot(mix, part).astype(jnp.bfloat16)
        for m in range(2):
            turned[:, h + 16 * m : h + 16 * m + 16, :] = both[:, 128 * m : 128 * m + 128].reshape(16, 16, 128)
    copies = []
    for r in range(0, ROWS, 2):
        both = dot(eye, turned[r : r + 2].reshape(256, 128), NT).astype(jnp.bfloat16)
        for m in range(2):
            out[r + m] = both[:HD, 128 * m : 128 * m + 128]
            out[r + m + ROWS] = both[HD:, 128 * m : 128 * m + 128]
        if r % 8 == 6:
            for first in (r - 6, r - 6 + ROWS):
                copy = pltpu.make_async_copy(
                    out.at[pl.ds(first, 8)], o_hbm.at[pl.ds(first, 8)], sems.at[len(copies)]
                )
                copy.start()
                copies.append(copy)
    for copy in copies:
        copy.wait()


VMEM = pl.BlockSpec(memory_space=pltpu.VMEM)
HBM = pl.BlockSpec(memory_space=pltpu.HBM)


def in_hbm(x):
    return pltpu.with_memory_space_constraint(x, pltpu.HBM)


def send_call(doc_bounds, q, k, v, q_gain, k_gain):
    return pl.pallas_call(
        send_kernel,
        out_shape=jax.ShapeDtypeStruct((HEADS, 48, 128), jnp.bfloat16),
        in_specs=[HBM] * 6,
        out_specs=VMEM,
        scratch_shapes=[
            pltpu.VMEM((1, DOCS + 1), jnp.int32),
            pltpu.VMEM((3, TOK, HD, HEADS), jnp.bfloat16),
            pltpu.VMEM((2, 1, HD), jnp.float32),
            pltpu.VMEM((2, ROWS, 128, HEADS), jnp.bfloat16),
            pltpu.VMEM((3, ROWS, HEADS, 128), jnp.bfloat16),
            pltpu.SemaphoreType.DMA((6,)),
        ],
        compiler_params=pltpu.CompilerParams(vmem_limit_bytes=32 << 20),
        name="send_side",
    )(*(in_hbm(x) for x in (doc_bounds, q, k, v, q_gain.reshape(1, HD), k_gain.reshape(1, HD))))


def attend_call(doc_bounds, mine):
    return pl.pallas_call(
        attend_kernel,
        out_shape=jax.ShapeDtypeStruct((2, 8, 4, 2, ROWS, 128), jnp.bfloat16),
        in_specs=[VMEM, VMEM],
        out_specs=VMEM,
        scratch_shapes=[
            pltpu.VMEM((NBLK + 1, HD, BLK), jnp.bfloat16),
            pltpu.VMEM((NBLK, BLK, 128), jnp.bfloat16),
            pltpu.VMEM((NBLK, HD, BLK), jnp.bfloat16),
            pltpu.VMEM((NBLK, 2, BLK, BLK), jnp.float32),
            pltpu.VMEM((FAR, BLK, BLK), jnp.float32),
            pltpu.VMEM((NBLK + 1, 8, BLK), jnp.float32),
            pltpu.VMEM((NBLK + 1, HD, BLK), jnp.float32),
            pltpu.SMEM((FAR,), jnp.int32),
        ],
        compiler_params=pltpu.CompilerParams(vmem_limit_bytes=44 << 20),
        name="attend",
    )(doc_bounds, mine)


def take_call(back):
    return pl.pallas_call(
        take_kernel,
        out_shape=jax.ShapeDtypeStruct((TOK, HD, HEADS), jnp.bfloat16),
        in_specs=[VMEM],
        out_specs=HBM,
        scratch_shapes=[
            pltpu.VMEM((ROWS, HEADS, 128), jnp.bfloat16),
            pltpu.VMEM((TOK, HD, HEADS), jnp.bfloat16),
            pltpu.SemaphoreType.DMA((4,)),
        ],
        compiler_params=pltpu.CompilerParams(vmem_limit_bytes=32 << 20),
        name="take_side",
    )(back)


def body(queries, keys, values, doc_bounds, q_gain, k_gain):
    doc_bounds = doc_bounds.reshape(1, DOCS + 1)
    inputs = [jnp.transpose(x, (0, 2, 1)) for x in (queries, keys, values)]
    packed = send_call(doc_bounds, *inputs, q_gain, k_gain)
    mine = lax.all_to_all(packed, ORDER, split_axis=0, concat_axis=0, tiled=True)
    result = attend_call(doc_bounds, mine.reshape(2, 8, 4, 2, 48, 128)).reshape(HEADS, ROWS, 128)
    back = lax.all_to_all(result, ORDER, split_axis=0, concat_axis=0, tiled=True)
    return jnp.transpose(take_call(back), (0, 2, 1))


def solution(mesh):
    fine = jax.sharding.Mesh(mesh.devices.reshape(8, 2, 4, 2, -1), ("zl", "c", "x", "zh", "dp"))
    tokens = P(("dp", "zl", "c", "x", "zh"), None, None)
    return jax.shard_map(
        body,
        mesh=fine,
        in_specs=(tokens, tokens, tokens, P("dp"), P(), P()),
        out_specs=tokens,
        check_vma=False,
    )
```

```python
import jax
import jax.numpy as jnp
from jax import lax
from jax.experimental import pallas as pl
from jax.experimental.pallas import tpu as pltpu
from jax.sharding import PartitionSpec as P

TOK = 32
ROWS = 16
HD = 64
HEADS = 128
DOCS = 8
SEQ = 4096
BLK = 256
PAIRS = BLK // 2
NBLK = SEQ // BLK
SRC = BLK // TOK
LONG, MIDDLE, SHORT = 16, 8, 4
FAR = (NBLK - 2) * (NBLK - 1) // 2 + LONG
NT = (((1,), (1,)), ((), ()))
NN = (((1,), (0,)), ((), ()))
BIG = 32768.0
SCALE = 1.4426950408889634 / 8.0
FIRST = -9.210340371976184


def run_of(z, x, c):
    return ((z % 8 * 2 + c) * 4 + x) * 2 + z // 8


ORDER = [run_of(7 * z % 16, x, c) for z in range(16) for x in range(4) for c in range(2)]
PLACE = [ORDER.index(s) for s in range(len(ORDER))]


def dot(a, b, dims=NN):
    return lax.dot_general(a, b, dims, preferred_element_type=jnp.float32)


def starts_of(token, bound):
    start = jnp.zeros_like(token)
    for d in range(1, DOCS):
        start = jnp.where(token >= bound(d), bound(d), start)
    return start


def identity(n):
    row = lax.broadcasted_iota(jnp.int32, (n, n), 0)
    col = lax.broadcasted_iota(jnp.int32, (n, n), 1)
    return (row == col).astype(jnp.float32).astype(jnp.bfloat16)


def interleave():
    row = lax.broadcasted_iota(jnp.int32, (256, 256), 0)
    col = lax.broadcasted_iota(jnp.int32, (256, 256), 1)
    return (col == (row % 16) * 16 + row // 16).astype(jnp.float32).astype(jnp.bfloat16)


def send_kernel(
    bounds_hbm, q_hbm, k_hbm, v_hbm, qg_hbm, kg_hbm, o_ref, bounds_ref, x_ref, g_ref, rot, turned, sems
):
    arriving = [
        pltpu.make_async_copy(source, target, sems.at[n])
        for n, (source, target) in enumerate(
            (
                (bounds_hbm, bounds_ref),
                (qg_hbm, g_ref.at[0]),
                (kg_hbm, g_ref.at[1]),
                (q_hbm, x_ref.at[0]),
                (v_hbm, x_ref.at[2]),
                (k_hbm, x_ref.at[1]),
            )
        )
    ]
    for c in arriving:
        c.start()
    for c in arriving[:3]:
        c.wait()
    lane = lax.broadcasted_iota(jnp.int32, (HD // 2, 128), 1)
    token = lax.axis_index("run") * TOK + lane
    start = starts_of(token, lambda d: bounds_ref[:, d : d + 1])
    place = (token - start).astype(jnp.float32)
    index = lax.broadcasted_iota(jnp.int32, (HD // 2, 128), 0).astype(jnp.float32)
    angle = place * jnp.exp(jnp.float32(FIRST) * index * 2.0 / HD)
    cosine = jnp.cos(angle)
    sine = jnp.sin(angle)
    eye = identity(HEADS)
    mix = interleave()

    def turn(n, r, rows):
        both = dot(eye, rows, NT).astype(jnp.bfloat16)
        turned[n, r] = both[:, :128]
        turned[n, r + 1] = both[:, 128:]

    def rotate(n):
        gain = jnp.transpose(jnp.broadcast_to(g_ref[n], (HEADS, HD)))
        for r in range(0, ROWS, 2):
            for t in (r, r + ROWS, r + 1, r + 1 + ROWS):
                c = jnp.broadcast_to(cosine[:, t : t + 1], (HD // 2, HEADS))
                s = jnp.broadcast_to(sine[:, t : t + 1], (HD // 2, HEADS))
                x = x_ref[n, t].astype(jnp.float32)
                scale = lax.rsqrt(jnp.mean(x * x, axis=0, keepdims=True) + 1e-06)
                x = x * scale * gain
                a, b = x[: HD // 2], x[HD // 2 :]
                y = jnp.concatenate([a * c - b * s, a * s + b * c], axis=0)
                rot[n, t % ROWS, pl.ds((t // ROWS) * HD, HD), :] = y.astype(jnp.bfloat16)
            turn(n, r, rot[n, r : r + 2].reshape(256, HEADS))

    def spread(n):
        for h in range(0, HEADS, 32):
            part = jnp.concatenate([turned[n, :, h + m : h + m + 16, :].reshape(256, 128) for m in (0, 16)], axis=1)
            both = dot(mix, part).astype(jnp.bfloat16)
            for m in range(2):
                heads = slice(h + 16 * m, h + 16 * m + 16)
                o_ref[heads, 16 * n : 16 * n + 16, :] = both[:, 128 * m : 128 * m + 128].reshape(16, 16, 128)

    for c in arriving[3:]:
        c.wait()

    def turn_values():
        for r in range(0, ROWS, 2):
            turn(2, r, jnp.concatenate([x_ref[2, t] for t in (r, r + ROWS, r + 1, r + 1 + ROWS)], axis=0))

    turn_values()
    rotate(0)
    spread(2)
    rotate(1)
    spread(0)
    spread(1)


def attend_kernel(bounds_ref, x_ref, o_ref, qt, kt, kf, vt, near, far, total, summed, items):

    def offsets(shape, axis):
        n = lax.broadcasted_iota(jnp.int32, shape, axis)
        return ((n % PAIRS) // 16) * 32 + n % 16 + (n // PAIRS) * 16

    below = offsets((BLK, BLK), 0) <= offsets((BLK, BLK), 1)
    q_off = offsets((16, BLK), 1)
    k_off = offsets((BLK, 128), 0)

    def bounds_along(shape, axis):
        n = lax.broadcasted_iota(jnp.int32, shape, axis)
        out = jnp.full(shape, SEQ, jnp.int32)
        for d in range(1, DOCS):
            out = jnp.where(n == d, bounds_ref[:, d : d + 1], out)
        return out

    q_bounds = bounds_along((16, BLK), 0)
    k_bounds = bounds_along((1, 128), 1)

    zero = jnp.zeros((HD, BLK), jnp.bfloat16)
    rest = jnp.zeros((128 - 16, BLK), jnp.bfloat16)

    def wide(x):
        t = jnp.transpose(x.astype(jnp.float32)).astype(jnp.bfloat16)
        return jnp.concatenate([t[:HD], t[HD:]], axis=1)

    def scores(j, q, flags):
        k2 = kt[j]
        low = dot(jnp.concatenate([k2, kf[j, :PAIRS]], axis=1), jnp.concatenate([q, zero, flags, rest], axis=0))
        high = dot(jnp.concatenate([k2, kf[j, PAIRS:]], axis=1), jnp.concatenate([zero, q, flags, rest], axis=0))
        return jnp.exp2(jnp.concatenate([low, high], axis=0) * jnp.float32(SCALE))

    def flags_of(i):
        return jnp.where(BLK * i + q_off >= q_bounds, jnp.float32(-BIG), jnp.float32(0.0)).astype(jnp.bfloat16)

    def partial_sum(e):
        return jnp.sum(e.reshape(BLK // 8, 8, BLK), axis=0)

    def tiles(i, row):
        runs = range(SRC * i, SRC * i + SRC)
        return jnp.concatenate([x_ref[PLACE[s], row : row + 16, :] for s in runs], axis=0)

    def near_scores(blocks):
        for i in blocks:
            q = wide(tiles(i, 0))
            kt[i] = tiles(i, 16)
            qt[i] = q
            vt[i] = wide(tiles(i, 32))
            flags = flags_of(i)
            kf[i] = jnp.where(BLK * i + k_off < k_bounds, jnp.float32(1.0), jnp.float32(0.0)).astype(jnp.bfloat16)
            e1 = jnp.where(below, scores(i, q, flags), jnp.float32(0.0))
            e0 = scores(max(i - 1, 0), q, flags)
            if i == 0:
                e0 = jnp.zeros_like(e0)
            near[i, 0] = e0
            near[i, 1] = e1
            total[i] = partial_sum(e0) + partial_sum(e1)

    scalars = [jnp.max(bounds_ref[:, d : d + 1]) for d in range(DOCS)]
    n_far = jnp.int32(0)
    for i in range(2, NBLK):
        start = starts_of(jnp.int32(BLK * i), lambda d: scalars[d])
        for j in range(i - 2, -1, -1):
            items[n_far] = NBLK * i + j
            n_far += (start < BLK * (j + 1)).astype(jnp.int32)
    near_scores(range(NBLK))
    for u in range(LONG - 1):
        items[n_far + u] = NBLK * NBLK
    trips = (n_far + LONG - MIDDLE - 1) // LONG
    left = n_far - LONG * trips
    passes = (
        (0, trips, LONG),
        (LONG * trips, (left > SHORT).astype(jnp.int32), MIDDLE),
        (LONG * trips, ((left > 0) & (left <= SHORT)).astype(jnp.int32), SHORT),
    )

    def far_blocks(work):
        for begin, trips, length in passes:

            def trip(w, _, begin=begin, length=length):
                for u in range(length):
                    n = begin + length * w + u
                    work(n, items[n] >> 4, items[n] & 15)
                return 0

            lax.fori_loop(0, trips, trip, 0)

    def far_scores(n, i, j):
        e = scores(j, qt[i], flags_of(i))
        far[n] = e
        total[i] += partial_sum(e)

    far_blocks(far_scores)
    for i in range(NBLK):
        inverse = 1.0 / jnp.sum(total[i], axis=0, keepdims=True)
        total[i] = jnp.broadcast_to(inverse, (8, BLK))
        summed[i] = jnp.zeros((HD, BLK), jnp.float32)

    def far_values(n, i, j):
        summed[i] += dot(vt[j], (far[n] * total[i][0:1]).astype(jnp.bfloat16))

    far_blocks(far_values)

    for i in range(NBLK):
        w = jnp.concatenate([(near[i, n] * total[i][0:1]).astype(jnp.bfloat16) for n in range(2)], axis=0)
        out = dot(jnp.concatenate([vt[max(i - 1, 0)], vt[i]], axis=1), w) + summed[i]
        both = jnp.transpose(jnp.concatenate([out[:, :PAIRS], out[:, PAIRS:]], axis=0))
        both = both.astype(jnp.bfloat16)
        for n in range(SRC):
            o_ref[PLACE[SRC * i + n]] = both[16 * n : 16 * n + 16]


def take_kernel(x_ref, o_hbm, turned, out, sems):
    mix = interleave()
    eye = identity(128)
    for h in range(0, HEADS, 32):
        part = jnp.concatenate([x_ref[h + m : h + m + 16].reshape(256, 128) for m in (0, 16)], axis=1)
        both = dot(mix, part).astype(jnp.bfloat16)
        for m in range(2):
            turned[:, h + 16 * m : h + 16 * m + 16, :] = both[:, 128 * m : 128 * m + 128].reshape(16, 16, 128)
    copies = []
    for r in range(0, ROWS, 2):
        both = dot(eye, turned[r : r + 2].reshape(256, 128), NT).astype(jnp.bfloat16)
        for m in range(2):
            out[r + m] = both[:HD, 128 * m : 128 * m + 128]
            out[r + m + ROWS] = both[HD:, 128 * m : 128 * m + 128]
        if r % 8 == 6:
            for first in (r - 6, r - 6 + ROWS):
                copy = pltpu.make_async_copy(
                    out.at[pl.ds(first, 8)], o_hbm.at[pl.ds(first, 8)], sems.at[len(copies)]
                )
                copy.start()
                copies.append(copy)
    for copy in copies:
        copy.wait()


VMEM = pl.BlockSpec(memory_space=pltpu.VMEM)
HBM = pl.BlockSpec(memory_space=pltpu.HBM)


def in_hbm(x):
    return pltpu.with_memory_space_constraint(x, pltpu.HBM)


def send_call(doc_bounds, q, k, v, q_gain, k_gain):
    return pl.pallas_call(
        send_kernel,
        out_shape=jax.ShapeDtypeStruct((HEADS, 48, 128), jnp.bfloat16),
        in_specs=[HBM] * 6,
        out_specs=VMEM,
        scratch_shapes=[
            pltpu.VMEM((1, DOCS + 1), jnp.int32),
            pltpu.VMEM((3, TOK, HD, HEADS), jnp.bfloat16),
            pltpu.VMEM((2, 1, HD), jnp.float32),
            pltpu.VMEM((2, ROWS, 128, HEADS), jnp.bfloat16),
            pltpu.VMEM((3, ROWS, HEADS, 128), jnp.bfloat16),
            pltpu.SemaphoreType.DMA((6,)),
        ],
        compiler_params=pltpu.CompilerParams(vmem_limit_bytes=32 << 20),
        name="send_side",
    )(*(in_hbm(x) for x in (doc_bounds, q, k, v, q_gain.reshape(1, HD), k_gain.reshape(1, HD))))


def attend_call(doc_bounds, mine):
    return pl.pallas_call(
        attend_kernel,
        out_shape=jax.ShapeDtypeStruct((SEQ // TOK, ROWS, 128), jnp.bfloat16),
        in_specs=[VMEM, VMEM],
        out_specs=VMEM,
        scratch_shapes=[
            pltpu.VMEM((NBLK + 1, HD, BLK), jnp.bfloat16),
            pltpu.VMEM((NBLK, PAIRS, 128), jnp.bfloat16),
            pltpu.VMEM((NBLK, BLK, 128), jnp.bfloat16),
            pltpu.VMEM((NBLK, HD, BLK), jnp.bfloat16),
            pltpu.VMEM((NBLK, 2, BLK, BLK), jnp.float32),
            pltpu.VMEM((FAR, BLK, BLK), jnp.float32),
            pltpu.VMEM((NBLK + 1, 8, BLK), jnp.float32),
            pltpu.VMEM((NBLK + 1, HD, BLK), jnp.float32),
            pltpu.SMEM((FAR,), jnp.int32),
        ],
        compiler_params=pltpu.CompilerParams(vmem_limit_bytes=44 << 20),
        name="attend",
    )(doc_bounds, mine)


def take_call(back):
    return pl.pallas_call(
        take_kernel,
        out_shape=jax.ShapeDtypeStruct((TOK, HD, HEADS), jnp.bfloat16),
        in_specs=[VMEM],
        out_specs=HBM,
        scratch_shapes=[
            pltpu.VMEM((ROWS, HEADS, 128), jnp.bfloat16),
            pltpu.VMEM((TOK, HD, HEADS), jnp.bfloat16),
            pltpu.SemaphoreType.DMA((4,)),
        ],
        compiler_params=pltpu.CompilerParams(vmem_limit_bytes=32 << 20),
        name="take_side",
    )(back)


def exchange(x):
    return lax.all_to_all(x, "run", split_axis=0, concat_axis=0, axis_index_groups=[ORDER], tiled=True)


def body(queries, keys, values, doc_bounds, q_gain, k_gain):
    doc_bounds = doc_bounds.reshape(1, DOCS + 1)
    inputs = [jnp.transpose(x, (0, 2, 1)) for x in (queries, keys, values)]
    packed = send_call(doc_bounds, *inputs, q_gain, k_gain)
    mine = exchange(packed)
    result = attend_call(doc_bounds, mine)
    back = exchange(result)
    return jnp.transpose(take_call(back), (0, 2, 1))


def solution(mesh):
    runs = jax.sharding.Mesh(mesh.devices.reshape(len(PLACE), -1), ("run", "dp"))
    tokens = P(("dp", "run"), None, None)
    return jax.shard_map(
        body,
        mesh=runs,
        in_specs=(tokens, tokens, tokens, P("dp"), P(), P()),
        out_specs=tokens,
        check_vma=False,
    )
```

```python
import jax
import jax.numpy as jnp
from jax import lax
from jax.experimental import pallas as pl
from jax.experimental.pallas import tpu as pltpu
from jax.sharding import PartitionSpec as P

TOK = 32
ROWS = 16
HD = 64
HEADS = 128
DOCS = 8
SEQ = 4096
BLK = 256
PAIRS = BLK // 2
NBLK = SEQ // BLK
SRC = BLK // TOK
LONG, MIDDLE, SHORT = 16, 8, 4
FAR = (NBLK - 2) * (NBLK - 1) // 2 + LONG
NT = (((1,), (1,)), ((), ()))
NN = (((1,), (0,)), ((), ()))
BIG = 32768.0
SCALE = 1.4426950408889634 / 8.0
FIRST = -9.210340371976184


def run_of(z, x, c):
    return ((z % 8 * 2 + c) * 4 + x) * 2 + z // 8


ORDER = [run_of(z, x, c) for x in range(4) for c in range(2) for z in range(16)]
PLACE = [ORDER.index(s) for s in range(len(ORDER))]


def dot(a, b, dims=NN):
    return lax.dot_general(a, b, dims, preferred_element_type=jnp.float32)


def starts_of(token, bound):
    start = jnp.zeros_like(token)
    for d in range(1, DOCS):
        start = jnp.where(token >= bound(d), bound(d), start)
    return start


def identity(n):
    row = lax.broadcasted_iota(jnp.int32, (n, n), 0)
    col = lax.broadcasted_iota(jnp.int32, (n, n), 1)
    return (row == col).astype(jnp.float32).astype(jnp.bfloat16)


def interleave():
    row = lax.broadcasted_iota(jnp.int32, (256, 256), 0)
    col = lax.broadcasted_iota(jnp.int32, (256, 256), 1)
    return (col == (row % 16) * 16 + row // 16).astype(jnp.float32).astype(jnp.bfloat16)


def send_kernel(
    bounds_hbm, q_hbm, k_hbm, v_hbm, qg_hbm, kg_hbm, o_ref, bounds_ref, x_ref, g_ref, rot, turned, sems
):
    arriving = [
        pltpu.make_async_copy(source, target, sems.at[n])
        for n, (source, target) in enumerate(
            (
                (bounds_hbm, bounds_ref),
                (qg_hbm, g_ref.at[0]),
                (kg_hbm, g_ref.at[1]),
                (q_hbm, x_ref.at[0]),
                (v_hbm, x_ref.at[2]),
                (k_hbm, x_ref.at[1]),
            )
        )
    ]
    for c in arriving:
        c.start()
    for c in arriving[:3]:
        c.wait()
    lane = lax.broadcasted_iota(jnp.int32, (HD // 2, 128), 1)
    token = lax.axis_index("run") * TOK + lane
    start = starts_of(token, lambda d: bounds_ref[:, d : d + 1])
    place = (token - start).astype(jnp.float32)
    index = lax.broadcasted_iota(jnp.int32, (HD // 2, 128), 0).astype(jnp.float32)
    angle = place * jnp.exp(jnp.float32(FIRST) * index * 2.0 / HD)
    cosine = jnp.cos(angle)
    sine = jnp.sin(angle)
    eye = identity(HEADS)
    mix = interleave()

    def turn(n, r, rows):
        both = dot(eye, rows, NT).astype(jnp.bfloat16)
        turned[n, r] = both[:, :128]
        turned[n, r + 1] = both[:, 128:]

    def rotate(n):
        gain = jnp.transpose(jnp.broadcast_to(g_ref[n], (HEADS, HD)))
        for r in range(0, ROWS, 2):
            for t in (r, r + ROWS, r + 1, r + 1 + ROWS):
                c = jnp.broadcast_to(cosine[:, t : t + 1], (HD // 2, HEADS))
                s = jnp.broadcast_to(sine[:, t : t + 1], (HD // 2, HEADS))
                x = x_ref[n, t].astype(jnp.float32)
                scale = lax.rsqrt(jnp.mean(x * x, axis=0, keepdims=True) + 1e-06)
                x = x * scale * gain
                a, b = x[: HD // 2], x[HD // 2 :]
                y = jnp.concatenate([a * c - b * s, a * s + b * c], axis=0)
                rot[n, t % ROWS, pl.ds((t // ROWS) * HD, HD), :] = y.astype(jnp.bfloat16)
            turn(n, r, rot[n, r : r + 2].reshape(256, HEADS))

    def spread(n):
        for h in range(0, HEADS, 32):
            part = jnp.concatenate([turned[n, :, h + m : h + m + 16, :].reshape(256, 128) for m in (0, 16)], axis=1)
            both = dot(mix, part).astype(jnp.bfloat16)
            for m in range(2):
                heads = slice(h + 16 * m, h + 16 * m + 16)
                o_ref[heads, 16 * n : 16 * n + 16, :] = both[:, 128 * m : 128 * m + 128].reshape(16, 16, 128)

    for c in arriving[3:]:
        c.wait()

    def turn_values():
        for r in range(0, ROWS, 2):
            turn(2, r, jnp.concatenate([x_ref[2, t] for t in (r, r + ROWS, r + 1, r + 1 + ROWS)], axis=0))

    turn_values()
    rotate(0)
    spread(2)
    rotate(1)
    spread(0)
    spread(1)


def attend_kernel(bounds_ref, x_ref, o_ref, qt, kt, kf, vt, near, far, total, summed, items):

    def offsets(shape, axis):
        n = lax.broadcasted_iota(jnp.int32, shape, axis)
        return ((n % PAIRS) // 16) * 32 + n % 16 + (n // PAIRS) * 16

    below = offsets((BLK, BLK), 0) <= offsets((BLK, BLK), 1)
    q_off = offsets((16, BLK), 1)
    k_off = offsets((BLK, 128), 0)

    def bounds_along(shape, axis):
        n = lax.broadcasted_iota(jnp.int32, shape, axis)
        out = jnp.full(shape, SEQ, jnp.int32)
        for d in range(1, DOCS):
            out = jnp.where(n == d, bounds_ref[:, d : d + 1], out)
        return out

    q_bounds = bounds_along((16, BLK), 0)
    k_bounds = bounds_along((1, 128), 1)

    zero = jnp.zeros((HD, BLK), jnp.bfloat16)
    rest = jnp.zeros((128 - 16, BLK), jnp.bfloat16)

    def wide(x):
        t = jnp.transpose(x.astype(jnp.float32)).astype(jnp.bfloat16)
        return jnp.concatenate([t[:HD], t[HD:]], axis=1)

    def scores(j, q, flags):
        k2 = kt[j]
        low = dot(jnp.concatenate([k2, kf[j, :PAIRS]], axis=1), jnp.concatenate([q, zero, flags, rest], axis=0))
        high = dot(jnp.concatenate([k2, kf[j, PAIRS:]], axis=1), jnp.concatenate([zero, q, flags, rest], axis=0))
        return jnp.exp2(jnp.concatenate([low, high], axis=0) * jnp.float32(SCALE))

    def flags_of(i):
        return jnp.where(BLK * i + q_off >= q_bounds, jnp.float32(-BIG), jnp.float32(0.0)).astype(jnp.bfloat16)

    def partial_sum(e):
        return jnp.sum(e.reshape(BLK // 8, 8, BLK), axis=0)

    def tiles(i, row):
        runs = range(SRC * i, SRC * i + SRC)
        return jnp.concatenate([x_ref[PLACE[s], row : row + 16, :] for s in runs], axis=0)

    def near_scores(blocks):
        for i in blocks:
            q = wide(tiles(i, 0))
            kt[i] = tiles(i, 16)
            qt[i] = q
            vt[i] = wide(tiles(i, 32))
            flags = flags_of(i)
            kf[i] = jnp.where(BLK * i + k_off < k_bounds, jnp.float32(1.0), jnp.float32(0.0)).astype(jnp.bfloat16)
            e1 = jnp.where(below, scores(i, q, flags), jnp.float32(0.0))
            e0 = scores(max(i - 1, 0), q, flags)
            if i == 0:
                e0 = jnp.zeros_like(e0)
            near[i, 0] = e0
            near[i, 1] = e1
            total[i] = partial_sum(e0) + partial_sum(e1)

    scalars = [jnp.max(bounds_ref[:, d : d + 1]) for d in range(DOCS)]
    n_far = jnp.int32(0)
    for i in range(2, NBLK):
        start = starts_of(jnp.int32(BLK * i), lambda d: scalars[d])
        for j in range(i - 2, -1, -1):
            items[n_far] = NBLK * i + j
            n_far += (start < BLK * (j + 1)).astype(jnp.int32)
    near_scores(range(NBLK))
    for u in range(LONG - 1):
        items[n_far + u] = NBLK * NBLK
    trips = (n_far + LONG - MIDDLE - 1) // LONG
    left = n_far - LONG * trips
    passes = (
        (0, trips, LONG),
        (LONG * trips, (left > SHORT).astype(jnp.int32), MIDDLE),
        (LONG * trips, ((left > 0) & (left <= SHORT)).astype(jnp.int32), SHORT),
    )

    def far_blocks(work):
        for begin, trips, length in passes:

            def trip(w, _, begin=begin, length=length):
                for u in range(length):
                    n = begin + length * w + u
                    work(n, items[n] >> 4, items[n] & 15)
                return 0

            lax.fori_loop(0, trips, trip, 0)

    def far_scores(n, i, j):
        e = scores(j, qt[i], flags_of(i))
        far[n] = e
        total[i] += partial_sum(e)

    far_blocks(far_scores)
    for i in range(NBLK):
        inverse = 1.0 / jnp.sum(total[i], axis=0, keepdims=True)
        total[i] = jnp.broadcast_to(inverse, (8, BLK))
        summed[i] = jnp.zeros((HD, BLK), jnp.float32)

    def far_values(n, i, j):
        summed[i] += dot(vt[j], (far[n] * total[i][0:1]).astype(jnp.bfloat16))

    far_blocks(far_values)

    for i in range(NBLK):
        w = jnp.concatenate([(near[i, n] * total[i][0:1]).astype(jnp.bfloat16) for n in range(2)], axis=0)
        out = dot(jnp.concatenate([vt[max(i - 1, 0)], vt[i]], axis=1), w) + summed[i]
        both = jnp.transpose(jnp.concatenate([out[:, :PAIRS], out[:, PAIRS:]], axis=0))
        both = both.astype(jnp.bfloat16)
        for n in range(SRC):
            o_ref[PLACE[SRC * i + n]] = both[16 * n : 16 * n + 16]


def take_kernel(x_ref, o_hbm, turned, out, sems):
    mix = interleave()
    eye = identity(128)
    for h in range(0, HEADS, 32):
        part = jnp.concatenate([x_ref[h + m : h + m + 16].reshape(256, 128) for m in (0, 16)], axis=1)
        both = dot(mix, part).astype(jnp.bfloat16)
        for m in range(2):
            turned[:, h + 16 * m : h + 16 * m + 16, :] = both[:, 128 * m : 128 * m + 128].reshape(16, 16, 128)
    copies = []
    for r in range(0, ROWS, 2):
        both = dot(eye, turned[r : r + 2].reshape(256, 128), NT).astype(jnp.bfloat16)
        for m in range(2):
            out[r + m] = both[:HD, 128 * m : 128 * m + 128]
            out[r + m + ROWS] = both[HD:, 128 * m : 128 * m + 128]
        if r % 8 == 6:
            for first in (r - 6, r - 6 + ROWS):
                copy = pltpu.make_async_copy(
                    out.at[pl.ds(first, 8)], o_hbm.at[pl.ds(first, 8)], sems.at[len(copies)]
                )
                copy.start()
                copies.append(copy)
    for copy in copies:
        copy.wait()


VMEM = pl.BlockSpec(memory_space=pltpu.VMEM)
HBM = pl.BlockSpec(memory_space=pltpu.HBM)


def in_hbm(x):
    return pltpu.with_memory_space_constraint(x, pltpu.HBM)


def send_call(doc_bounds, q, k, v, q_gain, k_gain):
    return pl.pallas_call(
        send_kernel,
        out_shape=jax.ShapeDtypeStruct((HEADS, 48, 128), jnp.bfloat16),
        in_specs=[HBM] * 6,
        out_specs=VMEM,
        scratch_shapes=[
            pltpu.VMEM((1, DOCS + 1), jnp.int32),
            pltpu.VMEM((3, TOK, HD, HEADS), jnp.bfloat16),
            pltpu.VMEM((2, 1, HD), jnp.float32),
            pltpu.VMEM((2, ROWS, 128, HEADS), jnp.bfloat16),
            pltpu.VMEM((3, ROWS, HEADS, 128), jnp.bfloat16),
            pltpu.SemaphoreType.DMA((6,)),
        ],
        compiler_params=pltpu.CompilerParams(vmem_limit_bytes=32 << 20),
        name="send_side",
    )(*(in_hbm(x) for x in (doc_bounds, q, k, v, q_gain.reshape(1, HD), k_gain.reshape(1, HD))))


def attend_call(doc_bounds, mine):
    return pl.pallas_call(
        attend_kernel,
        out_shape=jax.ShapeDtypeStruct((SEQ // TOK, ROWS, 128), jnp.bfloat16),
        in_specs=[VMEM, VMEM],
        out_specs=VMEM,
        scratch_shapes=[
            pltpu.VMEM((NBLK + 1, HD, BLK), jnp.bfloat16),
            pltpu.VMEM((NBLK, PAIRS, 128), jnp.bfloat16),
            pltpu.VMEM((NBLK, BLK, 128), jnp.bfloat16),
            pltpu.VMEM((NBLK, HD, BLK), jnp.bfloat16),
            pltpu.VMEM((NBLK, 2, BLK, BLK), jnp.float32),
            pltpu.VMEM((FAR, BLK, BLK), jnp.float32),
            pltpu.VMEM((NBLK + 1, 8, BLK), jnp.float32),
            pltpu.VMEM((NBLK + 1, HD, BLK), jnp.float32),
            pltpu.SMEM((FAR,), jnp.int32),
        ],
        compiler_params=pltpu.CompilerParams(vmem_limit_bytes=44 << 20),
        name="attend",
    )(doc_bounds, mine)


def take_call(back):
    return pl.pallas_call(
        take_kernel,
        out_shape=jax.ShapeDtypeStruct((TOK, HD, HEADS), jnp.bfloat16),
        in_specs=[VMEM],
        out_specs=HBM,
        scratch_shapes=[
            pltpu.VMEM((ROWS, HEADS, 128), jnp.bfloat16),
            pltpu.VMEM((TOK, HD, HEADS), jnp.bfloat16),
            pltpu.SemaphoreType.DMA((4,)),
        ],
        compiler_params=pltpu.CompilerParams(vmem_limit_bytes=32 << 20),
        name="take_side",
    )(back)


def exchange(x):
    return lax.all_to_all(x, "run", split_axis=0, concat_axis=0, axis_index_groups=[ORDER], tiled=True)


def body(queries, keys, values, doc_bounds, q_gain, k_gain):
    doc_bounds = doc_bounds.reshape(1, DOCS + 1)
    inputs = [jnp.transpose(x, (0, 2, 1)) for x in (queries, keys, values)]
    packed = send_call(doc_bounds, *inputs, q_gain, k_gain)
    mine = exchange(packed)
    result = attend_call(doc_bounds, mine)
    back = exchange(result)
    return jnp.transpose(take_call(back), (0, 2, 1))


def solution(mesh):
    runs = jax.sharding.Mesh(mesh.devices.reshape(len(PLACE), -1), ("run", "dp"))
    tokens = P(("dp", "run"), None, None)
    return jax.shard_map(
        body,
        mesh=runs,
        in_specs=(tokens, tokens, tokens, P("dp"), P(), P()),
        out_specs=tokens,
        check_vma=False,
    )
```

```python
import jax
import jax.numpy as jnp
from jax import lax
from jax.experimental import pallas as pl
from jax.experimental.pallas import tpu as pltpu
from jax.sharding import PartitionSpec as P

TOK = 32
ROWS = 16
HD = 64
HEADS = 128
DOCS = 8
SEQ = 4096
BLK = 256
PAIRS = BLK // 2
NBLK = SEQ // BLK
SRC = BLK // TOK
LONG, MIDDLE, SHORT = 16, 8, 4
FAR = (NBLK - 2) * (NBLK - 1) // 2 + LONG
NT = (((1,), (1,)), ((), ()))
NN = (((1,), (0,)), ((), ()))
BIG = 32768.0
SCALE = 1.4426950408889634 / 8.0
FIRST = -9.210340371976184


def run_of(z, x, c):
    return ((z % 8 * 2 + c) * 4 + x) * 2 + z // 8


ORDER = [run_of((8 + (n + 1) // 2 * (-1) ** n) % 16, x, c) for n in range(16) for x in range(4) for c in range(2)]
PLACE = [ORDER.index(s) for s in range(len(ORDER))]


def dot(a, b, dims=NN):
    return lax.dot_general(a, b, dims, preferred_element_type=jnp.float32)


def starts_of(token, bound):
    start = jnp.zeros_like(token)
    for d in range(1, DOCS):
        start = jnp.where(token >= bound(d), bound(d), start)
    return start


def identity(n):
    row = lax.broadcasted_iota(jnp.int32, (n, n), 0)
    col = lax.broadcasted_iota(jnp.int32, (n, n), 1)
    return (row == col).astype(jnp.float32).astype(jnp.bfloat16)


def interleave():
    row = lax.broadcasted_iota(jnp.int32, (256, 256), 0)
    col = lax.broadcasted_iota(jnp.int32, (256, 256), 1)
    return (col == (row % 16) * 16 + row // 16).astype(jnp.float32).astype(jnp.bfloat16)


def send_kernel(
    bounds_hbm, q_hbm, k_hbm, v_hbm, qg_hbm, kg_hbm, o_ref, bounds_ref, x_ref, g_ref, rot, turned, sems
):
    arriving = [
        pltpu.make_async_copy(source, target, sems.at[n])
        for n, (source, target) in enumerate(
            (
                (bounds_hbm, bounds_ref),
                (qg_hbm, g_ref.at[0]),
                (kg_hbm, g_ref.at[1]),
                (q_hbm, x_ref.at[0]),
                (v_hbm, x_ref.at[2]),
                (k_hbm, x_ref.at[1]),
            )
        )
    ]
    for c in arriving:
        c.start()
    for c in arriving[:3]:
        c.wait()
    lane = lax.broadcasted_iota(jnp.int32, (HD // 2, 128), 1)
    token = lax.axis_index("run") * TOK + lane
    start = starts_of(token, lambda d: bounds_ref[:, d : d + 1])
    place = (token - start).astype(jnp.float32)
    index = lax.broadcasted_iota(jnp.int32, (HD // 2, 128), 0).astype(jnp.float32)
    angle = place * jnp.exp(jnp.float32(FIRST) * index * 2.0 / HD)
    cosine = jnp.cos(angle)
    sine = jnp.sin(angle)
    eye = identity(HEADS)
    mix = interleave()

    def turn(n, r, rows):
        both = dot(eye, rows, NT).astype(jnp.bfloat16)
        turned[n, r] = both[:, :128]
        turned[n, r + 1] = both[:, 128:]

    def rotate(n):
        gain = jnp.transpose(jnp.broadcast_to(g_ref[n], (HEADS, HD)))
        for r in range(0, ROWS, 2):
            for t in (r, r + ROWS, r + 1, r + 1 + ROWS):
                c = jnp.broadcast_to(cosine[:, t : t + 1], (HD // 2, HEADS))
                s = jnp.broadcast_to(sine[:, t : t + 1], (HD // 2, HEADS))
                x = x_ref[n, t].astype(jnp.float32)
                scale = lax.rsqrt(jnp.mean(x * x, axis=0, keepdims=True) + 1e-06)
                x = x * scale * gain
                a, b = x[: HD // 2], x[HD // 2 :]
                y = jnp.concatenate([a * c - b * s, a * s + b * c], axis=0)
                rot[n, t % ROWS, pl.ds((t // ROWS) * HD, HD), :] = y.astype(jnp.bfloat16)
            turn(n, r, rot[n, r : r + 2].reshape(256, HEADS))

    def spread(n):
        for h in range(0, HEADS, 32):
            part = jnp.concatenate([turned[n, :, h + m : h + m + 16, :].reshape(256, 128) for m in (0, 16)], axis=1)
            both = dot(mix, part).astype(jnp.bfloat16)
            for m in range(2):
                heads = slice(h + 16 * m, h + 16 * m + 16)
                o_ref[heads, 16 * n : 16 * n + 16, :] = both[:, 128 * m : 128 * m + 128].reshape(16, 16, 128)

    for c in arriving[3:]:
        c.wait()

    def turn_values():
        for r in range(0, ROWS, 2):
            turn(2, r, jnp.concatenate([x_ref[2, t] for t in (r, r + ROWS, r + 1, r + 1 + ROWS)], axis=0))

    turn_values()
    rotate(0)
    spread(2)
    rotate(1)
    spread(0)
    spread(1)


def attend_kernel(bounds_ref, x_ref, o_ref, qt, kt, kf, vt, near, far, total, summed, items):

    def offsets(shape, axis):
        n = lax.broadcasted_iota(jnp.int32, shape, axis)
        return ((n % PAIRS) // 16) * 32 + n % 16 + (n // PAIRS) * 16

    below = offsets((BLK, BLK), 0) <= offsets((BLK, BLK), 1)
    q_off = offsets((16, BLK), 1)
    k_off = offsets((BLK, 128), 0)

    def bounds_along(shape, axis):
        n = lax.broadcasted_iota(jnp.int32, shape, axis)
        out = jnp.full(shape, SEQ, jnp.int32)
        for d in range(1, DOCS):
            out = jnp.where(n == d, bounds_ref[:, d : d + 1], out)
        return out

    q_bounds = bounds_along((16, BLK), 0)
    k_bounds = bounds_along((1, 128), 1)

    zero = jnp.zeros((HD, BLK), jnp.bfloat16)
    rest = jnp.zeros((128 - 16, BLK), jnp.bfloat16)

    def wide(x):
        t = jnp.transpose(x.astype(jnp.float32)).astype(jnp.bfloat16)
        return jnp.concatenate([t[:HD], t[HD:]], axis=1)

    def scores(j, q, flags):
        k2 = kt[j]
        low = dot(jnp.concatenate([k2, kf[j, :PAIRS]], axis=1), jnp.concatenate([q, zero, flags, rest], axis=0))
        high = dot(jnp.concatenate([k2, kf[j, PAIRS:]], axis=1), jnp.concatenate([zero, q, flags, rest], axis=0))
        return jnp.exp2(jnp.concatenate([low, high], axis=0) * jnp.float32(SCALE))

    def flags_of(i):
        return jnp.where(BLK * i + q_off >= q_bounds, jnp.float32(-BIG), jnp.float32(0.0)).astype(jnp.bfloat16)

    def partial_sum(e):
        return jnp.sum(e.reshape(BLK // 8, 8, BLK), axis=0)

    def tiles(i, row):
        runs = range(SRC * i, SRC * i + SRC)
        return jnp.concatenate([x_ref[PLACE[s], row : row + 16, :] for s in runs], axis=0)

    def near_scores(blocks):
        for i in blocks:
            q = wide(tiles(i, 0))
            kt[i] = tiles(i, 16)
            qt[i] = q
            vt[i] = wide(tiles(i, 32))
            flags = flags_of(i)
            kf[i] = jnp.where(BLK * i + k_off < k_bounds, jnp.float32(1.0), jnp.float32(0.0)).astype(jnp.bfloat16)
            e1 = jnp.where(below, scores(i, q, flags), jnp.float32(0.0))
            e0 = scores(max(i - 1, 0), q, flags)
            if i == 0:
                e0 = jnp.zeros_like(e0)
            near[i, 0] = e0
            near[i, 1] = e1
            total[i] = partial_sum(e0) + partial_sum(e1)

    scalars = [jnp.max(bounds_ref[:, d : d + 1]) for d in range(DOCS)]
    n_far = jnp.int32(0)
    for i in range(2, NBLK):
        start = starts_of(jnp.int32(BLK * i), lambda d: scalars[d])
        for j in range(i - 2, -1, -1):
            items[n_far] = NBLK * i + j
            n_far += (start < BLK * (j + 1)).astype(jnp.int32)
    near_scores(range(NBLK))
    for u in range(LONG - 1):
        items[n_far + u] = NBLK * NBLK
    trips = (n_far + LONG - MIDDLE - 1) // LONG
    left = n_far - LONG * trips
    passes = (
        (0, trips, LONG),
        (LONG * trips, (left > SHORT).astype(jnp.int32), MIDDLE),
        (LONG * trips, ((left > 0) & (left <= SHORT)).astype(jnp.int32), SHORT),
    )

    def far_blocks(work):
        for begin, trips, length in passes:

            def trip(w, _, begin=begin, length=length):
                for u in range(length):
                    n = begin + length * w + u
                    work(n, items[n] >> 4, items[n] & 15)
                return 0

            lax.fori_loop(0, trips, trip, 0)

    def far_scores(n, i, j):
        e = scores(j, qt[i], flags_of(i))
        far[n] = e
        total[i] += partial_sum(e)

    far_blocks(far_scores)
    for i in range(NBLK):
        inverse = 1.0 / jnp.sum(total[i], axis=0, keepdims=True)
        total[i] = jnp.broadcast_to(inverse, (8, BLK))
        summed[i] = jnp.zeros((HD, BLK), jnp.float32)

    def far_values(n, i, j):
        summed[i] += dot(vt[j], (far[n] * total[i][0:1]).astype(jnp.bfloat16))

    far_blocks(far_values)

    for i in range(NBLK):
        w = jnp.concatenate([(near[i, n] * total[i][0:1]).astype(jnp.bfloat16) for n in range(2)], axis=0)
        out = dot(jnp.concatenate([vt[max(i - 1, 0)], vt[i]], axis=1), w) + summed[i]
        both = jnp.transpose(jnp.concatenate([out[:, :PAIRS], out[:, PAIRS:]], axis=0))
        both = both.astype(jnp.bfloat16)
        for n in range(SRC):
            o_ref[PLACE[SRC * i + n]] = both[16 * n : 16 * n + 16]


def take_kernel(x_ref, o_hbm, turned, out, sems):
    mix = interleave()
    eye = identity(128)
    for h in range(0, HEADS, 32):
        part = jnp.concatenate([x_ref[h + m : h + m + 16].reshape(256, 128) for m in (0, 16)], axis=1)
        both = dot(mix, part).astype(jnp.bfloat16)
        for m in range(2):
            turned[:, h + 16 * m : h + 16 * m + 16, :] = both[:, 128 * m : 128 * m + 128].reshape(16, 16, 128)
    copies = []
    for r in range(0, ROWS, 2):
        both = dot(eye, turned[r : r + 2].reshape(256, 128), NT).astype(jnp.bfloat16)
        for m in range(2):
            out[r + m] = both[:HD, 128 * m : 128 * m + 128]
            out[r + m + ROWS] = both[HD:, 128 * m : 128 * m + 128]
        if r % 8 == 6:
            for first in (r - 6, r - 6 + ROWS):
                copy = pltpu.make_async_copy(
                    out.at[pl.ds(first, 8)], o_hbm.at[pl.ds(first, 8)], sems.at[len(copies)]
                )
                copy.start()
                copies.append(copy)
    for copy in copies:
        copy.wait()


VMEM = pl.BlockSpec(memory_space=pltpu.VMEM)
HBM = pl.BlockSpec(memory_space=pltpu.HBM)


def in_hbm(x):
    return pltpu.with_memory_space_constraint(x, pltpu.HBM)


def send_call(doc_bounds, q, k, v, q_gain, k_gain):
    return pl.pallas_call(
        send_kernel,
        out_shape=jax.ShapeDtypeStruct((HEADS, 48, 128), jnp.bfloat16),
        in_specs=[HBM] * 6,
        out_specs=VMEM,
        scratch_shapes=[
            pltpu.VMEM((1, DOCS + 1), jnp.int32),
            pltpu.VMEM((3, TOK, HD, HEADS), jnp.bfloat16),
            pltpu.VMEM((2, 1, HD), jnp.float32),
            pltpu.VMEM((2, ROWS, 128, HEADS), jnp.bfloat16),
            pltpu.VMEM((3, ROWS, HEADS, 128), jnp.bfloat16),
            pltpu.SemaphoreType.DMA((6,)),
        ],
        compiler_params=pltpu.CompilerParams(vmem_limit_bytes=32 << 20),
        name="send_side",
    )(*(in_hbm(x) for x in (doc_bounds, q, k, v, q_gain.reshape(1, HD), k_gain.reshape(1, HD))))


def attend_call(doc_bounds, mine):
    return pl.pallas_call(
        attend_kernel,
        out_shape=jax.ShapeDtypeStruct((SEQ // TOK, ROWS, 128), jnp.bfloat16),
        in_specs=[VMEM, VMEM],
        out_specs=VMEM,
        scratch_shapes=[
            pltpu.VMEM((NBLK + 1, HD, BLK), jnp.bfloat16),
            pltpu.VMEM((NBLK, PAIRS, 128), jnp.bfloat16),
            pltpu.VMEM((NBLK, BLK, 128), jnp.bfloat16),
            pltpu.VMEM((NBLK, HD, BLK), jnp.bfloat16),
            pltpu.VMEM((NBLK, 2, BLK, BLK), jnp.float32),
            pltpu.VMEM((FAR, BLK, BLK), jnp.float32),
            pltpu.VMEM((NBLK + 1, 8, BLK), jnp.float32),
            pltpu.VMEM((NBLK + 1, HD, BLK), jnp.float32),
            pltpu.SMEM((FAR,), jnp.int32),
        ],
        compiler_params=pltpu.CompilerParams(vmem_limit_bytes=44 << 20),
        name="attend",
    )(doc_bounds, mine)


def take_call(back):
    return pl.pallas_call(
        take_kernel,
        out_shape=jax.ShapeDtypeStruct((TOK, HD, HEADS), jnp.bfloat16),
        in_specs=[VMEM],
        out_specs=HBM,
        scratch_shapes=[
            pltpu.VMEM((ROWS, HEADS, 128), jnp.bfloat16),
            pltpu.VMEM((TOK, HD, HEADS), jnp.bfloat16),
            pltpu.SemaphoreType.DMA((4,)),
        ],
        compiler_params=pltpu.CompilerParams(vmem_limit_bytes=32 << 20),
        name="take_side",
    )(back)


def exchange(x):
    return lax.all_to_all(x, "run", split_axis=0, concat_axis=0, axis_index_groups=[ORDER], tiled=True)


def body(queries, keys, values, doc_bounds, q_gain, k_gain):
    doc_bounds = doc_bounds.reshape(1, DOCS + 1)
    inputs = [jnp.transpose(x, (0, 2, 1)) for x in (queries, keys, values)]
    packed = send_call(doc_bounds, *inputs, q_gain, k_gain)
    mine = exchange(packed)
    result = attend_call(doc_bounds, mine)
    back = exchange(result)
    return jnp.transpose(take_call(back), (0, 2, 1))


def solution(mesh):
    runs = jax.sharding.Mesh(mesh.devices.reshape(len(PLACE), -1), ("run", "dp"))
    tokens = P(("dp", "run"), None, None)
    return jax.shard_map(
        body,
        mesh=runs,
        in_specs=(tokens, tokens, tokens, P("dp"), P(), P()),
        out_specs=tokens,
        check_vma=False,
    )
```

```python
import jax
import jax.numpy as jnp
from jax import lax
from jax.experimental import pallas as pl
from jax.experimental.pallas import tpu as pltpu
from jax.sharding import PartitionSpec as P

TOK = 32
ROWS = 16
HD = 64
HEADS = 128
DOCS = 8
SEQ = 4096
BLK = 256
PAIRS = BLK // 2
NBLK = SEQ // BLK
SRC = BLK // TOK
LONG, MIDDLE, SHORT = 16, 8, 4
FAR = (NBLK - 2) * (NBLK - 1) // 2 + LONG
NT = (((1,), (1,)), ((), ()))
NN = (((1,), (0,)), ((), ()))
BIG = 32768.0
SCALE = 1.4426950408889634 / 8.0
FIRST = -9.210340371976184


def run_of(z, x, c):
    return ((z % 8 * 2 + c) * 4 + x) * 2 + z // 8


ORDER = [run_of((n + 1) // 2 * (-1) ** n % 16, x, c) for n in range(16) for x in range(4) for c in range(2)]
PLACE = [ORDER.index(s) for s in range(len(ORDER))]


def dot(a, b, dims=NN):
    return lax.dot_general(a, b, dims, preferred_element_type=jnp.float32)


def starts_of(token, bound):
    start = jnp.zeros_like(token)
    for d in range(1, DOCS):
        start = jnp.where(token >= bound(d), bound(d), start)
    return start


def identity(n):
    row = lax.broadcasted_iota(jnp.int32, (n, n), 0)
    col = lax.broadcasted_iota(jnp.int32, (n, n), 1)
    return (row == col).astype(jnp.float32).astype(jnp.bfloat16)


def interleave():
    row = lax.broadcasted_iota(jnp.int32, (256, 256), 0)
    col = lax.broadcasted_iota(jnp.int32, (256, 256), 1)
    return (col == (row % 16) * 16 + row // 16).astype(jnp.float32).astype(jnp.bfloat16)


def send_kernel(
    bounds_hbm, q_hbm, k_hbm, v_hbm, qg_hbm, kg_hbm, o_ref, bounds_ref, x_ref, g_ref, rot, turned, sems
):
    arriving = [
        pltpu.make_async_copy(source, target, sems.at[n])
        for n, (source, target) in enumerate(
            (
                (bounds_hbm, bounds_ref),
                (qg_hbm, g_ref.at[0]),
                (kg_hbm, g_ref.at[1]),
                (q_hbm, x_ref.at[0]),
                (v_hbm, x_ref.at[2]),
                (k_hbm, x_ref.at[1]),
            )
        )
    ]
    for c in arriving:
        c.start()
    for c in arriving[:3]:
        c.wait()
    lane = lax.broadcasted_iota(jnp.int32, (HD // 2, 128), 1)
    token = lax.axis_index("run") * TOK + lane
    start = starts_of(token, lambda d: bounds_ref[:, d : d + 1])
    place = (token - start).astype(jnp.float32)
    index = lax.broadcasted_iota(jnp.int32, (HD // 2, 128), 0).astype(jnp.float32)
    angle = place * jnp.exp(jnp.float32(FIRST) * index * 2.0 / HD)
    cosine = jnp.cos(angle)
    sine = jnp.sin(angle)
    eye = identity(HEADS)
    mix = interleave()

    def turn(n, r, rows):
        both = dot(eye, rows, NT).astype(jnp.bfloat16)
        turned[n, r] = both[:, :128]
        turned[n, r + 1] = both[:, 128:]

    def rotate(n):
        gain = jnp.transpose(jnp.broadcast_to(g_ref[n], (HEADS, HD)))
        for r in range(0, ROWS, 2):
            for t in (r, r + ROWS, r + 1, r + 1 + ROWS):
                c = jnp.broadcast_to(cosine[:, t : t + 1], (HD // 2, HEADS))
                s = jnp.broadcast_to(sine[:, t : t + 1], (HD // 2, HEADS))
                x = x_ref[n, t].astype(jnp.float32)
                scale = lax.rsqrt(jnp.mean(x * x, axis=0, keepdims=True) + 1e-06)
                x = x * scale * gain
                a, b = x[: HD // 2], x[HD // 2 :]
                y = jnp.concatenate([a * c - b * s, a * s + b * c], axis=0)
                rot[n, t % ROWS, pl.ds((t // ROWS) * HD, HD), :] = y.astype(jnp.bfloat16)
            turn(n, r, rot[n, r : r + 2].reshape(256, HEADS))

    def spread(n):
        for h in range(0, HEADS, 32):
            part = jnp.concatenate([turned[n, :, h + m : h + m + 16, :].reshape(256, 128) for m in (0, 16)], axis=1)
            both = dot(mix, part).astype(jnp.bfloat16)
            for m in range(2):
                heads = slice(h + 16 * m, h + 16 * m + 16)
                o_ref[heads, 16 * n : 16 * n + 16, :] = both[:, 128 * m : 128 * m + 128].reshape(16, 16, 128)

    for c in arriving[3:]:
        c.wait()

    def turn_values():
        for r in range(0, ROWS, 2):
            turn(2, r, jnp.concatenate([x_ref[2, t] for t in (r, r + ROWS, r + 1, r + 1 + ROWS)], axis=0))

    turn_values()
    rotate(0)
    spread(2)
    rotate(1)
    spread(0)
    spread(1)


def attend_kernel(bounds_ref, x_ref, o_ref, qt, kt, kf, vt, near, far, total, summed, items):

    def offsets(shape, axis):
        n = lax.broadcasted_iota(jnp.int32, shape, axis)
        return ((n % PAIRS) // 16) * 32 + n % 16 + (n // PAIRS) * 16

    below = offsets((BLK, BLK), 0) <= offsets((BLK, BLK), 1)
    q_off = offsets((16, BLK), 1)
    k_off = offsets((BLK, 128), 0)

    def bounds_along(shape, axis):
        n = lax.broadcasted_iota(jnp.int32, shape, axis)
        out = jnp.full(shape, SEQ, jnp.int32)
        for d in range(1, DOCS):
            out = jnp.where(n == d, bounds_ref[:, d : d + 1], out)
        return out

    q_bounds = bounds_along((16, BLK), 0)
    k_bounds = bounds_along((1, 128), 1)

    zero = jnp.zeros((HD, BLK), jnp.bfloat16)
    rest = jnp.zeros((128 - 16, BLK), jnp.bfloat16)

    def wide(x):
        t = jnp.transpose(x.astype(jnp.float32)).astype(jnp.bfloat16)
        return jnp.concatenate([t[:HD], t[HD:]], axis=1)

    def scores(j, q, flags):
        k2 = kt[j]
        low = dot(jnp.concatenate([k2, kf[j, :PAIRS]], axis=1), jnp.concatenate([q, zero, flags, rest], axis=0))
        high = dot(jnp.concatenate([k2, kf[j, PAIRS:]], axis=1), jnp.concatenate([zero, q, flags, rest], axis=0))
        return jnp.exp2(jnp.concatenate([low, high], axis=0) * jnp.float32(SCALE))

    def flags_of(i):
        return jnp.where(BLK * i + q_off >= q_bounds, jnp.float32(-BIG), jnp.float32(0.0)).astype(jnp.bfloat16)

    def partial_sum(e):
        return jnp.sum(e.reshape(BLK // 8, 8, BLK), axis=0)

    def tiles(i, row):
        runs = range(SRC * i, SRC * i + SRC)
        return jnp.concatenate([x_ref[PLACE[s], row : row + 16, :] for s in runs], axis=0)

    def near_scores(blocks):
        for i in blocks:
            q = wide(tiles(i, 0))
            kt[i] = tiles(i, 16)
            qt[i] = q
            vt[i] = wide(tiles(i, 32))
            flags = flags_of(i)
            kf[i] = jnp.where(BLK * i + k_off < k_bounds, jnp.float32(1.0), jnp.float32(0.0)).astype(jnp.bfloat16)
            e1 = jnp.where(below, scores(i, q, flags), jnp.float32(0.0))
            e0 = scores(max(i - 1, 0), q, flags)
            if i == 0:
                e0 = jnp.zeros_like(e0)
            near[i, 0] = e0
            near[i, 1] = e1
            total[i] = partial_sum(e0) + partial_sum(e1)

    scalars = [jnp.max(bounds_ref[:, d : d + 1]) for d in range(DOCS)]
    n_far = jnp.int32(0)
    for i in range(2, NBLK):
        start = starts_of(jnp.int32(BLK * i), lambda d: scalars[d])
        for j in range(i - 2, -1, -1):
            items[n_far] = NBLK * i + j
            n_far += (start < BLK * (j + 1)).astype(jnp.int32)
    near_scores(range(NBLK))
    for u in range(LONG - 1):
        items[n_far + u] = NBLK * NBLK
    trips = (n_far + LONG - MIDDLE - 1) // LONG
    left = n_far - LONG * trips
    passes = (
        (0, trips, LONG),
        (LONG * trips, (left > SHORT).astype(jnp.int32), MIDDLE),
        (LONG * trips, ((left > 0) & (left <= SHORT)).astype(jnp.int32), SHORT),
    )

    def far_blocks(work):
        for begin, trips, length in passes:

            def trip(w, _, begin=begin, length=length):
                for u in range(length):
                    n = begin + length * w + u
                    work(n, items[n] >> 4, items[n] & 15)
                return 0

            lax.fori_loop(0, trips, trip, 0)

    def far_scores(n, i, j):
        e = scores(j, qt[i], flags_of(i))
        far[n] = e
        total[i] += partial_sum(e)

    far_blocks(far_scores)
    for i in range(NBLK):
        inverse = 1.0 / jnp.sum(total[i], axis=0, keepdims=True)
        total[i] = jnp.broadcast_to(inverse, (8, BLK))
        summed[i] = jnp.zeros((HD, BLK), jnp.float32)

    def far_values(n, i, j):
        summed[i] += dot(vt[j], (far[n] * total[i][0:1]).astype(jnp.bfloat16))

    far_blocks(far_values)

    for i in range(NBLK):
        w = jnp.concatenate([(near[i, n] * total[i][0:1]).astype(jnp.bfloat16) for n in range(2)], axis=0)
        out = dot(jnp.concatenate([vt[max(i - 1, 0)], vt[i]], axis=1), w) + summed[i]
        both = jnp.transpose(jnp.concatenate([out[:, :PAIRS], out[:, PAIRS:]], axis=0))
        both = both.astype(jnp.bfloat16)
        for n in range(SRC):
            o_ref[PLACE[SRC * i + n]] = both[16 * n : 16 * n + 16]


def take_kernel(x_ref, o_hbm, turned, out, sems):
    mix = interleave()
    eye = identity(128)
    for h in range(0, HEADS, 32):
        part = jnp.concatenate([x_ref[h + m : h + m + 16].reshape(256, 128) for m in (0, 16)], axis=1)
        both = dot(mix, part).astype(jnp.bfloat16)
        for m in range(2):
            turned[:, h + 16 * m : h + 16 * m + 16, :] = both[:, 128 * m : 128 * m + 128].reshape(16, 16, 128)
    copies = []
    for r in range(0, ROWS, 2):
        both = dot(eye, turned[r : r + 2].reshape(256, 128), NT).astype(jnp.bfloat16)
        for m in range(2):
            out[r + m] = both[:HD, 128 * m : 128 * m + 128]
            out[r + m + ROWS] = both[HD:, 128 * m : 128 * m + 128]
        if r % 8 == 6:
            for first in (r - 6, r - 6 + ROWS):
                copy = pltpu.make_async_copy(
                    out.at[pl.ds(first, 8)], o_hbm.at[pl.ds(first, 8)], sems.at[len(copies)]
                )
                copy.start()
                copies.append(copy)
    for copy in copies:
        copy.wait()


VMEM = pl.BlockSpec(memory_space=pltpu.VMEM)
HBM = pl.BlockSpec(memory_space=pltpu.HBM)


def in_hbm(x):
    return pltpu.with_memory_space_constraint(x, pltpu.HBM)


def send_call(doc_bounds, q, k, v, q_gain, k_gain):
    return pl.pallas_call(
        send_kernel,
        out_shape=jax.ShapeDtypeStruct((HEADS, 48, 128), jnp.bfloat16),
        in_specs=[HBM] * 6,
        out_specs=VMEM,
        scratch_shapes=[
            pltpu.VMEM((1, DOCS + 1), jnp.int32),
            pltpu.VMEM((3, TOK, HD, HEADS), jnp.bfloat16),
            pltpu.VMEM((2, 1, HD), jnp.float32),
            pltpu.VMEM((2, ROWS, 128, HEADS), jnp.bfloat16),
            pltpu.VMEM((3, ROWS, HEADS, 128), jnp.bfloat16),
            pltpu.SemaphoreType.DMA((6,)),
        ],
        compiler_params=pltpu.CompilerParams(vmem_limit_bytes=32 << 20),
        name="send_side",
    )(*(in_hbm(x) for x in (doc_bounds, q, k, v, q_gain.reshape(1, HD), k_gain.reshape(1, HD))))


def attend_call(doc_bounds, mine):
    return pl.pallas_call(
        attend_kernel,
        out_shape=jax.ShapeDtypeStruct((SEQ // TOK, ROWS, 128), jnp.bfloat16),
        in_specs=[VMEM, VMEM],
        out_specs=VMEM,
        scratch_shapes=[
            pltpu.VMEM((NBLK + 1, HD, BLK), jnp.bfloat16),
            pltpu.VMEM((NBLK, PAIRS, 128), jnp.bfloat16),
            pltpu.VMEM((NBLK, BLK, 128), jnp.bfloat16),
            pltpu.VMEM((NBLK, HD, BLK), jnp.bfloat16),
            pltpu.VMEM((NBLK, 2, BLK, BLK), jnp.float32),
            pltpu.VMEM((FAR, BLK, BLK), jnp.float32),
            pltpu.VMEM((NBLK + 1, 8, BLK), jnp.float32),
            pltpu.VMEM((NBLK + 1, HD, BLK), jnp.float32),
            pltpu.SMEM((FAR,), jnp.int32),
        ],
        compiler_params=pltpu.CompilerParams(vmem_limit_bytes=44 << 20),
        name="attend",
    )(doc_bounds, mine)


def take_call(back):
    return pl.pallas_call(
        take_kernel,
        out_shape=jax.ShapeDtypeStruct((TOK, HD, HEADS), jnp.bfloat16),
        in_specs=[VMEM],
        out_specs=HBM,
        scratch_shapes=[
            pltpu.VMEM((ROWS, HEADS, 128), jnp.bfloat16),
            pltpu.VMEM((TOK, HD, HEADS), jnp.bfloat16),
            pltpu.SemaphoreType.DMA((4,)),
        ],
        compiler_params=pltpu.CompilerParams(vmem_limit_bytes=32 << 20),
        name="take_side",
    )(back)


def exchange(x):
    return lax.all_to_all(x, "run", split_axis=0, concat_axis=0, axis_index_groups=[ORDER], tiled=True)


def body(queries, keys, values, doc_bounds, q_gain, k_gain):
    doc_bounds = doc_bounds.reshape(1, DOCS + 1)
    inputs = [jnp.transpose(x, (0, 2, 1)) for x in (queries, keys, values)]
    packed = send_call(doc_bounds, *inputs, q_gain, k_gain)
    mine = exchange(packed)
    result = attend_call(doc_bounds, mine)
    back = exchange(result)
    return jnp.transpose(take_call(back), (0, 2, 1))


def solution(mesh):
    runs = jax.sharding.Mesh(mesh.devices.reshape(len(PLACE), -1), ("run", "dp"))
    tokens = P(("dp", "run"), None, None)
    return jax.shard_map(
        body,
        mesh=runs,
        in_specs=(tokens, tokens, tokens, P("dp"), P(), P()),
        out_specs=tokens,
        check_vma=False,
    )
```

```python
import jax
import jax.numpy as jnp
from jax import lax
from jax.experimental import pallas as pl
from jax.experimental.pallas import tpu as pltpu
from jax.sharding import PartitionSpec as P

TOK = 32
ROWS = 16
HD = 64
HEADS = 128
DOCS = 8
SEQ = 4096
BLK = 256
PAIRS = BLK // 2
NBLK = SEQ // BLK
SRC = BLK // TOK
LONG, MIDDLE, SHORT = 16, 8, 4
FAR = (NBLK - 2) * (NBLK - 1) // 2 + LONG
NT = (((1,), (1,)), ((), ()))
NN = (((1,), (0,)), ((), ()))
BIG = 32768.0
SCALE = 1.4426950408889634 / 8.0
FIRST = -9.210340371976184


def run_of(z, x, c):
    return ((z % 8 * 2 + c) * 4 + x) * 2 + z // 8


FIRST_Z = [8, 7, 9, 6, 10, 5, 11, 4, 12, 3, 13, 2, 14, 1, 15, 0]
THEN_Z = [0, 1, 2, 3, 4, 5, 6, 7, 8, 9, 10, 11, 12, 13, 14, 15]
ORDER_IN = [run_of(z, x, c) for z in FIRST_Z for x in range(4) for c in range(2)]
ORDER_OUT = [run_of(z, x, c) for z in THEN_Z for x in range(4) for c in range(2)]
PLACE_IN = [ORDER_IN.index(s) for s in range(len(ORDER_IN))]
PLACE_OUT = [ORDER_OUT.index(s) for s in range(len(ORDER_OUT))]


def dot(a, b, dims=NN):
    return lax.dot_general(a, b, dims, preferred_element_type=jnp.float32)


def starts_of(token, bound):
    start = jnp.zeros_like(token)
    for d in range(1, DOCS):
        start = jnp.where(token >= bound(d), bound(d), start)
    return start


def identity(n):
    row = lax.broadcasted_iota(jnp.int32, (n, n), 0)
    col = lax.broadcasted_iota(jnp.int32, (n, n), 1)
    return (row == col).astype(jnp.float32).astype(jnp.bfloat16)


def interleave():
    row = lax.broadcasted_iota(jnp.int32, (256, 256), 0)
    col = lax.broadcasted_iota(jnp.int32, (256, 256), 1)
    return (col == (row % 16) * 16 + row // 16).astype(jnp.float32).astype(jnp.bfloat16)


def send_kernel(
    bounds_hbm, q_hbm, k_hbm, v_hbm, qg_hbm, kg_hbm, o_ref, bounds_ref, x_ref, g_ref, rot, turned, sems
):
    arriving = [
        pltpu.make_async_copy(source, target, sems.at[n])
        for n, (source, target) in enumerate(
            (
                (bounds_hbm, bounds_ref),
                (qg_hbm, g_ref.at[0]),
                (kg_hbm, g_ref.at[1]),
                (q_hbm, x_ref.at[0]),
                (v_hbm, x_ref.at[2]),
                (k_hbm, x_ref.at[1]),
            )
        )
    ]
    for c in arriving:
        c.start()
    for c in arriving[:3]:
        c.wait()
    lane = lax.broadcasted_iota(jnp.int32, (HD // 2, 128), 1)
    token = lax.axis_index("run") * TOK + lane
    start = starts_of(token, lambda d: bounds_ref[:, d : d + 1])
    place = (token - start).astype(jnp.float32)
    index = lax.broadcasted_iota(jnp.int32, (HD // 2, 128), 0).astype(jnp.float32)
    angle = place * jnp.exp(jnp.float32(FIRST) * index * 2.0 / HD)
    cosine = jnp.cos(angle)
    sine = jnp.sin(angle)
    eye = identity(HEADS)
    mix = interleave()

    def turn(n, r, rows):
        both = dot(eye, rows, NT).astype(jnp.bfloat16)
        turned[n, r] = both[:, :128]
        turned[n, r + 1] = both[:, 128:]

    def rotate(n):
        gain = jnp.transpose(jnp.broadcast_to(g_ref[n], (HEADS, HD)))
        for r in range(0, ROWS, 2):
            for t in (r, r + ROWS, r + 1, r + 1 + ROWS):
                c = jnp.broadcast_to(cosine[:, t : t + 1], (HD // 2, HEADS))
                s = jnp.broadcast_to(sine[:, t : t + 1], (HD // 2, HEADS))
                x = x_ref[n, t].astype(jnp.float32)
                scale = lax.rsqrt(jnp.mean(x * x, axis=0, keepdims=True) + 1e-06)
                x = x * scale * gain
                a, b = x[: HD // 2], x[HD // 2 :]
                y = jnp.concatenate([a * c - b * s, a * s + b * c], axis=0)
                rot[n, t % ROWS, pl.ds((t // ROWS) * HD, HD), :] = y.astype(jnp.bfloat16)
            turn(n, r, rot[n, r : r + 2].reshape(256, HEADS))

    def spread(n):
        for h in range(0, HEADS, 32):
            part = jnp.concatenate([turned[n, :, h + m : h + m + 16, :].reshape(256, 128) for m in (0, 16)], axis=1)
            both = dot(mix, part).astype(jnp.bfloat16)
            for m in range(2):
                heads = slice(h + 16 * m, h + 16 * m + 16)
                o_ref[heads, 16 * n : 16 * n + 16, :] = both[:, 128 * m : 128 * m + 128].reshape(16, 16, 128)

    for c in arriving[3:]:
        c.wait()

    def turn_values():
        for r in range(0, ROWS, 2):
            turn(2, r, jnp.concatenate([x_ref[2, t] for t in (r, r + ROWS, r + 1, r + 1 + ROWS)], axis=0))

    turn_values()
    rotate(0)
    spread(2)
    rotate(1)
    spread(0)
    spread(1)


def attend_kernel(bounds_ref, x_ref, o_ref, qt, kt, kf, vt, near, far, total, summed, items):

    def offsets(shape, axis):
        n = lax.broadcasted_iota(jnp.int32, shape, axis)
        return ((n % PAIRS) // 16) * 32 + n % 16 + (n // PAIRS) * 16

    below = offsets((BLK, BLK), 0) <= offsets((BLK, BLK), 1)
    q_off = offsets((16, BLK), 1)
    k_off = offsets((BLK, 128), 0)

    def bounds_along(shape, axis):
        n = lax.broadcasted_iota(jnp.int32, shape, axis)
        out = jnp.full(shape, SEQ, jnp.int32)
        for d in range(1, DOCS):
            out = jnp.where(n == d, bounds_ref[:, d : d + 1], out)
        return out

    q_bounds = bounds_along((16, BLK), 0)
    k_bounds = bounds_along((1, 128), 1)

    zero = jnp.zeros((HD, BLK), jnp.bfloat16)
    rest = jnp.zeros((128 - 16, BLK), jnp.bfloat16)

    def wide(x):
        t = jnp.transpose(x.astype(jnp.float32)).astype(jnp.bfloat16)
        return jnp.concatenate([t[:HD], t[HD:]], axis=1)

    def scores(j, q, flags):
        k2 = kt[j]
        low = dot(jnp.concatenate([k2, kf[j, :PAIRS]], axis=1), jnp.concatenate([q, zero, flags, rest], axis=0))
        high = dot(jnp.concatenate([k2, kf[j, PAIRS:]], axis=1), jnp.concatenate([zero, q, flags, rest], axis=0))
        return jnp.exp2(jnp.concatenate([low, high], axis=0) * jnp.float32(SCALE))

    def flags_of(i):
        return jnp.where(BLK * i + q_off >= q_bounds, jnp.float32(-BIG), jnp.float32(0.0)).astype(jnp.bfloat16)

    def partial_sum(e):
        return jnp.sum(e.reshape(BLK // 8, 8, BLK), axis=0)

    def tiles(i, row):
        runs = range(SRC * i, SRC * i + SRC)
        return jnp.concatenate([x_ref[PLACE_IN[s], row : row + 16, :] for s in runs], axis=0)

    def near_scores(blocks):
        for i in blocks:
            q = wide(tiles(i, 0))
            kt[i] = tiles(i, 16)
            qt[i] = q
            vt[i] = wide(tiles(i, 32))
            flags = flags_of(i)
            kf[i] = jnp.where(BLK * i + k_off < k_bounds, jnp.float32(1.0), jnp.float32(0.0)).astype(jnp.bfloat16)
            e1 = jnp.where(below, scores(i, q, flags), jnp.float32(0.0))
            e0 = scores(max(i - 1, 0), q, flags)
            if i == 0:
                e0 = jnp.zeros_like(e0)
            near[i, 0] = e0
            near[i, 1] = e1
            total[i] = partial_sum(e0) + partial_sum(e1)

    scalars = [jnp.max(bounds_ref[:, d : d + 1]) for d in range(DOCS)]
    n_far = jnp.int32(0)
    for i in range(2, NBLK):
        start = starts_of(jnp.int32(BLK * i), lambda d: scalars[d])
        for j in range(i - 2, -1, -1):
            items[n_far] = NBLK * i + j
            n_far += (start < BLK * (j + 1)).astype(jnp.int32)
    near_scores(range(NBLK))
    for u in range(LONG - 1):
        items[n_far + u] = NBLK * NBLK
    trips = (n_far + LONG - MIDDLE - 1) // LONG
    left = n_far - LONG * trips
    passes = (
        (0, trips, LONG),
        (LONG * trips, (left > SHORT).astype(jnp.int32), MIDDLE),
        (LONG * trips, ((left > 0) & (left <= SHORT)).astype(jnp.int32), SHORT),
    )

    def far_blocks(work):
        for begin, trips, length in passes:

            def trip(w, _, begin=begin, length=length):
                for u in range(length):
                    n = begin + length * w + u
                    work(n, items[n] >> 4, items[n] & 15)
                return 0

            lax.fori_loop(0, trips, trip, 0)

    def far_scores(n, i, j):
        e = scores(j, qt[i], flags_of(i))
        far[n] = e
        total[i] += partial_sum(e)

    far_blocks(far_scores)
    for i in range(NBLK):
        inverse = 1.0 / jnp.sum(total[i], axis=0, keepdims=True)
        total[i] = jnp.broadcast_to(inverse, (8, BLK))
        summed[i] = jnp.zeros((HD, BLK), jnp.float32)

    def far_values(n, i, j):
        summed[i] += dot(vt[j], (far[n] * total[i][0:1]).astype(jnp.bfloat16))

    far_blocks(far_values)

    for i in range(NBLK):
        w = jnp.concatenate([(near[i, n] * total[i][0:1]).astype(jnp.bfloat16) for n in range(2)], axis=0)
        out = dot(jnp.concatenate([vt[max(i - 1, 0)], vt[i]], axis=1), w) + summed[i]
        both = jnp.transpose(jnp.concatenate([out[:, :PAIRS], out[:, PAIRS:]], axis=0))
        both = both.astype(jnp.bfloat16)
        for n in range(SRC):
            o_ref[PLACE_OUT[SRC * i + n]] = both[16 * n : 16 * n + 16]


def take_kernel(x_ref, o_hbm, turned, out, sems):
    mix = interleave()
    eye = identity(128)
    for h in range(0, HEADS, 32):
        tiles = [x_ref[PLACE_OUT[s]] for s in ORDER_IN[h : h + 32]]
        part = jnp.concatenate([jnp.concatenate(tiles[m : m + 16], axis=0) for m in (0, 16)], axis=1)
        both = dot(mix, part).astype(jnp.bfloat16)
        for m in range(2):
            turned[:, h + 16 * m : h + 16 * m + 16, :] = both[:, 128 * m : 128 * m + 128].reshape(16, 16, 128)
    copies = []
    for r in range(0, ROWS, 2):
        both = dot(eye, turned[r : r + 2].reshape(256, 128), NT).astype(jnp.bfloat16)
        for m in range(2):
            out[r + m] = both[:HD, 128 * m : 128 * m + 128]
            out[r + m + ROWS] = both[HD:, 128 * m : 128 * m + 128]
        if r % 8 == 6:
            for first in (r - 6, r - 6 + ROWS):
                copy = pltpu.make_async_copy(
                    out.at[pl.ds(first, 8)], o_hbm.at[pl.ds(first, 8)], sems.at[len(copies)]
                )
                copy.start()
                copies.append(copy)
    for copy in copies:
        copy.wait()


VMEM = pl.BlockSpec(memory_space=pltpu.VMEM)
HBM = pl.BlockSpec(memory_space=pltpu.HBM)


def in_hbm(x):
    return pltpu.with_memory_space_constraint(x, pltpu.HBM)


def send_call(doc_bounds, q, k, v, q_gain, k_gain):
    return pl.pallas_call(
        send_kernel,
        out_shape=jax.ShapeDtypeStruct((HEADS, 48, 128), jnp.bfloat16),
        in_specs=[HBM] * 6,
        out_specs=VMEM,
        scratch_shapes=[
            pltpu.VMEM((1, DOCS + 1), jnp.int32),
            pltpu.VMEM((3, TOK, HD, HEADS), jnp.bfloat16),
            pltpu.VMEM((2, 1, HD), jnp.float32),
            pltpu.VMEM((2, ROWS, 128, HEADS), jnp.bfloat16),
            pltpu.VMEM((3, ROWS, HEADS, 128), jnp.bfloat16),
            pltpu.SemaphoreType.DMA((6,)),
        ],
        compiler_params=pltpu.CompilerParams(vmem_limit_bytes=32 << 20),
        name="send_side",
    )(*(in_hbm(x) for x in (doc_bounds, q, k, v, q_gain.reshape(1, HD), k_gain.reshape(1, HD))))


def attend_call(doc_bounds, mine):
    return pl.pallas_call(
        attend_kernel,
        out_shape=jax.ShapeDtypeStruct((SEQ // TOK, ROWS, 128), jnp.bfloat16),
        in_specs=[VMEM, VMEM],
        out_specs=VMEM,
        scratch_shapes=[
            pltpu.VMEM((NBLK + 1, HD, BLK), jnp.bfloat16),
            pltpu.VMEM((NBLK, PAIRS, 128), jnp.bfloat16),
            pltpu.VMEM((NBLK, BLK, 128), jnp.bfloat16),
            pltpu.VMEM((NBLK, HD, BLK), jnp.bfloat16),
            pltpu.VMEM((NBLK, 2, BLK, BLK), jnp.float32),
            pltpu.VMEM((FAR, BLK, BLK), jnp.float32),
            pltpu.VMEM((NBLK + 1, 8, BLK), jnp.float32),
            pltpu.VMEM((NBLK + 1, HD, BLK), jnp.float32),
            pltpu.SMEM((FAR,), jnp.int32),
        ],
        compiler_params=pltpu.CompilerParams(vmem_limit_bytes=44 << 20),
        name="attend",
    )(doc_bounds, mine)


def take_call(back):
    return pl.pallas_call(
        take_kernel,
        out_shape=jax.ShapeDtypeStruct((TOK, HD, HEADS), jnp.bfloat16),
        in_specs=[VMEM],
        out_specs=HBM,
        scratch_shapes=[
            pltpu.VMEM((ROWS, HEADS, 128), jnp.bfloat16),
            pltpu.VMEM((TOK, HD, HEADS), jnp.bfloat16),
            pltpu.SemaphoreType.DMA((4,)),
        ],
        compiler_params=pltpu.CompilerParams(vmem_limit_bytes=32 << 20),
        name="take_side",
    )(back)


def exchange(x, order):
    return lax.all_to_all(x, "run", split_axis=0, concat_axis=0, axis_index_groups=[order], tiled=True)


def body(queries, keys, values, doc_bounds, q_gain, k_gain):
    doc_bounds = doc_bounds.reshape(1, DOCS + 1)
    inputs = [jnp.transpose(x, (0, 2, 1)) for x in (queries, keys, values)]
    packed = send_call(doc_bounds, *inputs, q_gain, k_gain)
    mine = exchange(packed, ORDER_IN)
    result = attend_call(doc_bounds, mine)
    back = exchange(result, ORDER_OUT)
    return jnp.transpose(take_call(back), (0, 2, 1))


def solution(mesh):
    runs = jax.sharding.Mesh(mesh.devices.reshape(len(ORDER_IN), -1), ("run", "dp"))
    tokens = P(("dp", "run"), None, None)
    return jax.shard_map(
        body,
        mesh=runs,
        in_specs=(tokens, tokens, tokens, P("dp"), P(), P()),
        out_specs=tokens,
        check_vma=False,
    )
```

```python
import jax
import jax.numpy as jnp
from jax import lax
from jax.experimental import pallas as pl
from jax.experimental.pallas import tpu as pltpu
from jax.sharding import PartitionSpec as P

TOK = 32
ROWS = 16
HD = 64
HEADS = 128
DOCS = 8
SEQ = 4096
BLK = 256
PAIRS = BLK // 2
NBLK = SEQ // BLK
SRC = BLK // TOK
LONG, MIDDLE, SHORT = 16, 8, 4
FAR = (NBLK - 2) * (NBLK - 1) // 2 + LONG
NT = (((1,), (1,)), ((), ()))
NN = (((1,), (0,)), ((), ()))
BIG = 32768.0
SCALE = 1.4426950408889634 / 8.0
FIRST = -9.210340371976184


def run_of(z, x, c):
    return ((z % 8 * 2 + c) * 4 + x) * 2 + z // 8


FIRST_Z = [8, 7, 9, 6, 10, 5, 11, 4, 12, 3, 13, 2, 14, 1, 15, 0]
THEN_Z = [0, 15, 1, 14, 2, 13, 3, 12, 4, 11, 5, 10, 6, 9, 7, 8]
ORDER_IN = [run_of(z, x, c) for z in FIRST_Z for x in range(4) for c in range(2)]
ORDER_OUT = [run_of(z, x, c) for z in THEN_Z for x in range(4) for c in range(2)]
PLACE_IN = [ORDER_IN.index(s) for s in range(len(ORDER_IN))]
PLACE_OUT = [ORDER_OUT.index(s) for s in range(len(ORDER_OUT))]


def dot(a, b, dims=NN):
    return lax.dot_general(a, b, dims, preferred_element_type=jnp.float32)


def starts_of(token, bound):
    start = jnp.zeros_like(token)
    for d in range(1, DOCS):
        start = jnp.where(token >= bound(d), bound(d), start)
    return start


def identity(n):
    row = lax.broadcasted_iota(jnp.int32, (n, n), 0)
    col = lax.broadcasted_iota(jnp.int32, (n, n), 1)
    return (row == col).astype(jnp.float32).astype(jnp.bfloat16)


def interleave():
    row = lax.broadcasted_iota(jnp.int32, (256, 256), 0)
    col = lax.broadcasted_iota(jnp.int32, (256, 256), 1)
    return (col == (row % 16) * 16 + row // 16).astype(jnp.float32).astype(jnp.bfloat16)


def send_kernel(
    bounds_hbm, q_hbm, k_hbm, v_hbm, qg_hbm, kg_hbm, o_ref, bounds_ref, x_ref, g_ref, rot, turned, sems
):
    arriving = [
        pltpu.make_async_copy(source, target, sems.at[n])
        for n, (source, target) in enumerate(
            (
                (bounds_hbm, bounds_ref),
                (qg_hbm, g_ref.at[0]),
                (kg_hbm, g_ref.at[1]),
                (q_hbm, x_ref.at[0]),
                (v_hbm, x_ref.at[2]),
                (k_hbm, x_ref.at[1]),
            )
        )
    ]
    for c in arriving:
        c.start()
    for c in arriving[:3]:
        c.wait()
    lane = lax.broadcasted_iota(jnp.int32, (HD // 2, 128), 1)
    token = lax.axis_index("run") * TOK + lane
    start = starts_of(token, lambda d: bounds_ref[:, d : d + 1])
    place = (token - start).astype(jnp.float32)
    index = lax.broadcasted_iota(jnp.int32, (HD // 2, 128), 0).astype(jnp.float32)
    angle = place * jnp.exp(jnp.float32(FIRST) * index * 2.0 / HD)
    cosine = jnp.cos(angle)
    sine = jnp.sin(angle)
    eye = identity(HEADS)
    mix = interleave()

    def turn(n, r, rows):
        both = dot(eye, rows, NT).astype(jnp.bfloat16)
        turned[n, r] = both[:, :128]
        turned[n, r + 1] = both[:, 128:]

    def rotate(n):
        gain = jnp.transpose(jnp.broadcast_to(g_ref[n], (HEADS, HD)))
        for r in range(0, ROWS, 2):
            for t in (r, r + ROWS, r + 1, r + 1 + ROWS):
                c = jnp.broadcast_to(cosine[:, t : t + 1], (HD // 2, HEADS))
                s = jnp.broadcast_to(sine[:, t : t + 1], (HD // 2, HEADS))
                x = x_ref[n, t].astype(jnp.float32)
                scale = lax.rsqrt(jnp.mean(x * x, axis=0, keepdims=True) + 1e-06)
                x = x * scale * gain
                a, b = x[: HD // 2], x[HD // 2 :]
                y = jnp.concatenate([a * c - b * s, a * s + b * c], axis=0)
                rot[n, t % ROWS, pl.ds((t // ROWS) * HD, HD), :] = y.astype(jnp.bfloat16)
            turn(n, r, rot[n, r : r + 2].reshape(256, HEADS))

    def spread(n):
        for h in range(0, HEADS, 32):
            part = jnp.concatenate([turned[n, :, h + m : h + m + 16, :].reshape(256, 128) for m in (0, 16)], axis=1)
            both = dot(mix, part).astype(jnp.bfloat16)
            for m in range(2):
                heads = slice(h + 16 * m, h + 16 * m + 16)
                o_ref[heads, 16 * n : 16 * n + 16, :] = both[:, 128 * m : 128 * m + 128].reshape(16, 16, 128)

    for c in arriving[3:]:
        c.wait()

    def turn_values():
        for r in range(0, ROWS, 2):
            turn(2, r, jnp.concatenate([x_ref[2, t] for t in (r, r + ROWS, r + 1, r + 1 + ROWS)], axis=0))

    turn_values()
    rotate(0)
    spread(2)
    rotate(1)
    spread(0)
    spread(1)


def attend_kernel(bounds_ref, x_ref, o_ref, qt, kt, kf, vt, near, far, total, summed, items):

    def offsets(shape, axis):
        n = lax.broadcasted_iota(jnp.int32, shape, axis)
        return ((n % PAIRS) // 16) * 32 + n % 16 + (n // PAIRS) * 16

    below = offsets((BLK, BLK), 0) <= offsets((BLK, BLK), 1)
    q_off = offsets((16, BLK), 1)
    k_off = offsets((BLK, 128), 0)

    def bounds_along(shape, axis):
        n = lax.broadcasted_iota(jnp.int32, shape, axis)
        out = jnp.full(shape, SEQ, jnp.int32)
        for d in range(1, DOCS):
            out = jnp.where(n == d, bounds_ref[:, d : d + 1], out)
        return out

    q_bounds = bounds_along((16, BLK), 0)
    k_bounds = bounds_along((1, 128), 1)

    zero = jnp.zeros((HD, BLK), jnp.bfloat16)
    rest = jnp.zeros((128 - 16, BLK), jnp.bfloat16)

    def wide(x):
        t = jnp.transpose(x.astype(jnp.float32)).astype(jnp.bfloat16)
        return jnp.concatenate([t[:HD], t[HD:]], axis=1)

    def scores(j, q, flags):
        k2 = kt[j]
        low = dot(jnp.concatenate([k2, kf[j, :PAIRS]], axis=1), jnp.concatenate([q, zero, flags, rest], axis=0))
        high = dot(jnp.concatenate([k2, kf[j, PAIRS:]], axis=1), jnp.concatenate([zero, q, flags, rest], axis=0))
        return jnp.exp2(jnp.concatenate([low, high], axis=0) * jnp.float32(SCALE))

    def flags_of(i):
        return jnp.where(BLK * i + q_off >= q_bounds, jnp.float32(-BIG), jnp.float32(0.0)).astype(jnp.bfloat16)

    def partial_sum(e):
        return jnp.sum(e.reshape(BLK // 8, 8, BLK), axis=0)

    def tiles(i, row):
        runs = range(SRC * i, SRC * i + SRC)
        return jnp.concatenate([x_ref[PLACE_IN[s], row : row + 16, :] for s in runs], axis=0)

    def near_scores(blocks):
        for i in blocks:
            q = wide(tiles(i, 0))
            kt[i] = tiles(i, 16)
            qt[i] = q
            vt[i] = wide(tiles(i, 32))
            flags = flags_of(i)
            kf[i] = jnp.where(BLK * i + k_off < k_bounds, jnp.float32(1.0), jnp.float32(0.0)).astype(jnp.bfloat16)
            e1 = jnp.where(below, scores(i, q, flags), jnp.float32(0.0))
            e0 = scores(max(i - 1, 0), q, flags)
            if i == 0:
                e0 = jnp.zeros_like(e0)
            near[i, 0] = e0
            near[i, 1] = e1
            total[i] = partial_sum(e0) + partial_sum(e1)

    scalars = [jnp.max(bounds_ref[:, d : d + 1]) for d in range(DOCS)]
    n_far = jnp.int32(0)
    for i in range(2, NBLK):
        start = starts_of(jnp.int32(BLK * i), lambda d: scalars[d])
        for j in range(i - 2, -1, -1):
            items[n_far] = NBLK * i + j
            n_far += (start < BLK * (j + 1)).astype(jnp.int32)
    near_scores(range(NBLK))
    for u in range(LONG - 1):
        items[n_far + u] = NBLK * NBLK
    trips = (n_far + LONG - MIDDLE - 1) // LONG
    left = n_far - LONG * trips
    passes = (
        (0, trips, LONG),
        (LONG * trips, (left > SHORT).astype(jnp.int32), MIDDLE),
        (LONG * trips, ((left > 0) & (left <= SHORT)).astype(jnp.int32), SHORT),
    )

    def far_blocks(work):
        for begin, trips, length in passes:

            def trip(w, _, begin=begin, length=length):
                for u in range(length):
                    n = begin + length * w + u
                    work(n, items[n] >> 4, items[n] & 15)
                return 0

            lax.fori_loop(0, trips, trip, 0)

    def far_scores(n, i, j):
        e = scores(j, qt[i], flags_of(i))
        far[n] = e
        total[i] += partial_sum(e)

    far_blocks(far_scores)
    for i in range(NBLK):
        inverse = 1.0 / jnp.sum(total[i], axis=0, keepdims=True)
        total[i] = jnp.broadcast_to(inverse, (8, BLK))
        summed[i] = jnp.zeros((HD, BLK), jnp.float32)

    def far_values(n, i, j):
        summed[i] += dot(vt[j], (far[n] * total[i][0:1]).astype(jnp.bfloat16))

    far_blocks(far_values)

    for i in range(NBLK):
        w = jnp.concatenate([(near[i, n] * total[i][0:1]).astype(jnp.bfloat16) for n in range(2)], axis=0)
        out = dot(jnp.concatenate([vt[max(i - 1, 0)], vt[i]], axis=1), w) + summed[i]
        both = jnp.transpose(jnp.concatenate([out[:, :PAIRS], out[:, PAIRS:]], axis=0))
        both = both.astype(jnp.bfloat16)
        for n in range(SRC):
            o_ref[PLACE_OUT[SRC * i + n]] = both[16 * n : 16 * n + 16]


def take_kernel(x_ref, o_hbm, turned, out, sems):
    mix = interleave()
    eye = identity(128)
    for h in range(0, HEADS, 32):
        tiles = [x_ref[PLACE_OUT[s]] for s in ORDER_IN[h : h + 32]]
        part = jnp.concatenate([jnp.concatenate(tiles[m : m + 16], axis=0) for m in (0, 16)], axis=1)
        both = dot(mix, part).astype(jnp.bfloat16)
        for m in range(2):
            turned[:, h + 16 * m : h + 16 * m + 16, :] = both[:, 128 * m : 128 * m + 128].reshape(16, 16, 128)
    copies = []
    for r in range(0, ROWS, 2):
        both = dot(eye, turned[r : r + 2].reshape(256, 128), NT).astype(jnp.bfloat16)
        for m in range(2):
            out[r + m] = both[:HD, 128 * m : 128 * m + 128]
            out[r + m + ROWS] = both[HD:, 128 * m : 128 * m + 128]
        if r % 8 == 6:
            for first in (r - 6, r - 6 + ROWS):
                copy = pltpu.make_async_copy(
                    out.at[pl.ds(first, 8)], o_hbm.at[pl.ds(first, 8)], sems.at[len(copies)]
                )
                copy.start()
                copies.append(copy)
    for copy in copies:
        copy.wait()


VMEM = pl.BlockSpec(memory_space=pltpu.VMEM)
HBM = pl.BlockSpec(memory_space=pltpu.HBM)


def in_hbm(x):
    return pltpu.with_memory_space_constraint(x, pltpu.HBM)


def send_call(doc_bounds, q, k, v, q_gain, k_gain):
    return pl.pallas_call(
        send_kernel,
        out_shape=jax.ShapeDtypeStruct((HEADS, 48, 128), jnp.bfloat16),
        in_specs=[HBM] * 6,
        out_specs=VMEM,
        scratch_shapes=[
            pltpu.VMEM((1, DOCS + 1), jnp.int32),
            pltpu.VMEM((3, TOK, HD, HEADS), jnp.bfloat16),
            pltpu.VMEM((2, 1, HD), jnp.float32),
            pltpu.VMEM((2, ROWS, 128, HEADS), jnp.bfloat16),
            pltpu.VMEM((3, ROWS, HEADS, 128), jnp.bfloat16),
            pltpu.SemaphoreType.DMA((6,)),
        ],
        compiler_params=pltpu.CompilerParams(vmem_limit_bytes=32 << 20),
        name="send_side",
    )(*(in_hbm(x) for x in (doc_bounds, q, k, v, q_gain.reshape(1, HD), k_gain.reshape(1, HD))))


def attend_call(doc_bounds, mine):
    return pl.pallas_call(
        attend_kernel,
        out_shape=jax.ShapeDtypeStruct((SEQ // TOK, ROWS, 128), jnp.bfloat16),
        in_specs=[VMEM, VMEM],
        out_specs=VMEM,
        scratch_shapes=[
            pltpu.VMEM((NBLK + 1, HD, BLK), jnp.bfloat16),
            pltpu.VMEM((NBLK, PAIRS, 128), jnp.bfloat16),
            pltpu.VMEM((NBLK, BLK, 128), jnp.bfloat16),
            pltpu.VMEM((NBLK, HD, BLK), jnp.bfloat16),
            pltpu.VMEM((NBLK, 2, BLK, BLK), jnp.float32),
            pltpu.VMEM((FAR, BLK, BLK), jnp.float32),
            pltpu.VMEM((NBLK + 1, 8, BLK), jnp.float32),
            pltpu.VMEM((NBLK + 1, HD, BLK), jnp.float32),
            pltpu.SMEM((FAR,), jnp.int32),
        ],
        compiler_params=pltpu.CompilerParams(vmem_limit_bytes=44 << 20),
        name="attend",
    )(doc_bounds, mine)


def take_call(back):
    return pl.pallas_call(
        take_kernel,
        out_shape=jax.ShapeDtypeStruct((TOK, HD, HEADS), jnp.bfloat16),
        in_specs=[VMEM],
        out_specs=HBM,
        scratch_shapes=[
            pltpu.VMEM((ROWS, HEADS, 128), jnp.bfloat16),
            pltpu.VMEM((TOK, HD, HEADS), jnp.bfloat16),
            pltpu.SemaphoreType.DMA((4,)),
        ],
        compiler_params=pltpu.CompilerParams(vmem_limit_bytes=32 << 20),
        name="take_side",
    )(back)


def exchange(x, order):
    return lax.all_to_all(x, "run", split_axis=0, concat_axis=0, axis_index_groups=[order], tiled=True)


def body(queries, keys, values, doc_bounds, q_gain, k_gain):
    doc_bounds = doc_bounds.reshape(1, DOCS + 1)
    inputs = [jnp.transpose(x, (0, 2, 1)) for x in (queries, keys, values)]
    packed = send_call(doc_bounds, *inputs, q_gain, k_gain)
    mine = exchange(packed, ORDER_IN)
    result = attend_call(doc_bounds, mine)
    back = exchange(result, ORDER_OUT)
    return jnp.transpose(take_call(back), (0, 2, 1))


def solution(mesh):
    runs = jax.sharding.Mesh(mesh.devices.reshape(len(ORDER_IN), -1), ("run", "dp"))
    tokens = P(("dp", "run"), None, None)
    return jax.shard_map(
        body,
        mesh=runs,
        in_specs=(tokens, tokens, tokens, P("dp"), P(), P()),
        out_specs=tokens,
        check_vma=False,
    )
```

```python
import jax
import jax.numpy as jnp
from jax import lax
from jax.experimental import pallas as pl
from jax.experimental.pallas import tpu as pltpu
from jax.sharding import PartitionSpec as P

TOK = 32
ROWS = 16
HD = 64
HEADS = 128
DOCS = 8
SEQ = 4096
BLK = 256
PAIRS = BLK // 2
NBLK = SEQ // BLK
SRC = BLK // TOK
LONG, MIDDLE, SHORT = 16, 8, 4
FAR = (NBLK - 2) * (NBLK - 1) // 2 + LONG
NT = (((1,), (1,)), ((), ()))
NN = (((1,), (0,)), ((), ()))
BIG = 32768.0
SCALE = 1.4426950408889634 / 8.0
FIRST = -9.210340371976184


def run_of(z, x, c):
    return ((z % 8 * 2 + c) * 4 + x) * 2 + z // 8


FIRST_Z = [11, 8, 5, 4, 1, 3, 9, 0, 12, 2, 13, 7, 15, 10, 6, 14]
THEN_Z = [1, 3, 0, 8, 9, 15, 13, 10, 5, 7, 11, 2, 6, 4, 12, 14]
ORDER_IN = [run_of(z, x, c) for z in FIRST_Z for x in range(4) for c in range(2)]
ORDER_OUT = [run_of(z, x, c) for z in THEN_Z for x in range(4) for c in range(2)]
PLACE_IN = [ORDER_IN.index(s) for s in range(len(ORDER_IN))]
PLACE_OUT = [ORDER_OUT.index(s) for s in range(len(ORDER_OUT))]


def dot(a, b, dims=NN):
    return lax.dot_general(a, b, dims, preferred_element_type=jnp.float32)


def starts_of(token, bound):
    start = jnp.zeros_like(token)
    for d in range(1, DOCS):
        start = jnp.where(token >= bound(d), bound(d), start)
    return start


def identity(n):
    row = lax.broadcasted_iota(jnp.int32, (n, n), 0)
    col = lax.broadcasted_iota(jnp.int32, (n, n), 1)
    return (row == col).astype(jnp.float32).astype(jnp.bfloat16)


def interleave():
    row = lax.broadcasted_iota(jnp.int32, (256, 256), 0)
    col = lax.broadcasted_iota(jnp.int32, (256, 256), 1)
    return (col == (row % 16) * 16 + row // 16).astype(jnp.float32).astype(jnp.bfloat16)


def send_kernel(
    bounds_hbm, q_hbm, k_hbm, v_hbm, qg_hbm, kg_hbm, o_ref, bounds_ref, x_ref, g_ref, rot, turned, sems
):
    arriving = [
        pltpu.make_async_copy(source, target, sems.at[n])
        for n, (source, target) in enumerate(
            (
                (bounds_hbm, bounds_ref),
                (qg_hbm, g_ref.at[0]),
                (kg_hbm, g_ref.at[1]),
                (q_hbm, x_ref.at[0]),
                (v_hbm, x_ref.at[2]),
                (k_hbm, x_ref.at[1]),
            )
        )
    ]
    for c in arriving:
        c.start()
    for c in arriving[:3]:
        c.wait()
    lane = lax.broadcasted_iota(jnp.int32, (HD // 2, 128), 1)
    token = lax.axis_index("run") * TOK + lane
    start = starts_of(token, lambda d: bounds_ref[:, d : d + 1])
    place = (token - start).astype(jnp.float32)
    index = lax.broadcasted_iota(jnp.int32, (HD // 2, 128), 0).astype(jnp.float32)
    angle = place * jnp.exp(jnp.float32(FIRST) * index * 2.0 / HD)
    cosine = jnp.cos(angle)
    sine = jnp.sin(angle)
    eye = identity(HEADS)
    mix = interleave()

    def turn(n, r, rows):
        both = dot(eye, rows, NT).astype(jnp.bfloat16)
        turned[n, r] = both[:, :128]
        turned[n, r + 1] = both[:, 128:]

    def rotate(n):
        gain = jnp.transpose(jnp.broadcast_to(g_ref[n], (HEADS, HD)))
        for r in range(0, ROWS, 2):
            for t in (r, r + ROWS, r + 1, r + 1 + ROWS):
                c = jnp.broadcast_to(cosine[:, t : t + 1], (HD // 2, HEADS))
                s = jnp.broadcast_to(sine[:, t : t + 1], (HD // 2, HEADS))
                x = x_ref[n, t].astype(jnp.float32)
                scale = lax.rsqrt(jnp.mean(x * x, axis=0, keepdims=True) + 1e-06)
                x = x * scale * gain
                a, b = x[: HD // 2], x[HD // 2 :]
                y = jnp.concatenate([a * c - b * s, a * s + b * c], axis=0)
                rot[n, t % ROWS, pl.ds((t // ROWS) * HD, HD), :] = y.astype(jnp.bfloat16)
            turn(n, r, rot[n, r : r + 2].reshape(256, HEADS))

    def spread(n):
        for h in range(0, HEADS, 32):
            part = jnp.concatenate([turned[n, :, h + m : h + m + 16, :].reshape(256, 128) for m in (0, 16)], axis=1)
            both = dot(mix, part).astype(jnp.bfloat16)
            for m in range(2):
                heads = slice(h + 16 * m, h + 16 * m + 16)
                o_ref[heads, 16 * n : 16 * n + 16, :] = both[:, 128 * m : 128 * m + 128].reshape(16, 16, 128)

    for c in arriving[3:]:
        c.wait()

    def turn_values():
        for r in range(0, ROWS, 2):
            turn(2, r, jnp.concatenate([x_ref[2, t] for t in (r, r + ROWS, r + 1, r + 1 + ROWS)], axis=0))

    turn_values()
    rotate(0)
    spread(2)
    rotate(1)
    spread(0)
    spread(1)


def attend_kernel(bounds_ref, x_ref, o_ref, qt, kt, kf, vt, near, far, total, summed, items):

    def offsets(shape, axis):
        n = lax.broadcasted_iota(jnp.int32, shape, axis)
        return ((n % PAIRS) // 16) * 32 + n % 16 + (n // PAIRS) * 16

    below = offsets((BLK, BLK), 0) <= offsets((BLK, BLK), 1)
    q_off = offsets((16, BLK), 1)
    k_off = offsets((BLK, 128), 0)

    def bounds_along(shape, axis):
        n = lax.broadcasted_iota(jnp.int32, shape, axis)
        out = jnp.full(shape, SEQ, jnp.int32)
        for d in range(1, DOCS):
            out = jnp.where(n == d, bounds_ref[:, d : d + 1], out)
        return out

    q_bounds = bounds_along((16, BLK), 0)
    k_bounds = bounds_along((1, 128), 1)

    zero = jnp.zeros((HD, BLK), jnp.bfloat16)
    rest = jnp.zeros((128 - 16, BLK), jnp.bfloat16)

    def wide(x):
        t = jnp.transpose(x.astype(jnp.float32)).astype(jnp.bfloat16)
        return jnp.concatenate([t[:HD], t[HD:]], axis=1)

    def scores(j, q, flags):
        k2 = kt[j]
        low = dot(jnp.concatenate([k2, kf[j, :PAIRS]], axis=1), jnp.concatenate([q, zero, flags, rest], axis=0))
        high = dot(jnp.concatenate([k2, kf[j, PAIRS:]], axis=1), jnp.concatenate([zero, q, flags, rest], axis=0))
        return jnp.exp2(jnp.concatenate([low, high], axis=0) * jnp.float32(SCALE))

    def flags_of(i):
        return jnp.where(BLK * i + q_off >= q_bounds, jnp.float32(-BIG), jnp.float32(0.0)).astype(jnp.bfloat16)

    def partial_sum(e):
        return jnp.sum(e.reshape(BLK // 8, 8, BLK), axis=0)

    def tiles(i, row):
        runs = range(SRC * i, SRC * i + SRC)
        return jnp.concatenate([x_ref[PLACE_IN[s], row : row + 16, :] for s in runs], axis=0)

    def near_scores(blocks):
        for i in blocks:
            q = wide(tiles(i, 0))
            kt[i] = tiles(i, 16)
            qt[i] = q
            vt[i] = wide(tiles(i, 32))
            flags = flags_of(i)
            kf[i] = jnp.where(BLK * i + k_off < k_bounds, jnp.float32(1.0), jnp.float32(0.0)).astype(jnp.bfloat16)
            e1 = jnp.where(below, scores(i, q, flags), jnp.float32(0.0))
            e0 = scores(max(i - 1, 0), q, flags)
            if i == 0:
                e0 = jnp.zeros_like(e0)
            near[i, 0] = e0
            near[i, 1] = e1
            total[i] = partial_sum(e0) + partial_sum(e1)

    scalars = [jnp.max(bounds_ref[:, d : d + 1]) for d in range(DOCS)]
    n_far = jnp.int32(0)
    for i in range(2, NBLK):
        start = starts_of(jnp.int32(BLK * i), lambda d: scalars[d])
        for j in range(i - 2, -1, -1):
            items[n_far] = NBLK * i + j
            n_far += (start < BLK * (j + 1)).astype(jnp.int32)
    near_scores(range(NBLK))
    for u in range(LONG - 1):
        items[n_far + u] = NBLK * NBLK
    trips = (n_far + LONG - MIDDLE - 1) // LONG
    left = n_far - LONG * trips
    passes = (
        (0, trips, LONG),
        (LONG * trips, (left > SHORT).astype(jnp.int32), MIDDLE),
        (LONG * trips, ((left > 0) & (left <= SHORT)).astype(jnp.int32), SHORT),
    )

    def far_blocks(work):
        for begin, trips, length in passes:

            def trip(w, _, begin=begin, length=length):
                for u in range(length):
                    n = begin + length * w + u
                    work(n, items[n] >> 4, items[n] & 15)
                return 0

            lax.fori_loop(0, trips, trip, 0)

    def far_scores(n, i, j):
        e = scores(j, qt[i], flags_of(i))
        far[n] = e
        total[i] += partial_sum(e)

    far_blocks(far_scores)
    for i in range(NBLK):
        inverse = 1.0 / jnp.sum(total[i], axis=0, keepdims=True)
        total[i] = jnp.broadcast_to(inverse, (8, BLK))
        summed[i] = jnp.zeros((HD, BLK), jnp.float32)

    def far_values(n, i, j):
        summed[i] += dot(vt[j], (far[n] * total[i][0:1]).astype(jnp.bfloat16))

    far_blocks(far_values)

    for i in range(NBLK):
        w = jnp.concatenate([(near[i, n] * total[i][0:1]).astype(jnp.bfloat16) for n in range(2)], axis=0)
        out = dot(jnp.concatenate([vt[max(i - 1, 0)], vt[i]], axis=1), w) + summed[i]
        both = jnp.transpose(jnp.concatenate([out[:, :PAIRS], out[:, PAIRS:]], axis=0))
        both = both.astype(jnp.bfloat16)
        for n in range(SRC):
            o_ref[PLACE_OUT[SRC * i + n]] = both[16 * n : 16 * n + 16]


def take_kernel(x_ref, o_hbm, turned, out, sems):
    mix = interleave()
    eye = identity(128)
    for h in range(0, HEADS, 32):
        tiles = [x_ref[PLACE_OUT[s]] for s in ORDER_IN[h : h + 32]]
        part = jnp.concatenate([jnp.concatenate(tiles[m : m + 16], axis=0) for m in (0, 16)], axis=1)
        both = dot(mix, part).astype(jnp.bfloat16)
        for m in range(2):
            turned[:, h + 16 * m : h + 16 * m + 16, :] = both[:, 128 * m : 128 * m + 128].reshape(16, 16, 128)
    copies = []
    for r in range(0, ROWS, 2):
        both = dot(eye, turned[r : r + 2].reshape(256, 128), NT).astype(jnp.bfloat16)
        for m in range(2):
            out[r + m] = both[:HD, 128 * m : 128 * m + 128]
            out[r + m + ROWS] = both[HD:, 128 * m : 128 * m + 128]
        if r % 8 == 6:
            for first in (r - 6, r - 6 + ROWS):
                copy = pltpu.make_async_copy(
                    out.at[pl.ds(first, 8)], o_hbm.at[pl.ds(first, 8)], sems.at[len(copies)]
                )
                copy.start()
                copies.append(copy)
    for copy in copies:
        copy.wait()


VMEM = pl.BlockSpec(memory_space=pltpu.VMEM)
HBM = pl.BlockSpec(memory_space=pltpu.HBM)


def in_hbm(x):
    return pltpu.with_memory_space_constraint(x, pltpu.HBM)


def send_call(doc_bounds, q, k, v, q_gain, k_gain):
    return pl.pallas_call(
        send_kernel,
        out_shape=jax.ShapeDtypeStruct((HEADS, 48, 128), jnp.bfloat16),
        in_specs=[HBM] * 6,
        out_specs=VMEM,
        scratch_shapes=[
            pltpu.VMEM((1, DOCS + 1), jnp.int32),
            pltpu.VMEM((3, TOK, HD, HEADS), jnp.bfloat16),
            pltpu.VMEM((2, 1, HD), jnp.float32),
            pltpu.VMEM((2, ROWS, 128, HEADS), jnp.bfloat16),
            pltpu.VMEM((3, ROWS, HEADS, 128), jnp.bfloat16),
            pltpu.SemaphoreType.DMA((6,)),
        ],
        compiler_params=pltpu.CompilerParams(vmem_limit_bytes=32 << 20),
        name="send_side",
    )(*(in_hbm(x) for x in (doc_bounds, q, k, v, q_gain.reshape(1, HD), k_gain.reshape(1, HD))))


def attend_call(doc_bounds, mine):
    return pl.pallas_call(
        attend_kernel,
        out_shape=jax.ShapeDtypeStruct((SEQ // TOK, ROWS, 128), jnp.bfloat16),
        in_specs=[VMEM, VMEM],
        out_specs=VMEM,
        scratch_shapes=[
            pltpu.VMEM((NBLK + 1, HD, BLK), jnp.bfloat16),
            pltpu.VMEM((NBLK, PAIRS, 128), jnp.bfloat16),
            pltpu.VMEM((NBLK, BLK, 128), jnp.bfloat16),
            pltpu.VMEM((NBLK, HD, BLK), jnp.bfloat16),
            pltpu.VMEM((NBLK, 2, BLK, BLK), jnp.float32),
            pltpu.VMEM((FAR, BLK, BLK), jnp.float32),
            pltpu.VMEM((NBLK + 1, 8, BLK), jnp.float32),
            pltpu.VMEM((NBLK + 1, HD, BLK), jnp.float32),
            pltpu.SMEM((FAR,), jnp.int32),
        ],
        compiler_params=pltpu.CompilerParams(vmem_limit_bytes=44 << 20),
        name="attend",
    )(doc_bounds, mine)


def take_call(back):
    return pl.pallas_call(
        take_kernel,
        out_shape=jax.ShapeDtypeStruct((TOK, HD, HEADS), jnp.bfloat16),
        in_specs=[VMEM],
        out_specs=HBM,
        scratch_shapes=[
            pltpu.VMEM((ROWS, HEADS, 128), jnp.bfloat16),
            pltpu.VMEM((TOK, HD, HEADS), jnp.bfloat16),
            pltpu.SemaphoreType.DMA((4,)),
        ],
        compiler_params=pltpu.CompilerParams(vmem_limit_bytes=32 << 20),
        name="take_side",
    )(back)


def exchange(x, order):
    return lax.all_to_all(x, "run", split_axis=0, concat_axis=0, axis_index_groups=[order], tiled=True)


def body(queries, keys, values, doc_bounds, q_gain, k_gain):
    doc_bounds = doc_bounds.reshape(1, DOCS + 1)
    inputs = [jnp.transpose(x, (0, 2, 1)) for x in (queries, keys, values)]
    packed = send_call(doc_bounds, *inputs, q_gain, k_gain)
    mine = exchange(packed, ORDER_IN)
    result = attend_call(doc_bounds, mine)
    back = exchange(result, ORDER_OUT)
    return jnp.transpose(take_call(back), (0, 2, 1))


def solution(mesh):
    runs = jax.sharding.Mesh(mesh.devices.reshape(len(ORDER_IN), -1), ("run", "dp"))
    tokens = P(("dp", "run"), None, None)
    return jax.shard_map(
        body,
        mesh=runs,
        in_specs=(tokens, tokens, tokens, P("dp"), P(), P()),
        out_specs=tokens,
        check_vma=False,
    )
```

```python
import jax
import jax.numpy as jnp
from jax import lax
from jax.experimental import pallas as pl
from jax.experimental.pallas import tpu as pltpu
from jax.sharding import PartitionSpec as P

TOK = 32
ROWS = 16
HD = 64
HEADS = 128
DOCS = 8
SEQ = 4096
BLK = 256
PAIRS = BLK // 2
NBLK = SEQ // BLK
SRC = BLK // TOK
LONG, MIDDLE, SHORT = 16, 8, 4
FAR = (NBLK - 2) * (NBLK - 1) // 2 + LONG
NT = (((1,), (1,)), ((), ()))
NN = (((1,), (0,)), ((), ()))
BIG = 32768.0
SCALE = 1.4426950408889634 / 8.0
FIRST = -9.210340371976184


def run_of(z, x, c):
    return ((z % 8 * 2 + c) * 4 + x) * 2 + z // 8


FIRST_Z = [8, 7, 9, 6, 10, 5, 11, 4, 12, 3, 13, 2, 14, 1, 15, 0]
THEN_Z = [11, 10, 12, 9, 13, 8, 14, 7, 15, 6, 0, 5, 1, 4, 2, 3]
ORDER_IN = [run_of(z, x, c) for z in FIRST_Z for x in range(4) for c in range(2)]
ORDER_OUT = [run_of(z, x, c) for z in THEN_Z for x in range(4) for c in range(2)]
PLACE_IN = [ORDER_IN.index(s) for s in range(len(ORDER_IN))]
PLACE_OUT = [ORDER_OUT.index(s) for s in range(len(ORDER_OUT))]


def dot(a, b, dims=NN):
    return lax.dot_general(a, b, dims, preferred_element_type=jnp.float32)


def starts_of(token, bound):
    start = jnp.zeros_like(token)
    for d in range(1, DOCS):
        start = jnp.where(token >= bound(d), bound(d), start)
    return start


def identity(n):
    row = lax.broadcasted_iota(jnp.int32, (n, n), 0)
    col = lax.broadcasted_iota(jnp.int32, (n, n), 1)
    return (row == col).astype(jnp.float32).astype(jnp.bfloat16)


def interleave():
    row = lax.broadcasted_iota(jnp.int32, (256, 256), 0)
    col = lax.broadcasted_iota(jnp.int32, (256, 256), 1)
    return (col == (row % 16) * 16 + row // 16).astype(jnp.float32).astype(jnp.bfloat16)


def send_kernel(
    bounds_hbm, q_hbm, k_hbm, v_hbm, qg_hbm, kg_hbm, o_ref, bounds_ref, x_ref, g_ref, rot, turned, sems
):
    arriving = [
        pltpu.make_async_copy(source, target, sems.at[n])
        for n, (source, target) in enumerate(
            (
                (bounds_hbm, bounds_ref),
                (qg_hbm, g_ref.at[0]),
                (kg_hbm, g_ref.at[1]),
                (q_hbm, x_ref.at[0]),
                (v_hbm, x_ref.at[2]),
                (k_hbm, x_ref.at[1]),
            )
        )
    ]
    for c in arriving:
        c.start()
    for c in arriving[:3]:
        c.wait()
    lane = lax.broadcasted_iota(jnp.int32, (HD // 2, 128), 1)
    token = lax.axis_index("run") * TOK + lane
    start = starts_of(token, lambda d: bounds_ref[:, d : d + 1])
    place = (token - start).astype(jnp.float32)
    index = lax.broadcasted_iota(jnp.int32, (HD // 2, 128), 0).astype(jnp.float32)
    angle = place * jnp.exp(jnp.float32(FIRST) * index * 2.0 / HD)
    cosine = jnp.cos(angle)
    sine = jnp.sin(angle)
    eye = identity(HEADS)
    mix = interleave()

    def turn(n, r, rows):
        both = dot(eye, rows, NT).astype(jnp.bfloat16)
        turned[n, r] = both[:, :128]
        turned[n, r + 1] = both[:, 128:]

    def rotate(n):
        gain = jnp.transpose(jnp.broadcast_to(g_ref[n], (HEADS, HD)))
        for r in range(0, ROWS, 2):
            for t in (r, r + ROWS, r + 1, r + 1 + ROWS):
                c = jnp.broadcast_to(cosine[:, t : t + 1], (HD // 2, HEADS))
                s = jnp.broadcast_to(sine[:, t : t + 1], (HD // 2, HEADS))
                x = x_ref[n, t].astype(jnp.float32)
                scale = lax.rsqrt(jnp.mean(x * x, axis=0, keepdims=True) + 1e-06)
                x = x * scale * gain
                a, b = x[: HD // 2], x[HD // 2 :]
                y = jnp.concatenate([a * c - b * s, a * s + b * c], axis=0)
                rot[n, t % ROWS, pl.ds((t // ROWS) * HD, HD), :] = y.astype(jnp.bfloat16)
            turn(n, r, rot[n, r : r + 2].reshape(256, HEADS))

    def spread(n):
        for h in range(0, HEADS, 32):
            part = jnp.concatenate([turned[n, :, h + m : h + m + 16, :].reshape(256, 128) for m in (0, 16)], axis=1)
            both = dot(mix, part).astype(jnp.bfloat16)
            for m in range(2):
                heads = slice(h + 16 * m, h + 16 * m + 16)
                o_ref[heads, 16 * n : 16 * n + 16, :] = both[:, 128 * m : 128 * m + 128].reshape(16, 16, 128)

    for c in arriving[3:]:
        c.wait()

    def turn_values():
        for r in range(0, ROWS, 2):
            turn(2, r, jnp.concatenate([x_ref[2, t] for t in (r, r + ROWS, r + 1, r + 1 + ROWS)], axis=0))

    turn_values()
    rotate(0)
    spread(2)
    rotate(1)
    spread(0)
    spread(1)


def attend_kernel(bounds_ref, x_ref, o_ref, qt, kt, kf, vt, near, far, total, summed, items):

    def offsets(shape, axis):
        n = lax.broadcasted_iota(jnp.int32, shape, axis)
        return ((n % PAIRS) // 16) * 32 + n % 16 + (n // PAIRS) * 16

    below = offsets((BLK, BLK), 0) <= offsets((BLK, BLK), 1)
    q_off = offsets((16, BLK), 1)
    k_off = offsets((BLK, 128), 0)

    def bounds_along(shape, axis):
        n = lax.broadcasted_iota(jnp.int32, shape, axis)
        out = jnp.full(shape, SEQ, jnp.int32)
        for d in range(1, DOCS):
            out = jnp.where(n == d, bounds_ref[:, d : d + 1], out)
        return out

    q_bounds = bounds_along((16, BLK), 0)
    k_bounds = bounds_along((1, 128), 1)

    zero = jnp.zeros((HD, BLK), jnp.bfloat16)
    rest = jnp.zeros((128 - 16, BLK), jnp.bfloat16)

    def wide(x):
        t = jnp.transpose(x.astype(jnp.float32)).astype(jnp.bfloat16)
        return jnp.concatenate([t[:HD], t[HD:]], axis=1)

    def scores(j, q, flags):
        k2 = kt[j]
        low = dot(jnp.concatenate([k2, kf[j, :PAIRS]], axis=1), jnp.concatenate([q, zero, flags, rest], axis=0))
        high = dot(jnp.concatenate([k2, kf[j, PAIRS:]], axis=1), jnp.concatenate([zero, q, flags, rest], axis=0))
        return jnp.exp2(jnp.concatenate([low, high], axis=0) * jnp.float32(SCALE))

    def flags_of(i):
        return jnp.where(BLK * i + q_off >= q_bounds, jnp.float32(-BIG), jnp.float32(0.0)).astype(jnp.bfloat16)

    def partial_sum(e):
        return jnp.sum(e.reshape(BLK // 8, 8, BLK), axis=0)

    def tiles(i, row):
        runs = range(SRC * i, SRC * i + SRC)
        return jnp.concatenate([x_ref[PLACE_IN[s], row : row + 16, :] for s in runs], axis=0)

    def near_scores(blocks):
        for i in blocks:
            q = wide(tiles(i, 0))
            kt[i] = tiles(i, 16)
            qt[i] = q
            vt[i] = wide(tiles(i, 32))
            flags = flags_of(i)
            kf[i] = jnp.where(BLK * i + k_off < k_bounds, jnp.float32(1.0), jnp.float32(0.0)).astype(jnp.bfloat16)
            e1 = jnp.where(below, scores(i, q, flags), jnp.float32(0.0))
            e0 = scores(max(i - 1, 0), q, flags)
            if i == 0:
                e0 = jnp.zeros_like(e0)
            near[i, 0] = e0
            near[i, 1] = e1
            total[i] = partial_sum(e0) + partial_sum(e1)

    scalars = [jnp.max(bounds_ref[:, d : d + 1]) for d in range(DOCS)]
    n_far = jnp.int32(0)
    for i in range(2, NBLK):
        start = starts_of(jnp.int32(BLK * i), lambda d: scalars[d])
        for j in range(i - 2, -1, -1):
            items[n_far] = NBLK * i + j
            n_far += (start < BLK * (j + 1)).astype(jnp.int32)
    near_scores(range(NBLK))
    for u in range(LONG - 1):
        items[n_far + u] = NBLK * NBLK
    trips = (n_far + LONG - MIDDLE - 1) // LONG
    left = n_far - LONG * trips
    passes = (
        (0, trips, LONG),
        (LONG * trips, (left > SHORT).astype(jnp.int32), MIDDLE),
        (LONG * trips, ((left > 0) & (left <= SHORT)).astype(jnp.int32), SHORT),
    )

    def far_blocks(work):
        for begin, trips, length in passes:

            def trip(w, _, begin=begin, length=length):
                for u in range(length):
                    n = begin + length * w + u
                    work(n, items[n] >> 4, items[n] & 15)
                return 0

            lax.fori_loop(0, trips, trip, 0)

    def far_scores(n, i, j):
        e = scores(j, qt[i], flags_of(i))
        far[n] = e
        total[i] += partial_sum(e)

    far_blocks(far_scores)
    for i in range(NBLK):
        inverse = 1.0 / jnp.sum(total[i], axis=0, keepdims=True)
        total[i] = jnp.broadcast_to(inverse, (8, BLK))
        summed[i] = jnp.zeros((HD, BLK), jnp.float32)

    def far_values(n, i, j):
        summed[i] += dot(vt[j], (far[n] * total[i][0:1]).astype(jnp.bfloat16))

    far_blocks(far_values)

    for i in range(NBLK):
        w = jnp.concatenate([(near[i, n] * total[i][0:1]).astype(jnp.bfloat16) for n in range(2)], axis=0)
        out = dot(jnp.concatenate([vt[max(i - 1, 0)], vt[i]], axis=1), w) + summed[i]
        both = jnp.transpose(jnp.concatenate([out[:, :PAIRS], out[:, PAIRS:]], axis=0))
        both = both.astype(jnp.bfloat16)
        for n in range(SRC):
            o_ref[PLACE_OUT[SRC * i + n]] = both[16 * n : 16 * n + 16]


def take_kernel(x_ref, o_hbm, turned, out, sems):
    mix = interleave()
    eye = identity(128)
    for h in range(0, HEADS, 32):
        tiles = [x_ref[PLACE_OUT[s]] for s in ORDER_IN[h : h + 32]]
        part = jnp.concatenate([jnp.concatenate(tiles[m : m + 16], axis=0) for m in (0, 16)], axis=1)
        both = dot(mix, part).astype(jnp.bfloat16)
        for m in range(2):
            turned[:, h + 16 * m : h + 16 * m + 16, :] = both[:, 128 * m : 128 * m + 128].reshape(16, 16, 128)
    copies = []
    for r in range(0, ROWS, 2):
        both = dot(eye, turned[r : r + 2].reshape(256, 128), NT).astype(jnp.bfloat16)
        for m in range(2):
            out[r + m] = both[:HD, 128 * m : 128 * m + 128]
            out[r + m + ROWS] = both[HD:, 128 * m : 128 * m + 128]
        if r % 8 == 6:
            for first in (r - 6, r - 6 + ROWS):
                copy = pltpu.make_async_copy(
                    out.at[pl.ds(first, 8)], o_hbm.at[pl.ds(first, 8)], sems.at[len(copies)]
                )
                copy.start()
                copies.append(copy)
    for copy in copies:
        copy.wait()


VMEM = pl.BlockSpec(memory_space=pltpu.VMEM)
HBM = pl.BlockSpec(memory_space=pltpu.HBM)


def in_hbm(x):
    return pltpu.with_memory_space_constraint(x, pltpu.HBM)


def send_call(doc_bounds, q, k, v, q_gain, k_gain):
    return pl.pallas_call(
        send_kernel,
        out_shape=jax.ShapeDtypeStruct((HEADS, 48, 128), jnp.bfloat16),
        in_specs=[HBM] * 6,
        out_specs=VMEM,
        scratch_shapes=[
            pltpu.VMEM((1, DOCS + 1), jnp.int32),
            pltpu.VMEM((3, TOK, HD, HEADS), jnp.bfloat16),
            pltpu.VMEM((2, 1, HD), jnp.float32),
            pltpu.VMEM((2, ROWS, 128, HEADS), jnp.bfloat16),
            pltpu.VMEM((3, ROWS, HEADS, 128), jnp.bfloat16),
            pltpu.SemaphoreType.DMA((6,)),
        ],
        compiler_params=pltpu.CompilerParams(vmem_limit_bytes=32 << 20),
        name="send_side",
    )(*(in_hbm(x) for x in (doc_bounds, q, k, v, q_gain.reshape(1, HD), k_gain.reshape(1, HD))))


def attend_call(doc_bounds, mine):
    return pl.pallas_call(
        attend_kernel,
        out_shape=jax.ShapeDtypeStruct((SEQ // TOK, ROWS, 128), jnp.bfloat16),
        in_specs=[VMEM, VMEM],
        out_specs=VMEM,
        scratch_shapes=[
            pltpu.VMEM((NBLK + 1, HD, BLK), jnp.bfloat16),
            pltpu.VMEM((NBLK, PAIRS, 128), jnp.bfloat16),
            pltpu.VMEM((NBLK, BLK, 128), jnp.bfloat16),
            pltpu.VMEM((NBLK, HD, BLK), jnp.bfloat16),
            pltpu.VMEM((NBLK, 2, BLK, BLK), jnp.float32),
            pltpu.VMEM((FAR, BLK, BLK), jnp.float32),
            pltpu.VMEM((NBLK + 1, 8, BLK), jnp.float32),
            pltpu.VMEM((NBLK + 1, HD, BLK), jnp.float32),
            pltpu.SMEM((FAR,), jnp.int32),
        ],
        compiler_params=pltpu.CompilerParams(vmem_limit_bytes=44 << 20),
        name="attend",
    )(doc_bounds, mine)


def take_call(back):
    return pl.pallas_call(
        take_kernel,
        out_shape=jax.ShapeDtypeStruct((TOK, HD, HEADS), jnp.bfloat16),
        in_specs=[VMEM],
        out_specs=HBM,
        scratch_shapes=[
            pltpu.VMEM((ROWS, HEADS, 128), jnp.bfloat16),
            pltpu.VMEM((TOK, HD, HEADS), jnp.bfloat16),
            pltpu.SemaphoreType.DMA((4,)),
        ],
        compiler_params=pltpu.CompilerParams(vmem_limit_bytes=32 << 20),
        name="take_side",
    )(back)


def exchange(x, order):
    return lax.all_to_all(x, "run", split_axis=0, concat_axis=0, axis_index_groups=[order], tiled=True)


def body(queries, keys, values, doc_bounds, q_gain, k_gain):
    doc_bounds = doc_bounds.reshape(1, DOCS + 1)
    inputs = [jnp.transpose(x, (0, 2, 1)) for x in (queries, keys, values)]
    packed = send_call(doc_bounds, *inputs, q_gain, k_gain)
    mine = exchange(packed, ORDER_IN)
    result = attend_call(doc_bounds, mine)
    back = exchange(result, ORDER_OUT)
    return jnp.transpose(take_call(back), (0, 2, 1))


def solution(mesh):
    runs = jax.sharding.Mesh(mesh.devices.reshape(len(ORDER_IN), -1), ("run", "dp"))
    tokens = P(("dp", "run"), None, None)
    return jax.shard_map(
        body,
        mesh=runs,
        in_specs=(tokens, tokens, tokens, P("dp"), P(), P()),
        out_specs=tokens,
        check_vma=False,
    )
```

```python
import jax
import jax.numpy as jnp
from jax import lax
from jax.experimental import pallas as pl
from jax.experimental.pallas import tpu as pltpu
from jax.sharding import PartitionSpec as P

TOK = 32
ROWS = 16
HD = 64
HEADS = 128
DOCS = 8
SEQ = 4096
BLK = 256
PAIRS = BLK // 2
NBLK = SEQ // BLK
SRC = BLK // TOK
LONG, MIDDLE, SHORT = 16, 8, 4
FAR = (NBLK - 2) * (NBLK - 1) // 2 + LONG
NT = (((1,), (1,)), ((), ()))
NN = (((1,), (0,)), ((), ()))
BIG = 32768.0
SCALE = 1.4426950408889634 / 8.0
FIRST = -9.210340371976184


def run_of(z, x, c):
    return ((z % 8 * 2 + c) * 4 + x) * 2 + z // 8


FIRST_Z = [10, 9, 11, 8, 12, 7, 13, 6, 14, 5, 15, 4, 0, 3, 1, 2]
THEN_Z = [6, 5, 7, 4, 8, 3, 9, 2, 10, 1, 11, 0, 12, 15, 13, 14]
ORDER_IN = [run_of(z, x, c) for z in FIRST_Z for x in range(4) for c in range(2)]
ORDER_OUT = [run_of(z, x, c) for z in THEN_Z for x in range(4) for c in range(2)]
PLACE_IN = [ORDER_IN.index(s) for s in range(len(ORDER_IN))]
PLACE_OUT = [ORDER_OUT.index(s) for s in range(len(ORDER_OUT))]


def dot(a, b, dims=NN):
    return lax.dot_general(a, b, dims, preferred_element_type=jnp.float32)


def starts_of(token, bound):
    start = jnp.zeros_like(token)
    for d in range(1, DOCS):
        start = jnp.where(token >= bound(d), bound(d), start)
    return start


def identity(n):
    row = lax.broadcasted_iota(jnp.int32, (n, n), 0)
    col = lax.broadcasted_iota(jnp.int32, (n, n), 1)
    return (row == col).astype(jnp.float32).astype(jnp.bfloat16)


def interleave():
    row = lax.broadcasted_iota(jnp.int32, (256, 256), 0)
    col = lax.broadcasted_iota(jnp.int32, (256, 256), 1)
    return (col == (row % 16) * 16 + row // 16).astype(jnp.float32).astype(jnp.bfloat16)


def send_kernel(
    bounds_hbm, q_hbm, k_hbm, v_hbm, qg_hbm, kg_hbm, o_ref, bounds_ref, x_ref, g_ref, rot, turned, sems
):
    arriving = [
        pltpu.make_async_copy(source, target, sems.at[n])
        for n, (source, target) in enumerate(
            (
                (bounds_hbm, bounds_ref),
                (qg_hbm, g_ref.at[0]),
                (kg_hbm, g_ref.at[1]),
                (q_hbm, x_ref.at[0]),
                (v_hbm, x_ref.at[2]),
                (k_hbm, x_ref.at[1]),
            )
        )
    ]
    for c in arriving:
        c.start()
    for c in arriving[:3]:
        c.wait()
    lane = lax.broadcasted_iota(jnp.int32, (HD // 2, 128), 1)
    token = lax.axis_index("run") * TOK + lane
    start = starts_of(token, lambda d: bounds_ref[:, d : d + 1])
    place = (token - start).astype(jnp.float32)
    index = lax.broadcasted_iota(jnp.int32, (HD // 2, 128), 0).astype(jnp.float32)
    angle = place * jnp.exp(jnp.float32(FIRST) * index * 2.0 / HD)
    cosine = jnp.cos(angle)
    sine = jnp.sin(angle)
    eye = identity(HEADS)
    mix = interleave()

    def turn(n, r, rows):
        both = dot(eye, rows, NT).astype(jnp.bfloat16)
        turned[n, r] = both[:, :128]
        turned[n, r + 1] = both[:, 128:]

    def rotate(n):
        gain = jnp.transpose(jnp.broadcast_to(g_ref[n], (HEADS, HD)))
        for r in range(0, ROWS, 2):
            for t in (r, r + ROWS, r + 1, r + 1 + ROWS):
                c = jnp.broadcast_to(cosine[:, t : t + 1], (HD // 2, HEADS))
                s = jnp.broadcast_to(sine[:, t : t + 1], (HD // 2, HEADS))
                x = x_ref[n, t].astype(jnp.float32)
                scale = lax.rsqrt(jnp.mean(x * x, axis=0, keepdims=True) + 1e-06)
                x = x * scale * gain
                a, b = x[: HD // 2], x[HD // 2 :]
                y = jnp.concatenate([a * c - b * s, a * s + b * c], axis=0)
                rot[n, t % ROWS, pl.ds((t // ROWS) * HD, HD), :] = y.astype(jnp.bfloat16)
            turn(n, r, rot[n, r : r + 2].reshape(256, HEADS))

    def spread(n):
        for h in range(0, HEADS, 32):
            part = jnp.concatenate([turned[n, :, h + m : h + m + 16, :].reshape(256, 128) for m in (0, 16)], axis=1)
            both = dot(mix, part).astype(jnp.bfloat16)
            for m in range(2):
                heads = slice(h + 16 * m, h + 16 * m + 16)
                o_ref[heads, 16 * n : 16 * n + 16, :] = both[:, 128 * m : 128 * m + 128].reshape(16, 16, 128)

    for c in arriving[3:]:
        c.wait()

    def turn_values():
        for r in range(0, ROWS, 2):
            turn(2, r, jnp.concatenate([x_ref[2, t] for t in (r, r + ROWS, r + 1, r + 1 + ROWS)], axis=0))

    turn_values()
    rotate(0)
    spread(2)
    rotate(1)
    spread(0)
    spread(1)


def attend_kernel(bounds_ref, x_ref, o_ref, qt, kt, kf, vt, near, far, total, summed, items):

    def offsets(shape, axis):
        n = lax.broadcasted_iota(jnp.int32, shape, axis)
        return ((n % PAIRS) // 16) * 32 + n % 16 + (n // PAIRS) * 16

    below = offsets((BLK, BLK), 0) <= offsets((BLK, BLK), 1)
    q_off = offsets((16, BLK), 1)
    k_off = offsets((BLK, 128), 0)

    def bounds_along(shape, axis):
        n = lax.broadcasted_iota(jnp.int32, shape, axis)
        out = jnp.full(shape, SEQ, jnp.int32)
        for d in range(1, DOCS):
            out = jnp.where(n == d, bounds_ref[:, d : d + 1], out)
        return out

    q_bounds = bounds_along((16, BLK), 0)
    k_bounds = bounds_along((1, 128), 1)

    zero = jnp.zeros((HD, BLK), jnp.bfloat16)
    rest = jnp.zeros((128 - 16, BLK), jnp.bfloat16)

    def wide(x):
        t = jnp.transpose(x.astype(jnp.float32)).astype(jnp.bfloat16)
        return jnp.concatenate([t[:HD], t[HD:]], axis=1)

    def scores(j, q, flags):
        k2 = kt[j]
        low = dot(jnp.concatenate([k2, kf[j, :PAIRS]], axis=1), jnp.concatenate([q, zero, flags, rest], axis=0))
        high = dot(jnp.concatenate([k2, kf[j, PAIRS:]], axis=1), jnp.concatenate([zero, q, flags, rest], axis=0))
        return jnp.exp2(jnp.concatenate([low, high], axis=0) * jnp.float32(SCALE))

    def flags_of(i):
        return jnp.where(BLK * i + q_off >= q_bounds, jnp.float32(-BIG), jnp.float32(0.0)).astype(jnp.bfloat16)

    def partial_sum(e):
        return jnp.sum(e.reshape(BLK // 8, 8, BLK), axis=0)

    def tiles(i, row):
        runs = range(SRC * i, SRC * i + SRC)
        return jnp.concatenate([x_ref[PLACE_IN[s], row : row + 16, :] for s in runs], axis=0)

    def near_scores(blocks):
        for i in blocks:
            q = wide(tiles(i, 0))
            kt[i] = tiles(i, 16)
            qt[i] = q
            vt[i] = wide(tiles(i, 32))
            flags = flags_of(i)
            kf[i] = jnp.where(BLK * i + k_off < k_bounds, jnp.float32(1.0), jnp.float32(0.0)).astype(jnp.bfloat16)
            e1 = jnp.where(below, scores(i, q, flags), jnp.float32(0.0))
            e0 = scores(max(i - 1, 0), q, flags)
            if i == 0:
                e0 = jnp.zeros_like(e0)
            near[i, 0] = e0
            near[i, 1] = e1
            total[i] = partial_sum(e0) + partial_sum(e1)

    scalars = [jnp.max(bounds_ref[:, d : d + 1]) for d in range(DOCS)]
    n_far = jnp.int32(0)
    for i in range(2, NBLK):
        start = starts_of(jnp.int32(BLK * i), lambda d: scalars[d])
        for j in range(i - 2, -1, -1):
            items[n_far] = NBLK * i + j
            n_far += (start < BLK * (j + 1)).astype(jnp.int32)
    near_scores(range(NBLK))
    for u in range(LONG - 1):
        items[n_far + u] = NBLK * NBLK
    trips = (n_far + LONG - MIDDLE - 1) // LONG
    left = n_far - LONG * trips
    passes = (
        (0, trips, LONG),
        (LONG * trips, (left > SHORT).astype(jnp.int32), MIDDLE),
        (LONG * trips, ((left > 0) & (left <= SHORT)).astype(jnp.int32), SHORT),
    )

    def far_blocks(work):
        for begin, trips, length in passes:

            def trip(w, _, begin=begin, length=length):
                for u in range(length):
                    n = begin + length * w + u
                    work(n, items[n] >> 4, items[n] & 15)
                return 0

            lax.fori_loop(0, trips, trip, 0)

    def far_scores(n, i, j):
        e = scores(j, qt[i], flags_of(i))
        far[n] = e
        total[i] += partial_sum(e)

    far_blocks(far_scores)
    for i in range(NBLK):
        inverse = 1.0 / jnp.sum(total[i], axis=0, keepdims=True)
        total[i] = jnp.broadcast_to(inverse, (8, BLK))
        summed[i] = jnp.zeros((HD, BLK), jnp.float32)

    def far_values(n, i, j):
        summed[i] += dot(vt[j], (far[n] * total[i][0:1]).astype(jnp.bfloat16))

    far_blocks(far_values)

    for i in range(NBLK):
        w = jnp.concatenate([(near[i, n] * total[i][0:1]).astype(jnp.bfloat16) for n in range(2)], axis=0)
        out = dot(jnp.concatenate([vt[max(i - 1, 0)], vt[i]], axis=1), w) + summed[i]
        both = jnp.transpose(jnp.concatenate([out[:, :PAIRS], out[:, PAIRS:]], axis=0))
        both = both.astype(jnp.bfloat16)
        for n in range(SRC):
            o_ref[PLACE_OUT[SRC * i + n]] = both[16 * n : 16 * n + 16]


def take_kernel(x_ref, o_hbm, turned, out, sems):
    mix = interleave()
    eye = identity(128)
    for h in range(0, HEADS, 32):
        tiles = [x_ref[PLACE_OUT[s]] for s in ORDER_IN[h : h + 32]]
        part = jnp.concatenate([jnp.concatenate(tiles[m : m + 16], axis=0) for m in (0, 16)], axis=1)
        both = dot(mix, part).astype(jnp.bfloat16)
        for m in range(2):
            turned[:, h + 16 * m : h + 16 * m + 16, :] = both[:, 128 * m : 128 * m + 128].reshape(16, 16, 128)
    copies = []
    for r in range(0, ROWS, 2):
        both = dot(eye, turned[r : r + 2].reshape(256, 128), NT).astype(jnp.bfloat16)
        for m in range(2):
            out[r + m] = both[:HD, 128 * m : 128 * m + 128]
            out[r + m + ROWS] = both[HD:, 128 * m : 128 * m + 128]
        if r % 8 == 6:
            for first in (r - 6, r - 6 + ROWS):
                copy = pltpu.make_async_copy(
                    out.at[pl.ds(first, 8)], o_hbm.at[pl.ds(first, 8)], sems.at[len(copies)]
                )
                copy.start()
                copies.append(copy)
    for copy in copies:
        copy.wait()


VMEM = pl.BlockSpec(memory_space=pltpu.VMEM)
HBM = pl.BlockSpec(memory_space=pltpu.HBM)


def in_hbm(x):
    return pltpu.with_memory_space_constraint(x, pltpu.HBM)


def send_call(doc_bounds, q, k, v, q_gain, k_gain):
    return pl.pallas_call(
        send_kernel,
        out_shape=jax.ShapeDtypeStruct((HEADS, 48, 128), jnp.bfloat16),
        in_specs=[HBM] * 6,
        out_specs=VMEM,
        scratch_shapes=[
            pltpu.VMEM((1, DOCS + 1), jnp.int32),
            pltpu.VMEM((3, TOK, HD, HEADS), jnp.bfloat16),
            pltpu.VMEM((2, 1, HD), jnp.float32),
            pltpu.VMEM((2, ROWS, 128, HEADS), jnp.bfloat16),
            pltpu.VMEM((3, ROWS, HEADS, 128), jnp.bfloat16),
            pltpu.SemaphoreType.DMA((6,)),
        ],
        compiler_params=pltpu.CompilerParams(vmem_limit_bytes=32 << 20),
        name="send_side",
    )(*(in_hbm(x) for x in (doc_bounds, q, k, v, q_gain.reshape(1, HD), k_gain.reshape(1, HD))))


def attend_call(doc_bounds, mine):
    return pl.pallas_call(
        attend_kernel,
        out_shape=jax.ShapeDtypeStruct((SEQ // TOK, ROWS, 128), jnp.bfloat16),
        in_specs=[VMEM, VMEM],
        out_specs=VMEM,
        scratch_shapes=[
            pltpu.VMEM((NBLK + 1, HD, BLK), jnp.bfloat16),
            pltpu.VMEM((NBLK, PAIRS, 128), jnp.bfloat16),
            pltpu.VMEM((NBLK, BLK, 128), jnp.bfloat16),
            pltpu.VMEM((NBLK, HD, BLK), jnp.bfloat16),
            pltpu.VMEM((NBLK, 2, BLK, BLK), jnp.float32),
            pltpu.VMEM((FAR, BLK, BLK), jnp.float32),
            pltpu.VMEM((NBLK + 1, 8, BLK), jnp.float32),
            pltpu.VMEM((NBLK + 1, HD, BLK), jnp.float32),
            pltpu.SMEM((FAR,), jnp.int32),
        ],
        compiler_params=pltpu.CompilerParams(vmem_limit_bytes=44 << 20),
        name="attend",
    )(doc_bounds, mine)


def take_call(back):
    return pl.pallas_call(
        take_kernel,
        out_shape=jax.ShapeDtypeStruct((TOK, HD, HEADS), jnp.bfloat16),
        in_specs=[VMEM],
        out_specs=HBM,
        scratch_shapes=[
            pltpu.VMEM((ROWS, HEADS, 128), jnp.bfloat16),
            pltpu.VMEM((TOK, HD, HEADS), jnp.bfloat16),
            pltpu.SemaphoreType.DMA((4,)),
        ],
        compiler_params=pltpu.CompilerParams(vmem_limit_bytes=32 << 20),
        name="take_side",
    )(back)


def exchange(x, order):
    return lax.all_to_all(x, "run", split_axis=0, concat_axis=0, axis_index_groups=[order], tiled=True)


def body(queries, keys, values, doc_bounds, q_gain, k_gain):
    doc_bounds = doc_bounds.reshape(1, DOCS + 1)
    inputs = [jnp.transpose(x, (0, 2, 1)) for x in (queries, keys, values)]
    packed = send_call(doc_bounds, *inputs, q_gain, k_gain)
    mine = exchange(packed, ORDER_IN)
    result = attend_call(doc_bounds, mine)
    back = exchange(result, ORDER_OUT)
    return jnp.transpose(take_call(back), (0, 2, 1))


def solution(mesh):
    runs = jax.sharding.Mesh(mesh.devices.reshape(len(ORDER_IN), -1), ("run", "dp"))
    tokens = P(("dp", "run"), None, None)
    return jax.shard_map(
        body,
        mesh=runs,
        in_specs=(tokens, tokens, tokens, P("dp"), P(), P()),
        out_specs=tokens,
        check_vma=False,
    )
```

```python
import jax
import jax.numpy as jnp
from jax import lax
from jax.experimental import pallas as pl
from jax.experimental.pallas import tpu as pltpu
from jax.sharding import PartitionSpec as P

TOK = 32
ROWS = 16
HD = 64
HEADS = 128
DOCS = 8
SEQ = 4096
BLK = 256
PAIRS = BLK // 2
NBLK = SEQ // BLK
SRC = BLK // TOK
LONG, MIDDLE, SHORT = 16, 8, 4
FAR = (NBLK - 2) * (NBLK - 1) // 2 + LONG
NT = (((1,), (1,)), ((), ()))
NN = (((1,), (0,)), ((), ()))
BIG = 32768.0
SCALE = 1.4426950408889634 / 8.0
FIRST = -9.210340371976184


def run_of(z, x, c):
    return ((z % 8 * 2 + c) * 4 + x) * 2 + z // 8


FIRST_Z = [8, 7, 9, 6, 10, 5, 11, 4, 12, 3, 13, 2, 14, 1, 15, 0]
THEN_Z = [8, 15, 6, 13, 4, 11, 2, 9, 0, 7, 14, 5, 12, 3, 10, 1]
ORDER_IN = [run_of(z, x, c) for z in FIRST_Z for x in range(4) for c in range(2)]
ORDER_OUT = [run_of(z, x, c) for z in THEN_Z for x in range(4) for c in range(2)]
PLACE_IN = [ORDER_IN.index(s) for s in range(len(ORDER_IN))]
PLACE_OUT = [ORDER_OUT.index(s) for s in range(len(ORDER_OUT))]


def dot(a, b, dims=NN):
    return lax.dot_general(a, b, dims, preferred_element_type=jnp.float32)


def starts_of(token, bound):
    start = jnp.zeros_like(token)
    for d in range(1, DOCS):
        start = jnp.where(token >= bound(d), bound(d), start)
    return start


def identity(n):
    row = lax.broadcasted_iota(jnp.int32, (n, n), 0)
    col = lax.broadcasted_iota(jnp.int32, (n, n), 1)
    return (row == col).astype(jnp.float32).astype(jnp.bfloat16)


def interleave():
    row = lax.broadcasted_iota(jnp.int32, (256, 256), 0)
    col = lax.broadcasted_iota(jnp.int32, (256, 256), 1)
    return (col == (row % 16) * 16 + row // 16).astype(jnp.float32).astype(jnp.bfloat16)


def send_kernel(
    bounds_hbm, q_hbm, k_hbm, v_hbm, qg_hbm, kg_hbm, o_ref, bounds_ref, x_ref, g_ref, rot, turned, sems
):
    arriving = [
        pltpu.make_async_copy(source, target, sems.at[n])
        for n, (source, target) in enumerate(
            (
                (bounds_hbm, bounds_ref),
                (qg_hbm, g_ref.at[0]),
                (kg_hbm, g_ref.at[1]),
                (q_hbm, x_ref.at[0]),
                (v_hbm, x_ref.at[2]),
                (k_hbm, x_ref.at[1]),
            )
        )
    ]
    for c in arriving:
        c.start()
    for c in arriving[:3]:
        c.wait()
    lane = lax.broadcasted_iota(jnp.int32, (HD // 2, 128), 1)
    token = lax.axis_index("run") * TOK + lane
    start = starts_of(token, lambda d: bounds_ref[:, d : d + 1])
    place = (token - start).astype(jnp.float32)
    index = lax.broadcasted_iota(jnp.int32, (HD // 2, 128), 0).astype(jnp.float32)
    angle = place * jnp.exp(jnp.float32(FIRST) * index * 2.0 / HD)
    cosine = jnp.cos(angle)
    sine = jnp.sin(angle)
    eye = identity(HEADS)
    mix = interleave()

    def turn(n, r, rows):
        both = dot(eye, rows, NT).astype(jnp.bfloat16)
        turned[n, r] = both[:, :128]
        turned[n, r + 1] = both[:, 128:]

    def rotate(n):
        gain = jnp.transpose(jnp.broadcast_to(g_ref[n], (HEADS, HD)))
        for r in range(0, ROWS, 2):
            for t in (r, r + ROWS, r + 1, r + 1 + ROWS):
                c = jnp.broadcast_to(cosine[:, t : t + 1], (HD // 2, HEADS))
                s = jnp.broadcast_to(sine[:, t : t + 1], (HD // 2, HEADS))
                x = x_ref[n, t].astype(jnp.float32)
                scale = lax.rsqrt(jnp.mean(x * x, axis=0, keepdims=True) + 1e-06)
                x = x * scale * gain
                a, b = x[: HD // 2], x[HD // 2 :]
                y = jnp.concatenate([a * c - b * s, a * s + b * c], axis=0)
                rot[n, t % ROWS, pl.ds((t // ROWS) * HD, HD), :] = y.astype(jnp.bfloat16)
            turn(n, r, rot[n, r : r + 2].reshape(256, HEADS))

    def spread(n):
        for h in range(0, HEADS, 32):
            part = jnp.concatenate([turned[n, :, h + m : h + m + 16, :].reshape(256, 128) for m in (0, 16)], axis=1)
            both = dot(mix, part).astype(jnp.bfloat16)
            for m in range(2):
                heads = slice(h + 16 * m, h + 16 * m + 16)
                o_ref[heads, 16 * n : 16 * n + 16, :] = both[:, 128 * m : 128 * m + 128].reshape(16, 16, 128)

    for c in arriving[3:]:
        c.wait()

    def turn_values():
        for r in range(0, ROWS, 2):
            turn(2, r, jnp.concatenate([x_ref[2, t] for t in (r, r + ROWS, r + 1, r + 1 + ROWS)], axis=0))

    turn_values()
    rotate(0)
    spread(2)
    rotate(1)
    spread(0)
    spread(1)


def attend_kernel(bounds_ref, x_ref, o_ref, qt, kt, kf, vt, near, far, total, summed, items):

    def offsets(shape, axis):
        n = lax.broadcasted_iota(jnp.int32, shape, axis)
        return ((n % PAIRS) // 16) * 32 + n % 16 + (n // PAIRS) * 16

    below = offsets((BLK, BLK), 0) <= offsets((BLK, BLK), 1)
    q_off = offsets((16, BLK), 1)
    k_off = offsets((BLK, 128), 0)

    def bounds_along(shape, axis):
        n = lax.broadcasted_iota(jnp.int32, shape, axis)
        out = jnp.full(shape, SEQ, jnp.int32)
        for d in range(1, DOCS):
            out = jnp.where(n == d, bounds_ref[:, d : d + 1], out)
        return out

    q_bounds = bounds_along((16, BLK), 0)
    k_bounds = bounds_along((1, 128), 1)

    zero = jnp.zeros((HD, BLK), jnp.bfloat16)
    rest = jnp.zeros((128 - 16, BLK), jnp.bfloat16)

    def wide(x):
        t = jnp.transpose(x.astype(jnp.float32)).astype(jnp.bfloat16)
        return jnp.concatenate([t[:HD], t[HD:]], axis=1)

    def scores(j, q, flags):
        k2 = kt[j]
        low = dot(jnp.concatenate([k2, kf[j, :PAIRS]], axis=1), jnp.concatenate([q, zero, flags, rest], axis=0))
        high = dot(jnp.concatenate([k2, kf[j, PAIRS:]], axis=1), jnp.concatenate([zero, q, flags, rest], axis=0))
        return jnp.exp2(jnp.concatenate([low, high], axis=0) * jnp.float32(SCALE))

    def flags_of(i):
        return jnp.where(BLK * i + q_off >= q_bounds, jnp.float32(-BIG), jnp.float32(0.0)).astype(jnp.bfloat16)

    def partial_sum(e):
        return jnp.sum(e.reshape(BLK // 8, 8, BLK), axis=0)

    def tiles(i, row):
        runs = range(SRC * i, SRC * i + SRC)
        return jnp.concatenate([x_ref[PLACE_IN[s], row : row + 16, :] for s in runs], axis=0)

    def near_scores(blocks):
        for i in blocks:
            q = wide(tiles(i, 0))
            kt[i] = tiles(i, 16)
            qt[i] = q
            vt[i] = wide(tiles(i, 32))
            flags = flags_of(i)
            kf[i] = jnp.where(BLK * i + k_off < k_bounds, jnp.float32(1.0), jnp.float32(0.0)).astype(jnp.bfloat16)
            e1 = jnp.where(below, scores(i, q, flags), jnp.float32(0.0))
            e0 = scores(max(i - 1, 0), q, flags)
            if i == 0:
                e0 = jnp.zeros_like(e0)
            near[i, 0] = e0
            near[i, 1] = e1
            total[i] = partial_sum(e0) + partial_sum(e1)

    scalars = [jnp.max(bounds_ref[:, d : d + 1]) for d in range(DOCS)]
    n_far = jnp.int32(0)
    for i in range(2, NBLK):
        start = starts_of(jnp.int32(BLK * i), lambda d: scalars[d])
        for j in range(i - 2, -1, -1):
            items[n_far] = NBLK * i + j
            n_far += (start < BLK * (j + 1)).astype(jnp.int32)
    near_scores(range(NBLK))
    for u in range(LONG - 1):
        items[n_far + u] = NBLK * NBLK
    trips = (n_far + LONG - MIDDLE - 1) // LONG
    left = n_far - LONG * trips
    passes = (
        (0, trips, LONG),
        (LONG * trips, (left > SHORT).astype(jnp.int32), MIDDLE),
        (LONG * trips, ((left > 0) & (left <= SHORT)).astype(jnp.int32), SHORT),
    )

    def far_blocks(work):
        for begin, trips, length in passes:

            def trip(w, _, begin=begin, length=length):
                for u in range(length):
                    n = begin + length * w + u
                    work(n, items[n] >> 4, items[n] & 15)
                return 0

            lax.fori_loop(0, trips, trip, 0)

    def far_scores(n, i, j):
        e = scores(j, qt[i], flags_of(i))
        far[n] = e
        total[i] += partial_sum(e)

    far_blocks(far_scores)
    for i in range(NBLK):
        inverse = 1.0 / jnp.sum(total[i], axis=0, keepdims=True)
        total[i] = jnp.broadcast_to(inverse, (8, BLK))
        summed[i] = jnp.zeros((HD, BLK), jnp.float32)

    def far_values(n, i, j):
        summed[i] += dot(vt[j], (far[n] * total[i][0:1]).astype(jnp.bfloat16))

    far_blocks(far_values)

    for i in range(NBLK):
        w = jnp.concatenate([(near[i, n] * total[i][0:1]).astype(jnp.bfloat16) for n in range(2)], axis=0)
        out = dot(jnp.concatenate([vt[max(i - 1, 0)], vt[i]], axis=1), w) + summed[i]
        both = jnp.transpose(jnp.concatenate([out[:, :PAIRS], out[:, PAIRS:]], axis=0))
        both = both.astype(jnp.bfloat16)
        for n in range(SRC):
            o_ref[PLACE_OUT[SRC * i + n]] = both[16 * n : 16 * n + 16]


def take_kernel(x_ref, o_hbm, turned, out, sems):
    mix = interleave()
    eye = identity(128)
    for h in range(0, HEADS, 32):
        tiles = [x_ref[PLACE_OUT[s]] for s in ORDER_IN[h : h + 32]]
        part = jnp.concatenate([jnp.concatenate(tiles[m : m + 16], axis=0) for m in (0, 16)], axis=1)
        both = dot(mix, part).astype(jnp.bfloat16)
        for m in range(2):
            turned[:, h + 16 * m : h + 16 * m + 16, :] = both[:, 128 * m : 128 * m + 128].reshape(16, 16, 128)
    copies = []
    for r in range(0, ROWS, 2):
        both = dot(eye, turned[r : r + 2].reshape(256, 128), NT).astype(jnp.bfloat16)
        for m in range(2):
            out[r + m] = both[:HD, 128 * m : 128 * m + 128]
            out[r + m + ROWS] = both[HD:, 128 * m : 128 * m + 128]
        if r % 8 == 6:
            for first in (r - 6, r - 6 + ROWS):
                copy = pltpu.make_async_copy(
                    out.at[pl.ds(first, 8)], o_hbm.at[pl.ds(first, 8)], sems.at[len(copies)]
                )
                copy.start()
                copies.append(copy)
    for copy in copies:
        copy.wait()


VMEM = pl.BlockSpec(memory_space=pltpu.VMEM)
HBM = pl.BlockSpec(memory_space=pltpu.HBM)


def in_hbm(x):
    return pltpu.with_memory_space_constraint(x, pltpu.HBM)


def send_call(doc_bounds, q, k, v, q_gain, k_gain):
    return pl.pallas_call(
        send_kernel,
        out_shape=jax.ShapeDtypeStruct((HEADS, 48, 128), jnp.bfloat16),
        in_specs=[HBM] * 6,
        out_specs=VMEM,
        scratch_shapes=[
            pltpu.VMEM((1, DOCS + 1), jnp.int32),
            pltpu.VMEM((3, TOK, HD, HEADS), jnp.bfloat16),
            pltpu.VMEM((2, 1, HD), jnp.float32),
            pltpu.VMEM((2, ROWS, 128, HEADS), jnp.bfloat16),
            pltpu.VMEM((3, ROWS, HEADS, 128), jnp.bfloat16),
            pltpu.SemaphoreType.DMA((6,)),
        ],
        compiler_params=pltpu.CompilerParams(vmem_limit_bytes=32 << 20),
        name="send_side",
    )(*(in_hbm(x) for x in (doc_bounds, q, k, v, q_gain.reshape(1, HD), k_gain.reshape(1, HD))))


def attend_call(doc_bounds, mine):
    return pl.pallas_call(
        attend_kernel,
        out_shape=jax.ShapeDtypeStruct((SEQ // TOK, ROWS, 128), jnp.bfloat16),
        in_specs=[VMEM, VMEM],
        out_specs=VMEM,
        scratch_shapes=[
            pltpu.VMEM((NBLK + 1, HD, BLK), jnp.bfloat16),
            pltpu.VMEM((NBLK, PAIRS, 128), jnp.bfloat16),
            pltpu.VMEM((NBLK, BLK, 128), jnp.bfloat16),
            pltpu.VMEM((NBLK, HD, BLK), jnp.bfloat16),
            pltpu.VMEM((NBLK, 2, BLK, BLK), jnp.float32),
            pltpu.VMEM((FAR, BLK, BLK), jnp.float32),
            pltpu.VMEM((NBLK + 1, 8, BLK), jnp.float32),
            pltpu.VMEM((NBLK + 1, HD, BLK), jnp.float32),
            pltpu.SMEM((FAR,), jnp.int32),
        ],
        compiler_params=pltpu.CompilerParams(vmem_limit_bytes=44 << 20),
        name="attend",
    )(doc_bounds, mine)


def take_call(back):
    return pl.pallas_call(
        take_kernel,
        out_shape=jax.ShapeDtypeStruct((TOK, HD, HEADS), jnp.bfloat16),
        in_specs=[VMEM],
        out_specs=HBM,
        scratch_shapes=[
            pltpu.VMEM((ROWS, HEADS, 128), jnp.bfloat16),
            pltpu.VMEM((TOK, HD, HEADS), jnp.bfloat16),
            pltpu.SemaphoreType.DMA((4,)),
        ],
        compiler_params=pltpu.CompilerParams(vmem_limit_bytes=32 << 20),
        name="take_side",
    )(back)


def exchange(x, order):
    return lax.all_to_all(x, "run", split_axis=0, concat_axis=0, axis_index_groups=[order], tiled=True)


def body(queries, keys, values, doc_bounds, q_gain, k_gain):
    doc_bounds = doc_bounds.reshape(1, DOCS + 1)
    inputs = [jnp.transpose(x, (0, 2, 1)) for x in (queries, keys, values)]
    packed = send_call(doc_bounds, *inputs, q_gain, k_gain)
    mine = exchange(packed, ORDER_IN)
    result = attend_call(doc_bounds, mine)
    back = exchange(result, ORDER_OUT)
    return jnp.transpose(take_call(back), (0, 2, 1))


def solution(mesh):
    runs = jax.sharding.Mesh(mesh.devices.reshape(len(ORDER_IN), -1), ("run", "dp"))
    tokens = P(("dp", "run"), None, None)
    return jax.shard_map(
        body,
        mesh=runs,
        in_specs=(tokens, tokens, tokens, P("dp"), P(), P()),
        out_specs=tokens,
        check_vma=False,
    )
```

```python
import jax
import jax.numpy as jnp
from jax import lax
from jax.experimental import pallas as pl
from jax.experimental.pallas import tpu as pltpu
from jax.sharding import PartitionSpec as P

TOK = 32
ROWS = 16
HD = 64
HEADS = 128
DOCS = 8
SEQ = 4096
BLK = 256
PAIRS = BLK // 2
NBLK = SEQ // BLK
SRC = BLK // TOK
LONG, MIDDLE, SHORT = 16, 8, 4
FAR = (NBLK - 2) * (NBLK - 1) // 2 + LONG
NT = (((1,), (1,)), ((), ()))
NN = (((1,), (0,)), ((), ()))
BIG = 32768.0
SCALE = 1.4426950408889634 / 8.0
FIRST = -9.210340371976184


def run_of(z, x, c):
    return ((z % 8 * 2 + c) * 4 + x) * 2 + z // 8


FIRST_Z = [8, 7, 9, 6, 10, 5, 11, 4, 12, 3, 13, 2, 14, 1, 15, 0]
THEN_Z = [8, 15, 6, 13, 4, 11, 2, 9, 0, 7, 14, 5, 12, 3, 10, 1]
ORDER_IN = [run_of(z, x, c) for z in FIRST_Z for x in range(4) for c in (1, 0)]
ORDER_OUT = [run_of(z, x, c) for z in THEN_Z for x in range(4) for c in (1, 0)]
PLACE_IN = [ORDER_IN.index(s) for s in range(len(ORDER_IN))]
PLACE_OUT = [ORDER_OUT.index(s) for s in range(len(ORDER_OUT))]


def dot(a, b, dims=NN):
    return lax.dot_general(a, b, dims, preferred_element_type=jnp.float32)


def starts_of(token, bound):
    start = jnp.zeros_like(token)
    for d in range(1, DOCS):
        start = jnp.where(token >= bound(d), bound(d), start)
    return start


def identity(n):
    row = lax.broadcasted_iota(jnp.int32, (n, n), 0)
    col = lax.broadcasted_iota(jnp.int32, (n, n), 1)
    return (row == col).astype(jnp.float32).astype(jnp.bfloat16)


def interleave():
    row = lax.broadcasted_iota(jnp.int32, (256, 256), 0)
    col = lax.broadcasted_iota(jnp.int32, (256, 256), 1)
    return (col == (row % 16) * 16 + row // 16).astype(jnp.float32).astype(jnp.bfloat16)


def send_kernel(
    bounds_hbm, q_hbm, k_hbm, v_hbm, qg_hbm, kg_hbm, o_ref, bounds_ref, x_ref, g_ref, rot, turned, sems
):
    arriving = [
        pltpu.make_async_copy(source, target, sems.at[n])
        for n, (source, target) in enumerate(
            (
                (bounds_hbm, bounds_ref),
                (qg_hbm, g_ref.at[0]),
                (kg_hbm, g_ref.at[1]),
                (q_hbm, x_ref.at[0]),
                (v_hbm, x_ref.at[2]),
                (k_hbm, x_ref.at[1]),
            )
        )
    ]
    for c in arriving:
        c.start()
    for c in arriving[:3]:
        c.wait()
    lane = lax.broadcasted_iota(jnp.int32, (HD // 2, 128), 1)
    token = lax.axis_index("run") * TOK + lane
    start = starts_of(token, lambda d: bounds_ref[:, d : d + 1])
    place = (token - start).astype(jnp.float32)
    index = lax.broadcasted_iota(jnp.int32, (HD // 2, 128), 0).astype(jnp.float32)
    angle = place * jnp.exp(jnp.float32(FIRST) * index * 2.0 / HD)
    cosine = jnp.cos(angle)
    sine = jnp.sin(angle)
    eye = identity(HEADS)
    mix = interleave()

    def turn(n, r, rows):
        both = dot(eye, rows, NT).astype(jnp.bfloat16)
        turned[n, r] = both[:, :128]
        turned[n, r + 1] = both[:, 128:]

    def rotate(n):
        gain = jnp.transpose(jnp.broadcast_to(g_ref[n], (HEADS, HD)))
        for r in range(0, ROWS, 2):
            for t in (r, r + ROWS, r + 1, r + 1 + ROWS):
                c = jnp.broadcast_to(cosine[:, t : t + 1], (HD // 2, HEADS))
                s = jnp.broadcast_to(sine[:, t : t + 1], (HD // 2, HEADS))
                x = x_ref[n, t].astype(jnp.float32)
                scale = lax.rsqrt(jnp.mean(x * x, axis=0, keepdims=True) + 1e-06)
                x = x * scale * gain
                a, b = x[: HD // 2], x[HD // 2 :]
                y = jnp.concatenate([a * c - b * s, a * s + b * c], axis=0)
                rot[n, t % ROWS, pl.ds((t // ROWS) * HD, HD), :] = y.astype(jnp.bfloat16)
            turn(n, r, rot[n, r : r + 2].reshape(256, HEADS))

    def spread(n):
        for h in range(0, HEADS, 32):
            part = jnp.concatenate([turned[n, :, h + m : h + m + 16, :].reshape(256, 128) for m in (0, 16)], axis=1)
            both = dot(mix, part).astype(jnp.bfloat16)
            for m in range(2):
                heads = slice(h + 16 * m, h + 16 * m + 16)
                o_ref[heads, 16 * n : 16 * n + 16, :] = both[:, 128 * m : 128 * m + 128].reshape(16, 16, 128)

    for c in arriving[3:]:
        c.wait()

    def turn_values():
        for r in range(0, ROWS, 2):
            turn(2, r, jnp.concatenate([x_ref[2, t] for t in (r, r + ROWS, r + 1, r + 1 + ROWS)], axis=0))

    turn_values()
    rotate(0)
    spread(2)
    rotate(1)
    spread(0)
    spread(1)


def attend_kernel(bounds_ref, x_ref, o_ref, qt, kt, kf, vt, near, far, total, summed, items):

    def offsets(shape, axis):
        n = lax.broadcasted_iota(jnp.int32, shape, axis)
        return ((n % PAIRS) // 16) * 32 + n % 16 + (n // PAIRS) * 16

    below = offsets((BLK, BLK), 0) <= offsets((BLK, BLK), 1)
    q_off = offsets((16, BLK), 1)
    k_off = offsets((BLK, 128), 0)

    def bounds_along(shape, axis):
        n = lax.broadcasted_iota(jnp.int32, shape, axis)
        out = jnp.full(shape, SEQ, jnp.int32)
        for d in range(1, DOCS):
            out = jnp.where(n == d, bounds_ref[:, d : d + 1], out)
        return out

    q_bounds = bounds_along((16, BLK), 0)
    k_bounds = bounds_along((1, 128), 1)

    zero = jnp.zeros((HD, BLK), jnp.bfloat16)
    rest = jnp.zeros((128 - 16, BLK), jnp.bfloat16)

    def wide(x):
        t = jnp.transpose(x.astype(jnp.float32)).astype(jnp.bfloat16)
        return jnp.concatenate([t[:HD], t[HD:]], axis=1)

    def scores(j, q, flags):
        k2 = kt[j]
        low = dot(jnp.concatenate([k2, kf[j, :PAIRS]], axis=1), jnp.concatenate([q, zero, flags, rest], axis=0))
        high = dot(jnp.concatenate([k2, kf[j, PAIRS:]], axis=1), jnp.concatenate([zero, q, flags, rest], axis=0))
        return jnp.exp2(jnp.concatenate([low, high], axis=0) * jnp.float32(SCALE))

    def flags_of(i):
        return jnp.where(BLK * i + q_off >= q_bounds, jnp.float32(-BIG), jnp.float32(0.0)).astype(jnp.bfloat16)

    def partial_sum(e):
        return jnp.sum(e.reshape(BLK // 8, 8, BLK), axis=0)

    def tiles(i, row):
        runs = range(SRC * i, SRC * i + SRC)
        return jnp.concatenate([x_ref[PLACE_IN[s], row : row + 16, :] for s in runs], axis=0)

    def near_scores(blocks):
        for i in blocks:
            q = wide(tiles(i, 0))
            kt[i] = tiles(i, 16)
            qt[i] = q
            vt[i] = wide(tiles(i, 32))
            flags = flags_of(i)
            kf[i] = jnp.where(BLK * i + k_off < k_bounds, jnp.float32(1.0), jnp.float32(0.0)).astype(jnp.bfloat16)
            e1 = jnp.where(below, scores(i, q, flags), jnp.float32(0.0))
            e0 = scores(max(i - 1, 0), q, flags)
            if i == 0:
                e0 = jnp.zeros_like(e0)
            near[i, 0] = e0
            near[i, 1] = e1
            total[i] = partial_sum(e0) + partial_sum(e1)

    scalars = [jnp.max(bounds_ref[:, d : d + 1]) for d in range(DOCS)]
    n_far = jnp.int32(0)
    for i in range(2, NBLK):
        start = starts_of(jnp.int32(BLK * i), lambda d: scalars[d])
        for j in range(i - 2, -1, -1):
            items[n_far] = NBLK * i + j
            n_far += (start < BLK * (j + 1)).astype(jnp.int32)
    near_scores(range(NBLK))
    for u in range(LONG - 1):
        items[n_far + u] = NBLK * NBLK
    trips = (n_far + LONG - MIDDLE - 1) // LONG
    left = n_far - LONG * trips
    passes = (
        (0, trips, LONG),
        (LONG * trips, (left > SHORT).astype(jnp.int32), MIDDLE),
        (LONG * trips, ((left > 0) & (left <= SHORT)).astype(jnp.int32), SHORT),
    )

    def far_blocks(work):
        for begin, trips, length in passes:

            def trip(w, _, begin=begin, length=length):
                for u in range(length):
                    n = begin + length * w + u
                    work(n, items[n] >> 4, items[n] & 15)
                return 0

            lax.fori_loop(0, trips, trip, 0)

    def far_scores(n, i, j):
        e = scores(j, qt[i], flags_of(i))
        far[n] = e
        total[i] += partial_sum(e)

    far_blocks(far_scores)
    for i in range(NBLK):
        inverse = 1.0 / jnp.sum(total[i], axis=0, keepdims=True)
        total[i] = jnp.broadcast_to(inverse, (8, BLK))
        summed[i] = jnp.zeros((HD, BLK), jnp.float32)

    def far_values(n, i, j):
        summed[i] += dot(vt[j], (far[n] * total[i][0:1]).astype(jnp.bfloat16))

    far_blocks(far_values)

    for i in range(NBLK):
        w = jnp.concatenate([(near[i, n] * total[i][0:1]).astype(jnp.bfloat16) for n in range(2)], axis=0)
        out = dot(jnp.concatenate([vt[max(i - 1, 0)], vt[i]], axis=1), w) + summed[i]
        both = jnp.transpose(jnp.concatenate([out[:, :PAIRS], out[:, PAIRS:]], axis=0))
        both = both.astype(jnp.bfloat16)
        for n in range(SRC):
            o_ref[PLACE_OUT[SRC * i + n]] = both[16 * n : 16 * n + 16]


def take_kernel(x_ref, o_hbm, turned, out, sems):
    mix = interleave()
    eye = identity(128)
    for h in range(0, HEADS, 32):
        tiles = [x_ref[PLACE_OUT[s]] for s in ORDER_IN[h : h + 32]]
        part = jnp.concatenate([jnp.concatenate(tiles[m : m + 16], axis=0) for m in (0, 16)], axis=1)
        both = dot(mix, part).astype(jnp.bfloat16)
        for m in range(2):
            turned[:, h + 16 * m : h + 16 * m + 16, :] = both[:, 128 * m : 128 * m + 128].reshape(16, 16, 128)
    copies = []
    for r in range(0, ROWS, 2):
        both = dot(eye, turned[r : r + 2].reshape(256, 128), NT).astype(jnp.bfloat16)
        for m in range(2):
            out[r + m] = both[:HD, 128 * m : 128 * m + 128]
            out[r + m + ROWS] = both[HD:, 128 * m : 128 * m + 128]
        if r % 8 == 6:
            for first in (r - 6, r - 6 + ROWS):
                copy = pltpu.make_async_copy(
                    out.at[pl.ds(first, 8)], o_hbm.at[pl.ds(first, 8)], sems.at[len(copies)]
                )
                copy.start()
                copies.append(copy)
    for copy in copies:
        copy.wait()


VMEM = pl.BlockSpec(memory_space=pltpu.VMEM)
HBM = pl.BlockSpec(memory_space=pltpu.HBM)


def in_hbm(x):
    return pltpu.with_memory_space_constraint(x, pltpu.HBM)


def send_call(doc_bounds, q, k, v, q_gain, k_gain):
    return pl.pallas_call(
        send_kernel,
        out_shape=jax.ShapeDtypeStruct((HEADS, 48, 128), jnp.bfloat16),
        in_specs=[HBM] * 6,
        out_specs=VMEM,
        scratch_shapes=[
            pltpu.VMEM((1, DOCS + 1), jnp.int32),
            pltpu.VMEM((3, TOK, HD, HEADS), jnp.bfloat16),
            pltpu.VMEM((2, 1, HD), jnp.float32),
            pltpu.VMEM((2, ROWS, 128, HEADS), jnp.bfloat16),
            pltpu.VMEM((3, ROWS, HEADS, 128), jnp.bfloat16),
            pltpu.SemaphoreType.DMA((6,)),
        ],
        compiler_params=pltpu.CompilerParams(vmem_limit_bytes=32 << 20),
        name="send_side",
    )(*(in_hbm(x) for x in (doc_bounds, q, k, v, q_gain.reshape(1, HD), k_gain.reshape(1, HD))))


def attend_call(doc_bounds, mine):
    return pl.pallas_call(
        attend_kernel,
        out_shape=jax.ShapeDtypeStruct((SEQ // TOK, ROWS, 128), jnp.bfloat16),
        in_specs=[VMEM, VMEM],
        out_specs=VMEM,
        scratch_shapes=[
            pltpu.VMEM((NBLK + 1, HD, BLK), jnp.bfloat16),
            pltpu.VMEM((NBLK, PAIRS, 128), jnp.bfloat16),
            pltpu.VMEM((NBLK, BLK, 128), jnp.bfloat16),
            pltpu.VMEM((NBLK, HD, BLK), jnp.bfloat16),
            pltpu.VMEM((NBLK, 2, BLK, BLK), jnp.float32),
            pltpu.VMEM((FAR, BLK, BLK), jnp.float32),
            pltpu.VMEM((NBLK + 1, 8, BLK), jnp.float32),
            pltpu.VMEM((NBLK + 1, HD, BLK), jnp.float32),
            pltpu.SMEM((FAR,), jnp.int32),
        ],
        compiler_params=pltpu.CompilerParams(vmem_limit_bytes=44 << 20),
        name="attend",
    )(doc_bounds, mine)


def take_call(back):
    return pl.pallas_call(
        take_kernel,
        out_shape=jax.ShapeDtypeStruct((TOK, HD, HEADS), jnp.bfloat16),
        in_specs=[VMEM],
        out_specs=HBM,
        scratch_shapes=[
            pltpu.VMEM((ROWS, HEADS, 128), jnp.bfloat16),
            pltpu.VMEM((TOK, HD, HEADS), jnp.bfloat16),
            pltpu.SemaphoreType.DMA((4,)),
        ],
        compiler_params=pltpu.CompilerParams(vmem_limit_bytes=32 << 20),
        name="take_side",
    )(back)


def exchange(x, order):
    return lax.all_to_all(x, "run", split_axis=0, concat_axis=0, axis_index_groups=[order], tiled=True)


def body(queries, keys, values, doc_bounds, q_gain, k_gain):
    doc_bounds = doc_bounds.reshape(1, DOCS + 1)
    inputs = [jnp.transpose(x, (0, 2, 1)) for x in (queries, keys, values)]
    packed = send_call(doc_bounds, *inputs, q_gain, k_gain)
    mine = exchange(packed, ORDER_IN)
    result = attend_call(doc_bounds, mine)
    back = exchange(result, ORDER_OUT)
    return jnp.transpose(take_call(back), (0, 2, 1))


def solution(mesh):
    runs = jax.sharding.Mesh(mesh.devices.reshape(len(ORDER_IN), -1), ("run", "dp"))
    tokens = P(("dp", "run"), None, None)
    return jax.shard_map(
        body,
        mesh=runs,
        in_specs=(tokens, tokens, tokens, P("dp"), P(), P()),
        out_specs=tokens,
        check_vma=False,
    )
```

```python
import jax
import jax.numpy as jnp
from jax import lax
from jax.experimental import pallas as pl
from jax.experimental.pallas import tpu as pltpu
from jax.sharding import PartitionSpec as P

TOK = 32
ROWS = 16
HD = 64
HEADS = 128
DOCS = 8
SEQ = 4096
BLK = 256
PAIRS = BLK // 2
NBLK = SEQ // BLK
SRC = BLK // TOK
LONG, MIDDLE, SHORT = 16, 8, 4
FAR = (NBLK - 2) * (NBLK - 1) // 2 + LONG
NT = (((1,), (1,)), ((), ()))
NN = (((1,), (0,)), ((), ()))
BIG = 32768.0
SCALE = 1.4426950408889634 / 8.0
FIRST = -9.210340371976184


def run_of(z, x, c):
    return ((z % 8 * 2 + c) * 4 + x) * 2 + z // 8


FIRST_Z = [8, 7, 9, 6, 10, 5, 11, 4, 12, 3, 13, 2, 14, 1, 15, 0]
THEN_Z = [8, 15, 6, 13, 4, 11, 2, 9, 0, 7, 14, 5, 12, 3, 10, 1]
ORDER_IN = [run_of(z, x, c) for z in FIRST_Z for x in (2, 1, 3, 0) for c in range(2)]
ORDER_OUT = [run_of(z, x, c) for z in THEN_Z for x in (2, 1, 3, 0) for c in range(2)]
PLACE_IN = [ORDER_IN.index(s) for s in range(len(ORDER_IN))]
PLACE_OUT = [ORDER_OUT.index(s) for s in range(len(ORDER_OUT))]


def dot(a, b, dims=NN):
    return lax.dot_general(a, b, dims, preferred_element_type=jnp.float32)


def starts_of(token, bound):
    start = jnp.zeros_like(token)
    for d in range(1, DOCS):
        start = jnp.where(token >= bound(d), bound(d), start)
    return start


def identity(n):
    row = lax.broadcasted_iota(jnp.int32, (n, n), 0)
    col = lax.broadcasted_iota(jnp.int32, (n, n), 1)
    return (row == col).astype(jnp.float32).astype(jnp.bfloat16)


def interleave():
    row = lax.broadcasted_iota(jnp.int32, (256, 256), 0)
    col = lax.broadcasted_iota(jnp.int32, (256, 256), 1)
    return (col == (row % 16) * 16 + row // 16).astype(jnp.float32).astype(jnp.bfloat16)


def send_kernel(
    bounds_hbm, q_hbm, k_hbm, v_hbm, qg_hbm, kg_hbm, o_ref, bounds_ref, x_ref, g_ref, rot, turned, sems
):
    arriving = [
        pltpu.make_async_copy(source, target, sems.at[n])
        for n, (source, target) in enumerate(
            (
                (bounds_hbm, bounds_ref),
                (qg_hbm, g_ref.at[0]),
                (kg_hbm, g_ref.at[1]),
                (q_hbm, x_ref.at[0]),
                (v_hbm, x_ref.at[2]),
                (k_hbm, x_ref.at[1]),
            )
        )
    ]
    for c in arriving:
        c.start()
    for c in arriving[:3]:
        c.wait()
    lane = lax.broadcasted_iota(jnp.int32, (HD // 2, 128), 1)
    token = lax.axis_index("run") * TOK + lane
    start = starts_of(token, lambda d: bounds_ref[:, d : d + 1])
    place = (token - start).astype(jnp.float32)
    index = lax.broadcasted_iota(jnp.int32, (HD // 2, 128), 0).astype(jnp.float32)
    angle = place * jnp.exp(jnp.float32(FIRST) * index * 2.0 / HD)
    cosine = jnp.cos(angle)
    sine = jnp.sin(angle)
    eye = identity(HEADS)
    mix = interleave()

    def turn(n, r, rows):
        both = dot(eye, rows, NT).astype(jnp.bfloat16)
        turned[n, r] = both[:, :128]
        turned[n, r + 1] = both[:, 128:]

    def rotate(n):
        gain = jnp.transpose(jnp.broadcast_to(g_ref[n], (HEADS, HD)))
        for r in range(0, ROWS, 2):
            for t in (r, r + ROWS, r + 1, r + 1 + ROWS):
                c = jnp.broadcast_to(cosine[:, t : t + 1], (HD // 2, HEADS))
                s = jnp.broadcast_to(sine[:, t : t + 1], (HD // 2, HEADS))
                x = x_ref[n, t].astype(jnp.float32)
                scale = lax.rsqrt(jnp.mean(x * x, axis=0, keepdims=True) + 1e-06)
                x = x * scale * gain
                a, b = x[: HD // 2], x[HD // 2 :]
                y = jnp.concatenate([a * c - b * s, a * s + b * c], axis=0)
                rot[n, t % ROWS, pl.ds((t // ROWS) * HD, HD), :] = y.astype(jnp.bfloat16)
            turn(n, r, rot[n, r : r + 2].reshape(256, HEADS))

    def spread(n):
        for h in range(0, HEADS, 32):
            part = jnp.concatenate([turned[n, :, h + m : h + m + 16, :].reshape(256, 128) for m in (0, 16)], axis=1)
            both = dot(mix, part).astype(jnp.bfloat16)
            for m in range(2):
                heads = slice(h + 16 * m, h + 16 * m + 16)
                o_ref[heads, 16 * n : 16 * n + 16, :] = both[:, 128 * m : 128 * m + 128].reshape(16, 16, 128)

    for c in arriving[3:]:
        c.wait()

    def turn_values():
        for r in range(0, ROWS, 2):
            turn(2, r, jnp.concatenate([x_ref[2, t] for t in (r, r + ROWS, r + 1, r + 1 + ROWS)], axis=0))

    turn_values()
    rotate(0)
    spread(2)
    rotate(1)
    spread(0)
    spread(1)


def attend_kernel(bounds_ref, x_ref, o_ref, qt, kt, kf, vt, near, far, total, summed, items):

    def offsets(shape, axis):
        n = lax.broadcasted_iota(jnp.int32, shape, axis)
        return ((n % PAIRS) // 16) * 32 + n % 16 + (n // PAIRS) * 16

    below = offsets((BLK, BLK), 0) <= offsets((BLK, BLK), 1)
    q_off = offsets((16, BLK), 1)
    k_off = offsets((BLK, 128), 0)

    def bounds_along(shape, axis):
        n = lax.broadcasted_iota(jnp.int32, shape, axis)
        out = jnp.full(shape, SEQ, jnp.int32)
        for d in range(1, DOCS):
            out = jnp.where(n == d, bounds_ref[:, d : d + 1], out)
        return out

    q_bounds = bounds_along((16, BLK), 0)
    k_bounds = bounds_along((1, 128), 1)

    zero = jnp.zeros((HD, BLK), jnp.bfloat16)
    rest = jnp.zeros((128 - 16, BLK), jnp.bfloat16)

    def wide(x):
        t = jnp.transpose(x.astype(jnp.float32)).astype(jnp.bfloat16)
        return jnp.concatenate([t[:HD], t[HD:]], axis=1)

    def scores(j, q, flags):
        k2 = kt[j]
        low = dot(jnp.concatenate([k2, kf[j, :PAIRS]], axis=1), jnp.concatenate([q, zero, flags, rest], axis=0))
        high = dot(jnp.concatenate([k2, kf[j, PAIRS:]], axis=1), jnp.concatenate([zero, q, flags, rest], axis=0))
        return jnp.exp2(jnp.concatenate([low, high], axis=0) * jnp.float32(SCALE))

    def flags_of(i):
        return jnp.where(BLK * i + q_off >= q_bounds, jnp.float32(-BIG), jnp.float32(0.0)).astype(jnp.bfloat16)

    def partial_sum(e):
        return jnp.sum(e.reshape(BLK // 8, 8, BLK), axis=0)

    def tiles(i, row):
        runs = range(SRC * i, SRC * i + SRC)
        return jnp.concatenate([x_ref[PLACE_IN[s], row : row + 16, :] for s in runs], axis=0)

    def near_scores(blocks):
        for i in blocks:
            q = wide(tiles(i, 0))
            kt[i] = tiles(i, 16)
            qt[i] = q
            vt[i] = wide(tiles(i, 32))
            flags = flags_of(i)
            kf[i] = jnp.where(BLK * i + k_off < k_bounds, jnp.float32(1.0), jnp.float32(0.0)).astype(jnp.bfloat16)
            e1 = jnp.where(below, scores(i, q, flags), jnp.float32(0.0))
            e0 = scores(max(i - 1, 0), q, flags)
            if i == 0:
                e0 = jnp.zeros_like(e0)
            near[i, 0] = e0
            near[i, 1] = e1
            total[i] = partial_sum(e0) + partial_sum(e1)

    scalars = [jnp.max(bounds_ref[:, d : d + 1]) for d in range(DOCS)]
    n_far = jnp.int32(0)
    for i in range(2, NBLK):
        start = starts_of(jnp.int32(BLK * i), lambda d: scalars[d])
        for j in range(i - 2, -1, -1):
            items[n_far] = NBLK * i + j
            n_far += (start < BLK * (j + 1)).astype(jnp.int32)
    near_scores(range(NBLK))
    for u in range(LONG - 1):
        items[n_far + u] = NBLK * NBLK
    trips = (n_far + LONG - MIDDLE - 1) // LONG
    left = n_far - LONG * trips
    passes = (
        (0, trips, LONG),
        (LONG * trips, (left > SHORT).astype(jnp.int32), MIDDLE),
        (LONG * trips, ((left > 0) & (left <= SHORT)).astype(jnp.int32), SHORT),
    )

    def far_blocks(work):
        for begin, trips, length in passes:

            def trip(w, _, begin=begin, length=length):
                for u in range(length):
                    n = begin + length * w + u
                    work(n, items[n] >> 4, items[n] & 15)
                return 0

            lax.fori_loop(0, trips, trip, 0)

    def far_scores(n, i, j):
        e = scores(j, qt[i], flags_of(i))
        far[n] = e
        total[i] += partial_sum(e)

    far_blocks(far_scores)
    for i in range(NBLK):
        inverse = 1.0 / jnp.sum(total[i], axis=0, keepdims=True)
        total[i] = jnp.broadcast_to(inverse, (8, BLK))
        summed[i] = jnp.zeros((HD, BLK), jnp.float32)

    def far_values(n, i, j):
        summed[i] += dot(vt[j], (far[n] * total[i][0:1]).astype(jnp.bfloat16))

    far_blocks(far_values)

    for i in range(NBLK):
        w = jnp.concatenate([(near[i, n] * total[i][0:1]).astype(jnp.bfloat16) for n in range(2)], axis=0)
        out = dot(jnp.concatenate([vt[max(i - 1, 0)], vt[i]], axis=1), w) + summed[i]
        both = jnp.transpose(jnp.concatenate([out[:, :PAIRS], out[:, PAIRS:]], axis=0))
        both = both.astype(jnp.bfloat16)
        for n in range(SRC):
            o_ref[PLACE_OUT[SRC * i + n]] = both[16 * n : 16 * n + 16]


def take_kernel(x_ref, o_hbm, turned, out, sems):
    mix = interleave()
    eye = identity(128)
    for h in range(0, HEADS, 32):
        tiles = [x_ref[PLACE_OUT[s]] for s in ORDER_IN[h : h + 32]]
        part = jnp.concatenate([jnp.concatenate(tiles[m : m + 16], axis=0) for m in (0, 16)], axis=1)
        both = dot(mix, part).astype(jnp.bfloat16)
        for m in range(2):
            turned[:, h + 16 * m : h + 16 * m + 16, :] = both[:, 128 * m : 128 * m + 128].reshape(16, 16, 128)
    copies = []
    for r in range(0, ROWS, 2):
        both = dot(eye, turned[r : r + 2].reshape(256, 128), NT).astype(jnp.bfloat16)
        for m in range(2):
            out[r + m] = both[:HD, 128 * m : 128 * m + 128]
            out[r + m + ROWS] = both[HD:, 128 * m : 128 * m + 128]
        if r % 8 == 6:
            for first in (r - 6, r - 6 + ROWS):
                copy = pltpu.make_async_copy(
                    out.at[pl.ds(first, 8)], o_hbm.at[pl.ds(first, 8)], sems.at[len(copies)]
                )
                copy.start()
                copies.append(copy)
    for copy in copies:
        copy.wait()


VMEM = pl.BlockSpec(memory_space=pltpu.VMEM)
HBM = pl.BlockSpec(memory_space=pltpu.HBM)


def in_hbm(x):
    return pltpu.with_memory_space_constraint(x, pltpu.HBM)


def send_call(doc_bounds, q, k, v, q_gain, k_gain):
    return pl.pallas_call(
        send_kernel,
        out_shape=jax.ShapeDtypeStruct((HEADS, 48, 128), jnp.bfloat16),
        in_specs=[HBM] * 6,
        out_specs=VMEM,
        scratch_shapes=[
            pltpu.VMEM((1, DOCS + 1), jnp.int32),
            pltpu.VMEM((3, TOK, HD, HEADS), jnp.bfloat16),
            pltpu.VMEM((2, 1, HD), jnp.float32),
            pltpu.VMEM((2, ROWS, 128, HEADS), jnp.bfloat16),
            pltpu.VMEM((3, ROWS, HEADS, 128), jnp.bfloat16),
            pltpu.SemaphoreType.DMA((6,)),
        ],
        compiler_params=pltpu.CompilerParams(vmem_limit_bytes=32 << 20),
        name="send_side",
    )(*(in_hbm(x) for x in (doc_bounds, q, k, v, q_gain.reshape(1, HD), k_gain.reshape(1, HD))))


def attend_call(doc_bounds, mine):
    return pl.pallas_call(
        attend_kernel,
        out_shape=jax.ShapeDtypeStruct((SEQ // TOK, ROWS, 128), jnp.bfloat16),
        in_specs=[VMEM, VMEM],
        out_specs=VMEM,
        scratch_shapes=[
            pltpu.VMEM((NBLK + 1, HD, BLK), jnp.bfloat16),
            pltpu.VMEM((NBLK, PAIRS, 128), jnp.bfloat16),
            pltpu.VMEM((NBLK, BLK, 128), jnp.bfloat16),
            pltpu.VMEM((NBLK, HD, BLK), jnp.bfloat16),
            pltpu.VMEM((NBLK, 2, BLK, BLK), jnp.float32),
            pltpu.VMEM((FAR, BLK, BLK), jnp.float32),
            pltpu.VMEM((NBLK + 1, 8, BLK), jnp.float32),
            pltpu.VMEM((NBLK + 1, HD, BLK), jnp.float32),
            pltpu.SMEM((FAR,), jnp.int32),
        ],
        compiler_params=pltpu.CompilerParams(vmem_limit_bytes=44 << 20),
        name="attend",
    )(doc_bounds, mine)


def take_call(back):
    return pl.pallas_call(
        take_kernel,
        out_shape=jax.ShapeDtypeStruct((TOK, HD, HEADS), jnp.bfloat16),
        in_specs=[VMEM],
        out_specs=HBM,
        scratch_shapes=[
            pltpu.VMEM((ROWS, HEADS, 128), jnp.bfloat16),
            pltpu.VMEM((TOK, HD, HEADS), jnp.bfloat16),
            pltpu.SemaphoreType.DMA((4,)),
        ],
        compiler_params=pltpu.CompilerParams(vmem_limit_bytes=32 << 20),
        name="take_side",
    )(back)


def exchange(x, order):
    return lax.all_to_all(x, "run", split_axis=0, concat_axis=0, axis_index_groups=[order], tiled=True)


def body(queries, keys, values, doc_bounds, q_gain, k_gain):
    doc_bounds = doc_bounds.reshape(1, DOCS + 1)
    inputs = [jnp.transpose(x, (0, 2, 1)) for x in (queries, keys, values)]
    packed = send_call(doc_bounds, *inputs, q_gain, k_gain)
    mine = exchange(packed, ORDER_IN)
    result = attend_call(doc_bounds, mine)
    back = exchange(result, ORDER_OUT)
    return jnp.transpose(take_call(back), (0, 2, 1))


def solution(mesh):
    runs = jax.sharding.Mesh(mesh.devices.reshape(len(ORDER_IN), -1), ("run", "dp"))
    tokens = P(("dp", "run"), None, None)
    return jax.shard_map(
        body,
        mesh=runs,
        in_specs=(tokens, tokens, tokens, P("dp"), P(), P()),
        out_specs=tokens,
        check_vma=False,
    )
```

```python
import jax
import jax.numpy as jnp
from jax import lax
from jax.experimental import pallas as pl
from jax.experimental.pallas import tpu as pltpu
from jax.sharding import PartitionSpec as P

TOK = 32
ROWS = 16
HD = 64
HEADS = 128
DOCS = 8
SEQ = 4096
BLK = 256
PAIRS = BLK // 2
NBLK = SEQ // BLK
SRC = BLK // TOK
LONG, MIDDLE, SHORT = 16, 8, 4
FAR = (NBLK - 2) * (NBLK - 1) // 2 + LONG
NT = (((1,), (1,)), ((), ()))
NN = (((1,), (0,)), ((), ()))
BIG = 32768.0
SCALE = 1.4426950408889634 / 8.0
FIRST = -9.210340371976184


def run_of(z, x, c):
    return ((z % 8 * 2 + c) * 4 + x) * 2 + z // 8


FIRST_Z = [9, 8, 10, 7, 11, 6, 12, 5, 13, 4, 14, 3, 15, 2, 0, 1]
THEN_Z = [8, 7, 9, 6, 10, 5, 11, 4, 12, 3, 13, 2, 14, 1, 15, 0]
ORDER_IN = [run_of(z, x, c) for z in FIRST_Z for x in (2, 1, 3, 0) for c in range(2)]
ORDER_OUT = [run_of(z, x, c) for z in THEN_Z for x in (2, 1, 3, 0) for c in range(2)]
PLACE_IN = [ORDER_IN.index(s) for s in range(len(ORDER_IN))]
PLACE_OUT = [ORDER_OUT.index(s) for s in range(len(ORDER_OUT))]


def dot(a, b, dims=NN):
    return lax.dot_general(a, b, dims, preferred_element_type=jnp.float32)


def starts_of(token, bound):
    start = jnp.zeros_like(token)
    for d in range(1, DOCS):
        start = jnp.where(token >= bound(d), bound(d), start)
    return start


def identity(n):
    row = lax.broadcasted_iota(jnp.int32, (n, n), 0)
    col = lax.broadcasted_iota(jnp.int32, (n, n), 1)
    return (row == col).astype(jnp.float32).astype(jnp.bfloat16)


def interleave():
    row = lax.broadcasted_iota(jnp.int32, (256, 256), 0)
    col = lax.broadcasted_iota(jnp.int32, (256, 256), 1)
    return (col == (row % 16) * 16 + row // 16).astype(jnp.float32).astype(jnp.bfloat16)


def send_kernel(
    bounds_hbm, q_hbm, k_hbm, v_hbm, qg_hbm, kg_hbm, o_ref, bounds_ref, x_ref, g_ref, rot, turned, sems
):
    arriving = [
        pltpu.make_async_copy(source, target, sems.at[n])
        for n, (source, target) in enumerate(
            (
                (bounds_hbm, bounds_ref),
                (qg_hbm, g_ref.at[0]),
                (kg_hbm, g_ref.at[1]),
                (q_hbm, x_ref.at[0]),
                (v_hbm, x_ref.at[2]),
                (k_hbm, x_ref.at[1]),
            )
        )
    ]
    for c in arriving:
        c.start()
    for c in arriving[:3]:
        c.wait()
    lane = lax.broadcasted_iota(jnp.int32, (HD // 2, 128), 1)
    token = lax.axis_index("run") * TOK + lane
    start = starts_of(token, lambda d: bounds_ref[:, d : d + 1])
    place = (token - start).astype(jnp.float32)
    index = lax.broadcasted_iota(jnp.int32, (HD // 2, 128), 0).astype(jnp.float32)
    angle = place * jnp.exp(jnp.float32(FIRST) * index * 2.0 / HD)
    cosine = jnp.cos(angle)
    sine = jnp.sin(angle)
    eye = identity(HEADS)
    mix = interleave()

    def turn(n, r, rows):
        both = dot(eye, rows, NT).astype(jnp.bfloat16)
        turned[n, r] = both[:, :128]
        turned[n, r + 1] = both[:, 128:]

    def rotate(n):
        gain = jnp.transpose(jnp.broadcast_to(g_ref[n], (HEADS, HD)))
        for r in range(0, ROWS, 2):
            for t in (r, r + ROWS, r + 1, r + 1 + ROWS):
                c = jnp.broadcast_to(cosine[:, t : t + 1], (HD // 2, HEADS))
                s = jnp.broadcast_to(sine[:, t : t + 1], (HD // 2, HEADS))
                x = x_ref[n, t].astype(jnp.float32)
                scale = lax.rsqrt(jnp.mean(x * x, axis=0, keepdims=True) + 1e-06)
                x = x * scale * gain
                a, b = x[: HD // 2], x[HD // 2 :]
                y = jnp.concatenate([a * c - b * s, a * s + b * c], axis=0)
                rot[n, t % ROWS, pl.ds((t // ROWS) * HD, HD), :] = y.astype(jnp.bfloat16)
            turn(n, r, rot[n, r : r + 2].reshape(256, HEADS))

    def spread(n):
        for h in range(0, HEADS, 32):
            part = jnp.concatenate([turned[n, :, h + m : h + m + 16, :].reshape(256, 128) for m in (0, 16)], axis=1)
            both = dot(mix, part).astype(jnp.bfloat16)
            for m in range(2):
                heads = slice(h + 16 * m, h + 16 * m + 16)
                o_ref[heads, 16 * n : 16 * n + 16, :] = both[:, 128 * m : 128 * m + 128].reshape(16, 16, 128)

    for c in arriving[3:]:
        c.wait()

    def turn_values():
        for r in range(0, ROWS, 2):
            turn(2, r, jnp.concatenate([x_ref[2, t] for t in (r, r + ROWS, r + 1, r + 1 + ROWS)], axis=0))

    turn_values()
    rotate(0)
    spread(2)
    rotate(1)
    spread(0)
    spread(1)


def attend_kernel(bounds_ref, x_ref, o_ref, qt, kt, kf, vt, near, far, total, summed, items):

    def offsets(shape, axis):
        n = lax.broadcasted_iota(jnp.int32, shape, axis)
        return ((n % PAIRS) // 16) * 32 + n % 16 + (n // PAIRS) * 16

    below = offsets((BLK, BLK), 0) <= offsets((BLK, BLK), 1)
    q_off = offsets((16, BLK), 1)
    k_off = offsets((BLK, 128), 0)

    def bounds_along(shape, axis):
        n = lax.broadcasted_iota(jnp.int32, shape, axis)
        out = jnp.full(shape, SEQ, jnp.int32)
        for d in range(1, DOCS):
            out = jnp.where(n == d, bounds_ref[:, d : d + 1], out)
        return out

    q_bounds = bounds_along((16, BLK), 0)
    k_bounds = bounds_along((1, 128), 1)

    zero = jnp.zeros((HD, BLK), jnp.bfloat16)
    rest = jnp.zeros((128 - 16, BLK), jnp.bfloat16)

    def wide(x):
        t = jnp.transpose(x.astype(jnp.float32)).astype(jnp.bfloat16)
        return jnp.concatenate([t[:HD], t[HD:]], axis=1)

    def scores(j, q, flags):
        k2 = kt[j]
        low = dot(jnp.concatenate([k2, kf[j, :PAIRS]], axis=1), jnp.concatenate([q, zero, flags, rest], axis=0))
        high = dot(jnp.concatenate([k2, kf[j, PAIRS:]], axis=1), jnp.concatenate([zero, q, flags, rest], axis=0))
        return jnp.exp2(jnp.concatenate([low, high], axis=0) * jnp.float32(SCALE))

    def flags_of(i):
        return jnp.where(BLK * i + q_off >= q_bounds, jnp.float32(-BIG), jnp.float32(0.0)).astype(jnp.bfloat16)

    def partial_sum(e):
        return jnp.sum(e.reshape(BLK // 8, 8, BLK), axis=0)

    def tiles(i, row):
        runs = range(SRC * i, SRC * i + SRC)
        return jnp.concatenate([x_ref[PLACE_IN[s], row : row + 16, :] for s in runs], axis=0)

    def near_scores(blocks):
        for i in blocks:
            q = wide(tiles(i, 0))
            kt[i] = tiles(i, 16)
            qt[i] = q
            vt[i] = wide(tiles(i, 32))
            flags = flags_of(i)
            kf[i] = jnp.where(BLK * i + k_off < k_bounds, jnp.float32(1.0), jnp.float32(0.0)).astype(jnp.bfloat16)
            e1 = jnp.where(below, scores(i, q, flags), jnp.float32(0.0))
            e0 = scores(max(i - 1, 0), q, flags)
            if i == 0:
                e0 = jnp.zeros_like(e0)
            near[i, 0] = e0
            near[i, 1] = e1
            total[i] = partial_sum(e0) + partial_sum(e1)

    scalars = [jnp.max(bounds_ref[:, d : d + 1]) for d in range(DOCS)]
    n_far = jnp.int32(0)
    for i in range(2, NBLK):
        start = starts_of(jnp.int32(BLK * i), lambda d: scalars[d])
        for j in range(i - 2, -1, -1):
            items[n_far] = NBLK * i + j
            n_far += (start < BLK * (j + 1)).astype(jnp.int32)
    near_scores(range(NBLK))
    for u in range(LONG - 1):
        items[n_far + u] = NBLK * NBLK
    trips = (n_far + LONG - MIDDLE - 1) // LONG
    left = n_far - LONG * trips
    passes = (
        (0, trips, LONG),
        (LONG * trips, (left > SHORT).astype(jnp.int32), MIDDLE),
        (LONG * trips, ((left > 0) & (left <= SHORT)).astype(jnp.int32), SHORT),
    )

    def far_blocks(work):
        for begin, trips, length in passes:

            def trip(w, _, begin=begin, length=length):
                for u in range(length):
                    n = begin + length * w + u
                    work(n, items[n] >> 4, items[n] & 15)
                return 0

            lax.fori_loop(0, trips, trip, 0)

    def far_scores(n, i, j):
        e = scores(j, qt[i], flags_of(i))
        far[n] = e
        total[i] += partial_sum(e)

    far_blocks(far_scores)
    for i in range(NBLK):
        inverse = 1.0 / jnp.sum(total[i], axis=0, keepdims=True)
        total[i] = jnp.broadcast_to(inverse, (8, BLK))
        summed[i] = jnp.zeros((HD, BLK), jnp.float32)

    def far_values(n, i, j):
        summed[i] += dot(vt[j], (far[n] * total[i][0:1]).astype(jnp.bfloat16))

    far_blocks(far_values)

    for i in range(NBLK):
        w = jnp.concatenate([(near[i, n] * total[i][0:1]).astype(jnp.bfloat16) for n in range(2)], axis=0)
        out = dot(jnp.concatenate([vt[max(i - 1, 0)], vt[i]], axis=1), w) + summed[i]
        both = jnp.transpose(jnp.concatenate([out[:, :PAIRS], out[:, PAIRS:]], axis=0))
        both = both.astype(jnp.bfloat16)
        for n in range(SRC):
            o_ref[PLACE_OUT[SRC * i + n]] = both[16 * n : 16 * n + 16]


def take_kernel(x_ref, o_hbm, turned, out, sems):
    mix = interleave()
    eye = identity(128)
    for h in range(0, HEADS, 32):
        tiles = [x_ref[PLACE_OUT[s]] for s in ORDER_IN[h : h + 32]]
        part = jnp.concatenate([jnp.concatenate(tiles[m : m + 16], axis=0) for m in (0, 16)], axis=1)
        both = dot(mix, part).astype(jnp.bfloat16)
        for m in range(2):
            turned[:, h + 16 * m : h + 16 * m + 16, :] = both[:, 128 * m : 128 * m + 128].reshape(16, 16, 128)
    copies = []
    for r in range(0, ROWS, 2):
        both = dot(eye, turned[r : r + 2].reshape(256, 128), NT).astype(jnp.bfloat16)
        for m in range(2):
            out[r + m] = both[:HD, 128 * m : 128 * m + 128]
            out[r + m + ROWS] = both[HD:, 128 * m : 128 * m + 128]
        if r % 8 == 6:
            for first in (r - 6, r - 6 + ROWS):
                copy = pltpu.make_async_copy(
                    out.at[pl.ds(first, 8)], o_hbm.at[pl.ds(first, 8)], sems.at[len(copies)]
                )
                copy.start()
                copies.append(copy)
    for copy in copies:
        copy.wait()


VMEM = pl.BlockSpec(memory_space=pltpu.VMEM)
HBM = pl.BlockSpec(memory_space=pltpu.HBM)


def in_hbm(x):
    return pltpu.with_memory_space_constraint(x, pltpu.HBM)


def send_call(doc_bounds, q, k, v, q_gain, k_gain):
    return pl.pallas_call(
        send_kernel,
        out_shape=jax.ShapeDtypeStruct((HEADS, 48, 128), jnp.bfloat16),
        in_specs=[HBM] * 6,
        out_specs=VMEM,
        scratch_shapes=[
            pltpu.VMEM((1, DOCS + 1), jnp.int32),
            pltpu.VMEM((3, TOK, HD, HEADS), jnp.bfloat16),
            pltpu.VMEM((2, 1, HD), jnp.float32),
            pltpu.VMEM((2, ROWS, 128, HEADS), jnp.bfloat16),
            pltpu.VMEM((3, ROWS, HEADS, 128), jnp.bfloat16),
            pltpu.SemaphoreType.DMA((6,)),
        ],
        compiler_params=pltpu.CompilerParams(vmem_limit_bytes=32 << 20),
        name="send_side",
    )(*(in_hbm(x) for x in (doc_bounds, q, k, v, q_gain.reshape(1, HD), k_gain.reshape(1, HD))))


def attend_call(doc_bounds, mine):
    return pl.pallas_call(
        attend_kernel,
        out_shape=jax.ShapeDtypeStruct((SEQ // TOK, ROWS, 128), jnp.bfloat16),
        in_specs=[VMEM, VMEM],
        out_specs=VMEM,
        scratch_shapes=[
            pltpu.VMEM((NBLK + 1, HD, BLK), jnp.bfloat16),
            pltpu.VMEM((NBLK, PAIRS, 128), jnp.bfloat16),
            pltpu.VMEM((NBLK, BLK, 128), jnp.bfloat16),
            pltpu.VMEM((NBLK, HD, BLK), jnp.bfloat16),
            pltpu.VMEM((NBLK, 2, BLK, BLK), jnp.float32),
            pltpu.VMEM((FAR, BLK, BLK), jnp.float32),
            pltpu.VMEM((NBLK + 1, 8, BLK), jnp.float32),
            pltpu.VMEM((NBLK + 1, HD, BLK), jnp.float32),
            pltpu.SMEM((FAR,), jnp.int32),
        ],
        compiler_params=pltpu.CompilerParams(vmem_limit_bytes=44 << 20),
        name="attend",
    )(doc_bounds, mine)


def take_call(back):
    return pl.pallas_call(
        take_kernel,
        out_shape=jax.ShapeDtypeStruct((TOK, HD, HEADS), jnp.bfloat16),
        in_specs=[VMEM],
        out_specs=HBM,
        scratch_shapes=[
            pltpu.VMEM((ROWS, HEADS, 128), jnp.bfloat16),
            pltpu.VMEM((TOK, HD, HEADS), jnp.bfloat16),
            pltpu.SemaphoreType.DMA((4,)),
        ],
        compiler_params=pltpu.CompilerParams(vmem_limit_bytes=32 << 20),
        name="take_side",
    )(back)


def exchange(x, order):
    return lax.all_to_all(x, "run", split_axis=0, concat_axis=0, axis_index_groups=[order], tiled=True)


def body(queries, keys, values, doc_bounds, q_gain, k_gain):
    doc_bounds = doc_bounds.reshape(1, DOCS + 1)
    inputs = [jnp.transpose(x, (0, 2, 1)) for x in (queries, keys, values)]
    packed = send_call(doc_bounds, *inputs, q_gain, k_gain)
    mine = exchange(packed, ORDER_IN)
    result = attend_call(doc_bounds, mine)
    back = exchange(result, ORDER_OUT)
    return jnp.transpose(take_call(back), (0, 2, 1))


def solution(mesh):
    runs = jax.sharding.Mesh(mesh.devices.reshape(len(ORDER_IN), -1), ("run", "dp"))
    tokens = P(("dp", "run"), None, None)
    return jax.shard_map(
        body,
        mesh=runs,
        in_specs=(tokens, tokens, tokens, P("dp"), P(), P()),
        out_specs=tokens,
        check_vma=False,
    )
```

```python
import jax
import jax.numpy as jnp
from jax import lax
from jax.experimental import pallas as pl
from jax.experimental.pallas import tpu as pltpu
from jax.sharding import PartitionSpec as P

TOK = 32
ROWS = 16
HD = 64
HEADS = 128
DOCS = 8
SEQ = 4096
BLK = 256
PAIRS = BLK // 2
NBLK = SEQ // BLK
SRC = BLK // TOK
LONG, MIDDLE, SHORT = 16, 8, 4
FAR = (NBLK - 2) * (NBLK - 1) // 2 + LONG
NT = (((1,), (1,)), ((), ()))
NN = (((1,), (0,)), ((), ()))
BIG = 32768.0
SCALE = 1.4426950408889634 / 8.0
FIRST = -9.210340371976184


def run_of(z, x, c):
    return ((z % 8 * 2 + c) * 4 + x) * 2 + z // 8


FIRST_Z = [8, 15, 6, 13, 4, 11, 2, 9, 0, 7, 14, 5, 12, 3, 10, 1]
THEN_Z = [8, 1, 10, 3, 12, 5, 14, 7, 0, 9, 2, 11, 4, 13, 6, 15]
ORDER_IN = [run_of(z, x, c) for z in FIRST_Z for x in (2, 1, 3, 0) for c in range(2)]
ORDER_OUT = [run_of(z, x, c) for z in THEN_Z for x in (2, 1, 3, 0) for c in range(2)]
PLACE_IN = [ORDER_IN.index(s) for s in range(len(ORDER_IN))]
PLACE_OUT = [ORDER_OUT.index(s) for s in range(len(ORDER_OUT))]


def dot(a, b, dims=NN):
    return lax.dot_general(a, b, dims, preferred_element_type=jnp.float32)


def starts_of(token, bound):
    start = jnp.zeros_like(token)
    for d in range(1, DOCS):
        start = jnp.where(token >= bound(d), bound(d), start)
    return start


def identity(n):
    row = lax.broadcasted_iota(jnp.int32, (n, n), 0)
    col = lax.broadcasted_iota(jnp.int32, (n, n), 1)
    return (row == col).astype(jnp.float32).astype(jnp.bfloat16)


def interleave():
    row = lax.broadcasted_iota(jnp.int32, (256, 256), 0)
    col = lax.broadcasted_iota(jnp.int32, (256, 256), 1)
    return (col == (row % 16) * 16 + row // 16).astype(jnp.float32).astype(jnp.bfloat16)


def send_kernel(
    bounds_hbm, q_hbm, k_hbm, v_hbm, qg_hbm, kg_hbm, o_ref, bounds_ref, x_ref, g_ref, rot, turned, sems
):
    arriving = [
        pltpu.make_async_copy(source, target, sems.at[n])
        for n, (source, target) in enumerate(
            (
                (bounds_hbm, bounds_ref),
                (qg_hbm, g_ref.at[0]),
                (kg_hbm, g_ref.at[1]),
                (q_hbm, x_ref.at[0]),
                (v_hbm, x_ref.at[2]),
                (k_hbm, x_ref.at[1]),
            )
        )
    ]
    for c in arriving:
        c.start()
    for c in arriving[:3]:
        c.wait()
    lane = lax.broadcasted_iota(jnp.int32, (HD // 2, 128), 1)
    token = lax.axis_index("run") * TOK + lane
    start = starts_of(token, lambda d: bounds_ref[:, d : d + 1])
    place = (token - start).astype(jnp.float32)
    index = lax.broadcasted_iota(jnp.int32, (HD // 2, 128), 0).astype(jnp.float32)
    angle = place * jnp.exp(jnp.float32(FIRST) * index * 2.0 / HD)
    cosine = jnp.cos(angle)
    sine = jnp.sin(angle)
    eye = identity(HEADS)
    mix = interleave()

    def turn(n, r, rows):
        both = dot(eye, rows, NT).astype(jnp.bfloat16)
        turned[n, r] = both[:, :128]
        turned[n, r + 1] = both[:, 128:]

    def rotate(n):
        gain = jnp.transpose(jnp.broadcast_to(g_ref[n], (HEADS, HD)))
        for r in range(0, ROWS, 2):
            for t in (r, r + ROWS, r + 1, r + 1 + ROWS):
                c = jnp.broadcast_to(cosine[:, t : t + 1], (HD // 2, HEADS))
                s = jnp.broadcast_to(sine[:, t : t + 1], (HD // 2, HEADS))
                x = x_ref[n, t].astype(jnp.float32)
                scale = lax.rsqrt(jnp.mean(x * x, axis=0, keepdims=True) + 1e-06)
                x = x * scale * gain
                a, b = x[: HD // 2], x[HD // 2 :]
                y = jnp.concatenate([a * c - b * s, a * s + b * c], axis=0)
                rot[n, t % ROWS, pl.ds((t // ROWS) * HD, HD), :] = y.astype(jnp.bfloat16)
            turn(n, r, rot[n, r : r + 2].reshape(256, HEADS))

    def spread(n):
        for h in range(0, HEADS, 32):
            part = jnp.concatenate([turned[n, :, h + m : h + m + 16, :].reshape(256, 128) for m in (0, 16)], axis=1)
            both = dot(mix, part).astype(jnp.bfloat16)
            for m in range(2):
                heads = slice(h + 16 * m, h + 16 * m + 16)
                o_ref[heads, 16 * n : 16 * n + 16, :] = both[:, 128 * m : 128 * m + 128].reshape(16, 16, 128)

    for c in arriving[3:]:
        c.wait()

    def turn_values():
        for r in range(0, ROWS, 2):
            turn(2, r, jnp.concatenate([x_ref[2, t] for t in (r, r + ROWS, r + 1, r + 1 + ROWS)], axis=0))

    turn_values()
    rotate(0)
    spread(2)
    rotate(1)
    spread(0)
    spread(1)


def attend_kernel(bounds_ref, x_ref, o_ref, qt, kt, kf, vt, near, far, total, summed, items):

    def offsets(shape, axis):
        n = lax.broadcasted_iota(jnp.int32, shape, axis)
        return ((n % PAIRS) // 16) * 32 + n % 16 + (n // PAIRS) * 16

    below = offsets((BLK, BLK), 0) <= offsets((BLK, BLK), 1)
    q_off = offsets((16, BLK), 1)
    k_off = offsets((BLK, 128), 0)

    def bounds_along(shape, axis):
        n = lax.broadcasted_iota(jnp.int32, shape, axis)
        out = jnp.full(shape, SEQ, jnp.int32)
        for d in range(1, DOCS):
            out = jnp.where(n == d, bounds_ref[:, d : d + 1], out)
        return out

    q_bounds = bounds_along((16, BLK), 0)
    k_bounds = bounds_along((1, 128), 1)

    zero = jnp.zeros((HD, BLK), jnp.bfloat16)
    rest = jnp.zeros((128 - 16, BLK), jnp.bfloat16)

    def wide(x):
        t = jnp.transpose(x.astype(jnp.float32)).astype(jnp.bfloat16)
        return jnp.concatenate([t[:HD], t[HD:]], axis=1)

    def scores(j, q, flags):
        k2 = kt[j]
        low = dot(jnp.concatenate([k2, kf[j, :PAIRS]], axis=1), jnp.concatenate([q, zero, flags, rest], axis=0))
        high = dot(jnp.concatenate([k2, kf[j, PAIRS:]], axis=1), jnp.concatenate([zero, q, flags, rest], axis=0))
        return jnp.exp2(jnp.concatenate([low, high], axis=0) * jnp.float32(SCALE))

    def flags_of(i):
        return jnp.where(BLK * i + q_off >= q_bounds, jnp.float32(-BIG), jnp.float32(0.0)).astype(jnp.bfloat16)

    def partial_sum(e):
        return jnp.sum(e.reshape(BLK // 8, 8, BLK), axis=0)

    def tiles(i, row):
        runs = range(SRC * i, SRC * i + SRC)
        return jnp.concatenate([x_ref[PLACE_IN[s], row : row + 16, :] for s in runs], axis=0)

    def near_scores(blocks):
        for i in blocks:
            q = wide(tiles(i, 0))
            kt[i] = tiles(i, 16)
            qt[i] = q
            vt[i] = wide(tiles(i, 32))
            flags = flags_of(i)
            kf[i] = jnp.where(BLK * i + k_off < k_bounds, jnp.float32(1.0), jnp.float32(0.0)).astype(jnp.bfloat16)
            e1 = jnp.where(below, scores(i, q, flags), jnp.float32(0.0))
            e0 = scores(max(i - 1, 0), q, flags)
            if i == 0:
                e0 = jnp.zeros_like(e0)
            near[i, 0] = e0
            near[i, 1] = e1
            total[i] = partial_sum(e0) + partial_sum(e1)

    scalars = [jnp.max(bounds_ref[:, d : d + 1]) for d in range(DOCS)]
    n_far = jnp.int32(0)
    for i in range(2, NBLK):
        start = starts_of(jnp.int32(BLK * i), lambda d: scalars[d])
        for j in range(i - 2, -1, -1):
            items[n_far] = NBLK * i + j
            n_far += (start < BLK * (j + 1)).astype(jnp.int32)
    near_scores(range(NBLK))
    for u in range(LONG - 1):
        items[n_far + u] = NBLK * NBLK
    trips = (n_far + LONG - MIDDLE - 1) // LONG
    left = n_far - LONG * trips
    passes = (
        (0, trips, LONG),
        (LONG * trips, (left > SHORT).astype(jnp.int32), MIDDLE),
        (LONG * trips, ((left > 0) & (left <= SHORT)).astype(jnp.int32), SHORT),
    )

    def far_blocks(work):
        for begin, trips, length in passes:

            def trip(w, _, begin=begin, length=length):
                for u in range(length):
                    n = begin + length * w + u
                    work(n, items[n] >> 4, items[n] & 15)
                return 0

            lax.fori_loop(0, trips, trip, 0)

    def far_scores(n, i, j):
        e = scores(j, qt[i], flags_of(i))
        far[n] = e
        total[i] += partial_sum(e)

    far_blocks(far_scores)
    for i in range(NBLK):
        inverse = 1.0 / jnp.sum(total[i], axis=0, keepdims=True)
        total[i] = jnp.broadcast_to(inverse, (8, BLK))
        summed[i] = jnp.zeros((HD, BLK), jnp.float32)

    def far_values(n, i, j):
        summed[i] += dot(vt[j], (far[n] * total[i][0:1]).astype(jnp.bfloat16))

    far_blocks(far_values)

    for i in range(NBLK):
        w = jnp.concatenate([(near[i, n] * total[i][0:1]).astype(jnp.bfloat16) for n in range(2)], axis=0)
        out = dot(jnp.concatenate([vt[max(i - 1, 0)], vt[i]], axis=1), w) + summed[i]
        both = jnp.transpose(jnp.concatenate([out[:, :PAIRS], out[:, PAIRS:]], axis=0))
        both = both.astype(jnp.bfloat16)
        for n in range(SRC):
            o_ref[PLACE_OUT[SRC * i + n]] = both[16 * n : 16 * n + 16]


def take_kernel(x_ref, o_hbm, turned, out, sems):
    mix = interleave()
    eye = identity(128)
    for h in range(0, HEADS, 32):
        tiles = [x_ref[PLACE_OUT[s]] for s in ORDER_IN[h : h + 32]]
        part = jnp.concatenate([jnp.concatenate(tiles[m : m + 16], axis=0) for m in (0, 16)], axis=1)
        both = dot(mix, part).astype(jnp.bfloat16)
        for m in range(2):
            turned[:, h + 16 * m : h + 16 * m + 16, :] = both[:, 128 * m : 128 * m + 128].reshape(16, 16, 128)
    copies = []
    for r in range(0, ROWS, 2):
        both = dot(eye, turned[r : r + 2].reshape(256, 128), NT).astype(jnp.bfloat16)
        for m in range(2):
            out[r + m] = both[:HD, 128 * m : 128 * m + 128]
            out[r + m + ROWS] = both[HD:, 128 * m : 128 * m + 128]
        if r % 8 == 6:
            for first in (r - 6, r - 6 + ROWS):
                copy = pltpu.make_async_copy(
                    out.at[pl.ds(first, 8)], o_hbm.at[pl.ds(first, 8)], sems.at[len(copies)]
                )
                copy.start()
                copies.append(copy)
    for copy in copies:
        copy.wait()


VMEM = pl.BlockSpec(memory_space=pltpu.VMEM)
HBM = pl.BlockSpec(memory_space=pltpu.HBM)


def in_hbm(x):
    return pltpu.with_memory_space_constraint(x, pltpu.HBM)


def send_call(doc_bounds, q, k, v, q_gain, k_gain):
    return pl.pallas_call(
        send_kernel,
        out_shape=jax.ShapeDtypeStruct((HEADS, 48, 128), jnp.bfloat16),
        in_specs=[HBM] * 6,
        out_specs=VMEM,
        scratch_shapes=[
            pltpu.VMEM((1, DOCS + 1), jnp.int32),
            pltpu.VMEM((3, TOK, HD, HEADS), jnp.bfloat16),
            pltpu.VMEM((2, 1, HD), jnp.float32),
            pltpu.VMEM((2, ROWS, 128, HEADS), jnp.bfloat16),
            pltpu.VMEM((3, ROWS, HEADS, 128), jnp.bfloat16),
            pltpu.SemaphoreType.DMA((6,)),
        ],
        compiler_params=pltpu.CompilerParams(vmem_limit_bytes=32 << 20),
        name="send_side",
    )(*(in_hbm(x) for x in (doc_bounds, q, k, v, q_gain.reshape(1, HD), k_gain.reshape(1, HD))))


def attend_call(doc_bounds, mine):
    return pl.pallas_call(
        attend_kernel,
        out_shape=jax.ShapeDtypeStruct((SEQ // TOK, ROWS, 128), jnp.bfloat16),
        in_specs=[VMEM, VMEM],
        out_specs=VMEM,
        scratch_shapes=[
            pltpu.VMEM((NBLK + 1, HD, BLK), jnp.bfloat16),
            pltpu.VMEM((NBLK, PAIRS, 128), jnp.bfloat16),
            pltpu.VMEM((NBLK, BLK, 128), jnp.bfloat16),
            pltpu.VMEM((NBLK, HD, BLK), jnp.bfloat16),
            pltpu.VMEM((NBLK, 2, BLK, BLK), jnp.float32),
            pltpu.VMEM((FAR, BLK, BLK), jnp.float32),
            pltpu.VMEM((NBLK + 1, 8, BLK), jnp.float32),
            pltpu.VMEM((NBLK + 1, HD, BLK), jnp.float32),
            pltpu.SMEM((FAR,), jnp.int32),
        ],
        compiler_params=pltpu.CompilerParams(vmem_limit_bytes=44 << 20),
        name="attend",
    )(doc_bounds, mine)


def take_call(back):
    return pl.pallas_call(
        take_kernel,
        out_shape=jax.ShapeDtypeStruct((TOK, HD, HEADS), jnp.bfloat16),
        in_specs=[VMEM],
        out_specs=HBM,
        scratch_shapes=[
            pltpu.VMEM((ROWS, HEADS, 128), jnp.bfloat16),
            pltpu.VMEM((TOK, HD, HEADS), jnp.bfloat16),
            pltpu.SemaphoreType.DMA((4,)),
        ],
        compiler_params=pltpu.CompilerParams(vmem_limit_bytes=32 << 20),
        name="take_side",
    )(back)


def exchange(x, order):
    return lax.all_to_all(x, "run", split_axis=0, concat_axis=0, axis_index_groups=[order], tiled=True)


def body(queries, keys, values, doc_bounds, q_gain, k_gain):
    doc_bounds = doc_bounds.reshape(1, DOCS + 1)
    inputs = [jnp.transpose(x, (0, 2, 1)) for x in (queries, keys, values)]
    packed = send_call(doc_bounds, *inputs, q_gain, k_gain)
    mine = exchange(packed, ORDER_IN)
    result = attend_call(doc_bounds, mine)
    back = exchange(result, ORDER_OUT)
    return jnp.transpose(take_call(back), (0, 2, 1))


def solution(mesh):
    runs = jax.sharding.Mesh(mesh.devices.reshape(len(ORDER_IN), -1), ("run", "dp"))
    tokens = P(("dp", "run"), None, None)
    return jax.shard_map(
        body,
        mesh=runs,
        in_specs=(tokens, tokens, tokens, P("dp"), P(), P()),
        out_specs=tokens,
        check_vma=False,
    )
```

```python
import jax
import jax.numpy as jnp
from jax import lax
from jax.experimental import pallas as pl
from jax.experimental.pallas import tpu as pltpu
from jax.sharding import PartitionSpec as P

TOK = 32
ROWS = 16
HD = 64
HEADS = 128
DOCS = 8
SEQ = 4096
BLK = 256
PAIRS = BLK // 2
NBLK = SEQ // BLK
SRC = BLK // TOK
LONG, MIDDLE, SHORT = 16, 8, 4
FAR = (NBLK - 2) * (NBLK - 1) // 2 + LONG
NT = (((1,), (1,)), ((), ()))
NN = (((1,), (0,)), ((), ()))
BIG = 32768.0
SCALE = 1.4426950408889634 / 8.0
FIRST = -9.210340371976184


def run_of(z, x, c):
    return ((z % 8 * 2 + c) * 4 + x) * 2 + z // 8


FIRST_Z = [9, 8, 10, 7, 11, 6, 12, 5, 13, 4, 14, 3, 15, 2, 0, 1]
THEN_Z = [8, 15, 6, 13, 4, 11, 2, 9, 0, 7, 14, 5, 12, 3, 10, 1]
ORDER_IN = [run_of(z, x, c) for z in FIRST_Z for x in (2, 1, 3, 0) for c in range(2)]
ORDER_OUT = [run_of(z, x, c) for z in THEN_Z for x in (2, 1, 3, 0) for c in range(2)]
PLACE_IN = [ORDER_IN.index(s) for s in range(len(ORDER_IN))]
PLACE_OUT = [ORDER_OUT.index(s) for s in range(len(ORDER_OUT))]


def dot(a, b, dims=NN):
    return lax.dot_general(a, b, dims, preferred_element_type=jnp.float32)


def starts_of(token, bound):
    start = jnp.zeros_like(token)
    for d in range(1, DOCS):
        start = jnp.where(token >= bound(d), bound(d), start)
    return start


def identity(n):
    row = lax.broadcasted_iota(jnp.int32, (n, n), 0)
    col = lax.broadcasted_iota(jnp.int32, (n, n), 1)
    return (row == col).astype(jnp.float32).astype(jnp.bfloat16)


def interleave():
    row = lax.broadcasted_iota(jnp.int32, (256, 256), 0)
    col = lax.broadcasted_iota(jnp.int32, (256, 256), 1)
    return (col == (row % 16) * 16 + row // 16).astype(jnp.float32).astype(jnp.bfloat16)


def send_kernel(
    bounds_hbm, q_hbm, k_hbm, v_hbm, qg_hbm, kg_hbm, o_ref, bounds_ref, x_ref, g_ref, rot, turned, sems
):
    arriving = [
        pltpu.make_async_copy(source, target, sems.at[n])
        for n, (source, target) in enumerate(
            (
                (bounds_hbm, bounds_ref),
                (qg_hbm, g_ref.at[0]),
                (kg_hbm, g_ref.at[1]),
                (q_hbm, x_ref.at[0]),
                (v_hbm, x_ref.at[2]),
                (k_hbm, x_ref.at[1]),
            )
        )
    ]
    for c in arriving:
        c.start()
    for c in arriving[:3]:
        c.wait()
    lane = lax.broadcasted_iota(jnp.int32, (HD // 2, 128), 1)
    token = lax.axis_index("run") * TOK + lane
    start = starts_of(token, lambda d: bounds_ref[:, d : d + 1])
    place = (token - start).astype(jnp.float32)
    index = lax.broadcasted_iota(jnp.int32, (HD // 2, 128), 0).astype(jnp.float32)
    angle = place * jnp.exp(jnp.float32(FIRST) * index * 2.0 / HD)
    cosine = jnp.cos(angle)
    sine = jnp.sin(angle)
    eye = identity(HEADS)
    mix = interleave()

    def turn(n, r, rows):
        both = dot(eye, rows, NT).astype(jnp.bfloat16)
        turned[n, r] = both[:, :128]
        turned[n, r + 1] = both[:, 128:]

    def rotate(n):
        gain = jnp.transpose(jnp.broadcast_to(g_ref[n], (HEADS, HD)))
        for r in range(0, ROWS, 2):
            for t in (r, r + ROWS, r + 1, r + 1 + ROWS):
                c = jnp.broadcast_to(cosine[:, t : t + 1], (HD // 2, HEADS))
                s = jnp.broadcast_to(sine[:, t : t + 1], (HD // 2, HEADS))
                x = x_ref[n, t].astype(jnp.float32)
                scale = lax.rsqrt(jnp.mean(x * x, axis=0, keepdims=True) + 1e-06)
                x = x * scale * gain
                a, b = x[: HD // 2], x[HD // 2 :]
                y = jnp.concatenate([a * c - b * s, a * s + b * c], axis=0)
                rot[n, t % ROWS, pl.ds((t // ROWS) * HD, HD), :] = y.astype(jnp.bfloat16)
            turn(n, r, rot[n, r : r + 2].reshape(256, HEADS))

    def spread(n):
        for h in range(0, HEADS, 32):
            part = jnp.concatenate([turned[n, :, h + m : h + m + 16, :].reshape(256, 128) for m in (0, 16)], axis=1)
            both = dot(mix, part).astype(jnp.bfloat16)
            for m in range(2):
                heads = slice(h + 16 * m, h + 16 * m + 16)
                o_ref[heads, 16 * n : 16 * n + 16, :] = both[:, 128 * m : 128 * m + 128].reshape(16, 16, 128)

    for c in arriving[3:]:
        c.wait()

    def turn_values():
        for r in range(0, ROWS, 2):
            turn(2, r, jnp.concatenate([x_ref[2, t] for t in (r, r + ROWS, r + 1, r + 1 + ROWS)], axis=0))

    turn_values()
    rotate(0)
    spread(2)
    rotate(1)
    spread(0)
    spread(1)


def attend_kernel(bounds_ref, x_ref, o_ref, qt, kt, kf, vt, near, far, total, summed, items):

    def offsets(shape, axis):
        n = lax.broadcasted_iota(jnp.int32, shape, axis)
        return ((n % PAIRS) // 16) * 32 + n % 16 + (n // PAIRS) * 16

    below = offsets((BLK, BLK), 0) <= offsets((BLK, BLK), 1)
    q_off = offsets((16, BLK), 1)
    k_off = offsets((BLK, 128), 0)

    def bounds_along(shape, axis):
        n = lax.broadcasted_iota(jnp.int32, shape, axis)
        out = jnp.full(shape, SEQ, jnp.int32)
        for d in range(1, DOCS):
            out = jnp.where(n == d, bounds_ref[:, d : d + 1], out)
        return out

    q_bounds = bounds_along((16, BLK), 0)
    k_bounds = bounds_along((1, 128), 1)

    zero = jnp.zeros((HD, BLK), jnp.bfloat16)
    rest = jnp.zeros((128 - 16, BLK), jnp.bfloat16)

    def wide(x):
        t = jnp.transpose(x.astype(jnp.float32)).astype(jnp.bfloat16)
        return jnp.concatenate([t[:HD], t[HD:]], axis=1)

    def scores(j, q, flags):
        k2 = kt[j]
        low = dot(jnp.concatenate([k2, kf[j, :PAIRS]], axis=1), jnp.concatenate([q, zero, flags, rest], axis=0))
        high = dot(jnp.concatenate([k2, kf[j, PAIRS:]], axis=1), jnp.concatenate([zero, q, flags, rest], axis=0))
        return jnp.exp2(jnp.concatenate([low, high], axis=0) * jnp.float32(SCALE))

    def flags_of(i):
        return jnp.where(BLK * i + q_off >= q_bounds, jnp.float32(-BIG), jnp.float32(0.0)).astype(jnp.bfloat16)

    def partial_sum(e):
        return jnp.sum(e.reshape(BLK // 8, 8, BLK), axis=0)

    def tiles(i, row):
        runs = range(SRC * i, SRC * i + SRC)
        return jnp.concatenate([x_ref[PLACE_IN[s], row : row + 16, :] for s in runs], axis=0)

    def near_scores(blocks):
        for i in blocks:
            q = wide(tiles(i, 0))
            kt[i] = tiles(i, 16)
            qt[i] = q
            vt[i] = wide(tiles(i, 32))
            flags = flags_of(i)
            kf[i] = jnp.where(BLK * i + k_off < k_bounds, jnp.float32(1.0), jnp.float32(0.0)).astype(jnp.bfloat16)
            e1 = jnp.where(below, scores(i, q, flags), jnp.float32(0.0))
            e0 = scores(max(i - 1, 0), q, flags)
            if i == 0:
                e0 = jnp.zeros_like(e0)
            near[i, 0] = e0
            near[i, 1] = e1
            total[i] = partial_sum(e0) + partial_sum(e1)

    scalars = [jnp.max(bounds_ref[:, d : d + 1]) for d in range(DOCS)]
    n_far = jnp.int32(0)
    for i in range(2, NBLK):
        start = starts_of(jnp.int32(BLK * i), lambda d: scalars[d])
        for j in range(i - 2, -1, -1):
            items[n_far] = NBLK * i + j
            n_far += (start < BLK * (j + 1)).astype(jnp.int32)
    near_scores(range(NBLK))
    for u in range(LONG - 1):
        items[n_far + u] = NBLK * NBLK
    trips = (n_far + LONG - MIDDLE - 1) // LONG
    left = n_far - LONG * trips
    passes = (
        (0, trips, LONG),
        (LONG * trips, (left > SHORT).astype(jnp.int32), MIDDLE),
        (LONG * trips, ((left > 0) & (left <= SHORT)).astype(jnp.int32), SHORT),
    )

    def far_blocks(work):
        for begin, trips, length in passes:

            def trip(w, _, begin=begin, length=length):
                for u in range(length):
                    n = begin + length * w + u
                    work(n, items[n] >> 4, items[n] & 15)
                return 0

            lax.fori_loop(0, trips, trip, 0)

    def far_scores(n, i, j):
        e = scores(j, qt[i], flags_of(i))
        far[n] = e
        total[i] += partial_sum(e)

    far_blocks(far_scores)
    for i in range(NBLK):
        inverse = 1.0 / jnp.sum(total[i], axis=0, keepdims=True)
        total[i] = jnp.broadcast_to(inverse, (8, BLK))
        summed[i] = jnp.zeros((HD, BLK), jnp.float32)

    def far_values(n, i, j):
        summed[i] += dot(vt[j], (far[n] * total[i][0:1]).astype(jnp.bfloat16))

    far_blocks(far_values)

    for i in range(NBLK):
        w = jnp.concatenate([(near[i, n] * total[i][0:1]).astype(jnp.bfloat16) for n in range(2)], axis=0)
        out = dot(jnp.concatenate([vt[max(i - 1, 0)], vt[i]], axis=1), w) + summed[i]
        both = jnp.transpose(jnp.concatenate([out[:, :PAIRS], out[:, PAIRS:]], axis=0))
        both = both.astype(jnp.bfloat16)
        for n in range(SRC):
            o_ref[PLACE_OUT[SRC * i + n]] = both[16 * n : 16 * n + 16]


def take_kernel(x_ref, o_hbm, turned, out, sems):
    mix = interleave()
    eye = identity(128)
    for h in range(0, HEADS, 32):
        tiles = [x_ref[PLACE_OUT[s]] for s in ORDER_IN[h : h + 32]]
        part = jnp.concatenate([jnp.concatenate(tiles[m : m + 16], axis=0) for m in (0, 16)], axis=1)
        both = dot(mix, part).astype(jnp.bfloat16)
        for m in range(2):
            turned[:, h + 16 * m : h + 16 * m + 16, :] = both[:, 128 * m : 128 * m + 128].reshape(16, 16, 128)
    copies = []
    for r in range(0, ROWS, 2):
        both = dot(eye, turned[r : r + 2].reshape(256, 128), NT).astype(jnp.bfloat16)
        for m in range(2):
            out[r + m] = both[:HD, 128 * m : 128 * m + 128]
            out[r + m + ROWS] = both[HD:, 128 * m : 128 * m + 128]
        if r % 8 == 6:
            for first in (r - 6, r - 6 + ROWS):
                copy = pltpu.make_async_copy(
                    out.at[pl.ds(first, 8)], o_hbm.at[pl.ds(first, 8)], sems.at[len(copies)]
                )
                copy.start()
                copies.append(copy)
    for copy in copies:
        copy.wait()


VMEM = pl.BlockSpec(memory_space=pltpu.VMEM)
HBM = pl.BlockSpec(memory_space=pltpu.HBM)


def in_hbm(x):
    return pltpu.with_memory_space_constraint(x, pltpu.HBM)


def send_call(doc_bounds, q, k, v, q_gain, k_gain):
    return pl.pallas_call(
        send_kernel,
        out_shape=jax.ShapeDtypeStruct((HEADS, 48, 128), jnp.bfloat16),
        in_specs=[HBM] * 6,
        out_specs=VMEM,
        scratch_shapes=[
            pltpu.VMEM((1, DOCS + 1), jnp.int32),
            pltpu.VMEM((3, TOK, HD, HEADS), jnp.bfloat16),
            pltpu.VMEM((2, 1, HD), jnp.float32),
            pltpu.VMEM((2, ROWS, 128, HEADS), jnp.bfloat16),
            pltpu.VMEM((3, ROWS, HEADS, 128), jnp.bfloat16),
            pltpu.SemaphoreType.DMA((6,)),
        ],
        compiler_params=pltpu.CompilerParams(vmem_limit_bytes=32 << 20),
        name="send_side",
    )(*(in_hbm(x) for x in (doc_bounds, q, k, v, q_gain.reshape(1, HD), k_gain.reshape(1, HD))))


def attend_call(doc_bounds, mine):
    return pl.pallas_call(
        attend_kernel,
        out_shape=jax.ShapeDtypeStruct((SEQ // TOK, ROWS, 128), jnp.bfloat16),
        in_specs=[VMEM, VMEM],
        out_specs=VMEM,
        scratch_shapes=[
            pltpu.VMEM((NBLK + 1, HD, BLK), jnp.bfloat16),
            pltpu.VMEM((NBLK, PAIRS, 128), jnp.bfloat16),
            pltpu.VMEM((NBLK, BLK, 128), jnp.bfloat16),
            pltpu.VMEM((NBLK, HD, BLK), jnp.bfloat16),
            pltpu.VMEM((NBLK, 2, BLK, BLK), jnp.float32),
            pltpu.VMEM((FAR, BLK, BLK), jnp.float32),
            pltpu.VMEM((NBLK + 1, 8, BLK), jnp.float32),
            pltpu.VMEM((NBLK + 1, HD, BLK), jnp.float32),
            pltpu.SMEM((FAR,), jnp.int32),
        ],
        compiler_params=pltpu.CompilerParams(vmem_limit_bytes=44 << 20),
        name="attend",
    )(doc_bounds, mine)


def take_call(back):
    return pl.pallas_call(
        take_kernel,
        out_shape=jax.ShapeDtypeStruct((TOK, HD, HEADS), jnp.bfloat16),
        in_specs=[VMEM],
        out_specs=HBM,
        scratch_shapes=[
            pltpu.VMEM((ROWS, HEADS, 128), jnp.bfloat16),
            pltpu.VMEM((TOK, HD, HEADS), jnp.bfloat16),
            pltpu.SemaphoreType.DMA((4,)),
        ],
        compiler_params=pltpu.CompilerParams(vmem_limit_bytes=32 << 20),
        name="take_side",
    )(back)


def exchange(x, order):
    return lax.all_to_all(x, "run", split_axis=0, concat_axis=0, axis_index_groups=[order], tiled=True)


def body(queries, keys, values, doc_bounds, q_gain, k_gain):
    doc_bounds = doc_bounds.reshape(1, DOCS + 1)
    inputs = [jnp.transpose(x, (0, 2, 1)) for x in (queries, keys, values)]
    packed = send_call(doc_bounds, *inputs, q_gain, k_gain)
    mine = exchange(packed, ORDER_IN)
    result = attend_call(doc_bounds, mine)
    back = exchange(result, ORDER_OUT)
    return jnp.transpose(take_call(back), (0, 2, 1))


def solution(mesh):
    runs = jax.sharding.Mesh(mesh.devices.reshape(len(ORDER_IN), -1), ("run", "dp"))
    tokens = P(("dp", "run"), None, None)
    return jax.shard_map(
        body,
        mesh=runs,
        in_specs=(tokens, tokens, tokens, P("dp"), P(), P()),
        out_specs=tokens,
        check_vma=False,
    )
```

```python
import jax
import jax.numpy as jnp
from jax import lax
from jax.experimental import pallas as pl
from jax.experimental.pallas import tpu as pltpu
from jax.sharding import PartitionSpec as P

TOK = 32
ROWS = 16
HD = 64
HEADS = 128
DOCS = 8
SEQ = 4096
BLK = 256
PAIRS = BLK // 2
NBLK = SEQ // BLK
SRC = BLK // TOK
LONG, MIDDLE, SHORT = 16, 8, 4
FAR = (NBLK - 2) * (NBLK - 1) // 2 + LONG
NT = (((1,), (1,)), ((), ()))
NN = (((1,), (0,)), ((), ()))
BIG = 32768.0
SCALE = 1.4426950408889634 / 8.0
FIRST = -9.210340371976184


def run_of(z, x, c):
    return ((z % 8 * 2 + c) * 4 + x) * 2 + z // 8


FIRST_Z = [8, 7, 9, 6, 10, 5, 11, 4, 12, 3, 13, 2, 14, 1, 15, 0]
THEN_Z = [8, 15, 6, 13, 4, 11, 2, 9, 0, 7, 14, 5, 12, 3, 10, 1]
ORDER_IN = [run_of(z, x, c) for x in (2, 1, 3, 0) for z in FIRST_Z for c in range(2)]
ORDER_OUT = [run_of(z, x, c) for c in range(2) for z in THEN_Z for x in (2, 1, 3, 0)]
PLACE_IN = [ORDER_IN.index(s) for s in range(len(ORDER_IN))]
PLACE_OUT = [ORDER_OUT.index(s) for s in range(len(ORDER_OUT))]


def dot(a, b, dims=NN):
    return lax.dot_general(a, b, dims, preferred_element_type=jnp.float32)


def starts_of(token, bound):
    start = jnp.zeros_like(token)
    for d in range(1, DOCS):
        start = jnp.where(token >= bound(d), bound(d), start)
    return start


def identity(n):
    row = lax.broadcasted_iota(jnp.int32, (n, n), 0)
    col = lax.broadcasted_iota(jnp.int32, (n, n), 1)
    return (row == col).astype(jnp.float32).astype(jnp.bfloat16)


def interleave():
    row = lax.broadcasted_iota(jnp.int32, (256, 256), 0)
    col = lax.broadcasted_iota(jnp.int32, (256, 256), 1)
    return (col == (row % 16) * 16 + row // 16).astype(jnp.float32).astype(jnp.bfloat16)


def send_kernel(
    bounds_hbm, q_hbm, k_hbm, v_hbm, qg_hbm, kg_hbm, o_ref, bounds_ref, x_ref, g_ref, rot, turned, sems
):
    arriving = [
        pltpu.make_async_copy(source, target, sems.at[n])
        for n, (source, target) in enumerate(
            (
                (bounds_hbm, bounds_ref),
                (qg_hbm, g_ref.at[0]),
                (kg_hbm, g_ref.at[1]),
                (q_hbm, x_ref.at[0]),
                (v_hbm, x_ref.at[2]),
                (k_hbm, x_ref.at[1]),
            )
        )
    ]
    for c in arriving:
        c.start()
    for c in arriving[:3]:
        c.wait()
    lane = lax.broadcasted_iota(jnp.int32, (HD // 2, 128), 1)
    token = lax.axis_index("run") * TOK + lane
    start = starts_of(token, lambda d: bounds_ref[:, d : d + 1])
    place = (token - start).astype(jnp.float32)
    index = lax.broadcasted_iota(jnp.int32, (HD // 2, 128), 0).astype(jnp.float32)
    angle = place * jnp.exp(jnp.float32(FIRST) * index * 2.0 / HD)
    cosine = jnp.cos(angle)
    sine = jnp.sin(angle)
    eye = identity(HEADS)
    mix = interleave()

    def turn(n, r, rows):
        both = dot(eye, rows, NT).astype(jnp.bfloat16)
        turned[n, r] = both[:, :128]
        turned[n, r + 1] = both[:, 128:]

    def rotate(n):
        gain = jnp.transpose(jnp.broadcast_to(g_ref[n], (HEADS, HD)))
        for r in range(0, ROWS, 2):
            for t in (r, r + ROWS, r + 1, r + 1 + ROWS):
                c = jnp.broadcast_to(cosine[:, t : t + 1], (HD // 2, HEADS))
                s = jnp.broadcast_to(sine[:, t : t + 1], (HD // 2, HEADS))
                x = x_ref[n, t].astype(jnp.float32)
                scale = lax.rsqrt(jnp.mean(x * x, axis=0, keepdims=True) + 1e-06)
                x = x * scale * gain
                a, b = x[: HD // 2], x[HD // 2 :]
                y = jnp.concatenate([a * c - b * s, a * s + b * c], axis=0)
                rot[n, t % ROWS, pl.ds((t // ROWS) * HD, HD), :] = y.astype(jnp.bfloat16)
            turn(n, r, rot[n, r : r + 2].reshape(256, HEADS))

    def spread(n):
        for h in range(0, HEADS, 32):
            part = jnp.concatenate([turned[n, :, h + m : h + m + 16, :].reshape(256, 128) for m in (0, 16)], axis=1)
            both = dot(mix, part).astype(jnp.bfloat16)
            for m in range(2):
                heads = slice(h + 16 * m, h + 16 * m + 16)
                o_ref[heads, 16 * n : 16 * n + 16, :] = both[:, 128 * m : 128 * m + 128].reshape(16, 16, 128)

    for c in arriving[3:]:
        c.wait()

    def turn_values():
        for r in range(0, ROWS, 2):
            turn(2, r, jnp.concatenate([x_ref[2, t] for t in (r, r + ROWS, r + 1, r + 1 + ROWS)], axis=0))

    turn_values()
    rotate(0)
    spread(2)
    rotate(1)
    spread(0)
    spread(1)


def attend_kernel(bounds_ref, x_ref, o_ref, qt, kt, kf, vt, near, far, total, summed, items):

    def offsets(shape, axis):
        n = lax.broadcasted_iota(jnp.int32, shape, axis)
        return ((n % PAIRS) // 16) * 32 + n % 16 + (n // PAIRS) * 16

    below = offsets((BLK, BLK), 0) <= offsets((BLK, BLK), 1)
    q_off = offsets((16, BLK), 1)
    k_off = offsets((BLK, 128), 0)

    def bounds_along(shape, axis):
        n = lax.broadcasted_iota(jnp.int32, shape, axis)
        out = jnp.full(shape, SEQ, jnp.int32)
        for d in range(1, DOCS):
            out = jnp.where(n == d, bounds_ref[:, d : d + 1], out)
        return out

    q_bounds = bounds_along((16, BLK), 0)
    k_bounds = bounds_along((1, 128), 1)

    zero = jnp.zeros((HD, BLK), jnp.bfloat16)
    rest = jnp.zeros((128 - 16, BLK), jnp.bfloat16)

    def wide(x):
        t = jnp.transpose(x.astype(jnp.float32)).astype(jnp.bfloat16)
        return jnp.concatenate([t[:HD], t[HD:]], axis=1)

    def scores(j, q, flags):
        k2 = kt[j]
        low = dot(jnp.concatenate([k2, kf[j, :PAIRS]], axis=1), jnp.concatenate([q, zero, flags, rest], axis=0))
        high = dot(jnp.concatenate([k2, kf[j, PAIRS:]], axis=1), jnp.concatenate([zero, q, flags, rest], axis=0))
        return jnp.exp2(jnp.concatenate([low, high], axis=0) * jnp.float32(SCALE))

    def flags_of(i):
        return jnp.where(BLK * i + q_off >= q_bounds, jnp.float32(-BIG), jnp.float32(0.0)).astype(jnp.bfloat16)

    def partial_sum(e):
        return jnp.sum(e.reshape(BLK // 8, 8, BLK), axis=0)

    def tiles(i, row):
        runs = range(SRC * i, SRC * i + SRC)
        return jnp.concatenate([x_ref[PLACE_IN[s], row : row + 16, :] for s in runs], axis=0)

    def near_scores(blocks):
        for i in blocks:
            q = wide(tiles(i, 0))
            kt[i] = tiles(i, 16)
            qt[i] = q
            vt[i] = wide(tiles(i, 32))
            flags = flags_of(i)
            kf[i] = jnp.where(BLK * i + k_off < k_bounds, jnp.float32(1.0), jnp.float32(0.0)).astype(jnp.bfloat16)
            e1 = jnp.where(below, scores(i, q, flags), jnp.float32(0.0))
            e0 = scores(max(i - 1, 0), q, flags)
            if i == 0:
                e0 = jnp.zeros_like(e0)
            near[i, 0] = e0
            near[i, 1] = e1
            total[i] = partial_sum(e0) + partial_sum(e1)

    scalars = [jnp.max(bounds_ref[:, d : d + 1]) for d in range(DOCS)]
    n_far = jnp.int32(0)
    for i in range(2, NBLK):
        start = starts_of(jnp.int32(BLK * i), lambda d: scalars[d])
        for j in range(i - 2, -1, -1):
            items[n_far] = NBLK * i + j
            n_far += (start < BLK * (j + 1)).astype(jnp.int32)
    near_scores(range(NBLK))
    for u in range(LONG - 1):
        items[n_far + u] = NBLK * NBLK
    trips = (n_far + LONG - MIDDLE - 1) // LONG
    left = n_far - LONG * trips
    passes = (
        (0, trips, LONG),
        (LONG * trips, (left > SHORT).astype(jnp.int32), MIDDLE),
        (LONG * trips, ((left > 0) & (left <= SHORT)).astype(jnp.int32), SHORT),
    )

    def far_blocks(work):
        for begin, trips, length in passes:

            def trip(w, _, begin=begin, length=length):
                for u in range(length):
                    n = begin + length * w + u
                    work(n, items[n] >> 4, items[n] & 15)
                return 0

            lax.fori_loop(0, trips, trip, 0)

    def far_scores(n, i, j):
        e = scores(j, qt[i], flags_of(i))
        far[n] = e
        total[i] += partial_sum(e)

    far_blocks(far_scores)
    for i in range(NBLK):
        inverse = 1.0 / jnp.sum(total[i], axis=0, keepdims=True)
        total[i] = jnp.broadcast_to(inverse, (8, BLK))
        summed[i] = jnp.zeros((HD, BLK), jnp.float32)

    def far_values(n, i, j):
        summed[i] += dot(vt[j], (far[n] * total[i][0:1]).astype(jnp.bfloat16))

    far_blocks(far_values)

    for i in range(NBLK):
        w = jnp.concatenate([(near[i, n] * total[i][0:1]).astype(jnp.bfloat16) for n in range(2)], axis=0)
        out = dot(jnp.concatenate([vt[max(i - 1, 0)], vt[i]], axis=1), w) + summed[i]
        both = jnp.transpose(jnp.concatenate([out[:, :PAIRS], out[:, PAIRS:]], axis=0))
        both = both.astype(jnp.bfloat16)
        for n in range(SRC):
            o_ref[PLACE_OUT[SRC * i + n]] = both[16 * n : 16 * n + 16]


def take_kernel(x_ref, o_hbm, turned, out, sems):
    mix = interleave()
    eye = identity(128)
    for h in range(0, HEADS, 32):
        tiles = [x_ref[PLACE_OUT[s]] for s in ORDER_IN[h : h + 32]]
        part = jnp.concatenate([jnp.concatenate(tiles[m : m + 16], axis=0) for m in (0, 16)], axis=1)
        both = dot(mix, part).astype(jnp.bfloat16)
        for m in range(2):
            turned[:, h + 16 * m : h + 16 * m + 16, :] = both[:, 128 * m : 128 * m + 128].reshape(16, 16, 128)
    copies = []
    for r in range(0, ROWS, 2):
        both = dot(eye, turned[r : r + 2].reshape(256, 128), NT).astype(jnp.bfloat16)
        for m in range(2):
            out[r + m] = both[:HD, 128 * m : 128 * m + 128]
            out[r + m + ROWS] = both[HD:, 128 * m : 128 * m + 128]
        if r % 8 == 6:
            for first in (r - 6, r - 6 + ROWS):
                copy = pltpu.make_async_copy(
                    out.at[pl.ds(first, 8)], o_hbm.at[pl.ds(first, 8)], sems.at[len(copies)]
                )
                copy.start()
                copies.append(copy)
    for copy in copies:
        copy.wait()


VMEM = pl.BlockSpec(memory_space=pltpu.VMEM)
HBM = pl.BlockSpec(memory_space=pltpu.HBM)


def in_hbm(x):
    return pltpu.with_memory_space_constraint(x, pltpu.HBM)


def send_call(doc_bounds, q, k, v, q_gain, k_gain):
    return pl.pallas_call(
        send_kernel,
        out_shape=jax.ShapeDtypeStruct((HEADS, 48, 128), jnp.bfloat16),
        in_specs=[HBM] * 6,
        out_specs=VMEM,
        scratch_shapes=[
            pltpu.VMEM((1, DOCS + 1), jnp.int32),
            pltpu.VMEM((3, TOK, HD, HEADS), jnp.bfloat16),
            pltpu.VMEM((2, 1, HD), jnp.float32),
            pltpu.VMEM((2, ROWS, 128, HEADS), jnp.bfloat16),
            pltpu.VMEM((3, ROWS, HEADS, 128), jnp.bfloat16),
            pltpu.SemaphoreType.DMA((6,)),
        ],
        compiler_params=pltpu.CompilerParams(vmem_limit_bytes=32 << 20),
        name="send_side",
    )(*(in_hbm(x) for x in (doc_bounds, q, k, v, q_gain.reshape(1, HD), k_gain.reshape(1, HD))))


def attend_call(doc_bounds, mine):
    return pl.pallas_call(
        attend_kernel,
        out_shape=jax.ShapeDtypeStruct((SEQ // TOK, ROWS, 128), jnp.bfloat16),
        in_specs=[VMEM, VMEM],
        out_specs=VMEM,
        scratch_shapes=[
            pltpu.VMEM((NBLK + 1, HD, BLK), jnp.bfloat16),
            pltpu.VMEM((NBLK, PAIRS, 128), jnp.bfloat16),
            pltpu.VMEM((NBLK, BLK, 128), jnp.bfloat16),
            pltpu.VMEM((NBLK, HD, BLK), jnp.bfloat16),
            pltpu.VMEM((NBLK, 2, BLK, BLK), jnp.float32),
            pltpu.VMEM((FAR, BLK, BLK), jnp.float32),
            pltpu.VMEM((NBLK + 1, 8, BLK), jnp.float32),
            pltpu.VMEM((NBLK + 1, HD, BLK), jnp.float32),
            pltpu.SMEM((FAR,), jnp.int32),
        ],
        compiler_params=pltpu.CompilerParams(vmem_limit_bytes=44 << 20),
        name="attend",
    )(doc_bounds, mine)


def take_call(back):
    return pl.pallas_call(
        take_kernel,
        out_shape=jax.ShapeDtypeStruct((TOK, HD, HEADS), jnp.bfloat16),
        in_specs=[VMEM],
        out_specs=HBM,
        scratch_shapes=[
            pltpu.VMEM((ROWS, HEADS, 128), jnp.bfloat16),
            pltpu.VMEM((TOK, HD, HEADS), jnp.bfloat16),
            pltpu.SemaphoreType.DMA((4,)),
        ],
        compiler_params=pltpu.CompilerParams(vmem_limit_bytes=32 << 20),
        name="take_side",
    )(back)


def exchange(x, order):
    return lax.all_to_all(x, "run", split_axis=0, concat_axis=0, axis_index_groups=[order], tiled=True)


def body(queries, keys, values, doc_bounds, q_gain, k_gain):
    doc_bounds = doc_bounds.reshape(1, DOCS + 1)
    inputs = [jnp.transpose(x, (0, 2, 1)) for x in (queries, keys, values)]
    packed = send_call(doc_bounds, *inputs, q_gain, k_gain)
    mine = exchange(packed, ORDER_IN)
    result = attend_call(doc_bounds, mine)
    back = exchange(result, ORDER_OUT)
    return jnp.transpose(take_call(back), (0, 2, 1))


def solution(mesh):
    runs = jax.sharding.Mesh(mesh.devices.reshape(len(ORDER_IN), -1), ("run", "dp"))
    tokens = P(("dp", "run"), None, None)
    return jax.shard_map(
        body,
        mesh=runs,
        in_specs=(tokens, tokens, tokens, P("dp"), P(), P()),
        out_specs=tokens,
        check_vma=False,
    )
```

```python
import jax
import jax.numpy as jnp
from jax import lax
from jax.experimental import pallas as pl
from jax.experimental.pallas import tpu as pltpu
from jax.sharding import PartitionSpec as P

TOK = 32
ROWS = 16
HD = 64
HEADS = 128
DOCS = 8
SEQ = 4096
BLK = 256
PAIRS = BLK // 2
NBLK = SEQ // BLK
SRC = BLK // TOK
LONG, MIDDLE, SHORT = 16, 8, 4
FAR = (NBLK - 2) * (NBLK - 1) // 2 + LONG
NT = (((1,), (1,)), ((), ()))
NN = (((1,), (0,)), ((), ()))
BIG = 32768.0
SCALE = 1.4426950408889634 / 8.0
FIRST = -9.210340371976184


def run_of(z, x, c):
    return ((z % 8 * 2 + c) * 4 + x) * 2 + z // 8


FIRST_Z = [8, 15, 6, 13, 4, 11, 2, 9, 0, 7, 14, 5, 12, 3, 10, 1]
THEN_Z = [8, 15, 6, 13, 4, 11, 2, 9, 0, 7, 14, 5, 12, 3, 10, 1]
ORDER_IN = [run_of(z, x, c) for z in FIRST_Z for x in (2, 1, 3, 0) for c in range(2)]
ORDER_OUT = [run_of(z, x, c) for z in THEN_Z for x in (2, 1, 3, 0) for c in range(2)]
PLACE_IN = [ORDER_IN.index(s) for s in range(len(ORDER_IN))]
PLACE_OUT = [ORDER_OUT.index(s) for s in range(len(ORDER_OUT))]


def dot(a, b, dims=NN):
    return lax.dot_general(a, b, dims, preferred_element_type=jnp.float32)


def starts_of(token, bound):
    start = jnp.zeros_like(token)
    for d in range(1, DOCS):
        start = jnp.where(token >= bound(d), bound(d), start)
    return start


def identity(n):
    row = lax.broadcasted_iota(jnp.int32, (n, n), 0)
    col = lax.broadcasted_iota(jnp.int32, (n, n), 1)
    return (row == col).astype(jnp.float32).astype(jnp.bfloat16)


def interleave():
    row = lax.broadcasted_iota(jnp.int32, (256, 256), 0)
    col = lax.broadcasted_iota(jnp.int32, (256, 256), 1)
    return (col == (row % 16) * 16 + row // 16).astype(jnp.float32).astype(jnp.bfloat16)


def send_kernel(
    bounds_hbm, q_hbm, k_hbm, v_hbm, qg_hbm, kg_hbm, o_ref, bounds_ref, x_ref, g_ref, rot, turned, sems
):
    arriving = [
        pltpu.make_async_copy(source, target, sems.at[n])
        for n, (source, target) in enumerate(
            (
                (bounds_hbm, bounds_ref),
                (qg_hbm, g_ref.at[0]),
                (kg_hbm, g_ref.at[1]),
                (q_hbm, x_ref.at[0]),
                (v_hbm, x_ref.at[2]),
                (k_hbm, x_ref.at[1]),
            )
        )
    ]
    for c in arriving:
        c.start()
    for c in arriving[:3]:
        c.wait()
    lane = lax.broadcasted_iota(jnp.int32, (HD // 2, 128), 1)
    token = lax.axis_index("run") * TOK + lane
    start = starts_of(token, lambda d: bounds_ref[:, d : d + 1])
    place = (token - start).astype(jnp.float32)
    index = lax.broadcasted_iota(jnp.int32, (HD // 2, 128), 0).astype(jnp.float32)
    angle = place * jnp.exp(jnp.float32(FIRST) * index * 2.0 / HD)
    cosine = jnp.cos(angle)
    sine = jnp.sin(angle)
    eye = identity(HEADS)
    mix = interleave()

    def turn(n, r, rows):
        both = dot(eye, rows, NT).astype(jnp.bfloat16)
        turned[n, r] = both[:, :128]
        turned[n, r + 1] = both[:, 128:]

    def rotate(n):
        gain = jnp.transpose(jnp.broadcast_to(g_ref[n], (HEADS, HD)))
        for r in range(0, ROWS, 2):
            for t in (r, r + ROWS, r + 1, r + 1 + ROWS):
                c = jnp.broadcast_to(cosine[:, t : t + 1], (HD // 2, HEADS))
                s = jnp.broadcast_to(sine[:, t : t + 1], (HD // 2, HEADS))
                x = x_ref[n, t].astype(jnp.float32)
                scale = lax.rsqrt(jnp.mean(x * x, axis=0, keepdims=True) + 1e-06)
                x = x * scale * gain
                a, b = x[: HD // 2], x[HD // 2 :]
                y = jnp.concatenate([a * c - b * s, a * s + b * c], axis=0)
                rot[n, t % ROWS, pl.ds((t // ROWS) * HD, HD), :] = y.astype(jnp.bfloat16)
            turn(n, r, rot[n, r : r + 2].reshape(256, HEADS))

    def spread(n):
        for h in range(0, HEADS, 32):
            part = jnp.concatenate([turned[n, :, h + m : h + m + 16, :].reshape(256, 128) for m in (0, 16)], axis=1)
            both = dot(mix, part).astype(jnp.bfloat16)
            for m in range(2):
                heads = slice(h + 16 * m, h + 16 * m + 16)
                o_ref[heads, 16 * n : 16 * n + 16, :] = both[:, 128 * m : 128 * m + 128].reshape(16, 16, 128)

    for c in arriving[3:]:
        c.wait()

    def turn_values():
        for r in range(0, ROWS, 2):
            turn(2, r, jnp.concatenate([x_ref[2, t] for t in (r, r + ROWS, r + 1, r + 1 + ROWS)], axis=0))

    turn_values()
    rotate(0)
    spread(2)
    rotate(1)
    spread(0)
    spread(1)


def attend_kernel(bounds_ref, x_ref, o_ref, qt, kt, kf, vt, near, far, total, summed, items):

    def offsets(shape, axis):
        n = lax.broadcasted_iota(jnp.int32, shape, axis)
        return ((n % PAIRS) // 16) * 32 + n % 16 + (n // PAIRS) * 16

    below = offsets((BLK, BLK), 0) <= offsets((BLK, BLK), 1)
    q_off = offsets((16, BLK), 1)
    k_off = offsets((BLK, 128), 0)

    def bounds_along(shape, axis):
        n = lax.broadcasted_iota(jnp.int32, shape, axis)
        out = jnp.full(shape, SEQ, jnp.int32)
        for d in range(1, DOCS):
            out = jnp.where(n == d, bounds_ref[:, d : d + 1], out)
        return out

    q_bounds = bounds_along((16, BLK), 0)
    k_bounds = bounds_along((1, 128), 1)

    zero = jnp.zeros((HD, BLK), jnp.bfloat16)
    rest = jnp.zeros((128 - 16, BLK), jnp.bfloat16)

    def wide(x):
        t = jnp.transpose(x.astype(jnp.float32)).astype(jnp.bfloat16)
        return jnp.concatenate([t[:HD], t[HD:]], axis=1)

    def scores(j, q, flags):
        k2 = kt[j]
        low = dot(jnp.concatenate([k2, kf[j, :PAIRS]], axis=1), jnp.concatenate([q, zero, flags, rest], axis=0))
        high = dot(jnp.concatenate([k2, kf[j, PAIRS:]], axis=1), jnp.concatenate([zero, q, flags, rest], axis=0))
        return jnp.exp2(jnp.concatenate([low, high], axis=0) * jnp.float32(SCALE))

    def flags_of(i):
        return jnp.where(BLK * i + q_off >= q_bounds, jnp.float32(-BIG), jnp.float32(0.0)).astype(jnp.bfloat16)

    def partial_sum(e):
        return jnp.sum(e.reshape(BLK // 8, 8, BLK), axis=0)

    def tiles(i, row):
        runs = range(SRC * i, SRC * i + SRC)
        return jnp.concatenate([x_ref[PLACE_IN[s], row : row + 16, :] for s in runs], axis=0)

    def near_scores(blocks):
        for i in blocks:
            q = wide(tiles(i, 0))
            kt[i] = tiles(i, 16)
            qt[i] = q
            vt[i] = wide(tiles(i, 32))
            flags = flags_of(i)
            kf[i] = jnp.where(BLK * i + k_off < k_bounds, jnp.float32(1.0), jnp.float32(0.0)).astype(jnp.bfloat16)
            e1 = jnp.where(below, scores(i, q, flags), jnp.float32(0.0))
            e0 = scores(max(i - 1, 0), q, flags)
            if i == 0:
                e0 = jnp.zeros_like(e0)
            near[i, 0] = e0
            near[i, 1] = e1
            total[i] = partial_sum(e0) + partial_sum(e1)

    scalars = [jnp.max(bounds_ref[:, d : d + 1]) for d in range(DOCS)]
    n_far = jnp.int32(0)
    for i in range(2, NBLK):
        start = starts_of(jnp.int32(BLK * i), lambda d: scalars[d])
        for j in range(i - 2, -1, -1):
            items[n_far] = NBLK * i + j
            n_far += (start < BLK * (j + 1)).astype(jnp.int32)
    near_scores(range(NBLK))
    for u in range(LONG - 1):
        items[n_far + u] = NBLK * NBLK
    trips = (n_far + LONG - MIDDLE - 1) // LONG
    left = n_far - LONG * trips
    passes = (
        (0, trips, LONG),
        (LONG * trips, (left > SHORT).astype(jnp.int32), MIDDLE),
        (LONG * trips, ((left > 0) & (left <= SHORT)).astype(jnp.int32), SHORT),
    )

    def far_blocks(work):
        for begin, trips, length in passes:

            def trip(w, _, begin=begin, length=length):
                for u in range(length):
                    n = begin + length * w + u
                    work(n, items[n] >> 4, items[n] & 15)
                return 0

            lax.fori_loop(0, trips, trip, 0)

    def far_scores(n, i, j):
        e = scores(j, qt[i], flags_of(i))
        far[n] = e
        total[i] += partial_sum(e)

    far_blocks(far_scores)
    for i in range(NBLK):
        inverse = 1.0 / jnp.sum(total[i], axis=0, keepdims=True)
        total[i] = jnp.broadcast_to(inverse, (8, BLK))
        summed[i] = jnp.zeros((HD, BLK), jnp.float32)

    def far_values(n, i, j):
        summed[i] += dot(vt[j], (far[n] * total[i][0:1]).astype(jnp.bfloat16))

    far_blocks(far_values)

    for i in range(NBLK):
        w = jnp.concatenate([(near[i, n] * total[i][0:1]).astype(jnp.bfloat16) for n in range(2)], axis=0)
        out = dot(jnp.concatenate([vt[max(i - 1, 0)], vt[i]], axis=1), w) + summed[i]
        both = jnp.transpose(jnp.concatenate([out[:, :PAIRS], out[:, PAIRS:]], axis=0))
        both = both.astype(jnp.bfloat16)
        for n in range(SRC):
            o_ref[PLACE_OUT[SRC * i + n]] = both[16 * n : 16 * n + 16]


def take_kernel(x_ref, o_hbm, turned, out, sems):
    mix = interleave()
    eye = identity(128)
    for h in range(0, HEADS, 32):
        tiles = [x_ref[PLACE_OUT[s]] for s in ORDER_IN[h : h + 32]]
        part = jnp.concatenate([jnp.concatenate(tiles[m : m + 16], axis=0) for m in (0, 16)], axis=1)
        both = dot(mix, part).astype(jnp.bfloat16)
        for m in range(2):
            turned[:, h + 16 * m : h + 16 * m + 16, :] = both[:, 128 * m : 128 * m + 128].reshape(16, 16, 128)
    copies = []
    for r in range(0, ROWS, 2):
        both = dot(eye, turned[r : r + 2].reshape(256, 128), NT).astype(jnp.bfloat16)
        for m in range(2):
            out[r + m] = both[:HD, 128 * m : 128 * m + 128]
            out[r + m + ROWS] = both[HD:, 128 * m : 128 * m + 128]
        if r % 8 == 6:
            for first in (r - 6, r - 6 + ROWS):
                copy = pltpu.make_async_copy(
                    out.at[pl.ds(first, 8)], o_hbm.at[pl.ds(first, 8)], sems.at[len(copies)]
                )
                copy.start()
                copies.append(copy)
    for copy in copies:
        copy.wait()


VMEM = pl.BlockSpec(memory_space=pltpu.VMEM)
HBM = pl.BlockSpec(memory_space=pltpu.HBM)


def in_hbm(x):
    return pltpu.with_memory_space_constraint(x, pltpu.HBM)


def send_call(doc_bounds, q, k, v, q_gain, k_gain):
    return pl.pallas_call(
        send_kernel,
        out_shape=jax.ShapeDtypeStruct((HEADS, 48, 128), jnp.bfloat16),
        in_specs=[HBM] * 6,
        out_specs=VMEM,
        scratch_shapes=[
            pltpu.VMEM((1, DOCS + 1), jnp.int32),
            pltpu.VMEM((3, TOK, HD, HEADS), jnp.bfloat16),
            pltpu.VMEM((2, 1, HD), jnp.float32),
            pltpu.VMEM((2, ROWS, 128, HEADS), jnp.bfloat16),
            pltpu.VMEM((3, ROWS, HEADS, 128), jnp.bfloat16),
            pltpu.SemaphoreType.DMA((6,)),
        ],
        compiler_params=pltpu.CompilerParams(vmem_limit_bytes=32 << 20),
        name="send_side",
    )(*(in_hbm(x) for x in (doc_bounds, q, k, v, q_gain.reshape(1, HD), k_gain.reshape(1, HD))))


def attend_call(doc_bounds, mine):
    return pl.pallas_call(
        attend_kernel,
        out_shape=jax.ShapeDtypeStruct((SEQ // TOK, ROWS, 128), jnp.bfloat16),
        in_specs=[VMEM, VMEM],
        out_specs=VMEM,
        scratch_shapes=[
            pltpu.VMEM((NBLK + 1, HD, BLK), jnp.bfloat16),
            pltpu.VMEM((NBLK, PAIRS, 128), jnp.bfloat16),
            pltpu.VMEM((NBLK, BLK, 128), jnp.bfloat16),
            pltpu.VMEM((NBLK, HD, BLK), jnp.bfloat16),
            pltpu.VMEM((NBLK, 2, BLK, BLK), jnp.float32),
            pltpu.VMEM((FAR, BLK, BLK), jnp.float32),
            pltpu.VMEM((NBLK + 1, 8, BLK), jnp.float32),
            pltpu.VMEM((NBLK + 1, HD, BLK), jnp.float32),
            pltpu.SMEM((FAR,), jnp.int32),
        ],
        compiler_params=pltpu.CompilerParams(vmem_limit_bytes=44 << 20),
        name="attend",
    )(doc_bounds, mine)


def take_call(back):
    return pl.pallas_call(
        take_kernel,
        out_shape=jax.ShapeDtypeStruct((TOK, HD, HEADS), jnp.bfloat16),
        in_specs=[VMEM],
        out_specs=HBM,
        scratch_shapes=[
            pltpu.VMEM((ROWS, HEADS, 128), jnp.bfloat16),
            pltpu.VMEM((TOK, HD, HEADS), jnp.bfloat16),
            pltpu.SemaphoreType.DMA((4,)),
        ],
        compiler_params=pltpu.CompilerParams(vmem_limit_bytes=32 << 20),
        name="take_side",
    )(back)


def exchange(x, order):
    return lax.all_to_all(x, "run", split_axis=0, concat_axis=0, axis_index_groups=[order], tiled=True)


def body(queries, keys, values, doc_bounds, q_gain, k_gain):
    doc_bounds = doc_bounds.reshape(1, DOCS + 1)
    inputs = [jnp.transpose(x, (0, 2, 1)) for x in (queries, keys, values)]
    packed = send_call(doc_bounds, *inputs, q_gain, k_gain)
    mine = exchange(packed, ORDER_IN)
    result = attend_call(doc_bounds, mine)
    back = exchange(result, ORDER_OUT)
    return jnp.transpose(take_call(back), (0, 2, 1))


def solution(mesh):
    runs = jax.sharding.Mesh(mesh.devices.reshape(len(ORDER_IN), -1), ("run", "dp"))
    tokens = P(("dp", "run"), None, None)
    return jax.shard_map(
        body,
        mesh=runs,
        in_specs=(tokens, tokens, tokens, P("dp"), P(), P()),
        out_specs=tokens,
        check_vma=False,
    )
```

```python
import jax
import jax.numpy as jnp
from jax import lax
from jax.experimental import pallas as pl
from jax.experimental.pallas import tpu as pltpu
from jax.sharding import PartitionSpec as P

TOK = 32
ROWS = 16
HD = 64
HEADS = 128
DOCS = 8
SEQ = 4096
BLK = 256
PAIRS = BLK // 2
NBLK = SEQ // BLK
SRC = BLK // TOK
LONG, MIDDLE, SHORT = 16, 8, 4
FAR = (NBLK - 2) * (NBLK - 1) // 2 + LONG
NT = (((1,), (1,)), ((), ()))
NN = (((1,), (0,)), ((), ()))
BIG = 32768.0
SCALE = 1.4426950408889634 / 8.0
FIRST = -9.210340371976184


def run_of(z, x, c):
    return ((z % 8 * 2 + c) * 4 + x) * 2 + z // 8


FIRST_Z = [10, 5, 11, 4, 12, 3, 13, 2, 14, 1, 15, 0, 8, 7, 9, 6]
THEN_Z = [10, 1, 8, 15, 6, 13, 4, 11, 2, 9, 0, 7, 14, 5, 12, 3]
ORDER_IN = [run_of(z, x, c) for z in FIRST_Z for x in (2, 1, 3, 0) for c in range(2)]
ORDER_OUT = [run_of(z, x, c) for z in THEN_Z for x in (2, 1, 3, 0) for c in range(2)]
PLACE_IN = [ORDER_IN.index(s) for s in range(len(ORDER_IN))]
PLACE_OUT = [ORDER_OUT.index(s) for s in range(len(ORDER_OUT))]


def dot(a, b, dims=NN):
    return lax.dot_general(a, b, dims, preferred_element_type=jnp.float32)


def starts_of(token, bound):
    start = jnp.zeros_like(token)
    for d in range(1, DOCS):
        start = jnp.where(token >= bound(d), bound(d), start)
    return start


def identity(n):
    row = lax.broadcasted_iota(jnp.int32, (n, n), 0)
    col = lax.broadcasted_iota(jnp.int32, (n, n), 1)
    return (row == col).astype(jnp.float32).astype(jnp.bfloat16)


def interleave():
    row = lax.broadcasted_iota(jnp.int32, (256, 256), 0)
    col = lax.broadcasted_iota(jnp.int32, (256, 256), 1)
    return (col == (row % 16) * 16 + row // 16).astype(jnp.float32).astype(jnp.bfloat16)


def send_kernel(
    bounds_hbm, q_hbm, k_hbm, v_hbm, qg_hbm, kg_hbm, o_ref, bounds_ref, x_ref, g_ref, rot, turned, sems
):
    arriving = [
        pltpu.make_async_copy(source, target, sems.at[n])
        for n, (source, target) in enumerate(
            (
                (bounds_hbm, bounds_ref),
                (qg_hbm, g_ref.at[0]),
                (kg_hbm, g_ref.at[1]),
                (q_hbm, x_ref.at[0]),
                (v_hbm, x_ref.at[2]),
                (k_hbm, x_ref.at[1]),
            )
        )
    ]
    for c in arriving:
        c.start()
    for c in arriving[:3]:
        c.wait()
    lane = lax.broadcasted_iota(jnp.int32, (HD // 2, 128), 1)
    token = lax.axis_index("run") * TOK + lane
    start = starts_of(token, lambda d: bounds_ref[:, d : d + 1])
    place = (token - start).astype(jnp.float32)
    index = lax.broadcasted_iota(jnp.int32, (HD // 2, 128), 0).astype(jnp.float32)
    angle = place * jnp.exp(jnp.float32(FIRST) * index * 2.0 / HD)
    cosine = jnp.cos(angle)
    sine = jnp.sin(angle)
    eye = identity(HEADS)
    mix = interleave()

    def turn(n, r, rows):
        both = dot(eye, rows, NT).astype(jnp.bfloat16)
        turned[n, r] = both[:, :128]
        turned[n, r + 1] = both[:, 128:]

    def rotate(n):
        gain = jnp.transpose(jnp.broadcast_to(g_ref[n], (HEADS, HD)))
        for r in range(0, ROWS, 2):
            for t in (r, r + ROWS, r + 1, r + 1 + ROWS):
                c = jnp.broadcast_to(cosine[:, t : t + 1], (HD // 2, HEADS))
                s = jnp.broadcast_to(sine[:, t : t + 1], (HD // 2, HEADS))
                x = x_ref[n, t].astype(jnp.float32)
                scale = lax.rsqrt(jnp.mean(x * x, axis=0, keepdims=True) + 1e-06)
                x = x * scale * gain
                a, b = x[: HD // 2], x[HD // 2 :]
                y = jnp.concatenate([a * c - b * s, a * s + b * c], axis=0)
                rot[n, t % ROWS, pl.ds((t // ROWS) * HD, HD), :] = y.astype(jnp.bfloat16)
            turn(n, r, rot[n, r : r + 2].reshape(256, HEADS))

    def spread(n):
        for h in range(0, HEADS, 32):
            part = jnp.concatenate([turned[n, :, h + m : h + m + 16, :].reshape(256, 128) for m in (0, 16)], axis=1)
            both = dot(mix, part).astype(jnp.bfloat16)
            for m in range(2):
                heads = slice(h + 16 * m, h + 16 * m + 16)
                o_ref[heads, 16 * n : 16 * n + 16, :] = both[:, 128 * m : 128 * m + 128].reshape(16, 16, 128)

    for c in arriving[3:]:
        c.wait()

    def turn_values():
        for r in range(0, ROWS, 2):
            turn(2, r, jnp.concatenate([x_ref[2, t] for t in (r, r + ROWS, r + 1, r + 1 + ROWS)], axis=0))

    turn_values()
    rotate(0)
    spread(2)
    rotate(1)
    spread(0)
    spread(1)


def attend_kernel(bounds_ref, x_ref, o_ref, qt, kt, kf, vt, near, far, total, summed, items):

    def offsets(shape, axis):
        n = lax.broadcasted_iota(jnp.int32, shape, axis)
        return ((n % PAIRS) // 16) * 32 + n % 16 + (n // PAIRS) * 16

    below = offsets((BLK, BLK), 0) <= offsets((BLK, BLK), 1)
    q_off = offsets((16, BLK), 1)
    k_off = offsets((BLK, 128), 0)

    def bounds_along(shape, axis):
        n = lax.broadcasted_iota(jnp.int32, shape, axis)
        out = jnp.full(shape, SEQ, jnp.int32)
        for d in range(1, DOCS):
            out = jnp.where(n == d, bounds_ref[:, d : d + 1], out)
        return out

    q_bounds = bounds_along((16, BLK), 0)
    k_bounds = bounds_along((1, 128), 1)

    zero = jnp.zeros((HD, BLK), jnp.bfloat16)
    rest = jnp.zeros((128 - 16, BLK), jnp.bfloat16)

    def wide(x):
        t = jnp.transpose(x.astype(jnp.float32)).astype(jnp.bfloat16)
        return jnp.concatenate([t[:HD], t[HD:]], axis=1)

    def scores(j, q, flags):
        k2 = kt[j]
        low = dot(jnp.concatenate([k2, kf[j, :PAIRS]], axis=1), jnp.concatenate([q, zero, flags, rest], axis=0))
        high = dot(jnp.concatenate([k2, kf[j, PAIRS:]], axis=1), jnp.concatenate([zero, q, flags, rest], axis=0))
        return jnp.exp2(jnp.concatenate([low, high], axis=0) * jnp.float32(SCALE))

    def flags_of(i):
        return jnp.where(BLK * i + q_off >= q_bounds, jnp.float32(-BIG), jnp.float32(0.0)).astype(jnp.bfloat16)

    def partial_sum(e):
        return jnp.sum(e.reshape(BLK // 8, 8, BLK), axis=0)

    def tiles(i, row):
        runs = range(SRC * i, SRC * i + SRC)
        return jnp.concatenate([x_ref[PLACE_IN[s], row : row + 16, :] for s in runs], axis=0)

    def near_scores(blocks):
        for i in blocks:
            q = wide(tiles(i, 0))
            kt[i] = tiles(i, 16)
            qt[i] = q
            vt[i] = wide(tiles(i, 32))
            flags = flags_of(i)
            kf[i] = jnp.where(BLK * i + k_off < k_bounds, jnp.float32(1.0), jnp.float32(0.0)).astype(jnp.bfloat16)
            e1 = jnp.where(below, scores(i, q, flags), jnp.float32(0.0))
            e0 = scores(max(i - 1, 0), q, flags)
            if i == 0:
                e0 = jnp.zeros_like(e0)
            near[i, 0] = e0
            near[i, 1] = e1
            total[i] = partial_sum(e0) + partial_sum(e1)

    scalars = [jnp.max(bounds_ref[:, d : d + 1]) for d in range(DOCS)]
    n_far = jnp.int32(0)
    for i in range(2, NBLK):
        start = starts_of(jnp.int32(BLK * i), lambda d: scalars[d])
        for j in range(i - 2, -1, -1):
            items[n_far] = NBLK * i + j
            n_far += (start < BLK * (j + 1)).astype(jnp.int32)
    near_scores(range(NBLK))
    for u in range(LONG - 1):
        items[n_far + u] = NBLK * NBLK
    trips = (n_far + LONG - MIDDLE - 1) // LONG
    left = n_far - LONG * trips
    passes = (
        (0, trips, LONG),
        (LONG * trips, (left > SHORT).astype(jnp.int32), MIDDLE),
        (LONG * trips, ((left > 0) & (left <= SHORT)).astype(jnp.int32), SHORT),
    )

    def far_blocks(work):
        for begin, trips, length in passes:

            def trip(w, _, begin=begin, length=length):
                for u in range(length):
                    n = begin + length * w + u
                    work(n, items[n] >> 4, items[n] & 15)
                return 0

            lax.fori_loop(0, trips, trip, 0)

    def far_scores(n, i, j):
        e = scores(j, qt[i], flags_of(i))
        far[n] = e
        total[i] += partial_sum(e)

    far_blocks(far_scores)
    for i in range(NBLK):
        inverse = 1.0 / jnp.sum(total[i], axis=0, keepdims=True)
        total[i] = jnp.broadcast_to(inverse, (8, BLK))
        summed[i] = jnp.zeros((HD, BLK), jnp.float32)

    def far_values(n, i, j):
        summed[i] += dot(vt[j], (far[n] * total[i][0:1]).astype(jnp.bfloat16))

    far_blocks(far_values)

    for i in range(NBLK):
        w = jnp.concatenate([(near[i, n] * total[i][0:1]).astype(jnp.bfloat16) for n in range(2)], axis=0)
        out = dot(jnp.concatenate([vt[max(i - 1, 0)], vt[i]], axis=1), w) + summed[i]
        both = jnp.transpose(jnp.concatenate([out[:, :PAIRS], out[:, PAIRS:]], axis=0))
        both = both.astype(jnp.bfloat16)
        for n in range(SRC):
            o_ref[PLACE_OUT[SRC * i + n]] = both[16 * n : 16 * n + 16]


def take_kernel(x_ref, o_hbm, turned, out, sems):
    mix = interleave()
    eye = identity(128)
    for h in range(0, HEADS, 32):
        tiles = [x_ref[PLACE_OUT[s]] for s in ORDER_IN[h : h + 32]]
        part = jnp.concatenate([jnp.concatenate(tiles[m : m + 16], axis=0) for m in (0, 16)], axis=1)
        both = dot(mix, part).astype(jnp.bfloat16)
        for m in range(2):
            turned[:, h + 16 * m : h + 16 * m + 16, :] = both[:, 128 * m : 128 * m + 128].reshape(16, 16, 128)
    copies = []
    for r in range(0, ROWS, 2):
        both = dot(eye, turned[r : r + 2].reshape(256, 128), NT).astype(jnp.bfloat16)
        for m in range(2):
            out[r + m] = both[:HD, 128 * m : 128 * m + 128]
            out[r + m + ROWS] = both[HD:, 128 * m : 128 * m + 128]
        if r % 8 == 6:
            for first in (r - 6, r - 6 + ROWS):
                copy = pltpu.make_async_copy(
                    out.at[pl.ds(first, 8)], o_hbm.at[pl.ds(first, 8)], sems.at[len(copies)]
                )
                copy.start()
                copies.append(copy)
    for copy in copies:
        copy.wait()


VMEM = pl.BlockSpec(memory_space=pltpu.VMEM)
HBM = pl.BlockSpec(memory_space=pltpu.HBM)


def in_hbm(x):
    return pltpu.with_memory_space_constraint(x, pltpu.HBM)


def send_call(doc_bounds, q, k, v, q_gain, k_gain):
    return pl.pallas_call(
        send_kernel,
        out_shape=jax.ShapeDtypeStruct((HEADS, 48, 128), jnp.bfloat16),
        in_specs=[HBM] * 6,
        out_specs=VMEM,
        scratch_shapes=[
            pltpu.VMEM((1, DOCS + 1), jnp.int32),
            pltpu.VMEM((3, TOK, HD, HEADS), jnp.bfloat16),
            pltpu.VMEM((2, 1, HD), jnp.float32),
            pltpu.VMEM((2, ROWS, 128, HEADS), jnp.bfloat16),
            pltpu.VMEM((3, ROWS, HEADS, 128), jnp.bfloat16),
            pltpu.SemaphoreType.DMA((6,)),
        ],
        compiler_params=pltpu.CompilerParams(vmem_limit_bytes=32 << 20),
        name="send_side",
    )(*(in_hbm(x) for x in (doc_bounds, q, k, v, q_gain.reshape(1, HD), k_gain.reshape(1, HD))))


def attend_call(doc_bounds, mine):
    return pl.pallas_call(
        attend_kernel,
        out_shape=jax.ShapeDtypeStruct((SEQ // TOK, ROWS, 128), jnp.bfloat16),
        in_specs=[VMEM, VMEM],
        out_specs=VMEM,
        scratch_shapes=[
            pltpu.VMEM((NBLK + 1, HD, BLK), jnp.bfloat16),
            pltpu.VMEM((NBLK, PAIRS, 128), jnp.bfloat16),
            pltpu.VMEM((NBLK, BLK, 128), jnp.bfloat16),
            pltpu.VMEM((NBLK, HD, BLK), jnp.bfloat16),
            pltpu.VMEM((NBLK, 2, BLK, BLK), jnp.float32),
            pltpu.VMEM((FAR, BLK, BLK), jnp.float32),
            pltpu.VMEM((NBLK + 1, 8, BLK), jnp.float32),
            pltpu.VMEM((NBLK + 1, HD, BLK), jnp.float32),
            pltpu.SMEM((FAR,), jnp.int32),
        ],
        compiler_params=pltpu.CompilerParams(vmem_limit_bytes=44 << 20),
        name="attend",
    )(doc_bounds, mine)


def take_call(back):
    return pl.pallas_call(
        take_kernel,
        out_shape=jax.ShapeDtypeStruct((TOK, HD, HEADS), jnp.bfloat16),
        in_specs=[VMEM],
        out_specs=HBM,
        scratch_shapes=[
            pltpu.VMEM((ROWS, HEADS, 128), jnp.bfloat16),
            pltpu.VMEM((TOK, HD, HEADS), jnp.bfloat16),
            pltpu.SemaphoreType.DMA((4,)),
        ],
        compiler_params=pltpu.CompilerParams(vmem_limit_bytes=32 << 20),
        name="take_side",
    )(back)


def exchange(x, order):
    return lax.all_to_all(x, "run", split_axis=0, concat_axis=0, axis_index_groups=[order], tiled=True)


def body(queries, keys, values, doc_bounds, q_gain, k_gain):
    doc_bounds = doc_bounds.reshape(1, DOCS + 1)
    inputs = [jnp.transpose(x, (0, 2, 1)) for x in (queries, keys, values)]
    packed = send_call(doc_bounds, *inputs, q_gain, k_gain)
    mine = exchange(packed, ORDER_IN)
    result = attend_call(doc_bounds, mine)
    back = exchange(result, ORDER_OUT)
    return jnp.transpose(take_call(back), (0, 2, 1))


def solution(mesh):
    runs = jax.sharding.Mesh(mesh.devices.reshape(len(ORDER_IN), -1), ("run", "dp"))
    tokens = P(("dp", "run"), None, None)
    return jax.shard_map(
        body,
        mesh=runs,
        in_specs=(tokens, tokens, tokens, P("dp"), P(), P()),
        out_specs=tokens,
        check_vma=False,
    )
```

```python
import jax
import jax.numpy as jnp
from jax import lax
from jax.experimental import pallas as pl
from jax.experimental.pallas import tpu as pltpu
from jax.sharding import PartitionSpec as P

TOK = 32
ROWS = 16
HD = 64
HEADS = 128
DOCS = 8
SEQ = 4096
BLK = 256
PAIRS = BLK // 2
NBLK = SEQ // BLK
SRC = BLK // TOK
LONG, MIDDLE, SHORT = 16, 8, 4
FAR = (NBLK - 2) * (NBLK - 1) // 2 + LONG
NT = (((1,), (1,)), ((), ()))
NN = (((1,), (0,)), ((), ()))
BIG = 32768.0
SCALE = 1.4426950408889634 / 8.0
FIRST = -9.210340371976184


def run_of(z, x, c):
    return ((z % 8 * 2 + c) * 4 + x) * 2 + z // 8


FIRST_Z = [8, 7, 9, 6, 10, 5, 11, 4, 12, 3, 13, 2, 14, 1, 15, 0]
THEN_Z = [8, 15, 6, 13, 4, 11, 2, 9, 0, 7, 14, 5, 12, 3, 10, 1]
ORDER_IN = [run_of(z, x, c) for z in FIRST_Z for x in (2, 1, 3, 0) for c in range(2)]
ORDER_OUT = [run_of(z, x, c) for z in THEN_Z for x in (2, 1, 3, 0) for c in range(2)]
ORDER_IN, ORDER_OUT = ORDER_IN[1:] + ORDER_IN[:1], ORDER_OUT[1:] + ORDER_OUT[:1]
PLACE_IN = [ORDER_IN.index(s) for s in range(len(ORDER_IN))]
PLACE_OUT = [ORDER_OUT.index(s) for s in range(len(ORDER_OUT))]


def dot(a, b, dims=NN):
    return lax.dot_general(a, b, dims, preferred_element_type=jnp.float32)


def starts_of(token, bound):
    start = jnp.zeros_like(token)
    for d in range(1, DOCS):
        start = jnp.where(token >= bound(d), bound(d), start)
    return start


def identity(n):
    row = lax.broadcasted_iota(jnp.int32, (n, n), 0)
    col = lax.broadcasted_iota(jnp.int32, (n, n), 1)
    return (row == col).astype(jnp.float32).astype(jnp.bfloat16)


def interleave():
    row = lax.broadcasted_iota(jnp.int32, (256, 256), 0)
    col = lax.broadcasted_iota(jnp.int32, (256, 256), 1)
    return (col == (row % 16) * 16 + row // 16).astype(jnp.float32).astype(jnp.bfloat16)


def send_kernel(
    bounds_hbm, q_hbm, k_hbm, v_hbm, qg_hbm, kg_hbm, o_ref, bounds_ref, x_ref, g_ref, rot, turned, sems
):
    arriving = [
        pltpu.make_async_copy(source, target, sems.at[n])
        for n, (source, target) in enumerate(
            (
                (bounds_hbm, bounds_ref),
                (qg_hbm, g_ref.at[0]),
                (kg_hbm, g_ref.at[1]),
                (q_hbm, x_ref.at[0]),
                (v_hbm, x_ref.at[2]),
                (k_hbm, x_ref.at[1]),
            )
        )
    ]
    for c in arriving:
        c.start()
    for c in arriving[:3]:
        c.wait()
    lane = lax.broadcasted_iota(jnp.int32, (HD // 2, 128), 1)
    token = lax.axis_index("run") * TOK + lane
    start = starts_of(token, lambda d: bounds_ref[:, d : d + 1])
    place = (token - start).astype(jnp.float32)
    index = lax.broadcasted_iota(jnp.int32, (HD // 2, 128), 0).astype(jnp.float32)
    angle = place * jnp.exp(jnp.float32(FIRST) * index * 2.0 / HD)
    cosine = jnp.cos(angle)
    sine = jnp.sin(angle)
    eye = identity(HEADS)
    mix = interleave()

    def turn(n, r, rows):
        both = dot(eye, rows, NT).astype(jnp.bfloat16)
        turned[n, r] = both[:, :128]
        turned[n, r + 1] = both[:, 128:]

    def rotate(n):
        gain = jnp.transpose(jnp.broadcast_to(g_ref[n], (HEADS, HD)))
        for r in range(0, ROWS, 2):
            for t in (r, r + ROWS, r + 1, r + 1 + ROWS):
                c = jnp.broadcast_to(cosine[:, t : t + 1], (HD // 2, HEADS))
                s = jnp.broadcast_to(sine[:, t : t + 1], (HD // 2, HEADS))
                x = x_ref[n, t].astype(jnp.float32)
                scale = lax.rsqrt(jnp.mean(x * x, axis=0, keepdims=True) + 1e-06)
                x = x * scale * gain
                a, b = x[: HD // 2], x[HD // 2 :]
                y = jnp.concatenate([a * c - b * s, a * s + b * c], axis=0)
                rot[n, t % ROWS, pl.ds((t // ROWS) * HD, HD), :] = y.astype(jnp.bfloat16)
            turn(n, r, rot[n, r : r + 2].reshape(256, HEADS))

    def spread(n):
        for h in range(0, HEADS, 32):
            part = jnp.concatenate([turned[n, :, h + m : h + m + 16, :].reshape(256, 128) for m in (0, 16)], axis=1)
            both = dot(mix, part).astype(jnp.bfloat16)
            for m in range(2):
                heads = slice(h + 16 * m, h + 16 * m + 16)
                o_ref[heads, 16 * n : 16 * n + 16, :] = both[:, 128 * m : 128 * m + 128].reshape(16, 16, 128)

    for c in arriving[3:]:
        c.wait()

    def turn_values():
        for r in range(0, ROWS, 2):
            turn(2, r, jnp.concatenate([x_ref[2, t] for t in (r, r + ROWS, r + 1, r + 1 + ROWS)], axis=0))

    turn_values()
    rotate(0)
    spread(2)
    rotate(1)
    spread(0)
    spread(1)


def attend_kernel(bounds_ref, x_ref, o_ref, qt, kt, kf, vt, near, far, total, summed, items):

    def offsets(shape, axis):
        n = lax.broadcasted_iota(jnp.int32, shape, axis)
        return ((n % PAIRS) // 16) * 32 + n % 16 + (n // PAIRS) * 16

    below = offsets((BLK, BLK), 0) <= offsets((BLK, BLK), 1)
    q_off = offsets((16, BLK), 1)
    k_off = offsets((BLK, 128), 0)

    def bounds_along(shape, axis):
        n = lax.broadcasted_iota(jnp.int32, shape, axis)
        out = jnp.full(shape, SEQ, jnp.int32)
        for d in range(1, DOCS):
            out = jnp.where(n == d, bounds_ref[:, d : d + 1], out)
        return out

    q_bounds = bounds_along((16, BLK), 0)
    k_bounds = bounds_along((1, 128), 1)

    zero = jnp.zeros((HD, BLK), jnp.bfloat16)
    rest = jnp.zeros((128 - 16, BLK), jnp.bfloat16)

    def wide(x):
        t = jnp.transpose(x.astype(jnp.float32)).astype(jnp.bfloat16)
        return jnp.concatenate([t[:HD], t[HD:]], axis=1)

    def scores(j, q, flags):
        k2 = kt[j]
        low = dot(jnp.concatenate([k2, kf[j, :PAIRS]], axis=1), jnp.concatenate([q, zero, flags, rest], axis=0))
        high = dot(jnp.concatenate([k2, kf[j, PAIRS:]], axis=1), jnp.concatenate([zero, q, flags, rest], axis=0))
        return jnp.exp2(jnp.concatenate([low, high], axis=0) * jnp.float32(SCALE))

    def flags_of(i):
        return jnp.where(BLK * i + q_off >= q_bounds, jnp.float32(-BIG), jnp.float32(0.0)).astype(jnp.bfloat16)

    def partial_sum(e):
        return jnp.sum(e.reshape(BLK // 8, 8, BLK), axis=0)

    def tiles(i, row):
        runs = range(SRC * i, SRC * i + SRC)
        return jnp.concatenate([x_ref[PLACE_IN[s], row : row + 16, :] for s in runs], axis=0)

    def near_scores(blocks):
        for i in blocks:
            q = wide(tiles(i, 0))
            kt[i] = tiles(i, 16)
            qt[i] = q
            vt[i] = wide(tiles(i, 32))
            flags = flags_of(i)
            kf[i] = jnp.where(BLK * i + k_off < k_bounds, jnp.float32(1.0), jnp.float32(0.0)).astype(jnp.bfloat16)
            e1 = jnp.where(below, scores(i, q, flags), jnp.float32(0.0))
            e0 = scores(max(i - 1, 0), q, flags)
            if i == 0:
                e0 = jnp.zeros_like(e0)
            near[i, 0] = e0
            near[i, 1] = e1
            total[i] = partial_sum(e0) + partial_sum(e1)

    scalars = [jnp.max(bounds_ref[:, d : d + 1]) for d in range(DOCS)]
    n_far = jnp.int32(0)
    for i in range(2, NBLK):
        start = starts_of(jnp.int32(BLK * i), lambda d: scalars[d])
        for j in range(i - 2, -1, -1):
            items[n_far] = NBLK * i + j
            n_far += (start < BLK * (j + 1)).astype(jnp.int32)
    near_scores(range(NBLK))
    for u in range(LONG - 1):
        items[n_far + u] = NBLK * NBLK
    trips = (n_far + LONG - MIDDLE - 1) // LONG
    left = n_far - LONG * trips
    passes = (
        (0, trips, LONG),
        (LONG * trips, (left > SHORT).astype(jnp.int32), MIDDLE),
        (LONG * trips, ((left > 0) & (left <= SHORT)).astype(jnp.int32), SHORT),
    )

    def far_blocks(work):
        for begin, trips, length in passes:

            def trip(w, _, begin=begin, length=length):
                for u in range(length):
                    n = begin + length * w + u
                    work(n, items[n] >> 4, items[n] & 15)
                return 0

            lax.fori_loop(0, trips, trip, 0)

    def far_scores(n, i, j):
        e = scores(j, qt[i], flags_of(i))
        far[n] = e
        total[i] += partial_sum(e)

    far_blocks(far_scores)
    for i in range(NBLK):
        inverse = 1.0 / jnp.sum(total[i], axis=0, keepdims=True)
        total[i] = jnp.broadcast_to(inverse, (8, BLK))
        summed[i] = jnp.zeros((HD, BLK), jnp.float32)

    def far_values(n, i, j):
        summed[i] += dot(vt[j], (far[n] * total[i][0:1]).astype(jnp.bfloat16))

    far_blocks(far_values)

    for i in range(NBLK):
        w = jnp.concatenate([(near[i, n] * total[i][0:1]).astype(jnp.bfloat16) for n in range(2)], axis=0)
        out = dot(jnp.concatenate([vt[max(i - 1, 0)], vt[i]], axis=1), w) + summed[i]
        both = jnp.transpose(jnp.concatenate([out[:, :PAIRS], out[:, PAIRS:]], axis=0))
        both = both.astype(jnp.bfloat16)
        for n in range(SRC):
            o_ref[PLACE_OUT[SRC * i + n]] = both[16 * n : 16 * n + 16]


def take_kernel(x_ref, o_hbm, turned, out, sems):
    mix = interleave()
    eye = identity(128)
    for h in range(0, HEADS, 32):
        tiles = [x_ref[PLACE_OUT[s]] for s in ORDER_IN[h : h + 32]]
        part = jnp.concatenate([jnp.concatenate(tiles[m : m + 16], axis=0) for m in (0, 16)], axis=1)
        both = dot(mix, part).astype(jnp.bfloat16)
        for m in range(2):
            turned[:, h + 16 * m : h + 16 * m + 16, :] = both[:, 128 * m : 128 * m + 128].reshape(16, 16, 128)
    copies = []
    for r in range(0, ROWS, 2):
        both = dot(eye, turned[r : r + 2].reshape(256, 128), NT).astype(jnp.bfloat16)
        for m in range(2):
            out[r + m] = both[:HD, 128 * m : 128 * m + 128]
            out[r + m + ROWS] = both[HD:, 128 * m : 128 * m + 128]
        if r % 8 == 6:
            for first in (r - 6, r - 6 + ROWS):
                copy = pltpu.make_async_copy(
                    out.at[pl.ds(first, 8)], o_hbm.at[pl.ds(first, 8)], sems.at[len(copies)]
                )
                copy.start()
                copies.append(copy)
    for copy in copies:
        copy.wait()


VMEM = pl.BlockSpec(memory_space=pltpu.VMEM)
HBM = pl.BlockSpec(memory_space=pltpu.HBM)


def in_hbm(x):
    return pltpu.with_memory_space_constraint(x, pltpu.HBM)


def send_call(doc_bounds, q, k, v, q_gain, k_gain):
    return pl.pallas_call(
        send_kernel,
        out_shape=jax.ShapeDtypeStruct((HEADS, 48, 128), jnp.bfloat16),
        in_specs=[HBM] * 6,
        out_specs=VMEM,
        scratch_shapes=[
            pltpu.VMEM((1, DOCS + 1), jnp.int32),
            pltpu.VMEM((3, TOK, HD, HEADS), jnp.bfloat16),
            pltpu.VMEM((2, 1, HD), jnp.float32),
            pltpu.VMEM((2, ROWS, 128, HEADS), jnp.bfloat16),
            pltpu.VMEM((3, ROWS, HEADS, 128), jnp.bfloat16),
            pltpu.SemaphoreType.DMA((6,)),
        ],
        compiler_params=pltpu.CompilerParams(vmem_limit_bytes=32 << 20),
        name="send_side",
    )(*(in_hbm(x) for x in (doc_bounds, q, k, v, q_gain.reshape(1, HD), k_gain.reshape(1, HD))))


def attend_call(doc_bounds, mine):
    return pl.pallas_call(
        attend_kernel,
        out_shape=jax.ShapeDtypeStruct((SEQ // TOK, ROWS, 128), jnp.bfloat16),
        in_specs=[VMEM, VMEM],
        out_specs=VMEM,
        scratch_shapes=[
            pltpu.VMEM((NBLK + 1, HD, BLK), jnp.bfloat16),
            pltpu.VMEM((NBLK, PAIRS, 128), jnp.bfloat16),
            pltpu.VMEM((NBLK, BLK, 128), jnp.bfloat16),
            pltpu.VMEM((NBLK, HD, BLK), jnp.bfloat16),
            pltpu.VMEM((NBLK, 2, BLK, BLK), jnp.float32),
            pltpu.VMEM((FAR, BLK, BLK), jnp.float32),
            pltpu.VMEM((NBLK + 1, 8, BLK), jnp.float32),
            pltpu.VMEM((NBLK + 1, HD, BLK), jnp.float32),
            pltpu.SMEM((FAR,), jnp.int32),
        ],
        compiler_params=pltpu.CompilerParams(vmem_limit_bytes=44 << 20),
        name="attend",
    )(doc_bounds, mine)


def take_call(back):
    return pl.pallas_call(
        take_kernel,
        out_shape=jax.ShapeDtypeStruct((TOK, HD, HEADS), jnp.bfloat16),
        in_specs=[VMEM],
        out_specs=HBM,
        scratch_shapes=[
            pltpu.VMEM((ROWS, HEADS, 128), jnp.bfloat16),
            pltpu.VMEM((TOK, HD, HEADS), jnp.bfloat16),
            pltpu.SemaphoreType.DMA((4,)),
        ],
        compiler_params=pltpu.CompilerParams(vmem_limit_bytes=32 << 20),
        name="take_side",
    )(back)


def exchange(x, order):
    return lax.all_to_all(x, "run", split_axis=0, concat_axis=0, axis_index_groups=[order], tiled=True)


def body(queries, keys, values, doc_bounds, q_gain, k_gain):
    doc_bounds = doc_bounds.reshape(1, DOCS + 1)
    inputs = [jnp.transpose(x, (0, 2, 1)) for x in (queries, keys, values)]
    packed = send_call(doc_bounds, *inputs, q_gain, k_gain)
    mine = exchange(packed, ORDER_IN)
    result = attend_call(doc_bounds, mine)
    back = exchange(result, ORDER_OUT)
    return jnp.transpose(take_call(back), (0, 2, 1))


def solution(mesh):
    runs = jax.sharding.Mesh(mesh.devices.reshape(len(ORDER_IN), -1), ("run", "dp"))
    tokens = P(("dp", "run"), None, None)
    return jax.shard_map(
        body,
        mesh=runs,
        in_specs=(tokens, tokens, tokens, P("dp"), P(), P()),
        out_specs=tokens,
        check_vma=False,
    )
```

```python
import jax
import jax.numpy as jnp
from jax import lax
from jax.experimental import pallas as pl
from jax.experimental.pallas import tpu as pltpu
from jax.sharding import PartitionSpec as P

TOK = 32
ROWS = 16
HD = 64
HEADS = 128
DOCS = 8
SEQ = 4096
BLK = 256
PAIRS = BLK // 2
NBLK = SEQ // BLK
SRC = BLK // TOK
LONG, MIDDLE, SHORT = 20, 12, 6
FAR = (NBLK - 2) * (NBLK - 1) // 2 + LONG
NT = (((1,), (1,)), ((), ()))
NN = (((1,), (0,)), ((), ()))
BIG = 32768.0
SCALE = 1.4426950408889634 / 8.0
FIRST = -9.210340371976184


def run_of(z, x, c):
    return ((z % 8 * 2 + c) * 4 + x) * 2 + z // 8


FIRST_Z = [8, 7, 9, 6, 10, 5, 11, 4, 12, 3, 13, 2, 14, 1, 15, 0]
THEN_Z = [8, 15, 6, 13, 4, 11, 2, 9, 0, 7, 14, 5, 12, 3, 10, 1]
ORDER_IN = [run_of(z, x, c) for z in FIRST_Z for x in (2, 1, 3, 0) for c in range(2)]
ORDER_OUT = [run_of(z, x, c) for z in THEN_Z for x in (2, 1, 3, 0) for c in range(2)]
PLACE_IN = [ORDER_IN.index(s) for s in range(len(ORDER_IN))]
PLACE_OUT = [ORDER_OUT.index(s) for s in range(len(ORDER_OUT))]


def dot(a, b, dims=NN):
    return lax.dot_general(a, b, dims, preferred_element_type=jnp.float32)


def starts_of(token, bound):
    start = jnp.zeros_like(token)
    for d in range(1, DOCS):
        start = jnp.where(token >= bound(d), bound(d), start)
    return start


def identity(n):
    row = lax.broadcasted_iota(jnp.int32, (n, n), 0)
    col = lax.broadcasted_iota(jnp.int32, (n, n), 1)
    return (row == col).astype(jnp.float32).astype(jnp.bfloat16)


def interleave():
    row = lax.broadcasted_iota(jnp.int32, (256, 256), 0)
    col = lax.broadcasted_iota(jnp.int32, (256, 256), 1)
    return (col == (row % 16) * 16 + row // 16).astype(jnp.float32).astype(jnp.bfloat16)


def send_kernel(
    bounds_hbm, q_hbm, k_hbm, v_hbm, qg_hbm, kg_hbm, o_ref, bounds_ref, x_ref, g_ref, rot, turned, sems
):
    arriving = [
        pltpu.make_async_copy(source, target, sems.at[n])
        for n, (source, target) in enumerate(
            (
                (bounds_hbm, bounds_ref),
                (qg_hbm, g_ref.at[0]),
                (kg_hbm, g_ref.at[1]),
                (q_hbm, x_ref.at[0]),
                (v_hbm, x_ref.at[2]),
                (k_hbm, x_ref.at[1]),
            )
        )
    ]
    for c in arriving:
        c.start()
    for c in arriving[:3]:
        c.wait()
    lane = lax.broadcasted_iota(jnp.int32, (HD // 2, 128), 1)
    token = lax.axis_index("run") * TOK + lane
    start = starts_of(token, lambda d: bounds_ref[:, d : d + 1])
    place = (token - start).astype(jnp.float32)
    index = lax.broadcasted_iota(jnp.int32, (HD // 2, 128), 0).astype(jnp.float32)
    angle = place * jnp.exp(jnp.float32(FIRST) * index * 2.0 / HD)
    cosine = jnp.cos(angle)
    sine = jnp.sin(angle)
    eye = identity(HEADS)
    mix = interleave()

    def turn(n, r, rows):
        both = dot(eye, rows, NT).astype(jnp.bfloat16)
        turned[n, r] = both[:, :128]
        turned[n, r + 1] = both[:, 128:]

    def rotate(n):
        gain = jnp.transpose(jnp.broadcast_to(g_ref[n], (HEADS, HD)))
        for r in range(0, ROWS, 2):
            for t in (r, r + ROWS, r + 1, r + 1 + ROWS):
                c = jnp.broadcast_to(cosine[:, t : t + 1], (HD // 2, HEADS))
                s = jnp.broadcast_to(sine[:, t : t + 1], (HD // 2, HEADS))
                x = x_ref[n, t].astype(jnp.float32)
                scale = lax.rsqrt(jnp.mean(x * x, axis=0, keepdims=True) + 1e-06)
                x = x * scale * gain
                a, b = x[: HD // 2], x[HD // 2 :]
                y = jnp.concatenate([a * c - b * s, a * s + b * c], axis=0)
                rot[n, t % ROWS, pl.ds((t // ROWS) * HD, HD), :] = y.astype(jnp.bfloat16)
            turn(n, r, rot[n, r : r + 2].reshape(256, HEADS))

    def spread(n):
        for h in range(0, HEADS, 32):
            part = jnp.concatenate([turned[n, :, h + m : h + m + 16, :].reshape(256, 128) for m in (0, 16)], axis=1)
            both = dot(mix, part).astype(jnp.bfloat16)
            for m in range(2):
                heads = slice(h + 16 * m, h + 16 * m + 16)
                o_ref[heads, 16 * n : 16 * n + 16, :] = both[:, 128 * m : 128 * m + 128].reshape(16, 16, 128)

    for c in arriving[3:]:
        c.wait()

    def turn_values():
        for r in range(0, ROWS, 2):
            turn(2, r, jnp.concatenate([x_ref[2, t] for t in (r, r + ROWS, r + 1, r + 1 + ROWS)], axis=0))

    turn_values()
    rotate(0)
    spread(2)
    rotate(1)
    spread(0)
    spread(1)


def attend_kernel(bounds_ref, x_ref, o_ref, qt, kt, kf, vt, near, far, total, summed, items):

    def offsets(shape, axis):
        n = lax.broadcasted_iota(jnp.int32, shape, axis)
        return ((n % PAIRS) // 16) * 32 + n % 16 + (n // PAIRS) * 16

    below = offsets((BLK, BLK), 0) <= offsets((BLK, BLK), 1)
    q_off = offsets((16, BLK), 1)
    k_off = offsets((BLK, 128), 0)

    def bounds_along(shape, axis):
        n = lax.broadcasted_iota(jnp.int32, shape, axis)
        out = jnp.full(shape, SEQ, jnp.int32)
        for d in range(1, DOCS):
            out = jnp.where(n == d, bounds_ref[:, d : d + 1], out)
        return out

    q_bounds = bounds_along((16, BLK), 0)
    k_bounds = bounds_along((1, 128), 1)

    zero = jnp.zeros((HD, BLK), jnp.bfloat16)
    rest = jnp.zeros((128 - 16, BLK), jnp.bfloat16)

    def wide(x):
        t = jnp.transpose(x.astype(jnp.float32)).astype(jnp.bfloat16)
        return jnp.concatenate([t[:HD], t[HD:]], axis=1)

    def scores(j, q, flags):
        k2 = kt[j]
        low = dot(jnp.concatenate([k2, kf[j, :PAIRS]], axis=1), jnp.concatenate([q, zero, flags, rest], axis=0))
        high = dot(jnp.concatenate([k2, kf[j, PAIRS:]], axis=1), jnp.concatenate([zero, q, flags, rest], axis=0))
        return jnp.exp2(jnp.concatenate([low, high], axis=0) * jnp.float32(SCALE))

    def flags_of(i):
        return jnp.where(BLK * i + q_off >= q_bounds, jnp.float32(-BIG), jnp.float32(0.0)).astype(jnp.bfloat16)

    def partial_sum(e):
        return jnp.sum(e.reshape(BLK // 8, 8, BLK), axis=0)

    def tiles(i, row):
        runs = range(SRC * i, SRC * i + SRC)
        return jnp.concatenate([x_ref[PLACE_IN[s], row : row + 16, :] for s in runs], axis=0)

    def near_scores(blocks):
        for i in blocks:
            q = wide(tiles(i, 0))
            kt[i] = tiles(i, 16)
            qt[i] = q
            vt[i] = wide(tiles(i, 32))
            flags = flags_of(i)
            kf[i] = jnp.where(BLK * i + k_off < k_bounds, jnp.float32(1.0), jnp.float32(0.0)).astype(jnp.bfloat16)
            e1 = jnp.where(below, scores(i, q, flags), jnp.float32(0.0))
            e0 = scores(max(i - 1, 0), q, flags)
            if i == 0:
                e0 = jnp.zeros_like(e0)
            near[i, 0] = e0
            near[i, 1] = e1
            total[i] = partial_sum(e0) + partial_sum(e1)

    scalars = [jnp.max(bounds_ref[:, d : d + 1]) for d in range(DOCS)]
    n_far = jnp.int32(0)
    for i in range(2, NBLK):
        start = starts_of(jnp.int32(BLK * i), lambda d: scalars[d])
        for j in range(i - 2, -1, -1):
            items[n_far] = NBLK * i + j
            n_far += (start < BLK * (j + 1)).astype(jnp.int32)
    near_scores(range(NBLK))
    for u in range(LONG - 1):
        items[n_far + u] = NBLK * NBLK
    trips = (n_far + LONG - MIDDLE - 1) // LONG
    left = n_far - LONG * trips
    passes = (
        (0, trips, LONG),
        (LONG * trips, (left > SHORT).astype(jnp.int32), MIDDLE),
        (LONG * trips, ((left > 0) & (left <= SHORT)).astype(jnp.int32), SHORT),
    )

    def far_blocks(work):
        for begin, trips, length in passes:

            def trip(w, _, begin=begin, length=length):
                for u in range(length):
                    n = begin + length * w + u
                    work(n, items[n] >> 4, items[n] & 15)
                return 0

            lax.fori_loop(0, trips, trip, 0)

    def far_scores(n, i, j):
        e = scores(j, qt[i], flags_of(i))
        far[n] = e
        total[i] += partial_sum(e)

    far_blocks(far_scores)
    for i in range(NBLK):
        inverse = 1.0 / jnp.sum(total[i], axis=0, keepdims=True)
        total[i] = jnp.broadcast_to(inverse, (8, BLK))
        summed[i] = jnp.zeros((HD, BLK), jnp.float32)

    def far_values(n, i, j):
        summed[i] += dot(vt[j], (far[n] * total[i][0:1]).astype(jnp.bfloat16))

    far_blocks(far_values)

    for i in range(NBLK):
        w = jnp.concatenate([(near[i, n] * total[i][0:1]).astype(jnp.bfloat16) for n in range(2)], axis=0)
        out = dot(jnp.concatenate([vt[max(i - 1, 0)], vt[i]], axis=1), w) + summed[i]
        both = jnp.transpose(jnp.concatenate([out[:, :PAIRS], out[:, PAIRS:]], axis=0))
        both = both.astype(jnp.bfloat16)
        for n in range(SRC):
            o_ref[PLACE_OUT[SRC * i + n]] = both[16 * n : 16 * n + 16]


def take_kernel(x_ref, o_hbm, turned, out, sems):
    mix = interleave()
    eye = identity(128)
    for h in range(0, HEADS, 32):
        tiles = [x_ref[PLACE_OUT[s]] for s in ORDER_IN[h : h + 32]]
        part = jnp.concatenate([jnp.concatenate(tiles[m : m + 16], axis=0) for m in (0, 16)], axis=1)
        both = dot(mix, part).astype(jnp.bfloat16)
        for m in range(2):
            turned[:, h + 16 * m : h + 16 * m + 16, :] = both[:, 128 * m : 128 * m + 128].reshape(16, 16, 128)
    copies = []
    for r in range(0, ROWS, 2):
        both = dot(eye, turned[r : r + 2].reshape(256, 128), NT).astype(jnp.bfloat16)
        for m in range(2):
            out[r + m] = both[:HD, 128 * m : 128 * m + 128]
            out[r + m + ROWS] = both[HD:, 128 * m : 128 * m + 128]
        if r % 8 == 6:
            for first in (r - 6, r - 6 + ROWS):
                copy = pltpu.make_async_copy(
                    out.at[pl.ds(first, 8)], o_hbm.at[pl.ds(first, 8)], sems.at[len(copies)]
                )
                copy.start()
                copies.append(copy)
    for copy in copies:
        copy.wait()


VMEM = pl.BlockSpec(memory_space=pltpu.VMEM)
HBM = pl.BlockSpec(memory_space=pltpu.HBM)


def in_hbm(x):
    return pltpu.with_memory_space_constraint(x, pltpu.HBM)


def send_call(doc_bounds, q, k, v, q_gain, k_gain):
    return pl.pallas_call(
        send_kernel,
        out_shape=jax.ShapeDtypeStruct((HEADS, 48, 128), jnp.bfloat16),
        in_specs=[HBM] * 6,
        out_specs=VMEM,
        scratch_shapes=[
            pltpu.VMEM((1, DOCS + 1), jnp.int32),
            pltpu.VMEM((3, TOK, HD, HEADS), jnp.bfloat16),
            pltpu.VMEM((2, 1, HD), jnp.float32),
            pltpu.VMEM((2, ROWS, 128, HEADS), jnp.bfloat16),
            pltpu.VMEM((3, ROWS, HEADS, 128), jnp.bfloat16),
            pltpu.SemaphoreType.DMA((6,)),
        ],
        compiler_params=pltpu.CompilerParams(vmem_limit_bytes=32 << 20),
        name="send_side",
    )(*(in_hbm(x) for x in (doc_bounds, q, k, v, q_gain.reshape(1, HD), k_gain.reshape(1, HD))))


def attend_call(doc_bounds, mine):
    return pl.pallas_call(
        attend_kernel,
        out_shape=jax.ShapeDtypeStruct((SEQ // TOK, ROWS, 128), jnp.bfloat16),
        in_specs=[VMEM, VMEM],
        out_specs=VMEM,
        scratch_shapes=[
            pltpu.VMEM((NBLK + 1, HD, BLK), jnp.bfloat16),
            pltpu.VMEM((NBLK, PAIRS, 128), jnp.bfloat16),
            pltpu.VMEM((NBLK, BLK, 128), jnp.bfloat16),
            pltpu.VMEM((NBLK, HD, BLK), jnp.bfloat16),
            pltpu.VMEM((NBLK, 2, BLK, BLK), jnp.float32),
            pltpu.VMEM((FAR, BLK, BLK), jnp.float32),
            pltpu.VMEM((NBLK + 1, 8, BLK), jnp.float32),
            pltpu.VMEM((NBLK + 1, HD, BLK), jnp.float32),
            pltpu.SMEM((FAR,), jnp.int32),
        ],
        compiler_params=pltpu.CompilerParams(vmem_limit_bytes=44 << 20),
        name="attend",
    )(doc_bounds, mine)


def take_call(back):
    return pl.pallas_call(
        take_kernel,
        out_shape=jax.ShapeDtypeStruct((TOK, HD, HEADS), jnp.bfloat16),
        in_specs=[VMEM],
        out_specs=HBM,
        scratch_shapes=[
            pltpu.VMEM((ROWS, HEADS, 128), jnp.bfloat16),
            pltpu.VMEM((TOK, HD, HEADS), jnp.bfloat16),
            pltpu.SemaphoreType.DMA((4,)),
        ],
        compiler_params=pltpu.CompilerParams(vmem_limit_bytes=32 << 20),
        name="take_side",
    )(back)


def exchange(x, order):
    return lax.all_to_all(x, "run", split_axis=0, concat_axis=0, axis_index_groups=[order], tiled=True)


def body(queries, keys, values, doc_bounds, q_gain, k_gain):
    doc_bounds = doc_bounds.reshape(1, DOCS + 1)
    inputs = [jnp.transpose(x, (0, 2, 1)) for x in (queries, keys, values)]
    packed = send_call(doc_bounds, *inputs, q_gain, k_gain)
    mine = exchange(packed, ORDER_IN)
    result = attend_call(doc_bounds, mine)
    back = exchange(result, ORDER_OUT)
    return jnp.transpose(take_call(back), (0, 2, 1))


def solution(mesh):
    runs = jax.sharding.Mesh(mesh.devices.reshape(len(ORDER_IN), -1), ("run", "dp"))
    tokens = P(("dp", "run"), None, None)
    return jax.shard_map(
        body,
        mesh=runs,
        in_specs=(tokens, tokens, tokens, P("dp"), P(), P()),
        out_specs=tokens,
        check_vma=False,
    )
```

```python
import jax
import jax.numpy as jnp
from jax import lax
from jax.experimental import pallas as pl
from jax.experimental.pallas import tpu as pltpu
from jax.sharding import PartitionSpec as P

TOK = 32
ROWS = 16
HD = 64
HEADS = 128
DOCS = 8
SEQ = 4096
BLK = 256
PAIRS = BLK // 2
NBLK = SEQ // BLK
SRC = BLK // TOK
LONG, MIDDLE, SHORT = 20, 12, 6
FAR = (NBLK - 2) * (NBLK - 1) // 2 + LONG
NT = (((1,), (1,)), ((), ()))
NN = (((1,), (0,)), ((), ()))
BIG = 32768.0
SCALE = 1.4426950408889634 / 8.0
FIRST = -9.210340371976184


def run_of(z, x, c):
    return ((z % 8 * 2 + c) * 4 + x) * 2 + z // 8


FIRST_Z = [8, 7, 9, 6, 10, 5, 11, 4, 12, 3, 13, 2, 14, 1, 15, 0]
THEN_Z = [8, 15, 6, 13, 4, 11, 2, 9, 0, 7, 14, 5, 12, 3, 10, 1]
ORDER_IN = [run_of(z, x, c) for z in FIRST_Z for x in (2, 3, 1, 0) for c in range(2)]
ORDER_OUT = [run_of(z, x, c) for z in THEN_Z for x in (2, 3, 1, 0) for c in range(2)]
PLACE_IN = [ORDER_IN.index(s) for s in range(len(ORDER_IN))]
PLACE_OUT = [ORDER_OUT.index(s) for s in range(len(ORDER_OUT))]


def dot(a, b, dims=NN):
    return lax.dot_general(a, b, dims, preferred_element_type=jnp.float32)


def starts_of(token, bound):
    start = jnp.zeros_like(token)
    for d in range(1, DOCS):
        start = jnp.where(token >= bound(d), bound(d), start)
    return start


def identity(n):
    row = lax.broadcasted_iota(jnp.int32, (n, n), 0)
    col = lax.broadcasted_iota(jnp.int32, (n, n), 1)
    return (row == col).astype(jnp.float32).astype(jnp.bfloat16)


def interleave():
    row = lax.broadcasted_iota(jnp.int32, (256, 256), 0)
    col = lax.broadcasted_iota(jnp.int32, (256, 256), 1)
    return (col == (row % 16) * 16 + row // 16).astype(jnp.float32).astype(jnp.bfloat16)


def send_kernel(
    bounds_hbm, q_hbm, k_hbm, v_hbm, qg_hbm, kg_hbm, o_ref, bounds_ref, x_ref, g_ref, rot, turned, sems
):
    arriving = [
        pltpu.make_async_copy(source, target, sems.at[n])
        for n, (source, target) in enumerate(
            (
                (bounds_hbm, bounds_ref),
                (qg_hbm, g_ref.at[0]),
                (kg_hbm, g_ref.at[1]),
                (q_hbm, x_ref.at[0]),
                (v_hbm, x_ref.at[2]),
                (k_hbm, x_ref.at[1]),
            )
        )
    ]
    for c in arriving:
        c.start()
    for c in arriving[:3]:
        c.wait()
    lane = lax.broadcasted_iota(jnp.int32, (HD // 2, 128), 1)
    token = lax.axis_index("run") * TOK + lane
    start = starts_of(token, lambda d: bounds_ref[:, d : d + 1])
    place = (token - start).astype(jnp.float32)
    index = lax.broadcasted_iota(jnp.int32, (HD // 2, 128), 0).astype(jnp.float32)
    angle = place * jnp.exp(jnp.float32(FIRST) * index * 2.0 / HD)
    cosine = jnp.cos(angle)
    sine = jnp.sin(angle)
    eye = identity(HEADS)
    mix = interleave()

    def turn(n, r, rows):
        both = dot(eye, rows, NT).astype(jnp.bfloat16)
        turned[n, r] = both[:, :128]
        turned[n, r + 1] = both[:, 128:]

    def rotate(n):
        gain = jnp.transpose(jnp.broadcast_to(g_ref[n], (HEADS, HD)))
        for r in range(0, ROWS, 2):
            for t in (r, r + ROWS, r + 1, r + 1 + ROWS):
                c = jnp.broadcast_to(cosine[:, t : t + 1], (HD // 2, HEADS))
                s = jnp.broadcast_to(sine[:, t : t + 1], (HD // 2, HEADS))
                x = x_ref[n, t].astype(jnp.float32)
                scale = lax.rsqrt(jnp.mean(x * x, axis=0, keepdims=True) + 1e-06)
                x = x * scale * gain
                a, b = x[: HD // 2], x[HD // 2 :]
                y = jnp.concatenate([a * c - b * s, a * s + b * c], axis=0)
                rot[n, t % ROWS, pl.ds((t // ROWS) * HD, HD), :] = y.astype(jnp.bfloat16)
            turn(n, r, rot[n, r : r + 2].reshape(256, HEADS))

    def spread(n):
        for h in range(0, HEADS, 32):
            part = jnp.concatenate([turned[n, :, h + m : h + m + 16, :].reshape(256, 128) for m in (0, 16)], axis=1)
            both = dot(mix, part).astype(jnp.bfloat16)
            for m in range(2):
                heads = slice(h + 16 * m, h + 16 * m + 16)
                o_ref[heads, 16 * n : 16 * n + 16, :] = both[:, 128 * m : 128 * m + 128].reshape(16, 16, 128)

    for c in arriving[3:]:
        c.wait()

    def turn_values():
        for r in range(0, ROWS, 2):
            turn(2, r, jnp.concatenate([x_ref[2, t] for t in (r, r + ROWS, r + 1, r + 1 + ROWS)], axis=0))

    turn_values()
    rotate(0)
    spread(2)
    rotate(1)
    spread(0)
    spread(1)


def attend_kernel(bounds_ref, x_ref, o_ref, qt, kt, kf, vt, near, far, total, summed, items):

    def offsets(shape, axis):
        n = lax.broadcasted_iota(jnp.int32, shape, axis)
        return ((n % PAIRS) // 16) * 32 + n % 16 + (n // PAIRS) * 16

    below = offsets((BLK, BLK), 0) <= offsets((BLK, BLK), 1)
    q_off = offsets((16, BLK), 1)
    k_off = offsets((BLK, 128), 0)

    def bounds_along(shape, axis):
        n = lax.broadcasted_iota(jnp.int32, shape, axis)
        out = jnp.full(shape, SEQ, jnp.int32)
        for d in range(1, DOCS):
            out = jnp.where(n == d, bounds_ref[:, d : d + 1], out)
        return out

    q_bounds = bounds_along((16, BLK), 0)
    k_bounds = bounds_along((1, 128), 1)

    zero = jnp.zeros((HD, BLK), jnp.bfloat16)
    rest = jnp.zeros((128 - 16, BLK), jnp.bfloat16)

    def wide(x):
        t = jnp.transpose(x.astype(jnp.float32)).astype(jnp.bfloat16)
        return jnp.concatenate([t[:HD], t[HD:]], axis=1)

    def scores(j, q, flags):
        k2 = kt[j]
        low = dot(jnp.concatenate([k2, kf[j, :PAIRS]], axis=1), jnp.concatenate([q, zero, flags, rest], axis=0))
        high = dot(jnp.concatenate([k2, kf[j, PAIRS:]], axis=1), jnp.concatenate([zero, q, flags, rest], axis=0))
        return jnp.exp2(jnp.concatenate([low, high], axis=0) * jnp.float32(SCALE))

    def flags_of(i):
        return jnp.where(BLK * i + q_off >= q_bounds, jnp.float32(-BIG), jnp.float32(0.0)).astype(jnp.bfloat16)

    def partial_sum(e):
        return jnp.sum(e.reshape(BLK // 8, 8, BLK), axis=0)

    def tiles(i, row):
        runs = range(SRC * i, SRC * i + SRC)
        return jnp.concatenate([x_ref[PLACE_IN[s], row : row + 16, :] for s in runs], axis=0)

    def near_scores(blocks):
        for i in blocks:
            q = wide(tiles(i, 0))
            kt[i] = tiles(i, 16)
            qt[i] = q
            vt[i] = wide(tiles(i, 32))
            flags = flags_of(i)
            kf[i] = jnp.where(BLK * i + k_off < k_bounds, jnp.float32(1.0), jnp.float32(0.0)).astype(jnp.bfloat16)
            e1 = jnp.where(below, scores(i, q, flags), jnp.float32(0.0))
            e0 = scores(max(i - 1, 0), q, flags)
            if i == 0:
                e0 = jnp.zeros_like(e0)
            near[i, 0] = e0
            near[i, 1] = e1
            total[i] = partial_sum(e0) + partial_sum(e1)

    scalars = [jnp.max(bounds_ref[:, d : d + 1]) for d in range(DOCS)]
    n_far = jnp.int32(0)
    for i in range(2, NBLK):
        start = starts_of(jnp.int32(BLK * i), lambda d: scalars[d])
        for j in range(i - 2, -1, -1):
            items[n_far] = NBLK * i + j
            n_far += (start < BLK * (j + 1)).astype(jnp.int32)
    near_scores(range(NBLK))
    for u in range(LONG - 1):
        items[n_far + u] = NBLK * NBLK
    trips = (n_far + LONG - MIDDLE - 1) // LONG
    left = n_far - LONG * trips
    passes = (
        (0, trips, LONG),
        (LONG * trips, (left > SHORT).astype(jnp.int32), MIDDLE),
        (LONG * trips, ((left > 0) & (left <= SHORT)).astype(jnp.int32), SHORT),
    )

    def far_blocks(work):
        for begin, trips, length in passes:

            def trip(w, _, begin=begin, length=length):
                for u in range(length):
                    n = begin + length * w + u
                    work(n, items[n] >> 4, items[n] & 15)
                return 0

            lax.fori_loop(0, trips, trip, 0)

    def far_scores(n, i, j):
        e = scores(j, qt[i], flags_of(i))
        far[n] = e
        total[i] += partial_sum(e)

    far_blocks(far_scores)
    for i in range(NBLK):
        inverse = 1.0 / jnp.sum(total[i], axis=0, keepdims=True)
        total[i] = jnp.broadcast_to(inverse, (8, BLK))
        summed[i] = jnp.zeros((HD, BLK), jnp.float32)

    def far_values(n, i, j):
        summed[i] += dot(vt[j], (far[n] * total[i][0:1]).astype(jnp.bfloat16))

    far_blocks(far_values)

    for i in range(NBLK):
        w = jnp.concatenate([(near[i, n] * total[i][0:1]).astype(jnp.bfloat16) for n in range(2)], axis=0)
        out = dot(jnp.concatenate([vt[max(i - 1, 0)], vt[i]], axis=1), w) + summed[i]
        both = jnp.transpose(jnp.concatenate([out[:, :PAIRS], out[:, PAIRS:]], axis=0))
        both = both.astype(jnp.bfloat16)
        for n in range(SRC):
            o_ref[PLACE_OUT[SRC * i + n]] = both[16 * n : 16 * n + 16]


def take_kernel(x_ref, o_hbm, turned, out, sems):
    mix = interleave()
    eye = identity(128)
    for h in range(0, HEADS, 32):
        tiles = [x_ref[PLACE_OUT[s]] for s in ORDER_IN[h : h + 32]]
        part = jnp.concatenate([jnp.concatenate(tiles[m : m + 16], axis=0) for m in (0, 16)], axis=1)
        both = dot(mix, part).astype(jnp.bfloat16)
        for m in range(2):
            turned[:, h + 16 * m : h + 16 * m + 16, :] = both[:, 128 * m : 128 * m + 128].reshape(16, 16, 128)
    copies = []
    for r in range(0, ROWS, 2):
        both = dot(eye, turned[r : r + 2].reshape(256, 128), NT).astype(jnp.bfloat16)
        for m in range(2):
            out[r + m] = both[:HD, 128 * m : 128 * m + 128]
            out[r + m + ROWS] = both[HD:, 128 * m : 128 * m + 128]
        if r % 8 == 6:
            for first in (r - 6, r - 6 + ROWS):
                copy = pltpu.make_async_copy(
                    out.at[pl.ds(first, 8)], o_hbm.at[pl.ds(first, 8)], sems.at[len(copies)]
                )
                copy.start()
                copies.append(copy)
    for copy in copies:
        copy.wait()


VMEM = pl.BlockSpec(memory_space=pltpu.VMEM)
HBM = pl.BlockSpec(memory_space=pltpu.HBM)


def in_hbm(x):
    return pltpu.with_memory_space_constraint(x, pltpu.HBM)


def send_call(doc_bounds, q, k, v, q_gain, k_gain):
    return pl.pallas_call(
        send_kernel,
        out_shape=jax.ShapeDtypeStruct((HEADS, 48, 128), jnp.bfloat16),
        in_specs=[HBM] * 6,
        out_specs=VMEM,
        scratch_shapes=[
            pltpu.VMEM((1, DOCS + 1), jnp.int32),
            pltpu.VMEM((3, TOK, HD, HEADS), jnp.bfloat16),
            pltpu.VMEM((2, 1, HD), jnp.float32),
            pltpu.VMEM((2, ROWS, 128, HEADS), jnp.bfloat16),
            pltpu.VMEM((3, ROWS, HEADS, 128), jnp.bfloat16),
            pltpu.SemaphoreType.DMA((6,)),
        ],
        compiler_params=pltpu.CompilerParams(vmem_limit_bytes=32 << 20),
        name="send_side",
    )(*(in_hbm(x) for x in (doc_bounds, q, k, v, q_gain.reshape(1, HD), k_gain.reshape(1, HD))))


def attend_call(doc_bounds, mine):
    return pl.pallas_call(
        attend_kernel,
        out_shape=jax.ShapeDtypeStruct((SEQ // TOK, ROWS, 128), jnp.bfloat16),
        in_specs=[VMEM, VMEM],
        out_specs=VMEM,
        scratch_shapes=[
            pltpu.VMEM((NBLK + 1, HD, BLK), jnp.bfloat16),
            pltpu.VMEM((NBLK, PAIRS, 128), jnp.bfloat16),
            pltpu.VMEM((NBLK, BLK, 128), jnp.bfloat16),
            pltpu.VMEM((NBLK, HD, BLK), jnp.bfloat16),
            pltpu.VMEM((NBLK, 2, BLK, BLK), jnp.float32),
            pltpu.VMEM((FAR, BLK, BLK), jnp.float32),
            pltpu.VMEM((NBLK + 1, 8, BLK), jnp.float32),
            pltpu.VMEM((NBLK + 1, HD, BLK), jnp.float32),
            pltpu.SMEM((FAR,), jnp.int32),
        ],
        compiler_params=pltpu.CompilerParams(vmem_limit_bytes=44 << 20),
        name="attend",
    )(doc_bounds, mine)


def take_call(back):
    return pl.pallas_call(
        take_kernel,
        out_shape=jax.ShapeDtypeStruct((TOK, HD, HEADS), jnp.bfloat16),
        in_specs=[VMEM],
        out_specs=HBM,
        scratch_shapes=[
            pltpu.VMEM((ROWS, HEADS, 128), jnp.bfloat16),
            pltpu.VMEM((TOK, HD, HEADS), jnp.bfloat16),
            pltpu.SemaphoreType.DMA((4,)),
        ],
        compiler_params=pltpu.CompilerParams(vmem_limit_bytes=32 << 20),
        name="take_side",
    )(back)


def exchange(x, order):
    return lax.all_to_all(x, "run", split_axis=0, concat_axis=0, axis_index_groups=[order], tiled=True)


def body(queries, keys, values, doc_bounds, q_gain, k_gain):
    doc_bounds = doc_bounds.reshape(1, DOCS + 1)
    inputs = [jnp.transpose(x, (0, 2, 1)) for x in (queries, keys, values)]
    packed = send_call(doc_bounds, *inputs, q_gain, k_gain)
    mine = exchange(packed, ORDER_IN)
    result = attend_call(doc_bounds, mine)
    back = exchange(result, ORDER_OUT)
    return jnp.transpose(take_call(back), (0, 2, 1))


def solution(mesh):
    runs = jax.sharding.Mesh(mesh.devices.reshape(len(ORDER_IN), -1), ("run", "dp"))
    tokens = P(("dp", "run"), None, None)
    return jax.shard_map(
        body,
        mesh=runs,
        in_specs=(tokens, tokens, tokens, P("dp"), P(), P()),
        out_specs=tokens,
        check_vma=False,
    )
```

```python
import jax
import jax.numpy as jnp
from jax import lax
from jax.experimental import pallas as pl
from jax.experimental.pallas import tpu as pltpu
from jax.sharding import PartitionSpec as P

TOK = 32
ROWS = 16
HD = 64
HEADS = 128
DOCS = 8
SEQ = 4096
BLK = 256
PAIRS = BLK // 2
NBLK = SEQ // BLK
SRC = BLK // TOK
LONG, MIDDLE, SHORT = 20, 12, 6
FAR = (NBLK - 2) * (NBLK - 1) // 2 + LONG
NT = (((1,), (1,)), ((), ()))
NN = (((1,), (0,)), ((), ()))
BIG = 32768.0
SCALE = 1.4426950408889634 / 8.0
FIRST = -9.210340371976184


def run_of(z, x, c):
    return ((z % 8 * 2 + c) * 4 + x) * 2 + z // 8


FIRST_Z = [8, 9, 7, 10, 6, 11, 5, 12, 4, 13, 3, 14, 2, 15, 1, 0]
THEN_Z = [8, 15, 6, 13, 4, 11, 2, 9, 0, 7, 14, 5, 12, 3, 10, 1]
ORDER_IN = [run_of(z, x, c) for z in FIRST_Z for x in (2, 1, 3, 0) for c in range(2)]
ORDER_OUT = [run_of(z, x, c) for z in THEN_Z for x in (2, 1, 3, 0) for c in range(2)]
PLACE_IN = [ORDER_IN.index(s) for s in range(len(ORDER_IN))]
PLACE_OUT = [ORDER_OUT.index(s) for s in range(len(ORDER_OUT))]


def dot(a, b, dims=NN):
    return lax.dot_general(a, b, dims, preferred_element_type=jnp.float32)


def starts_of(token, bound):
    start = jnp.zeros_like(token)
    for d in range(1, DOCS):
        start = jnp.where(token >= bound(d), bound(d), start)
    return start


def identity(n):
    row = lax.broadcasted_iota(jnp.int32, (n, n), 0)
    col = lax.broadcasted_iota(jnp.int32, (n, n), 1)
    return (row == col).astype(jnp.float32).astype(jnp.bfloat16)


def interleave():
    row = lax.broadcasted_iota(jnp.int32, (256, 256), 0)
    col = lax.broadcasted_iota(jnp.int32, (256, 256), 1)
    return (col == (row % 16) * 16 + row // 16).astype(jnp.float32).astype(jnp.bfloat16)


def send_kernel(
    bounds_hbm, q_hbm, k_hbm, v_hbm, qg_hbm, kg_hbm, o_ref, bounds_ref, x_ref, g_ref, rot, turned, sems
):
    arriving = [
        pltpu.make_async_copy(source, target, sems.at[n])
        for n, (source, target) in enumerate(
            (
                (bounds_hbm, bounds_ref),
                (qg_hbm, g_ref.at[0]),
                (kg_hbm, g_ref.at[1]),
                (q_hbm, x_ref.at[0]),
                (v_hbm, x_ref.at[2]),
                (k_hbm, x_ref.at[1]),
            )
        )
    ]
    for c in arriving:
        c.start()
    for c in arriving[:3]:
        c.wait()
    lane = lax.broadcasted_iota(jnp.int32, (HD // 2, 128), 1)
    token = lax.axis_index("run") * TOK + lane
    start = starts_of(token, lambda d: bounds_ref[:, d : d + 1])
    place = (token - start).astype(jnp.float32)
    index = lax.broadcasted_iota(jnp.int32, (HD // 2, 128), 0).astype(jnp.float32)
    angle = place * jnp.exp(jnp.float32(FIRST) * index * 2.0 / HD)
    cosine = jnp.cos(angle)
    sine = jnp.sin(angle)
    eye = identity(HEADS)
    mix = interleave()

    def turn(n, r, rows):
        both = dot(eye, rows, NT).astype(jnp.bfloat16)
        turned[n, r] = both[:, :128]
        turned[n, r + 1] = both[:, 128:]

    def rotate(n):
        gain = jnp.transpose(jnp.broadcast_to(g_ref[n], (HEADS, HD)))
        for r in range(0, ROWS, 2):
            for t in (r, r + ROWS, r + 1, r + 1 + ROWS):
                c = jnp.broadcast_to(cosine[:, t : t + 1], (HD // 2, HEADS))
                s = jnp.broadcast_to(sine[:, t : t + 1], (HD // 2, HEADS))
                x = x_ref[n, t].astype(jnp.float32)
                scale = lax.rsqrt(jnp.mean(x * x, axis=0, keepdims=True) + 1e-06)
                x = x * scale * gain
                a, b = x[: HD // 2], x[HD // 2 :]
                y = jnp.concatenate([a * c - b * s, a * s + b * c], axis=0)
                rot[n, t % ROWS, pl.ds((t // ROWS) * HD, HD), :] = y.astype(jnp.bfloat16)
            turn(n, r, rot[n, r : r + 2].reshape(256, HEADS))

    def spread(n):
        for h in range(0, HEADS, 32):
            part = jnp.concatenate([turned[n, :, h + m : h + m + 16, :].reshape(256, 128) for m in (0, 16)], axis=1)
            both = dot(mix, part).astype(jnp.bfloat16)
            for m in range(2):
                heads = slice(h + 16 * m, h + 16 * m + 16)
                o_ref[heads, 16 * n : 16 * n + 16, :] = both[:, 128 * m : 128 * m + 128].reshape(16, 16, 128)

    for c in arriving[3:]:
        c.wait()

    def turn_values():
        for r in range(0, ROWS, 2):
            turn(2, r, jnp.concatenate([x_ref[2, t] for t in (r, r + ROWS, r + 1, r + 1 + ROWS)], axis=0))

    turn_values()
    rotate(0)
    spread(2)
    rotate(1)
    spread(0)
    spread(1)


def attend_kernel(bounds_ref, x_ref, o_ref, qt, kt, kf, vt, near, far, total, summed, items):

    def offsets(shape, axis):
        n = lax.broadcasted_iota(jnp.int32, shape, axis)
        return ((n % PAIRS) // 16) * 32 + n % 16 + (n // PAIRS) * 16

    below = offsets((BLK, BLK), 0) <= offsets((BLK, BLK), 1)
    q_off = offsets((16, BLK), 1)
    k_off = offsets((BLK, 128), 0)

    def bounds_along(shape, axis):
        n = lax.broadcasted_iota(jnp.int32, shape, axis)
        out = jnp.full(shape, SEQ, jnp.int32)
        for d in range(1, DOCS):
            out = jnp.where(n == d, bounds_ref[:, d : d + 1], out)
        return out

    q_bounds = bounds_along((16, BLK), 0)
    k_bounds = bounds_along((1, 128), 1)

    zero = jnp.zeros((HD, BLK), jnp.bfloat16)
    rest = jnp.zeros((128 - 16, BLK), jnp.bfloat16)

    def wide(x):
        t = jnp.transpose(x.astype(jnp.float32)).astype(jnp.bfloat16)
        return jnp.concatenate([t[:HD], t[HD:]], axis=1)

    def scores(j, q, flags):
        k2 = kt[j]
        low = dot(jnp.concatenate([k2, kf[j, :PAIRS]], axis=1), jnp.concatenate([q, zero, flags, rest], axis=0))
        high = dot(jnp.concatenate([k2, kf[j, PAIRS:]], axis=1), jnp.concatenate([zero, q, flags, rest], axis=0))
        return jnp.exp2(jnp.concatenate([low, high], axis=0) * jnp.float32(SCALE))

    def flags_of(i):
        return jnp.where(BLK * i + q_off >= q_bounds, jnp.float32(-BIG), jnp.float32(0.0)).astype(jnp.bfloat16)

    def partial_sum(e):
        return jnp.sum(e.reshape(BLK // 8, 8, BLK), axis=0)

    def tiles(i, row):
        runs = range(SRC * i, SRC * i + SRC)
        return jnp.concatenate([x_ref[PLACE_IN[s], row : row + 16, :] for s in runs], axis=0)

    def near_scores(blocks):
        for i in blocks:
            q = wide(tiles(i, 0))
            kt[i] = tiles(i, 16)
            qt[i] = q
            vt[i] = wide(tiles(i, 32))
            flags = flags_of(i)
            kf[i] = jnp.where(BLK * i + k_off < k_bounds, jnp.float32(1.0), jnp.float32(0.0)).astype(jnp.bfloat16)
            e1 = jnp.where(below, scores(i, q, flags), jnp.float32(0.0))
            e0 = scores(max(i - 1, 0), q, flags)
            if i == 0:
                e0 = jnp.zeros_like(e0)
            near[i, 0] = e0
            near[i, 1] = e1
            total[i] = partial_sum(e0) + partial_sum(e1)

    scalars = [jnp.max(bounds_ref[:, d : d + 1]) for d in range(DOCS)]
    n_far = jnp.int32(0)
    for i in range(2, NBLK):
        start = starts_of(jnp.int32(BLK * i), lambda d: scalars[d])
        for j in range(i - 2, -1, -1):
            items[n_far] = NBLK * i + j
            n_far += (start < BLK * (j + 1)).astype(jnp.int32)
    near_scores(range(NBLK))
    for u in range(LONG - 1):
        items[n_far + u] = NBLK * NBLK
    trips = (n_far + LONG - MIDDLE - 1) // LONG
    left = n_far - LONG * trips
    passes = (
        (0, trips, LONG),
        (LONG * trips, (left > SHORT).astype(jnp.int32), MIDDLE),
        (LONG * trips, ((left > 0) & (left <= SHORT)).astype(jnp.int32), SHORT),
    )

    def far_blocks(work):
        for begin, trips, length in passes:

            def trip(w, _, begin=begin, length=length):
                for u in range(length):
                    n = begin + length * w + u
                    work(n, items[n] >> 4, items[n] & 15)
                return 0

            lax.fori_loop(0, trips, trip, 0)

    def far_scores(n, i, j):
        e = scores(j, qt[i], flags_of(i))
        far[n] = e
        total[i] += partial_sum(e)

    far_blocks(far_scores)
    for i in range(NBLK):
        inverse = 1.0 / jnp.sum(total[i], axis=0, keepdims=True)
        total[i] = jnp.broadcast_to(inverse, (8, BLK))
        summed[i] = jnp.zeros((HD, BLK), jnp.float32)

    def far_values(n, i, j):
        summed[i] += dot(vt[j], (far[n] * total[i][0:1]).astype(jnp.bfloat16))

    far_blocks(far_values)

    for i in range(NBLK):
        w = jnp.concatenate([(near[i, n] * total[i][0:1]).astype(jnp.bfloat16) for n in range(2)], axis=0)
        out = dot(jnp.concatenate([vt[max(i - 1, 0)], vt[i]], axis=1), w) + summed[i]
        both = jnp.transpose(jnp.concatenate([out[:, :PAIRS], out[:, PAIRS:]], axis=0))
        both = both.astype(jnp.bfloat16)
        for n in range(SRC):
            o_ref[PLACE_OUT[SRC * i + n]] = both[16 * n : 16 * n + 16]


def take_kernel(x_ref, o_hbm, turned, out, sems):
    mix = interleave()
    eye = identity(128)
    for h in range(0, HEADS, 32):
        tiles = [x_ref[PLACE_OUT[s]] for s in ORDER_IN[h : h + 32]]
        part = jnp.concatenate([jnp.concatenate(tiles[m : m + 16], axis=0) for m in (0, 16)], axis=1)
        both = dot(mix, part).astype(jnp.bfloat16)
        for m in range(2):
            turned[:, h + 16 * m : h + 16 * m + 16, :] = both[:, 128 * m : 128 * m + 128].reshape(16, 16, 128)
    copies = []
    for r in range(0, ROWS, 2):
        both = dot(eye, turned[r : r + 2].reshape(256, 128), NT).astype(jnp.bfloat16)
        for m in range(2):
            out[r + m] = both[:HD, 128 * m : 128 * m + 128]
            out[r + m + ROWS] = both[HD:, 128 * m : 128 * m + 128]
        if r % 8 == 6:
            for first in (r - 6, r - 6 + ROWS):
                copy = pltpu.make_async_copy(
                    out.at[pl.ds(first, 8)], o_hbm.at[pl.ds(first, 8)], sems.at[len(copies)]
                )
                copy.start()
                copies.append(copy)
    for copy in copies:
        copy.wait()


VMEM = pl.BlockSpec(memory_space=pltpu.VMEM)
HBM = pl.BlockSpec(memory_space=pltpu.HBM)


def in_hbm(x):
    return pltpu.with_memory_space_constraint(x, pltpu.HBM)


def send_call(doc_bounds, q, k, v, q_gain, k_gain):
    return pl.pallas_call(
        send_kernel,
        out_shape=jax.ShapeDtypeStruct((HEADS, 48, 128), jnp.bfloat16),
        in_specs=[HBM] * 6,
        out_specs=VMEM,
        scratch_shapes=[
            pltpu.VMEM((1, DOCS + 1), jnp.int32),
            pltpu.VMEM((3, TOK, HD, HEADS), jnp.bfloat16),
            pltpu.VMEM((2, 1, HD), jnp.float32),
            pltpu.VMEM((2, ROWS, 128, HEADS), jnp.bfloat16),
            pltpu.VMEM((3, ROWS, HEADS, 128), jnp.bfloat16),
            pltpu.SemaphoreType.DMA((6,)),
        ],
        compiler_params=pltpu.CompilerParams(vmem_limit_bytes=32 << 20),
        name="send_side",
    )(*(in_hbm(x) for x in (doc_bounds, q, k, v, q_gain.reshape(1, HD), k_gain.reshape(1, HD))))


def attend_call(doc_bounds, mine):
    return pl.pallas_call(
        attend_kernel,
        out_shape=jax.ShapeDtypeStruct((SEQ // TOK, ROWS, 128), jnp.bfloat16),
        in_specs=[VMEM, VMEM],
        out_specs=VMEM,
        scratch_shapes=[
            pltpu.VMEM((NBLK + 1, HD, BLK), jnp.bfloat16),
            pltpu.VMEM((NBLK, PAIRS, 128), jnp.bfloat16),
            pltpu.VMEM((NBLK, BLK, 128), jnp.bfloat16),
            pltpu.VMEM((NBLK, HD, BLK), jnp.bfloat16),
            pltpu.VMEM((NBLK, 2, BLK, BLK), jnp.float32),
            pltpu.VMEM((FAR, BLK, BLK), jnp.float32),
            pltpu.VMEM((NBLK + 1, 8, BLK), jnp.float32),
            pltpu.VMEM((NBLK + 1, HD, BLK), jnp.float32),
            pltpu.SMEM((FAR,), jnp.int32),
        ],
        compiler_params=pltpu.CompilerParams(vmem_limit_bytes=44 << 20),
        name="attend",
    )(doc_bounds, mine)


def take_call(back):
    return pl.pallas_call(
        take_kernel,
        out_shape=jax.ShapeDtypeStruct((TOK, HD, HEADS), jnp.bfloat16),
        in_specs=[VMEM],
        out_specs=HBM,
        scratch_shapes=[
            pltpu.VMEM((ROWS, HEADS, 128), jnp.bfloat16),
            pltpu.VMEM((TOK, HD, HEADS), jnp.bfloat16),
            pltpu.SemaphoreType.DMA((4,)),
        ],
        compiler_params=pltpu.CompilerParams(vmem_limit_bytes=32 << 20),
        name="take_side",
    )(back)


def exchange(x, order):
    return lax.all_to_all(x, "run", split_axis=0, concat_axis=0, axis_index_groups=[order], tiled=True)


def body(queries, keys, values, doc_bounds, q_gain, k_gain):
    doc_bounds = doc_bounds.reshape(1, DOCS + 1)
    inputs = [jnp.transpose(x, (0, 2, 1)) for x in (queries, keys, values)]
    packed = send_call(doc_bounds, *inputs, q_gain, k_gain)
    mine = exchange(packed, ORDER_IN)
    result = attend_call(doc_bounds, mine)
    back = exchange(result, ORDER_OUT)
    return jnp.transpose(take_call(back), (0, 2, 1))


def solution(mesh):
    runs = jax.sharding.Mesh(mesh.devices.reshape(len(ORDER_IN), -1), ("run", "dp"))
    tokens = P(("dp", "run"), None, None)
    return jax.shard_map(
        body,
        mesh=runs,
        in_specs=(tokens, tokens, tokens, P("dp"), P(), P()),
        out_specs=tokens,
        check_vma=False,
    )
```

```python
import jax
import jax.numpy as jnp
from jax import lax
from jax.experimental import pallas as pl
from jax.experimental.pallas import tpu as pltpu
from jax.sharding import PartitionSpec as P

TOK = 32
ROWS = 16
HD = 64
HEADS = 128
DOCS = 8
SEQ = 4096
BLK = 256
PAIRS = BLK // 2
NBLK = SEQ // BLK
SRC = BLK // TOK
LONG, MIDDLE, SHORT = 20, 12, 6
FAR = (NBLK - 2) * (NBLK - 1) // 2 + LONG
NT = (((1,), (1,)), ((), ()))
NN = (((1,), (0,)), ((), ()))
BIG = 32768.0
SCALE = 1.4426950408889634 / 8.0
FIRST = -9.210340371976184


def run_of(z, x, c):
    return ((z % 8 * 2 + c) * 4 + x) * 2 + z // 8


FIRST_Z = [8, 7, 9, 6, 10, 5, 11, 4, 12, 3, 13, 2, 14, 1, 15, 0]
THEN_Z = [8, 15, 6, 13, 4, 11, 2, 9, 0, 7, 14, 5, 12, 3, 10, 1]
ORDER_IN = [run_of(z, x, c) for z in FIRST_Z for x in (2, 1, 3, 0) for c in range(2)]
ORDER_OUT = [run_of(z, x, c) for z in THEN_Z for x in (2, 1, 3, 0) for c in (1, 0)]
PLACE_IN = [ORDER_IN.index(s) for s in range(len(ORDER_IN))]
PLACE_OUT = [ORDER_OUT.index(s) for s in range(len(ORDER_OUT))]


def dot(a, b, dims=NN):
    return lax.dot_general(a, b, dims, preferred_element_type=jnp.float32)


def starts_of(token, bound):
    start = jnp.zeros_like(token)
    for d in range(1, DOCS):
        start = jnp.where(token >= bound(d), bound(d), start)
    return start


def identity(n):
    row = lax.broadcasted_iota(jnp.int32, (n, n), 0)
    col = lax.broadcasted_iota(jnp.int32, (n, n), 1)
    return (row == col).astype(jnp.float32).astype(jnp.bfloat16)


def interleave():
    row = lax.broadcasted_iota(jnp.int32, (256, 256), 0)
    col = lax.broadcasted_iota(jnp.int32, (256, 256), 1)
    return (col == (row % 16) * 16 + row // 16).astype(jnp.float32).astype(jnp.bfloat16)


def send_kernel(
    bounds_hbm, q_hbm, k_hbm, v_hbm, qg_hbm, kg_hbm, o_ref, bounds_ref, x_ref, g_ref, rot, turned, sems
):
    arriving = [
        pltpu.make_async_copy(source, target, sems.at[n])
        for n, (source, target) in enumerate(
            (
                (bounds_hbm, bounds_ref),
                (qg_hbm, g_ref.at[0]),
                (kg_hbm, g_ref.at[1]),
                (q_hbm, x_ref.at[0]),
                (v_hbm, x_ref.at[2]),
                (k_hbm, x_ref.at[1]),
            )
        )
    ]
    for c in arriving:
        c.start()
    for c in arriving[:3]:
        c.wait()
    lane = lax.broadcasted_iota(jnp.int32, (HD // 2, 128), 1)
    token = lax.axis_index("run") * TOK + lane
    start = starts_of(token, lambda d: bounds_ref[:, d : d + 1])
    place = (token - start).astype(jnp.float32)
    index = lax.broadcasted_iota(jnp.int32, (HD // 2, 128), 0).astype(jnp.float32)
    angle = place * jnp.exp(jnp.float32(FIRST) * index * 2.0 / HD)
    cosine = jnp.cos(angle)
    sine = jnp.sin(angle)
    eye = identity(HEADS)
    mix = interleave()

    def turn(n, r, rows):
        both = dot(eye, rows, NT).astype(jnp.bfloat16)
        turned[n, r] = both[:, :128]
        turned[n, r + 1] = both[:, 128:]

    def rotate(n):
        gain = jnp.transpose(jnp.broadcast_to(g_ref[n], (HEADS, HD)))
        for r in range(0, ROWS, 2):
            for t in (r, r + ROWS, r + 1, r + 1 + ROWS):
                c = jnp.broadcast_to(cosine[:, t : t + 1], (HD // 2, HEADS))
                s = jnp.broadcast_to(sine[:, t : t + 1], (HD // 2, HEADS))
                x = x_ref[n, t].astype(jnp.float32)
                scale = lax.rsqrt(jnp.mean(x * x, axis=0, keepdims=True) + 1e-06)
                x = x * scale * gain
                a, b = x[: HD // 2], x[HD // 2 :]
                y = jnp.concatenate([a * c - b * s, a * s + b * c], axis=0)
                rot[n, t % ROWS, pl.ds((t // ROWS) * HD, HD), :] = y.astype(jnp.bfloat16)
            turn(n, r, rot[n, r : r + 2].reshape(256, HEADS))

    def spread(n):
        for h in range(0, HEADS, 32):
            part = jnp.concatenate([turned[n, :, h + m : h + m + 16, :].reshape(256, 128) for m in (0, 16)], axis=1)
            both = dot(mix, part).astype(jnp.bfloat16)
            for m in range(2):
                heads = slice(h + 16 * m, h + 16 * m + 16)
                o_ref[heads, 16 * n : 16 * n + 16, :] = both[:, 128 * m : 128 * m + 128].reshape(16, 16, 128)

    for c in arriving[3:]:
        c.wait()

    def turn_values():
        for r in range(0, ROWS, 2):
            turn(2, r, jnp.concatenate([x_ref[2, t] for t in (r, r + ROWS, r + 1, r + 1 + ROWS)], axis=0))

    turn_values()
    rotate(0)
    spread(2)
    rotate(1)
    spread(0)
    spread(1)


def attend_kernel(bounds_ref, x_ref, o_ref, qt, kt, kf, vt, near, far, total, summed, items):

    def offsets(shape, axis):
        n = lax.broadcasted_iota(jnp.int32, shape, axis)
        return ((n % PAIRS) // 16) * 32 + n % 16 + (n // PAIRS) * 16

    below = offsets((BLK, BLK), 0) <= offsets((BLK, BLK), 1)
    q_off = offsets((16, BLK), 1)
    k_off = offsets((BLK, 128), 0)

    def bounds_along(shape, axis):
        n = lax.broadcasted_iota(jnp.int32, shape, axis)
        out = jnp.full(shape, SEQ, jnp.int32)
        for d in range(1, DOCS):
            out = jnp.where(n == d, bounds_ref[:, d : d + 1], out)
        return out

    q_bounds = bounds_along((16, BLK), 0)
    k_bounds = bounds_along((1, 128), 1)

    zero = jnp.zeros((HD, BLK), jnp.bfloat16)
    rest = jnp.zeros((128 - 16, BLK), jnp.bfloat16)

    def wide(x):
        t = jnp.transpose(x.astype(jnp.float32)).astype(jnp.bfloat16)
        return jnp.concatenate([t[:HD], t[HD:]], axis=1)

    def scores(j, q, flags):
        k2 = kt[j]
        low = dot(jnp.concatenate([k2, kf[j, :PAIRS]], axis=1), jnp.concatenate([q, zero, flags, rest], axis=0))
        high = dot(jnp.concatenate([k2, kf[j, PAIRS:]], axis=1), jnp.concatenate([zero, q, flags, rest], axis=0))
        return jnp.exp2(jnp.concatenate([low, high], axis=0) * jnp.float32(SCALE))

    def flags_of(i):
        return jnp.where(BLK * i + q_off >= q_bounds, jnp.float32(-BIG), jnp.float32(0.0)).astype(jnp.bfloat16)

    def partial_sum(e):
        return jnp.sum(e.reshape(BLK // 8, 8, BLK), axis=0)

    def tiles(i, row):
        runs = range(SRC * i, SRC * i + SRC)
        return jnp.concatenate([x_ref[PLACE_IN[s], row : row + 16, :] for s in runs], axis=0)

    def near_scores(blocks):
        for i in blocks:
            q = wide(tiles(i, 0))
            kt[i] = tiles(i, 16)
            qt[i] = q
            vt[i] = wide(tiles(i, 32))
            flags = flags_of(i)
            kf[i] = jnp.where(BLK * i + k_off < k_bounds, jnp.float32(1.0), jnp.float32(0.0)).astype(jnp.bfloat16)
            e1 = jnp.where(below, scores(i, q, flags), jnp.float32(0.0))
            e0 = scores(max(i - 1, 0), q, flags)
            if i == 0:
                e0 = jnp.zeros_like(e0)
            near[i, 0] = e0
            near[i, 1] = e1
            total[i] = partial_sum(e0) + partial_sum(e1)

    scalars = [jnp.max(bounds_ref[:, d : d + 1]) for d in range(DOCS)]
    n_far = jnp.int32(0)
    for i in range(2, NBLK):
        start = starts_of(jnp.int32(BLK * i), lambda d: scalars[d])
        for j in range(i - 2, -1, -1):
            items[n_far] = NBLK * i + j
            n_far += (start < BLK * (j + 1)).astype(jnp.int32)
    near_scores(range(NBLK))
    for u in range(LONG - 1):
        items[n_far + u] = NBLK * NBLK
    trips = (n_far + LONG - MIDDLE - 1) // LONG
    left = n_far - LONG * trips
    passes = (
        (0, trips, LONG),
        (LONG * trips, (left > SHORT).astype(jnp.int32), MIDDLE),
        (LONG * trips, ((left > 0) & (left <= SHORT)).astype(jnp.int32), SHORT),
    )

    def far_blocks(work):
        for begin, trips, length in passes:

            def trip(w, _, begin=begin, length=length):
                for u in range(length):
                    n = begin + length * w + u
                    work(n, items[n] >> 4, items[n] & 15)
                return 0

            lax.fori_loop(0, trips, trip, 0)

    def far_scores(n, i, j):
        e = scores(j, qt[i], flags_of(i))
        far[n] = e
        total[i] += partial_sum(e)

    far_blocks(far_scores)
    for i in range(NBLK):
        inverse = 1.0 / jnp.sum(total[i], axis=0, keepdims=True)
        total[i] = jnp.broadcast_to(inverse, (8, BLK))
        summed[i] = jnp.zeros((HD, BLK), jnp.float32)

    def far_values(n, i, j):
        summed[i] += dot(vt[j], (far[n] * total[i][0:1]).astype(jnp.bfloat16))

    far_blocks(far_values)

    for i in range(NBLK):
        w = jnp.concatenate([(near[i, n] * total[i][0:1]).astype(jnp.bfloat16) for n in range(2)], axis=0)
        out = dot(jnp.concatenate([vt[max(i - 1, 0)], vt[i]], axis=1), w) + summed[i]
        both = jnp.transpose(jnp.concatenate([out[:, :PAIRS], out[:, PAIRS:]], axis=0))
        both = both.astype(jnp.bfloat16)
        for n in range(SRC):
            o_ref[PLACE_OUT[SRC * i + n]] = both[16 * n : 16 * n + 16]


def take_kernel(x_ref, o_hbm, turned, out, sems):
    mix = interleave()
    eye = identity(128)
    for h in range(0, HEADS, 32):
        tiles = [x_ref[PLACE_OUT[s]] for s in ORDER_IN[h : h + 32]]
        part = jnp.concatenate([jnp.concatenate(tiles[m : m + 16], axis=0) for m in (0, 16)], axis=1)
        both = dot(mix, part).astype(jnp.bfloat16)
        for m in range(2):
            turned[:, h + 16 * m : h + 16 * m + 16, :] = both[:, 128 * m : 128 * m + 128].reshape(16, 16, 128)
    copies = []
    for r in range(0, ROWS, 2):
        both = dot(eye, turned[r : r + 2].reshape(256, 128), NT).astype(jnp.bfloat16)
        for m in range(2):
            out[r + m] = both[:HD, 128 * m : 128 * m + 128]
            out[r + m + ROWS] = both[HD:, 128 * m : 128 * m + 128]
        if r % 8 == 6:
            for first in (r - 6, r - 6 + ROWS):
                copy = pltpu.make_async_copy(
                    out.at[pl.ds(first, 8)], o_hbm.at[pl.ds(first, 8)], sems.at[len(copies)]
                )
                copy.start()
                copies.append(copy)
    for copy in copies:
        copy.wait()


VMEM = pl.BlockSpec(memory_space=pltpu.VMEM)
HBM = pl.BlockSpec(memory_space=pltpu.HBM)


def in_hbm(x):
    return pltpu.with_memory_space_constraint(x, pltpu.HBM)


def send_call(doc_bounds, q, k, v, q_gain, k_gain):
    return pl.pallas_call(
        send_kernel,
        out_shape=jax.ShapeDtypeStruct((HEADS, 48, 128), jnp.bfloat16),
        in_specs=[HBM] * 6,
        out_specs=VMEM,
        scratch_shapes=[
            pltpu.VMEM((1, DOCS + 1), jnp.int32),
            pltpu.VMEM((3, TOK, HD, HEADS), jnp.bfloat16),
            pltpu.VMEM((2, 1, HD), jnp.float32),
            pltpu.VMEM((2, ROWS, 128, HEADS), jnp.bfloat16),
            pltpu.VMEM((3, ROWS, HEADS, 128), jnp.bfloat16),
            pltpu.SemaphoreType.DMA((6,)),
        ],
        compiler_params=pltpu.CompilerParams(vmem_limit_bytes=32 << 20),
        name="send_side",
    )(*(in_hbm(x) for x in (doc_bounds, q, k, v, q_gain.reshape(1, HD), k_gain.reshape(1, HD))))


def attend_call(doc_bounds, mine):
    return pl.pallas_call(
        attend_kernel,
        out_shape=jax.ShapeDtypeStruct((SEQ // TOK, ROWS, 128), jnp.bfloat16),
        in_specs=[VMEM, VMEM],
        out_specs=VMEM,
        scratch_shapes=[
            pltpu.VMEM((NBLK + 1, HD, BLK), jnp.bfloat16),
            pltpu.VMEM((NBLK, PAIRS, 128), jnp.bfloat16),
            pltpu.VMEM((NBLK, BLK, 128), jnp.bfloat16),
            pltpu.VMEM((NBLK, HD, BLK), jnp.bfloat16),
            pltpu.VMEM((NBLK, 2, BLK, BLK), jnp.float32),
            pltpu.VMEM((FAR, BLK, BLK), jnp.float32),
            pltpu.VMEM((NBLK + 1, 8, BLK), jnp.float32),
            pltpu.VMEM((NBLK + 1, HD, BLK), jnp.float32),
            pltpu.SMEM((FAR,), jnp.int32),
        ],
        compiler_params=pltpu.CompilerParams(vmem_limit_bytes=44 << 20),
        name="attend",
    )(doc_bounds, mine)


def take_call(back):
    return pl.pallas_call(
        take_kernel,
        out_shape=jax.ShapeDtypeStruct((TOK, HD, HEADS), jnp.bfloat16),
        in_specs=[VMEM],
        out_specs=HBM,
        scratch_shapes=[
            pltpu.VMEM((ROWS, HEADS, 128), jnp.bfloat16),
            pltpu.VMEM((TOK, HD, HEADS), jnp.bfloat16),
            pltpu.SemaphoreType.DMA((4,)),
        ],
        compiler_params=pltpu.CompilerParams(vmem_limit_bytes=32 << 20),
        name="take_side",
    )(back)


def exchange(x, order):
    return lax.all_to_all(x, "run", split_axis=0, concat_axis=0, axis_index_groups=[order], tiled=True)


def body(queries, keys, values, doc_bounds, q_gain, k_gain):
    doc_bounds = doc_bounds.reshape(1, DOCS + 1)
    inputs = [jnp.transpose(x, (0, 2, 1)) for x in (queries, keys, values)]
    packed = send_call(doc_bounds, *inputs, q_gain, k_gain)
    mine = exchange(packed, ORDER_IN)
    result = attend_call(doc_bounds, mine)
    back = exchange(result, ORDER_OUT)
    return jnp.transpose(take_call(back), (0, 2, 1))


def solution(mesh):
    runs = jax.sharding.Mesh(mesh.devices.reshape(len(ORDER_IN), -1), ("run", "dp"))
    tokens = P(("dp", "run"), None, None)
    return jax.shard_map(
        body,
        mesh=runs,
        in_specs=(tokens, tokens, tokens, P("dp"), P(), P()),
        out_specs=tokens,
        check_vma=False,
    )
```
